8 devices in a mesh: rep: 2 (over z, y), fsdp: 4 (over x, core).
Axes of the slice: x: 2, y: 2, z: 1, core: 2. Of those that a mesh axis runs over, the one named last changes fastest.
Arguments:
- tokens: bfloat16 [8192, 2048], P(('rep', 'fsdp')), parts along dimension 0
- seg_ids: int32 [8192], P(('rep', 'fsdp')), parts along dimension 0
- w_q: bfloat16 [2, 2048, 2048], P(None, 'fsdp')
- w_k: bfloat16 [2, 2048, 256], P(None, 'fsdp')
- w_v: bfloat16 [2, 2048, 256], P(None, 'fsdp')
- w_o: bfloat16 [2, 2048, 2048], P(None, 'fsdp')
- w_gate: bfloat16 [2, 2048, 11008], P(None, 'fsdp')
- w_up: bfloat16 [2, 2048, 11008], P(None, 'fsdp')
- w_down: bfloat16 [2, 11008, 2048], P(None, 'fsdp')
- g_attn: bfloat16 [2, 2048], replicated
- g_mlp: bfloat16 [2, 2048], replicated
Outputs:
- output: float32 [8192, 2048], P(('rep', 'fsdp')), parts along dimension 0
There are 2 independent parts. The reference program is written for one: setup_inputs(seed, part) draws one part's arguments, and reference() takes and returns one part's arrays. A program takes and returns all parts, laid end to end along the dimension named above; an argument that names none is the same for every part.
All inputs are finite; a program needn't handle non-finite values.
Results may differ from the reference program's by a relative error of at most 0.0135712.
Values are sent between devices in bfloat16 or wider.
A program may use at most 1 GiB of HBM per device.

```python
import jax
import jax.numpy as jnp
from jax import lax

D = 2048
FF = 11008
HEADS = 16
KV_HEADS = 2
HEAD = 128
TOKENS_DEV = 1024
GROUP = 4
LAYERS = 2
PART_TOKENS = GROUP * TOKENS_DEV
MEAN_LEN = max(2, TOKENS_DEV // 4)
Q_GROUP = HEADS // KV_HEADS
EPS = 1e-5
ROPE_BASE = 10000.0


def draw_segments(seg_key):
    tok_idx = jnp.arange(PART_TOKENS, dtype=jnp.int32)
    new_req = (jax.random.randint(seg_key, (PART_TOKENS,), 0, MEAN_LEN) == 0) | (tok_idx % TOKENS_DEV == 0)
    return (jnp.cumsum(new_req.astype(jnp.int32)) - 1).astype(jnp.int32)


def weight_draw(w_key, shape, scale):
    return (jax.random.normal(w_key, shape, jnp.float32) * scale).astype(jnp.bfloat16)


def setup_inputs(seed: int = 0, part: int = 0) -> dict:
    root_key = jax.random.key(seed)
    part_key = jax.random.fold_in(root_key, part)
    tok_key, seg_key = jax.random.split(part_key)
    key_list = jax.random.split(root_key, 9)
    q_width = HEADS * HEAD
    kv_width = KV_HEADS * HEAD
    d_scale = D ** -0.5
    qk_scale = 1.5 * d_scale
    o_scale = q_width ** -0.5
    down_scale = FF ** -0.5
    tokens = jax.random.normal(tok_key, (PART_TOKENS, D), jnp.float32).astype(jnp.bfloat16)
    gain_a = 1.0 + 0.3 * jax.random.normal(key_list[7], (LAYERS, D), jnp.float32)
    gain_m = 1.0 + 0.3 * jax.random.normal(key_list[8], (LAYERS, D), jnp.float32)
    return {
        "tokens": tokens,
        "seg_ids": draw_segments(seg_key),
        "w_q": weight_draw(key_list[0], (LAYERS, D, q_width), qk_scale),
        "w_k": weight_draw(key_list[1], (LAYERS, D, kv_width), qk_scale),
        "w_v": weight_draw(key_list[2], (LAYERS, D, kv_width), d_scale),
        "w_o": weight_draw(key_list[3], (LAYERS, q_width, D), o_scale),
        "w_gate": weight_draw(key_list[4], (LAYERS, D, FF), d_scale),
        "w_up": weight_draw(key_list[5], (LAYERS, D, FF), d_scale),
        "w_down": weight_draw(key_list[6], (LAYERS, FF, D), down_scale),
        "g_attn": gain_a.astype(jnp.bfloat16),
        "g_mlp": gain_m.astype(jnp.bfloat16),
    }


def rms_norm(hidden, gain):
    inv_rms = lax.rsqrt(jnp.mean(hidden * hidden, axis=-1, keepdims=True) + EPS)
    return (hidden * inv_rms * gain.astype(jnp.float32)).astype(jnp.bfloat16)


def rotary(vals, tok_pos):
    half_dim = HEAD // 2
    inv_freq = ROPE_BASE ** (-jnp.arange(half_dim, dtype=jnp.float32) / half_dim)
    angles = tok_pos[:, None] * inv_freq[None, :]
    bcast_shape = (vals.shape[0],) + (1,) * (vals.ndim - 2) + (half_dim,)
    cos_wide = jnp.cos(angles).reshape(bcast_shape)
    sin_wide = jnp.sin(angles).reshape(bcast_shape)
    first_half = vals[..., :half_dim].astype(jnp.float32)
    second_half = vals[..., half_dim:].astype(jnp.float32)
    rotated = jnp.concatenate([first_half * cos_wide - second_half * sin_wide, second_half * cos_wide + first_half * sin_wide], axis=-1)
    return rotated.astype(jnp.bfloat16)


def attend_block(block_in):
    q_blk, k_blk, v_blk, seg_blk = block_in
    tok_idx = jnp.arange(TOKENS_DEV, dtype=jnp.int32)
    is_first = jnp.concatenate([tok_idx[:1] == 0, seg_blk[1:] != seg_blk[:-1]])
    req_start = lax.cummax(jnp.where(is_first, tok_idx, 0), axis=0)
    tok_pos = (tok_idx - req_start).astype(jnp.float32)
    q_rot = rotary(q_blk, tok_pos)
    k_rot = rotary(k_blk, tok_pos)
    scores = jnp.einsum("tkgd,skd->kgts", q_rot.astype(jnp.float32), k_rot.astype(jnp.float32)) * HEAD ** -0.5
    allowed = (seg_blk[:, None] == seg_blk[None, :]) & (tok_idx[None, :] <= tok_idx[:, None])
    scores = jnp.where(allowed, scores, -1e30)
    probs = jax.nn.softmax(scores, axis=-1).astype(jnp.bfloat16)
    mixed = jnp.einsum("kgts,skd->tkgd", probs.astype(jnp.float32), v_blk.astype(jnp.float32))
    return mixed.astype(jnp.bfloat16)


def reference(tokens, seg_ids, w_q, w_k, w_v, w_o, w_gate, w_up, w_down, g_attn, g_mlp):
    seg_blocks = seg_ids.reshape(GROUP, TOKENS_DEV)

    def layer_step(hidden, layer_w):
        lw_q, lw_k, lw_v, lw_o, lw_gate, lw_up, lw_down, lg_attn, lg_mlp = layer_w
        normed = rms_norm(hidden, lg_attn)
        q_all = jnp.dot(normed, lw_q, preferred_element_type=jnp.float32).astype(jnp.bfloat16)
        k_all = jnp.dot(normed, lw_k, preferred_element_type=jnp.float32).astype(jnp.bfloat16)
        v_all = jnp.dot(normed, lw_v, preferred_element_type=jnp.float32).astype(jnp.bfloat16)
        q_blocks = q_all.reshape(GROUP, TOKENS_DEV, KV_HEADS, Q_GROUP, HEAD)
        k_blocks = k_all.reshape(GROUP, TOKENS_DEV, KV_HEADS, HEAD)
        v_blocks = v_all.reshape(GROUP, TOKENS_DEV, KV_HEADS, HEAD)
        mixed = lax.map(attend_block, (q_blocks, k_blocks, v_blocks, seg_blocks))
        hidden = hidden + jnp.dot(mixed.reshape(PART_TOKENS, HEADS * HEAD), lw_o, preferred_element_type=jnp.float32)
        normed = rms_norm(hidden, lg_mlp)
        gate_proj = jnp.dot(normed, lw_gate, preferred_element_type=jnp.float32)
        up_proj = jnp.dot(normed, lw_up, preferred_element_type=jnp.float32)
        act_val = (jax.nn.silu(gate_proj) * up_proj).astype(jnp.bfloat16)
        hidden = hidden + jnp.dot(act_val, lw_down, preferred_element_type=jnp.float32)
        return hidden, None

    hidden_out, _ = lax.scan(layer_step, tokens.astype(jnp.float32), (w_q, w_k, w_v, w_o, w_gate, w_up, w_down, g_attn, g_mlp))
    return hidden_out
```

```python
import functools

import jax
import jax.numpy as jnp
from jax import lax
from jax.experimental import pallas as pl
from jax.experimental.pallas import tpu as pltpu
from jax.sharding import PartitionSpec as P

HEAD = 128
EPS = 1e-5
ROPE_BASE = 10000.0
MESH = pl.DeviceIdType.MESH

LAYERS = 2
SLOTS = 16
AHEAD = 4
AHEAD0 = 2

N_Q = 4
N_GU = 21
N_D = 10
CH_Q = 1
CH_O = CH_Q + N_Q
CH_GU = CH_O + N_Q
CH_GL = CH_GU + N_GU
CH_D = CH_GL + 1
CH_DR = CH_D + N_D
PER_LAYER = CH_DR + 1
CHUNKS = LAYERS * PER_LAYER
NAMES = ("q", "k", "v", "o", "g", "u", "d")


def gather_kernel(*refs):
    own = dict(zip(NAMES, refs[:7]))
    b1 = dict(zip(NAMES, refs[7:14]))
    b2 = dict(zip(NAMES, refs[14:21]))
    b3 = dict(zip(NAMES, refs[21:28]))
    s0s, s0r, s1s, s1r, s2s, s2r, s3s, s3r = refs[28:]
    y = lax.axis_index("rep")
    d = lax.axis_index("fsdp")
    core = lax.rem(d, 2)
    x_dev = (y, lax.rem(d + 2, 4))
    y_dev = (1 - y, d)
    c_dev = (y, d + 1 - 2 * core)

    barrier = pltpu.get_barrier_semaphore()
    for dev in (x_dev, y_dev, c_dev):
        pl.semaphore_signal(barrier, inc=1, device_id=dev, device_id_type=MESH)
    pl.semaphore_wait(barrier, 3)

    def for_chunk(k, fn, lo=0, hi=CHUNKS):
        layer = k // PER_LAYER
        i = lax.rem(k, PER_LAYER)
        slot = lax.rem(k, SLOTS)
        ok = (k >= lo) & (k < hi)

        def case(cond, items):
            @pl.when(ok & cond)
            def _():
                for n, (name, r0, nr, c0, nc) in enumerate(items):
                    fn(name, layer, r0, nr, c0, nc, slot, n)

        case(i == 0, [("k", 0, 512, 0, 256), ("v", 0, 512, 0, 256)])
        jq = pl.multiple_of((i - CH_Q) * 512, 512)
        case((i >= CH_Q) & (i < CH_O), [("q", 0, 512, jq, 512)])
        jo = pl.multiple_of((i - CH_O) * 512, 512)
        case((i >= CH_O) & (i < CH_GU), [("o", 0, 512, jo, 512)])
        jg = pl.multiple_of((i - CH_GU) * 512, 512)
        case((i >= CH_GU) & (i < CH_GL), [("g", 0, 512, jg, 512), ("u", 0, 512, jg, 512)])
        case(i == CH_GL, [("g", 0, 512, N_GU * 512, 256), ("u", 0, 512, N_GU * 512, 256)])
        jd = core * 192 + (i - CH_D) * 256
        case((i >= CH_D) & (i < CH_DR), [("d", jd, 256, 0, 2048)])
        case(i == CH_DR, [("d", (1 - core) * 2560, 192, 0, 2048)])

    def view(bufs, name, layer, r0, nr, c0, nc, half):
        if half:
            nr = nr // 2
            r0 = r0 + y * nr
        r0 = pl.multiple_of(r0, 32)
        return bufs[name].at[layer, pl.ds(r0, nr), pl.ds(c0, nc)]

    def copy0(name, layer, r0, nr, c0, nc, slot, n):
        return pltpu.make_async_remote_copy(
            src_ref=view(own, name, layer, r0, nr, c0, nc, False),
            dst_ref=view(b1, name, layer, r0, nr, c0, nc, False),
            send_sem=s0s.at[slot, n], recv_sem=s0r.at[slot, n], device_id=c_dev, device_id_type=MESH)

    def copy1(name, layer, r0, nr, c0, nc, slot, n):
        return pltpu.make_async_remote_copy(
            src_ref=view(own, name, layer, r0, nr, c0, nc, True),
            dst_ref=view(b2, name, layer, r0, nr, c0, nc, True),
            send_sem=s1s.at[slot, n], recv_sem=s1r.at[slot, n], device_id=x_dev, device_id_type=MESH)

    def copy2(name, layer, r0, nr, c0, nc, slot, n):
        return pltpu.make_async_remote_copy(
            src_ref=view(b2, name, layer, r0, nr, c0, nc, True),
            dst_ref=view(b2, name, layer, r0, nr, c0, nc, True),
            send_sem=s2s.at[slot, n], recv_sem=s2r.at[slot, n], device_id=y_dev, device_id_type=MESH)

    def copy3(name, layer, r0, nr, c0, nc, slot, n):
        return pltpu.make_async_remote_copy(
            src_ref=view(b2, name, layer, r0, nr, c0, nc, False),
            dst_ref=view(b3, name, layer, r0, nr, c0, nc, False),
            send_sem=s3s.at[slot, n], recv_sem=s3r.at[slot, n], device_id=c_dev, device_id_type=MESH)

    def start1(*a):
        copy1(*a).start()

    def start0(*a):
        copy0(*a).start()

    def relay2(*a):
        copy1(*a).wait_recv()
        copy2(*a).start()

    def relay3(*a):
        copy2(*a).wait_recv()
        copy3(*a).start()

    def finish(*a):
        copy0(*a).wait_recv()
        copy3(*a).wait_recv()
        copy0(*a).wait_send()
        copy1(*a).wait_send()
        copy2(*a).wait_send()
        copy3(*a).wait_send()

    def tick(k):
        for_chunk(k + AHEAD, start1, AHEAD)
        for_chunk(k + AHEAD0, start0, AHEAD0)
        for_chunk(k, relay2)
        for_chunk(k - 1, relay3)
        for_chunk(k - 2, finish)

    @pl.loop(0, AHEAD)
    def _(k):
        for_chunk(k, start1)

    @pl.loop(0, AHEAD0)
    def _(k):
        for_chunk(k, start0)

    @pl.loop(0, CHUNKS + 2)
    def _(k):
        tick(k)


def gather_all(*weights):
    shapes = [jax.ShapeDtypeStruct(w.shape, w.dtype) for w in weights]
    sem = pltpu.SemaphoreType.DMA((SLOTS, 2))
    outs = pl.pallas_call(
        gather_kernel,
        out_shape=shapes * 3,
        in_specs=[pl.BlockSpec(memory_space=pl.ANY)] * 7,
        out_specs=[pl.BlockSpec(memory_space=pl.ANY)] * 21,
        scratch_shapes=[sem] * 8,
        compiler_params=pltpu.CompilerParams(collective_id=0, has_side_effects=True),
        name="gather_weights",
    )(*weights)
    return outs[:7], outs[7:14], outs[14:21]


def rms_norm(hidden, gain):
    inv_rms = lax.rsqrt(jnp.mean(hidden * hidden, axis=-1, keepdims=True) + EPS)
    return (hidden * inv_rms * gain.astype(jnp.float32)).astype(jnp.bfloat16)


def rope_tables(seg_blk):
    tok_idx = lax.broadcasted_iota(jnp.int32, seg_blk.shape, 1)
    is_first = jnp.concatenate([tok_idx[:, :1] == 0, seg_blk[:, 1:] != seg_blk[:, :-1]], axis=1)
    req_start = lax.cummax(jnp.where(is_first, tok_idx, 0), axis=1)
    tok_pos = (tok_idx - req_start).astype(jnp.float32)
    half_dim = HEAD // 2
    inv_freq = ROPE_BASE ** (-jnp.arange(half_dim, dtype=jnp.float32) / half_dim)
    angles = tok_pos[:, :, None] * inv_freq
    return jnp.cos(angles), jnp.sin(angles)


def attention_mask(seg_blk):
    tok_idx = jnp.arange(seg_blk.shape[1], dtype=jnp.int32)
    causal = tok_idx[:, None] >= tok_idx[None, :]
    same_req = seg_blk[:, :, None] == seg_blk[:, None, :]
    return (same_req & causal)[:, None, None]


def apply_rope(vals, cos_tab, sin_tab):
    half_dim = HEAD // 2
    bcast_shape = cos_tab.shape[:2] + (1,) * (vals.ndim - 3) + (half_dim,)
    cos_wide = cos_tab.reshape(bcast_shape)
    sin_wide = sin_tab.reshape(bcast_shape)
    first_half = vals[..., :half_dim].astype(jnp.float32)
    second_half = vals[..., half_dim:].astype(jnp.float32)
    rotated = jnp.concatenate([first_half * cos_wide - second_half * sin_wide, second_half * cos_wide + first_half * sin_wide], axis=-1)
    return rotated.astype(jnp.bfloat16)


def attend(q_proj, k_proj, v_proj, allowed, cos_tab, sin_tab):
    n_blk = q_proj.shape[0]
    n_tok = q_proj.shape[1]
    kv_heads = k_proj.shape[2] // HEAD
    group_size = q_proj.shape[2] // k_proj.shape[2]
    q_rot = apply_rope(q_proj.reshape(n_blk, n_tok, kv_heads, group_size, HEAD), cos_tab, sin_tab)
    k_rot = apply_rope(k_proj.reshape(n_blk, n_tok, kv_heads, HEAD), cos_tab, sin_tab)
    v_heads = v_proj.reshape(n_blk, n_tok, kv_heads, HEAD)
    scores = jnp.einsum("btkgd,bskd->bkgts", q_rot, k_rot, preferred_element_type=jnp.float32) * HEAD ** -0.5
    scores = jnp.where(allowed, scores, -1e30)
    probs = jax.nn.softmax(scores, axis=-1).astype(jnp.bfloat16)
    mixed = jnp.einsum("bkgts,bskd->btkgd", probs, v_heads, preferred_element_type=jnp.float32)
    return mixed.astype(jnp.bfloat16).reshape(n_blk, n_tok, q_proj.shape[2])


def decoder_layer(hidden, allowed, cos_tab, sin_tab, full, perm, g_attn, g_mlp):
    def mul(lhs, name):
        return jnp.dot(perm(lhs), full[name], preferred_element_type=jnp.float32)

    normed = rms_norm(hidden, g_attn)
    q_proj = mul(normed, "q").astype(jnp.bfloat16)
    k_proj = mul(normed, "k").astype(jnp.bfloat16)
    v_proj = mul(normed, "v").astype(jnp.bfloat16)
    mixed = attend(q_proj, k_proj, v_proj, allowed, cos_tab, sin_tab)
    hidden = hidden + mul(mixed, "o")
    normed = rms_norm(hidden, g_mlp)
    act_val = (jax.nn.silu(mul(normed, "g")) * mul(normed, "u")).astype(jnp.bfloat16)
    return hidden + mul(act_val, "d")


def solution(mesh):
    tok_spec = P(("rep", "fsdp"), None)
    seg_spec = P(("rep", "fsdp"))
    mat_spec = P(None, "fsdp", None)
    gain_spec = P(None, None)

    def per_device(tokens, seg_ids, w_q, w_k, w_v, w_o, w_gate, w_up, w_down, g_attn, g_mlp):
        n_tok, width = tokens.shape
        seg_blk = seg_ids.reshape(1, n_tok)
        cos_tab, sin_tab = rope_tables(seg_blk)
        allowed = attention_mask(seg_blk)
        weights = (w_q, w_k, w_v, w_o, w_gate, w_up, w_down)
        b1, b2, b3 = gather_all(*weights)
        d = lax.axis_index("fsdp")
        order = jnp.stack([d, d + 1 - 2 * lax.rem(d, 2), lax.rem(d + 2, 4), 3 - d])

        def perm(lhs):
            blocks = lhs.reshape(lhs.shape[:-1] + (4, lhs.shape[-1] // 4))
            return jnp.take(blocks, order, axis=-2).reshape(lhs.shape)

        hidden = tokens.astype(jnp.float32).reshape(1, n_tok, width)
        for layer in range(LAYERS):
            full = {n: jnp.concatenate([w[layer], p[layer], q[layer], r[layer]], axis=0)
                    for n, w, p, q, r in zip(NAMES, weights, b1, b2, b3)}
            hidden = decoder_layer(hidden, allowed, cos_tab, sin_tab, full, perm, g_attn[layer], g_mlp[layer])
        return hidden.reshape(n_tok, width)

    return jax.shard_map(per_device, mesh=mesh, in_specs=(tok_spec, seg_spec, mat_spec, mat_spec, mat_spec, mat_spec, mat_spec, mat_spec, mat_spec, gain_spec, gain_spec), out_specs=tok_spec, check_vma=False)
```

```python
import functools

import jax
import jax.numpy as jnp
from jax import lax
from jax.experimental import pallas as pl
from jax.experimental.pallas import tpu as pltpu
from jax.sharding import PartitionSpec as P

D = 2048
FF = 11008
HEADS = 16
HEAD = 128
TOK = 1024
EPS = 1e-5
ROPE_BASE = 10000.0
MESH = pl.DeviceIdType.MESH
F32 = jnp.float32
BF16 = jnp.bfloat16

LAYERS = 2
SLOTS = 16
AHEAD = 4
AHEAD0 = 2
ROWS = D // 4
FF_ROWS = FF // 4
TAIL = 192
NAMES = ("q", "k", "v", "o", "g", "u", "d")

N_Q = 4
N_GU = 21
N_D = 10
CH_Q = 1
CH_O = CH_Q + N_Q
CH_GU = CH_O + N_Q
CH_GL = CH_GU + N_GU
CH_D = CH_GL + 1
CH_DR = CH_D + N_D
PER_LAYER = CH_DR + 1
CHUNKS = LAYERS * PER_LAYER
TICKS = CHUNKS + 2

N_GT = FF // 256
ST_Q = 1
ST_A = ST_Q + N_Q
ST_O = ST_A + HEADS
ST_G = ST_O + 4
ST_D = ST_G + N_GT
ST_T = ST_D + 20
STEPS = ST_T + 2
ALL_STEPS = LAYERS * STEPS

MB = 256
NB = 128
QB = 256


def layer_kernel(*refs):
    tok, cos_ref, sin_ref, first_ref, gain_ref = refs[:5]
    own = dict(zip(NAMES, refs[5:12]))
    out = refs[12]
    b1 = dict(zip(NAMES, refs[13:20]))
    b2 = dict(zip(NAMES, refs[20:27]))
    b3 = dict(zip(NAMES, refs[27:34]))
    x_ref, h_ref, q_ref, kv_ref, a_ref, wbuf, dbuf, wsem, dsem, iosem = refs[34:44]
    s0s, s0r, s1s, s1r, s2s, s2r, s3s, s3r = refs[44:]
    sources = (own, b1, b2, b3)
    y = lax.axis_index("rep")
    d = lax.axis_index("fsdp")
    side = d // 2
    core = lax.rem(d, 2)
    x_dev = (y, lax.rem(d + 2, 4))
    y_dev = (1 - y, d)
    c_dev = (y, d + 1 - 2 * core)

    def rel(block):
        return 2 * lax.rem(block // 2 + side, 2) + lax.rem(block + core, 2)

    load_tok = pltpu.make_async_copy(tok, q_ref, iosem)
    load_tok.start()

    barrier = pltpu.get_barrier_semaphore()
    for dev in (x_dev, y_dev, c_dev):
        pl.semaphore_signal(barrier, inc=1, device_id=dev, device_id_type=MESH)
    pl.semaphore_wait(barrier, 3)

    def for_chunk(k, fn, lo=0):
        layer = k // PER_LAYER
        i = lax.rem(k, PER_LAYER)
        slot = lax.rem(k, SLOTS)
        ok = (k >= lo) & (k < CHUNKS)

        def case(cond, items):
            @pl.when(ok & cond)
            def _():
                for n, (name, r0, nr, c0, nc) in enumerate(items):
                    fn(name, layer, r0, nr, c0, nc, slot, n)

        case(i == 0, [("k", 0, ROWS, 0, 256), ("v", 0, ROWS, 0, 256)])
        jq = pl.multiple_of((i - CH_Q) * 512, 512)
        case((i >= CH_Q) & (i < CH_O), [("q", 0, ROWS, jq, 512)])
        jo = pl.multiple_of((i - CH_O) * 512, 512)
        case((i >= CH_O) & (i < CH_GU), [("o", 0, ROWS, jo, 512)])
        jg = pl.multiple_of((i - CH_GU) * 512, 512)
        case((i >= CH_GU) & (i < CH_GL), [("g", 0, ROWS, jg, 512), ("u", 0, ROWS, jg, 512)])
        case(i == CH_GL, [("g", 0, ROWS, N_GU * 512, 256), ("u", 0, ROWS, N_GU * 512, 256)])
        jd = core * TAIL + (i - CH_D) * 256
        case((i >= CH_D) & (i < CH_DR), [("d", jd, 256, 0, D)])
        case(i == CH_DR, [("d", (1 - core) * 2560, TAIL, 0, D)])

    def view(bufs, name, layer, r0, nr, c0, nc, half):
        if half:
            nr = nr // 2
            r0 = r0 + y * nr
        r0 = pl.multiple_of(r0, 32)
        return bufs[name].at[layer, pl.ds(r0, nr), pl.ds(c0, nc)]

    def remote(src, dst, ss, rs, dev, half):
        def make(name, layer, r0, nr, c0, nc, slot, n):
            return pltpu.make_async_remote_copy(
                src_ref=view(src, name, layer, r0, nr, c0, nc, half),
                dst_ref=view(dst, name, layer, r0, nr, c0, nc, half),
                send_sem=ss.at[slot, n], recv_sem=rs.at[slot, n], device_id=dev, device_id_type=MESH)
        return make

    copy0 = remote(own, b1, s0s, s0r, c_dev, False)
    copy1 = remote(own, b2, s1s, s1r, x_dev, True)
    copy2 = remote(b2, b2, s2s, s2r, y_dev, True)
    copy3 = remote(b2, b3, s3s, s3r, c_dev, False)

    def start0(*a):
        copy0(*a).start()

    def start1(*a):
        copy1(*a).start()

    def relay2(*a):
        copy1(*a).wait_recv()
        copy2(*a).start()

    def relay3(*a):
        copy2(*a).wait_recv()
        copy3(*a).start()

    def finish(*a):
        copy0(*a).wait_recv()
        copy3(*a).wait_recv()
        copy0(*a).wait_send()
        copy1(*a).wait_send()
        copy2(*a).wait_send()
        copy3(*a).wait_send()

    def tick(k):
        for_chunk(k + AHEAD, start1, AHEAD)
        for_chunk(k + AHEAD0, start0, AHEAD0)
        for_chunk(k, relay2)
        for_chunk(k - 1, relay3)
        for_chunk(k - 2, finish)

    def need(s):
        layer = s // STEPS
        i = lax.rem(s, STEPS)
        v = jnp.where(i < ST_A, 3 + i,
            jnp.where(i < ST_O, 7 + (i - ST_A + 1) * 5 // HEADS,
            jnp.where(i < ST_G, 12,
            jnp.where(i < ST_D, 12 + (i - ST_G) // 2,
            jnp.where(i < ST_T, CH_D + 4 + 2 * ((i - ST_D) // 4), CH_DR + 3)))))
        return jnp.minimum(layer * PER_LAYER + v, TICKS)

    def ticks(lo, hi):
        @pl.loop(lo, hi)
        def _(k):
            tick(k)

    def load_tile(s):
        layer = s // STEPS
        i = lax.rem(s, STEPS)
        slot = lax.rem(s, 2)

        def cols(name, c0, nc, w0):
            for r, src in enumerate(sources):
                pltpu.make_async_copy(src[name].at[layer, :, pl.ds(c0, nc)],
                                      wbuf.at[slot, pl.ds(r * ROWS, ROWS), pl.ds(w0, nc)], wsem.at[slot]).start()

        @pl.when(i == 0)
        def _():
            cols("k", 0, 256, 0)
            cols("v", 0, 256, 256)

        @pl.when((i >= ST_Q) & (i < ST_A))
        def _():
            cols("q", pl.multiple_of((i - ST_Q) * 512, 512), 512, 0)

        @pl.when((i >= ST_O) & (i < ST_G))
        def _():
            cols("o", pl.multiple_of((i - ST_O) * 512, 512), 512, 0)

        @pl.when((i >= ST_G) & (i < ST_D))
        def _():
            c0 = pl.multiple_of((i - ST_G) * 256, 256)
            cols("g", c0, 256, 0)
            cols("u", c0, 256, 256)

        for r, src in enumerate(sources):
            src_core = core if r % 2 == 0 else 1 - core

            @pl.when((i >= ST_D) & (i < ST_T) & (lax.rem(i - ST_D, 4) == r))
            def _():
                r0 = pl.multiple_of(src_core * TAIL + (i - ST_D) // 4 * 512, 64)
                pltpu.make_async_copy(src["d"].at[layer, pl.ds(r0, 512), :], dbuf.at[slot], dsem.at[slot]).start()

            @pl.when(i == ST_T + r // 2)
            def _():
                r0 = pl.multiple_of((1 - src_core) * 2560, 512)
                w0 = pl.multiple_of(src_core * TAIL, TAIL)
                pltpu.make_async_copy(src["d"].at[layer, pl.ds(r0, TAIL), :], dbuf.at[slot, pl.ds(w0, TAIL), :],
                                      dsem.at[slot]).start()

    def norm(layer, which):
        @pl.loop(0, TOK // NB)
        def _(m):
            rows = pl.ds(pl.multiple_of(m * NB, NB), NB)
            total = jnp.zeros((NB, 1), F32)
            for b in range(4):
                blk = x_ref[rows, pl.ds(b * ROWS, ROWS)]
                total = total + jnp.sum(blk * blk, axis=1, keepdims=True)
            inv = lax.rsqrt(total * (1.0 / D) + EPS)
            for b in range(4):
                blk = x_ref[rows, pl.ds(b * ROWS, ROWS)]
                gain = gain_ref[which * LAYERS + layer, :, pl.ds(b * ROWS, ROWS)]
                c0 = pl.multiple_of(rel(b) * ROWS, ROWS)
                h_ref[rows, pl.ds(c0, ROWS)] = (blk * inv * gain).astype(BF16)

    def rotate(vals, rows):
        vals = vals.astype(BF16).astype(F32)
        turned = pltpu.roll(vals, HEAD // 2, 1)
        return (vals * cos_ref[rows, :] + turned * sin_ref[rows, :]).astype(BF16)

    def tile_product(slot, finish_rows):
        @pl.loop(0, TOK // MB)
        def _(m):
            rows = pl.ds(pl.multiple_of(m * MB, MB), MB)
            finish_rows(rows, jnp.dot(h_ref[rows, :], wbuf[slot], preferred_element_type=F32))

    def kv_step(slot):
        def fin(rows, acc):
            for b in range(2):
                kv_ref[rows, pl.ds(b * HEAD, HEAD)] = rotate(acc[:, b * HEAD:(b + 1) * HEAD], rows)
            kv_ref[rows, pl.ds(256, 256)] = acc[:, 256:].astype(BF16)
        tile_product(slot, fin)

    def q_step(slot, j):
        def fin(rows, acc):
            for b in range(4):
                c0 = pl.multiple_of(j * 512 + b * HEAD, HEAD)
                q_ref[rows, pl.ds(c0, HEAD)] = rotate(acc[:, b * HEAD:(b + 1) * HEAD], rows)
        tile_product(slot, fin)

    def o_step(slot, j):
        def fin(rows, acc):
            c0 = pl.ds(pl.multiple_of(j * 512, 512), 512)
            x_ref[rows, c0] = x_ref[rows, c0] + acc
        tile_product(slot, fin)

    def g_step(slot, j):
        def fin(rows, acc):
            gate = acc[:, :256]
            up = acc[:, 256:]
            c0 = pl.multiple_of(j * 256, 256)
            a_ref[rows, pl.ds(c0, 256)] = (gate * jax.nn.sigmoid(gate) * up).astype(BF16)
        tile_product(slot, fin)

    def attend(head):
        kv = head // 8
        q0 = pl.multiple_of(head * HEAD, HEAD)
        k0 = pl.multiple_of(kv * HEAD, HEAD)
        v0 = pl.multiple_of(256 + kv * HEAD, HEAD)
        o0 = pl.multiple_of(rel(head // 4) * ROWS + lax.rem(head, 4) * HEAD, HEAD)
        scale = HEAD ** -0.5
        for b in range(TOK // QB):
            keys = (b + 1) * QB
            rows = pl.ds(b * QB, QB)
            scores = lax.dot_general(q_ref[rows, pl.ds(q0, HEAD)], kv_ref[pl.ds(0, keys), pl.ds(k0, HEAD)],
                                     (((1,), (1,)), ((), ())), preferred_element_type=F32)
            key_idx = lax.broadcasted_iota(jnp.int32, (QB, keys), 1)
            row_idx = lax.broadcasted_iota(jnp.int32, (QB, keys), 0) + b * QB
            ok = (key_idx >= first_ref[rows, :]) & (key_idx <= row_idx)
            scores = jnp.where(ok, scores, -1e30)
            top = jnp.max(scores, axis=1, keepdims=True)
            probs = jnp.exp((scores - top) * scale)
            inv = 1.0 / jnp.sum(probs, axis=1, keepdims=True)
            probs = (probs * inv).astype(BF16)
            mixed = jnp.dot(probs, kv_ref[pl.ds(0, keys), pl.ds(v0, HEAD)], preferred_element_type=F32)
            h_ref[rows, pl.ds(o0, HEAD)] = mixed.astype(BF16)

    def d_step(slot, i):
        r = lax.rem(i, 4)
        src_side = lax.rem(side + r // 2, 2)
        src_core = lax.rem(core + r, 2)
        c0 = pl.multiple_of(src_side * (2 * FF_ROWS) + src_core * (FF_ROWS + TAIL) + i // 4 * 512, HEAD)

        @pl.loop(0, TOK // MB)
        def _(m):
            rows = pl.ds(pl.multiple_of(m * MB, MB), MB)
            x_ref[rows, :] = x_ref[rows, :] + jnp.dot(a_ref[rows, pl.ds(c0, 512)], dbuf[slot], preferred_element_type=F32)

    def t_step(slot, i):
        src_side = lax.rem(side + i, 2)
        c0 = pl.multiple_of(src_side * (2 * FF_ROWS) + 2560, HEAD)

        @pl.loop(0, TOK // MB)
        def _(m):
            rows = pl.ds(pl.multiple_of(m * MB, MB), MB)
            x_ref[rows, :] = x_ref[rows, :] + jnp.dot(a_ref[rows, pl.ds(c0, 2 * TAIL)], dbuf[slot, pl.ds(0, 2 * TAIL), :],
                                                      preferred_element_type=F32)

    def wait_w(slot):
        pltpu.make_async_copy(wbuf.at[slot], wbuf.at[slot], wsem.at[slot]).wait()

    def step(s):
        ticks(need(s), need(s + 1))

        @pl.when(s + 1 < ALL_STEPS)
        def _():
            load_tile(s + 1)

        layer = s // STEPS
        i = lax.rem(s, STEPS)
        slot = lax.rem(s, 2)

        @pl.when((i == 0) | (i == ST_G))
        def _():
            norm(layer, jnp.where(i == 0, 0, 1))

        @pl.when((i < ST_A) | ((i >= ST_O) & (i < ST_D)))
        def _():
            wait_w(slot)

        @pl.when(i == 0)
        def _():
            kv_step(slot)

        @pl.when((i >= ST_Q) & (i < ST_A))
        def _():
            q_step(slot, i - ST_Q)

        @pl.when((i >= ST_A) & (i < ST_O))
        def _():
            attend(i - ST_A)

        @pl.when((i >= ST_O) & (i < ST_G))
        def _():
            o_step(slot, i - ST_O)

        @pl.when((i >= ST_G) & (i < ST_D))
        def _():
            g_step(slot, i - ST_G)

        @pl.when((i >= ST_D) & (i < ST_T))
        def _():
            pltpu.make_async_copy(dbuf.at[slot], dbuf.at[slot], dsem.at[slot]).wait()
            d_step(slot, i - ST_D)

        @pl.when(i >= ST_T)
        def _():
            whole = dbuf.at[slot, pl.ds(0, 2 * TAIL), :]
            pltpu.make_async_copy(whole, whole, dsem.at[slot]).wait()
            t_step(slot, i - ST_T)

    @pl.loop(0, AHEAD)
    def _(k):
        for_chunk(k, start1)

    @pl.loop(0, AHEAD0)
    def _(k):
        for_chunk(k, start0)

    load_tok.wait()

    @pl.loop(0, TOK // NB)
    def _(m):
        rows = pl.ds(pl.multiple_of(m * NB, NB), NB)
        x_ref[rows, :] = q_ref[rows, :].astype(F32)

    ticks(0, need(0))
    load_tile(0)

    @pl.loop(0, ALL_STEPS)
    def _(s):
        step(s)

    store = pltpu.make_async_copy(x_ref, out, iosem)
    store.start()
    store.wait()


def run_layers(tokens, cos_tab, sin_tab, first, gains, weights):
    shapes = [jax.ShapeDtypeStruct(w.shape, w.dtype) for w in weights]
    sem = pltpu.SemaphoreType.DMA((SLOTS, 2))
    any_spec = pl.BlockSpec(memory_space=pl.ANY)
    vmem_spec = pl.BlockSpec(memory_space=pltpu.VMEM)
    outs = pl.pallas_call(
        layer_kernel,
        out_shape=[jax.ShapeDtypeStruct((TOK, D), F32)] + shapes * 3,
        in_specs=[any_spec] + [vmem_spec] * 4 + [any_spec] * 7,
        out_specs=[any_spec] * 22,
        scratch_shapes=[
            pltpu.VMEM((TOK, D), F32),
            pltpu.VMEM((TOK, D), BF16),
            pltpu.VMEM((TOK, D), BF16),
            pltpu.VMEM((TOK, 512), BF16),
            pltpu.VMEM((TOK, FF), BF16),
            pltpu.VMEM((2, D, 512), BF16),
            pltpu.VMEM((2, 512, D), BF16),
            pltpu.SemaphoreType.DMA((2,)),
            pltpu.SemaphoreType.DMA((2,)),
            pltpu.SemaphoreType.DMA,
        ] + [sem] * 8,
        compiler_params=pltpu.CompilerParams(collective_id=0, has_side_effects=True, vmem_limit_bytes=66 * 1000 * 1000),
        name="two_layers",
    )(tokens, cos_tab, sin_tab, first, gains, *weights)
    return outs[0]


def rope_tables(seg_ids):
    tok_idx = lax.iota(jnp.int32, TOK)
    is_first = jnp.concatenate([tok_idx[:1] == 0, seg_ids[1:] != seg_ids[:-1]])
    first = lax.cummax(jnp.where(is_first, tok_idx, 0), axis=0)
    tok_pos = (tok_idx - first).astype(F32)
    half_dim = HEAD // 2
    inv_freq = ROPE_BASE ** (-jnp.arange(half_dim, dtype=F32) / half_dim)
    angles = tok_pos[:, None] * inv_freq[None, :]
    cos, sin = jnp.cos(angles), jnp.sin(angles)
    return jnp.concatenate([cos, cos], axis=1), jnp.concatenate([-sin, sin], axis=1), first[:, None]


def solution(mesh):
    tok_spec = P(("rep", "fsdp"), None)
    seg_spec = P(("rep", "fsdp"))
    mat_spec = P(None, "fsdp", None)
    gain_spec = P(None, None)

    def per_device(tokens, seg_ids, w_q, w_k, w_v, w_o, w_gate, w_up, w_down, g_attn, g_mlp):
        cos_tab, sin_tab, first = rope_tables(seg_ids)
        gains = jnp.concatenate([g_attn, g_mlp], axis=0).astype(F32).reshape(2 * LAYERS, 1, D)
        return run_layers(tokens, cos_tab, sin_tab, first, gains, (w_q, w_k, w_v, w_o, w_gate, w_up, w_down))

    return jax.shard_map(per_device, mesh=mesh, in_specs=(tok_spec, seg_spec, mat_spec, mat_spec, mat_spec, mat_spec, mat_spec, mat_spec, mat_spec, gain_spec, gain_spec), out_specs=tok_spec, check_vma=False)
```

```python
import functools

import jax
import jax.numpy as jnp
from jax import lax
from jax.experimental import pallas as pl
from jax.experimental.pallas import tpu as pltpu
from jax.sharding import PartitionSpec as P

D = 2048
FF = 11008
HEADS = 16
HEAD = 128
TOK = 1024
EPS = 1e-5
ROPE_BASE = 10000.0
MESH = pl.DeviceIdType.MESH
F32 = jnp.float32
BF16 = jnp.bfloat16

LAYERS = 2
SLOTS = 16
AHEAD = 8
AHEAD0 = 2
LAG3 = 2
LAGF = 3
ROWS = D // 4
FF_ROWS = FF // 4
TAIL = 192
NAMES = ("q", "k", "v", "o", "g", "u", "d")

N_Q = 4
N_GU = 21
N_D = 10
CH_Q = 1
CH_O = CH_Q + N_Q
CH_GU = CH_O + N_Q
CH_GL = CH_GU + N_GU
CH_D = CH_GL + 1
CH_DR = CH_D + N_D
PER_LAYER = CH_DR + 1
CHUNKS = LAYERS * PER_LAYER
TICKS = CHUNKS + LAGF

N_GT = FF // 256
ST_Q = 1
ST_A = ST_Q + N_Q
ST_O = ST_A + HEADS
ST_G = ST_O + 4
ST_D = ST_G + N_GT
ST_T = ST_D + 20
STEPS = ST_T + 2
ALL_STEPS = LAYERS * STEPS
FIRST = 1 + LAGF

MB = 256
NB = 128
QB = 256


def layer_kernel(*refs):
    tok, cos_ref, sin_ref, first_ref, gain_ref = refs[:5]
    own = dict(zip(NAMES, refs[5:12]))
    out = refs[12]
    b1 = dict(zip(NAMES, refs[13:20]))
    b2 = dict(zip(NAMES, refs[20:27]))
    b3 = dict(zip(NAMES, refs[27:34]))
    x_ref, h_ref, q_ref, kv_ref, a_ref, wbuf, dbuf, wsem, dsem, iosem = refs[34:44]
    s0s, s0r, s1s, s1r, s2s, s2r, s3s, s3r = refs[44:]
    sources = (own, b1, b2, b3)
    y = lax.axis_index("rep")
    d = lax.axis_index("fsdp")
    side = d // 2
    core = lax.rem(d, 2)
    x_dev = (y, lax.rem(d + 2, 4))
    y_dev = (1 - y, d)
    c_dev = (y, d + 1 - 2 * core)

    def rel(block):
        return 2 * lax.rem(block // 2 + side, 2) + lax.rem(block + core, 2)

    load_tok = pltpu.make_async_copy(tok, q_ref, iosem)
    load_tok.start()

    barrier = pltpu.get_barrier_semaphore()
    for dev in (x_dev, y_dev, c_dev):
        pl.semaphore_signal(barrier, inc=1, device_id=dev, device_id_type=MESH)
    pl.semaphore_wait(barrier, 3)

    def for_chunk(k, fn, lo=0):
        layer = k // PER_LAYER
        i = lax.rem(k, PER_LAYER)
        slot = lax.rem(k, SLOTS)
        ok = (k >= lo) & (k < CHUNKS)

        def case(cond, items):
            @pl.when(ok & cond)
            def _():
                for n, (name, r0, nr, c0, nc) in enumerate(items):
                    fn(name, layer, r0, nr, c0, nc, slot, n)

        case(i == 0, [("k", 0, ROWS, 0, 256), ("v", 0, ROWS, 0, 256)])
        jq = pl.multiple_of((i - CH_Q) * 512, 512)
        case((i >= CH_Q) & (i < CH_O), [("q", 0, ROWS, jq, 512)])
        jo = pl.multiple_of((i - CH_O) * 512, 512)
        case((i >= CH_O) & (i < CH_GU), [("o", 0, ROWS, jo, 512)])
        jg = pl.multiple_of((i - CH_GU) * 512, 512)
        case((i >= CH_GU) & (i < CH_GL), [("g", 0, ROWS, jg, 512), ("u", 0, ROWS, jg, 512)])
        case(i == CH_GL, [("g", 0, ROWS, N_GU * 512, 256), ("u", 0, ROWS, N_GU * 512, 256)])
        jd = core * TAIL + (i - CH_D) * 256
        case((i >= CH_D) & (i < CH_DR), [("d", jd, 256, 0, D)])
        case(i == CH_DR, [("d", (1 - core) * 2560, TAIL, 0, D)])

    def view(bufs, name, layer, r0, nr, c0, nc, half):
        if half:
            nr = nr // 2
            r0 = r0 + y * nr
        r0 = pl.multiple_of(r0, 32)
        return bufs[name].at[layer, pl.ds(r0, nr), pl.ds(c0, nc)]

    def remote(src, dst, ss, rs, dev, half):
        def make(name, layer, r0, nr, c0, nc, slot, n):
            return pltpu.make_async_remote_copy(
                src_ref=view(src, name, layer, r0, nr, c0, nc, half),
                dst_ref=view(dst, name, layer, r0, nr, c0, nc, half),
                send_sem=ss.at[slot, n], recv_sem=rs.at[slot, n], device_id=dev, device_id_type=MESH)
        return make

    copy0 = remote(own, b1, s0s, s0r, c_dev, False)
    copy1 = remote(own, b2, s1s, s1r, x_dev, True)
    copy2 = remote(b2, b2, s2s, s2r, y_dev, True)
    copy3 = remote(b2, b3, s3s, s3r, c_dev, False)

    def start0(*a):
        copy0(*a).start()

    def start1(*a):
        copy1(*a).start()

    def relay2(*a):
        copy1(*a).wait_recv()
        copy2(*a).start()

    def relay3(*a):
        copy2(*a).wait_recv()
        copy3(*a).start()

    def finish(*a):
        copy0(*a).wait_recv()
        copy3(*a).wait_recv()
        copy0(*a).wait_send()
        copy1(*a).wait_send()
        copy2(*a).wait_send()
        copy3(*a).wait_send()

    def tick(k):
        for_chunk(k, relay2)
        for_chunk(k + AHEAD, start1, AHEAD)
        for_chunk(k + AHEAD0, start0, AHEAD0)
        for_chunk(k - LAG3, relay3)
        for_chunk(k - LAGF, finish)

    def target(s):
        i = lax.rem(s, STEPS)
        lead = jnp.where(i < ST_A, jnp.minimum(8, 5 + i),
               jnp.where(i < 35, 9 + (i - ST_A) // 4,
               jnp.where(i < ST_D, 16 + (i - 34) // 2,
               jnp.where(i < 84, 34 + 2 * ((i - ST_D) // 4) + jnp.minimum(1, lax.rem(i - ST_D, 4)), 44 + (i - 84) // 2))))
        lead = lead + s // STEPS * PER_LAYER
        i = lax.rem(s + 1, STEPS)
        data = jnp.where(i < ST_A, i,
               jnp.where(i < ST_O, 0,
               jnp.where(i < ST_G, CH_O + i - ST_O,
               jnp.where(i < ST_D, CH_GU + (i - ST_G) // 2,
               jnp.where(i < ST_T, CH_D + 1 + 2 * ((i - ST_D) // 4), CH_DR)))))
        data = data + 1 + LAGF + (s + 1) // STEPS * PER_LAYER
        return jnp.minimum(jnp.maximum(lead, data), TICKS)

    def ticks(lo, hi):
        @pl.loop(lo, hi)
        def _(k):
            tick(k)

    def load_tile(s):
        layer = s // STEPS
        i = lax.rem(s, STEPS)
        slot = lax.rem(s, 2)

        def cols(name, c0, nc, w0):
            for r, src in enumerate(sources):
                pltpu.make_async_copy(src[name].at[layer, :, pl.ds(c0, nc)],
                                      wbuf.at[slot, pl.ds(r * ROWS, ROWS), pl.ds(w0, nc)], wsem.at[slot]).start()

        @pl.when(i == 0)
        def _():
            cols("k", 0, 256, 0)
            cols("v", 0, 256, 256)

        @pl.when((i >= ST_Q) & (i < ST_A))
        def _():
            cols("q", pl.multiple_of((i - ST_Q) * 512, 512), 512, 0)

        @pl.when((i >= ST_O) & (i < ST_G))
        def _():
            cols("o", pl.multiple_of((i - ST_O) * 512, 512), 512, 0)

        @pl.when((i >= ST_G) & (i < ST_D))
        def _():
            c0 = pl.multiple_of((i - ST_G) * 256, 256)
            cols("g", c0, 256, 0)
            cols("u", c0, 256, 256)

        for r, src in enumerate(sources):
            src_core = core if r % 2 == 0 else 1 - core

            @pl.when((i >= ST_D) & (i < ST_T) & (lax.rem(i - ST_D, 4) == r))
            def _():
                r0 = pl.multiple_of(src_core * TAIL + (i - ST_D) // 4 * 512, 64)
                pltpu.make_async_copy(src["d"].at[layer, pl.ds(r0, 512), :], dbuf.at[slot], dsem.at[slot]).start()

            @pl.when(i == ST_T + r // 2)
            def _():
                r0 = pl.multiple_of((1 - src_core) * 2560, 512)
                w0 = pl.multiple_of(src_core * TAIL, TAIL)
                pltpu.make_async_copy(src["d"].at[layer, pl.ds(r0, TAIL), :], dbuf.at[slot, pl.ds(w0, TAIL), :],
                                      dsem.at[slot]).start()

    def norm(layer, which):
        @pl.loop(0, TOK // NB)
        def _(m):
            rows = pl.ds(pl.multiple_of(m * NB, NB), NB)
            total = jnp.zeros((NB, 1), F32)
            for b in range(4):
                blk = x_ref[rows, pl.ds(b * ROWS, ROWS)]
                total = total + jnp.sum(blk * blk, axis=1, keepdims=True)
            inv = lax.rsqrt(total * (1.0 / D) + EPS)
            for b in range(4):
                blk = x_ref[rows, pl.ds(b * ROWS, ROWS)]
                gain = gain_ref[which * LAYERS + layer, :, pl.ds(b * ROWS, ROWS)]
                c0 = pl.multiple_of(rel(b) * ROWS, ROWS)
                h_ref[rows, pl.ds(c0, ROWS)] = (blk * inv * gain).astype(BF16)

    def rotate(vals, rows):
        vals = vals.astype(BF16).astype(F32)
        turned = pltpu.roll(vals, HEAD // 2, 1)
        return (vals * cos_ref[rows, :] + turned * sin_ref[rows, :]).astype(BF16)

    def tile_product(slot, finish_rows):
        @pl.loop(0, TOK // MB)
        def _(m):
            rows = pl.ds(pl.multiple_of(m * MB, MB), MB)
            finish_rows(rows, jnp.dot(h_ref[rows, :], wbuf[slot], preferred_element_type=F32))

    def kv_step(slot):
        def fin(rows, acc):
            for b in range(2):
                kv_ref[rows, pl.ds(b * HEAD, HEAD)] = rotate(acc[:, b * HEAD:(b + 1) * HEAD], rows)
            kv_ref[rows, pl.ds(256, 256)] = acc[:, 256:].astype(BF16)
        tile_product(slot, fin)

    def q_step(slot, j):
        def fin(rows, acc):
            for b in range(4):
                c0 = pl.multiple_of(j * 512 + b * HEAD, HEAD)
                q_ref[rows, pl.ds(c0, HEAD)] = rotate(acc[:, b * HEAD:(b + 1) * HEAD], rows)
        tile_product(slot, fin)

    def o_step(slot, j):
        def fin(rows, acc):
            c0 = pl.ds(pl.multiple_of(j * 512, 512), 512)
            x_ref[rows, c0] = x_ref[rows, c0] + acc
        tile_product(slot, fin)

    def g_step(slot, j):
        def fin(rows, acc):
            gate = acc[:, :256]
            up = acc[:, 256:]
            c0 = pl.multiple_of(j * 256, 256)
            a_ref[rows, pl.ds(c0, 256)] = (gate * jax.nn.sigmoid(gate) * up).astype(BF16)
        tile_product(slot, fin)

    def attend(head):
        kv = head // 8
        q0 = pl.multiple_of(head * HEAD, HEAD)
        k0 = pl.multiple_of(kv * HEAD, HEAD)
        v0 = pl.multiple_of(256 + kv * HEAD, HEAD)
        o0 = pl.multiple_of(rel(head // 4) * ROWS + lax.rem(head, 4) * HEAD, HEAD)
        scale = HEAD ** -0.5
        for b in range(TOK // QB):
            keys = (b + 1) * QB
            rows = pl.ds(b * QB, QB)
            scores = lax.dot_general(q_ref[rows, pl.ds(q0, HEAD)], kv_ref[pl.ds(0, keys), pl.ds(k0, HEAD)],
                                     (((1,), (1,)), ((), ())), preferred_element_type=F32)
            key_idx = lax.broadcasted_iota(jnp.int32, (QB, keys), 1)
            row_idx = lax.broadcasted_iota(jnp.int32, (QB, keys), 0) + b * QB
            ok = (key_idx >= first_ref[rows, :]) & (key_idx <= row_idx)
            scores = jnp.where(ok, scores, -1e30)
            top = jnp.max(scores, axis=1, keepdims=True)
            probs = jnp.exp((scores - top) * scale)
            inv = 1.0 / jnp.sum(probs, axis=1, keepdims=True)
            probs = (probs * inv).astype(BF16)
            mixed = jnp.dot(probs, kv_ref[pl.ds(0, keys), pl.ds(v0, HEAD)], preferred_element_type=F32)
            h_ref[rows, pl.ds(o0, HEAD)] = mixed.astype(BF16)

    def d_step(slot, i):
        r = lax.rem(i, 4)
        src_side = lax.rem(side + r // 2, 2)
        src_core = lax.rem(core + r, 2)
        c0 = pl.multiple_of(src_side * (2 * FF_ROWS) + src_core * (FF_ROWS + TAIL) + i // 4 * 512, HEAD)

        @pl.loop(0, TOK // MB)
        def _(m):
            rows = pl.ds(pl.multiple_of(m * MB, MB), MB)
            x_ref[rows, :] = x_ref[rows, :] + jnp.dot(a_ref[rows, pl.ds(c0, 512)], dbuf[slot], preferred_element_type=F32)

    def t_step(slot, i):
        src_side = lax.rem(side + i, 2)
        c0 = pl.multiple_of(src_side * (2 * FF_ROWS) + 2560, HEAD)

        @pl.loop(0, TOK // MB)
        def _(m):
            rows = pl.ds(pl.multiple_of(m * MB, MB), MB)
            x_ref[rows, :] = x_ref[rows, :] + jnp.dot(a_ref[rows, pl.ds(c0, 2 * TAIL)], dbuf[slot, pl.ds(0, 2 * TAIL), :],
                                                      preferred_element_type=F32)

    def wait_w(slot):
        pltpu.make_async_copy(wbuf.at[slot], wbuf.at[slot], wsem.at[slot]).wait()

    def step(s):
        ticks(jnp.where(s == 0, FIRST, target(s - 1)), target(s))

        @pl.when(s + 1 < ALL_STEPS)
        def _():
            load_tile(s + 1)

        layer = s // STEPS
        i = lax.rem(s, STEPS)
        slot = lax.rem(s, 2)

        @pl.when((i == 0) | (i == ST_G))
        def _():
            norm(layer, jnp.where(i == 0, 0, 1))

        @pl.when((i < ST_A) | ((i >= ST_O) & (i < ST_D)))
        def _():
            wait_w(slot)

        @pl.when(i == 0)
        def _():
            kv_step(slot)

        @pl.when((i >= ST_Q) & (i < ST_A))
        def _():
            q_step(slot, i - ST_Q)

        @pl.when((i >= ST_A) & (i < ST_O))
        def _():
            attend(i - ST_A)

        @pl.when((i >= ST_O) & (i < ST_G))
        def _():
            o_step(slot, i - ST_O)

        @pl.when((i >= ST_G) & (i < ST_D))
        def _():
            g_step(slot, i - ST_G)

        @pl.when((i >= ST_D) & (i < ST_T))
        def _():
            pltpu.make_async_copy(dbuf.at[slot], dbuf.at[slot], dsem.at[slot]).wait()
            d_step(slot, i - ST_D)

        @pl.when(i >= ST_T)
        def _():
            whole = dbuf.at[slot, pl.ds(0, 2 * TAIL), :]
            pltpu.make_async_copy(whole, whole, dsem.at[slot]).wait()
            t_step(slot, i - ST_T)

    @pl.loop(0, AHEAD)
    def _(k):
        for_chunk(k, start1)

    @pl.loop(0, AHEAD0)
    def _(k):
        for_chunk(k, start0)

    load_tok.wait()

    @pl.loop(0, TOK // NB)
    def _(m):
        rows = pl.ds(pl.multiple_of(m * NB, NB), NB)
        x_ref[rows, :] = q_ref[rows, :].astype(F32)

    ticks(0, FIRST)
    load_tile(0)

    @pl.loop(0, ALL_STEPS)
    def _(s):
        step(s)

    store = pltpu.make_async_copy(x_ref, out, iosem)
    store.start()
    store.wait()


def run_layers(tokens, cos_tab, sin_tab, first, gains, weights):
    shapes = [jax.ShapeDtypeStruct(w.shape, w.dtype) for w in weights]
    sem = pltpu.SemaphoreType.DMA((SLOTS, 2))
    any_spec = pl.BlockSpec(memory_space=pl.ANY)
    vmem_spec = pl.BlockSpec(memory_space=pltpu.VMEM)
    outs = pl.pallas_call(
        layer_kernel,
        out_shape=[jax.ShapeDtypeStruct((TOK, D), F32)] + shapes * 3,
        in_specs=[any_spec] + [vmem_spec] * 4 + [any_spec] * 7,
        out_specs=[any_spec] * 22,
        scratch_shapes=[
            pltpu.VMEM((TOK, D), F32),
            pltpu.VMEM((TOK, D), BF16),
            pltpu.VMEM((TOK, D), BF16),
            pltpu.VMEM((TOK, 512), BF16),
            pltpu.VMEM((TOK, FF), BF16),
            pltpu.VMEM((2, D, 512), BF16),
            pltpu.VMEM((2, 512, D), BF16),
            pltpu.SemaphoreType.DMA((2,)),
            pltpu.SemaphoreType.DMA((2,)),
            pltpu.SemaphoreType.DMA,
        ] + [sem] * 8,
        compiler_params=pltpu.CompilerParams(collective_id=0, has_side_effects=True, vmem_limit_bytes=66 * 1000 * 1000),
        name="two_layers",
    )(tokens, cos_tab, sin_tab, first, gains, *weights)
    return outs[0]


def rope_tables(seg_ids):
    tok_idx = lax.iota(jnp.int32, TOK)
    is_first = jnp.concatenate([tok_idx[:1] == 0, seg_ids[1:] != seg_ids[:-1]])
    first = lax.cummax(jnp.where(is_first, tok_idx, 0), axis=0)
    tok_pos = (tok_idx - first).astype(F32)
    half_dim = HEAD // 2
    inv_freq = ROPE_BASE ** (-jnp.arange(half_dim, dtype=F32) / half_dim)
    angles = tok_pos[:, None] * inv_freq[None, :]
    cos, sin = jnp.cos(angles), jnp.sin(angles)
    return jnp.concatenate([cos, cos], axis=1), jnp.concatenate([-sin, sin], axis=1), first[:, None]


def solution(mesh):
    tok_spec = P(("rep", "fsdp"), None)
    seg_spec = P(("rep", "fsdp"))
    mat_spec = P(None, "fsdp", None)
    gain_spec = P(None, None)

    def per_device(tokens, seg_ids, w_q, w_k, w_v, w_o, w_gate, w_up, w_down, g_attn, g_mlp):
        cos_tab, sin_tab, first = rope_tables(seg_ids)
        gains = jnp.concatenate([g_attn, g_mlp], axis=0).astype(F32).reshape(2 * LAYERS, 1, D)
        return run_layers(tokens, cos_tab, sin_tab, first, gains, (w_q, w_k, w_v, w_o, w_gate, w_up, w_down))

    return jax.shard_map(per_device, mesh=mesh, in_specs=(tok_spec, seg_spec, mat_spec, mat_spec, mat_spec, mat_spec, mat_spec, mat_spec, mat_spec, gain_spec, gain_spec), out_specs=tok_spec, check_vma=False)
```

```python
import functools

import jax
import jax.numpy as jnp
import numpy as np
from jax import lax
from jax.experimental import pallas as pl
from jax.experimental.pallas import tpu as pltpu
from jax.sharding import PartitionSpec as P

D = 2048
FF = 11008
HEADS = 16
HEAD = 128
TOK = 1024
EPS = 1e-5
ROPE_BASE = 10000.0
MESH = pl.DeviceIdType.MESH
F32 = jnp.float32
BF16 = jnp.bfloat16

LAYERS = 2
SLOTS = 16
AHEAD = 8
AHEAD0 = 2
LAG3 = 2
LAGF = 3
ROWS = D // 4
FF_ROWS = FF // 4
TAIL = 192
NAMES = ("q", "k", "v", "o", "g", "u", "d")

N_Q = 4
N_GU = 21
N_D = 10
CH_Q = 1
CH_O = CH_Q + N_Q
CH_GU = CH_O + N_Q
CH_GL = CH_GU + N_GU
CH_D = CH_GL + 1
CH_DR = CH_D + N_D
PER_LAYER = CH_DR + 1
CHUNKS = LAYERS * PER_LAYER

N_GT = FF // 256
ST_Q = 1
ST_A = ST_Q + N_Q
ST_O = ST_A + HEADS
ST_G = ST_O + 4
ST_D = ST_G + N_GT
ST_T = ST_D + 4 * N_D
STEPS = ST_T + 2
ALL_STEPS = LAYERS * STEPS
LATE = 5

MB = 256
NB = 128
QB = 256


def layer_kernel(*refs):
    tok, seg, freq, g_attn, g_mlp = refs[:5]
    own = dict(zip(NAMES, refs[5:12]))
    out = refs[12]
    b1 = dict(zip(NAMES, refs[13:20]))
    b2 = dict(zip(NAMES, refs[20:27]))
    b3 = dict(zip(NAMES, refs[27:34]))
    (x_ref, h_ref, q_ref, kv_ref, a_ref, wbuf, dbuf, cos_ref, sin_ref, first_ref, gain_ref,
     seg_ref, freq_ref, ga_ref, gm_ref, wsem, dsem, iosem, outsem) = refs[34:53]
    s0s, s0r, s1s, s1r, s2s, s2r, s3s, s3r = refs[53:]
    sources = (own, b1, b2, b3)
    y = lax.axis_index("rep")
    d = lax.axis_index("fsdp")
    side = d // 2
    core = lax.rem(d, 2)
    x_dev = (y, lax.rem(d + 2, 4))
    y_dev = (1 - y, d)
    c_dev = (y, d + 1 - 2 * core)

    def rel(block):
        return 2 * lax.rem(block // 2 + side, 2) + lax.rem(block + core, 2)

    inputs = [pltpu.make_async_copy(src, dst, iosem.at[n]) for n, (src, dst) in enumerate(
        ((tok, q_ref), (seg, seg_ref), (freq, freq_ref), (g_attn, ga_ref), (g_mlp, gm_ref)))]
    for copy in inputs:
        copy.start()

    barrier = pltpu.get_barrier_semaphore()
    for dev in (x_dev, y_dev, c_dev):
        pl.semaphore_signal(barrier, inc=1, device_id=dev, device_id_type=MESH)
    pl.semaphore_wait(barrier, 3)

    def for_chunk(k, fn, lo=0):
        layer = k // PER_LAYER
        i = lax.rem(k, PER_LAYER)
        slot = lax.rem(k, SLOTS)
        ok = (k >= lo) & (k < CHUNKS)

        def case(cond, items, direct=False):
            @pl.when(ok & cond)
            def _():
                for n, (name, r0, nr, c0, nc) in enumerate(items):
                    fn(direct, name, layer, r0, nr, c0, nc, slot, n)

        case(i == 0, [("k", 0, ROWS, 0, 256), ("v", 0, ROWS, 0, 256)])
        jq = pl.multiple_of((i - CH_Q) * 512, 512)
        case((i >= CH_Q) & (i < CH_O), [("q", 0, ROWS, jq, 512)])
        jo = pl.multiple_of((i - CH_O) * 512, 512)
        case((i >= CH_O) & (i < CH_GU), [("o", 0, ROWS, jo, 512)])
        jg = pl.multiple_of((i - CH_GU) * 512, 512)
        case((i >= CH_GU) & (i < CH_GL), [("g", 0, ROWS, jg, 512), ("u", 0, ROWS, jg, 512)])
        case(i == CH_GL, [("g", 0, ROWS, N_GU * 512, 256), ("u", 0, ROWS, N_GU * 512, 256)])
        jd = core * TAIL + (i - CH_D) * 256
        case((i >= CH_D) & (i < CH_DR), [("d", jd, 256, 0, D)])
        last = [("d", (1 - core) * 2560, TAIL, 0, D)]
        case((i == CH_DR) & (k < CHUNKS - 1), last)
        case((i == CH_DR) & (k == CHUNKS - 1), last, True)

    def view(bufs, name, layer, r0, nr, c0, nc, half):
        if half:
            nr = nr // 2
            r0 = r0 + y * nr
        r0 = pl.multiple_of(r0, 32)
        return bufs[name].at[layer, pl.ds(r0, nr), pl.ds(c0, nc)]

    def remote(src, dst, ss, rs, dev, half):
        def make(direct, name, layer, r0, nr, c0, nc, slot, n):
            part = half and not direct
            return pltpu.make_async_remote_copy(
                src_ref=view(src, name, layer, r0, nr, c0, nc, part),
                dst_ref=view(dst, name, layer, r0, nr, c0, nc, part),
                send_sem=ss.at[slot, n], recv_sem=rs.at[slot, n], device_id=dev, device_id_type=MESH)
        return make

    copy0 = remote(own, b1, s0s, s0r, c_dev, False)
    copy1 = remote(own, b2, s1s, s1r, x_dev, True)
    copy2 = remote(b2, b2, s2s, s2r, y_dev, True)
    copy3 = remote(b2, b3, s3s, s3r, c_dev, False)

    def start0(*a):
        copy0(*a).start()

    def start1(*a):
        copy1(*a).start()

    def relay2(*a):
        copy0(*a).wait_recv()
        copy1(*a).wait_recv()
        if not a[0]:
            copy2(*a).start()

    def relay3(*a):
        if not a[0]:
            copy2(*a).wait_recv()
        copy3(*a).start()

    def finish(*a):
        copy3(*a).wait_recv()
        copy0(*a).wait_send()
        copy1(*a).wait_send()
        if not a[0]:
            copy2(*a).wait_send()
        copy3(*a).wait_send()

    def targets(s):
        i = lax.rem(s, STEPS)
        lead = jnp.where(i < ST_A, 5 + i,
               jnp.where(i < ST_D, jnp.maximum(11 + (i - ST_A) // 3, i // 2),
               jnp.where(i < ST_T, 17 + i // 4, 46)))
        lead = jnp.minimum(lead + s // STEPS * PER_LAYER, jnp.where(s < ALL_STEPS - LATE, CHUNKS - 1, CHUNKS))
        i = lax.rem(s + 1, STEPS)
        base = (s + 1) // STEPS * PER_LAYER
        part = lax.rem(i - ST_D + STEPS * 4, 4)
        in_d = (i >= ST_D) & (i < ST_T)
        chunk = jnp.where(i < ST_A, i,
                jnp.where(i < ST_O, ST_A - 1,
                jnp.where(i < ST_G, CH_O + i - ST_O,
                jnp.where(i < ST_D, CH_GU + (i - ST_G) // 2,
                jnp.where(i < ST_T, CH_D + (i - ST_D) // 4, CH_DR)))))
        chunk = jnp.minimum(chunk + base, CHUNKS - 1)
        need2 = chunk + jnp.where(in_d & (part == 0), 0, 1)
        need3 = chunk + jnp.where(in_d & (part < 2), 0, 1)
        needf = chunk + jnp.where((in_d & (part < 3)) | (i == ST_T), 0, 1)
        tf = jnp.maximum(lead - LAGF, needf)
        t3 = jnp.maximum(jnp.maximum(lead - LAG3, need3), tf)
        t2 = jnp.maximum(jnp.maximum(lead, need2), t3)
        return t2, t3, tf

    def relays(old, new):
        @pl.loop(old[0], new[0])
        def _(k):
            for_chunk(k, relay2)
            for_chunk(k + AHEAD, start1, AHEAD)
            for_chunk(k + AHEAD0, start0, AHEAD0)

        @pl.loop(old[1], new[1])
        def _(k):
            for_chunk(k, relay3)

        @pl.loop(old[2], new[2])
        def _(k):
            for_chunk(k, finish)

    def load_tile(s):
        layer = s // STEPS
        i = lax.rem(s, STEPS)
        slot = lax.rem(s, 2)

        def cols(name, c0, nc, w0):
            for r, src in enumerate(sources):
                pltpu.make_async_copy(src[name].at[layer, :, pl.ds(c0, nc)],
                                      wbuf.at[slot, pl.ds(r * ROWS, ROWS), pl.ds(w0, nc)], wsem.at[slot]).start()

        @pl.when(i == 0)
        def _():
            cols("k", 0, 256, 0)
            cols("v", 0, 256, 256)

        @pl.when((i >= ST_Q) & (i < ST_A))
        def _():
            cols("q", pl.multiple_of((i - ST_Q) * 512, 512), 512, 0)

        @pl.when((i >= ST_O) & (i < ST_G))
        def _():
            cols("o", pl.multiple_of((i - ST_O) * 512, 512), 512, 0)

        @pl.when((i >= ST_G) & (i < ST_D))
        def _():
            c0 = pl.multiple_of((i - ST_G) * 256, 256)
            cols("g", c0, 256, 0)
            cols("u", c0, 256, 256)

        for r, src in enumerate(sources):
            src_core = core if r % 2 == 0 else 1 - core

            @pl.when((i >= ST_D) & (i < ST_T) & (lax.rem(i - ST_D, 4) == r))
            def _():
                r0 = pl.multiple_of(src_core * TAIL + (i - ST_D) // 4 * 256, 64)
                pltpu.make_async_copy(src["d"].at[layer, pl.ds(r0, 256), :], dbuf.at[slot, pl.ds(0, 256), :], dsem.at[slot]).start()

            @pl.when(i == ST_T + r // 2)
            def _():
                r0 = pl.multiple_of((1 - src_core) * 2560, 512)
                w0 = pl.multiple_of(src_core * TAIL, TAIL)
                pltpu.make_async_copy(src["d"].at[layer, pl.ds(r0, TAIL), :], dbuf.at[slot, pl.ds(w0, TAIL), :],
                                      dsem.at[slot]).start()

    def norm(layer, which):
        @pl.loop(0, TOK // NB)
        def _(m):
            rows = pl.ds(pl.multiple_of(m * NB, NB), NB)
            total = jnp.zeros((NB, 1), F32)
            for b in range(4):
                blk = x_ref[rows, pl.ds(b * ROWS, ROWS)]
                total = total + jnp.sum(blk * blk, axis=1, keepdims=True)
            inv = lax.rsqrt(total * (1.0 / D) + EPS)
            for b in range(4):
                blk = x_ref[rows, pl.ds(b * ROWS, ROWS)]
                gain = gain_ref[which * LAYERS + layer, :, pl.ds(b * ROWS, ROWS)]
                c0 = pl.multiple_of(rel(b) * ROWS, ROWS)
                h_ref[rows, pl.ds(c0, ROWS)] = (blk * inv * gain).astype(BF16)

    def rotate(vals, rows):
        vals = vals.astype(BF16).astype(F32)
        turned = pltpu.roll(vals, HEAD // 2, 1)
        return (vals * cos_ref[rows, :] + turned * sin_ref[rows, :]).astype(BF16)

    def tile_product(slot, finish_rows):
        @pl.loop(0, TOK // MB)
        def _(m):
            rows = pl.ds(pl.multiple_of(m * MB, MB), MB)
            finish_rows(rows, jnp.dot(h_ref[rows, :], wbuf[slot], preferred_element_type=F32))

    def kv_step(slot):
        def fin(rows, acc):
            for b in range(2):
                kv_ref[rows, pl.ds(b * HEAD, HEAD)] = rotate(acc[:, b * HEAD:(b + 1) * HEAD], rows)
            kv_ref[rows, pl.ds(256, 256)] = acc[:, 256:].astype(BF16)
        tile_product(slot, fin)

    def q_step(slot, j):
        def fin(rows, acc):
            for b in range(4):
                c0 = pl.multiple_of(j * 512 + b * HEAD, HEAD)
                q_ref[rows, pl.ds(c0, HEAD)] = rotate(acc[:, b * HEAD:(b + 1) * HEAD], rows)
        tile_product(slot, fin)

    def o_step(slot, j):
        def fin(rows, acc):
            c0 = pl.ds(pl.multiple_of(j * 512, 512), 512)
            x_ref[rows, c0] = x_ref[rows, c0] + acc
        tile_product(slot, fin)

    def g_step(slot, j):
        def fin(rows, acc):
            gate = acc[:, :256]
            up = acc[:, 256:]
            c0 = pl.multiple_of(j * 256, 256)
            a_ref[rows, pl.ds(c0, 256)] = (gate * jax.nn.sigmoid(gate) * up).astype(BF16)
        tile_product(slot, fin)

    def attend(head):
        kv = head // 8
        q0 = pl.multiple_of(head * HEAD, HEAD)
        k0 = pl.multiple_of(kv * HEAD, HEAD)
        v0 = pl.multiple_of(256 + kv * HEAD, HEAD)
        o0 = pl.multiple_of(rel(head // 4) * ROWS + lax.rem(head, 4) * HEAD, HEAD)
        scale = HEAD ** -0.5
        for b in range(TOK // QB):
            keys = (b + 1) * QB
            rows = pl.ds(b * QB, QB)
            scores = lax.dot_general(q_ref[rows, pl.ds(q0, HEAD)], kv_ref[pl.ds(0, keys), pl.ds(k0, HEAD)],
                                     (((1,), (1,)), ((), ())), preferred_element_type=F32)
            key_idx = lax.broadcasted_iota(jnp.int32, (QB, keys), 1)
            row_idx = lax.broadcasted_iota(jnp.int32, (QB, keys), 0) + b * QB
            first = jnp.concatenate([first_ref[rows, :]] * (keys // HEAD), axis=1)
            ok = (key_idx >= first) & (key_idx <= row_idx)
            scores = jnp.where(ok, scores, -1e30)
            top = jnp.max(scores, axis=1, keepdims=True)
            probs = jnp.exp((scores - top) * scale)
            inv = 1.0 / jnp.sum(probs, axis=1, keepdims=True)
            probs = (probs * inv).astype(BF16)
            mixed = jnp.dot(probs, kv_ref[pl.ds(0, keys), pl.ds(v0, HEAD)], preferred_element_type=F32)
            h_ref[rows, pl.ds(o0, HEAD)] = mixed.astype(BF16)

    def add_product(slot, c0, depth, final):
        @pl.loop(0, TOK // MB)
        def _(m):
            rows = pl.ds(pl.multiple_of(m * MB, MB), MB)
            x_ref[rows, :] = x_ref[rows, :] + jnp.dot(a_ref[rows, pl.ds(c0, depth)], dbuf[slot, pl.ds(0, depth), :],
                                                      preferred_element_type=F32)

            @pl.when(final)
            def _():
                pltpu.make_async_copy(x_ref.at[rows, :], out.at[rows, :], outsem.at[m]).start()

    def d_step(slot, i):
        r = lax.rem(i, 4)
        src_side = lax.rem(side + r // 2, 2)
        src_core = lax.rem(core + r, 2)
        c0 = pl.multiple_of(src_side * (2 * FF_ROWS) + src_core * (FF_ROWS + TAIL) + i // 4 * 256, HEAD)
        add_product(slot, c0, 256, False)

    def t_step(slot, i, final):
        src_side = lax.rem(side + i, 2)
        c0 = pl.multiple_of(src_side * (2 * FF_ROWS) + 2560, HEAD)
        add_product(slot, c0, 2 * TAIL, final)

    def wait_w(slot):
        pltpu.make_async_copy(wbuf.at[slot], wbuf.at[slot], wsem.at[slot]).wait()

    def step(s):
        relays(targets(s - 1), targets(s))

        @pl.when(s + 1 < ALL_STEPS)
        def _():
            load_tile(s + 1)

        layer = s // STEPS
        i = lax.rem(s, STEPS)
        slot = lax.rem(s, 2)

        @pl.when((i == 0) | (i == ST_G))
        def _():
            norm(layer, jnp.where(i == 0, 0, 1))

        @pl.when((i < ST_A) | ((i >= ST_O) & (i < ST_D)))
        def _():
            wait_w(slot)

        @pl.when(i == 0)
        def _():
            kv_step(slot)

        @pl.when((i >= ST_Q) & (i < ST_A))
        def _():
            q_step(slot, i - ST_Q)

        @pl.when((i >= ST_A) & (i < ST_O))
        def _():
            attend(i - ST_A)

        @pl.when((i >= ST_O) & (i < ST_G))
        def _():
            o_step(slot, i - ST_O)

        @pl.when((i >= ST_G) & (i < ST_D))
        def _():
            g_step(slot, i - ST_G)

        @pl.when((i >= ST_D) & (i < ST_T))
        def _():
            whole = dbuf.at[slot, pl.ds(0, 256), :]
            pltpu.make_async_copy(whole, whole, dsem.at[slot]).wait()
            d_step(slot, i - ST_D)

        @pl.when(i >= ST_T)
        def _():
            whole = dbuf.at[slot, pl.ds(0, 2 * TAIL), :]
            pltpu.make_async_copy(whole, whole, dsem.at[slot]).wait()
            t_step(slot, i - ST_T, s == ALL_STEPS - 1)

    @pl.loop(0, AHEAD)
    def _(k):
        for_chunk(k, start1)

    @pl.loop(0, AHEAD0)
    def _(k):
        for_chunk(k, start0)

    for copy in inputs:
        copy.wait()

    for n, ref in enumerate((ga_ref, gm_ref)):
        for layer in range(LAYERS):
            gain_ref[n * LAYERS + layer] = ref[pl.ds(layer, 1), :].astype(F32)
    ids = seg_ref[...].astype(F32)
    lane = lax.broadcasted_iota(jnp.int32, (128, HEAD), 1)
    for b in range(TOK // 128):
        rows = pl.ds(b * 128, 128)
        mine = jnp.transpose(jnp.broadcast_to(ids[b:b + 1, :], (128, 128)))
        before = jnp.zeros((128, 128), F32)
        for c in range(TOK // 128):
            before = before + jnp.where(ids[c:c + 1, :] < mine, 1.0, 0.0)
        first = jnp.sum(before, axis=1, keepdims=True)
        pos = lax.broadcasted_iota(jnp.int32, (128, 128), 0).astype(F32) + (b * 128.0) - first
        angles = pos * freq_ref[...]
        cos_ref[rows, :] = jnp.cos(angles)
        sin = jnp.sin(angles)
        sin_ref[rows, :] = jnp.where(lane < HEAD // 2, -sin, sin)
        first_ref[rows, :] = jnp.broadcast_to(first, (128, 128)).astype(jnp.int32)

    @pl.loop(0, TOK // NB)
    def _(m):
        rows = pl.ds(pl.multiple_of(m * NB, NB), NB)
        x_ref[rows, :] = q_ref[rows, :].astype(F32)

    relays((0, 0, 0), (1, 1, 1))
    load_tile(0)

    @pl.loop(0, ALL_STEPS)
    def _(s):
        step(s)

    for m in range(TOK // MB):
        rows = pl.ds(m * MB, MB)
        pltpu.make_async_copy(x_ref.at[rows, :], out.at[rows, :], outsem.at[m]).wait()


def run_layers(tokens, seg_ids, g_attn, g_mlp, weights):
    shapes = [jax.ShapeDtypeStruct(w.shape, w.dtype) for w in weights]
    half_dim = HEAD // 2
    freq = np.float32(ROPE_BASE) ** (-np.arange(half_dim, dtype=np.float32) / np.float32(half_dim))
    freq = jnp.asarray(np.concatenate([freq, freq]).reshape(1, HEAD))
    sem = pltpu.SemaphoreType.DMA((SLOTS, 2))
    any_spec = pl.BlockSpec(memory_space=pl.ANY)
    outs = pl.pallas_call(
        layer_kernel,
        out_shape=[jax.ShapeDtypeStruct((TOK, D), F32)] + shapes * 3,
        in_specs=[any_spec] * 12,
        out_specs=[any_spec] * 22,
        scratch_shapes=[
            pltpu.VMEM((TOK, D), F32),
            pltpu.VMEM((TOK, D), BF16),
            pltpu.VMEM((TOK, D), BF16),
            pltpu.VMEM((TOK, 512), BF16),
            pltpu.VMEM((TOK, FF), BF16),
            pltpu.VMEM((2, D, 512), BF16),
            pltpu.VMEM((2, 2 * TAIL, D), BF16),
            pltpu.VMEM((TOK, HEAD), F32),
            pltpu.VMEM((TOK, HEAD), F32),
            pltpu.VMEM((TOK, HEAD), jnp.int32),
            pltpu.VMEM((2 * LAYERS, 1, D), F32),
            pltpu.VMEM((TOK // 128, 128), jnp.int32),
            pltpu.VMEM((1, HEAD), F32),
            pltpu.VMEM((LAYERS, D), BF16),
            pltpu.VMEM((LAYERS, D), BF16),
            pltpu.SemaphoreType.DMA((2,)),
            pltpu.SemaphoreType.DMA((2,)),
            pltpu.SemaphoreType.DMA((5,)),
            pltpu.SemaphoreType.DMA((TOK // MB,)),
        ] + [sem] * 8,
        compiler_params=pltpu.CompilerParams(collective_id=0, has_side_effects=True, vmem_limit_bytes=66 * 1000 * 1000),
        name="two_layers",
    )(tokens, seg_ids.reshape(TOK // 128, 128), freq, g_attn, g_mlp, *weights)
    return outs[0]


def solution(mesh):
    tok_spec = P(("rep", "fsdp"), None)
    seg_spec = P(("rep", "fsdp"))
    mat_spec = P(None, "fsdp", None)
    gain_spec = P(None, None)

    def per_device(tokens, seg_ids, w_q, w_k, w_v, w_o, w_gate, w_up, w_down, g_attn, g_mlp):
        return run_layers(tokens, seg_ids, g_attn, g_mlp, (w_q, w_k, w_v, w_o, w_gate, w_up, w_down))

    return jax.shard_map(per_device, mesh=mesh, in_specs=(tok_spec, seg_spec, mat_spec, mat_spec, mat_spec, mat_spec, mat_spec, mat_spec, mat_spec, gain_spec, gain_spec), out_specs=tok_spec, check_vma=False)
```

```python
import functools

import jax
import jax.numpy as jnp
import numpy as np
from jax import lax
from jax.experimental import pallas as pl
from jax.experimental.pallas import tpu as pltpu
from jax.sharding import PartitionSpec as P

D = 2048
FF = 11008
HEADS = 16
HEAD = 128
TOK = 1024
EPS = 1e-5
ROPE_BASE = 10000.0
MESH = pl.DeviceIdType.MESH
F32 = jnp.float32
BF16 = jnp.bfloat16

LAYERS = 2
SLOTS = 16
AHEAD = 8
AHEAD0 = 2
LAG3 = 2
LAGF = 3
ROWS = D // 4
FF_ROWS = FF // 4
TAIL = 192
NAMES = ("q", "k", "v", "o", "g", "u", "d")

N_Q = 4
N_GU = 21
N_D = 10
CH_Q = 1
CH_O = CH_Q + N_Q
CH_GU = CH_O + N_Q
CH_GL = CH_GU + N_GU
CH_D = CH_GL + 1
CH_DR = CH_D + N_D
PER_LAYER = CH_DR + 1
CHUNKS = LAYERS * PER_LAYER

N_GT = FF // 256
ST_Q = 1
ST_A = ST_Q + N_Q
ST_O = ST_A + HEADS
ST_G = ST_O + 4
ST_D = ST_G + N_GT
ST_T = ST_D + 4 * N_D - 2
STEPS = ST_D + 4 * N_D + 2
ALL_STEPS = LAYERS * STEPS - 3
FIRST = (3, 2, 1)
FINAL_K = 256 + 256 + 2 * TAIL

MB = 256
NB = 128
QB = 256


def layer_kernel(*refs):
    tok, seg, freq, g_attn, g_mlp = refs[:5]
    own = dict(zip(NAMES, refs[5:12]))
    out, last_out = refs[12:14]
    b1 = dict(zip(NAMES, refs[14:21]))
    b2 = dict(zip(NAMES, refs[21:28]))
    b3 = dict(zip(NAMES, refs[28:35]))
    (x_ref, h_ref, q_ref, kv_ref, a_ref, wbuf, dbuf, cos_ref, sin_ref, first_ref, gain_ref,
     seg_ref, freq_ref, ga_ref, gm_ref, wsem, dsem, iosem, outsem, lastsem) = refs[35:55]
    s0s, s0r, s1s, s1r, s2s, s2r, s3s, s3r = refs[55:]
    sources = (own, b1, b2, b3)
    y = lax.axis_index("rep")
    d = lax.axis_index("fsdp")
    side = d // 2
    core = lax.rem(d, 2)
    x_dev = (y, lax.rem(d + 2, 4))
    y_dev = (1 - y, d)
    c_dev = (y, d + 1 - 2 * core)

    def rel(block):
        return 2 * lax.rem(block // 2 + side, 2) + lax.rem(block + core, 2)

    inputs = [pltpu.make_async_copy(src, dst, iosem.at[n]) for n, (src, dst) in enumerate(
        ((tok, q_ref), (seg, seg_ref), (freq, freq_ref), (g_attn, ga_ref), (g_mlp, gm_ref)))]
    for copy in inputs:
        copy.start()

    barrier = pltpu.get_barrier_semaphore()
    for dev in (x_dev, y_dev, c_dev):
        pl.semaphore_signal(barrier, inc=1, device_id=dev, device_id_type=MESH)
    pl.semaphore_wait(barrier, 3)

    def for_chunk(k, fn, lo=0):
        layer = k // PER_LAYER
        i = lax.rem(k, PER_LAYER)
        slot = lax.rem(k, SLOTS)
        ok = (k >= lo) & (k < CHUNKS)

        def case(cond, items, direct=False):
            @pl.when(ok & cond)
            def _():
                for n, (name, r0, nr, c0, nc) in enumerate(items):
                    fn(direct, name, layer, r0, nr, c0, nc, slot, n)

        case(i == 0, [("k", 0, ROWS, 0, 256), ("v", 0, ROWS, 0, 256)])
        jq = pl.multiple_of((i - CH_Q) * 512, 512)
        case((i >= CH_Q) & (i < CH_O), [("q", 0, ROWS, jq, 512)])
        jo = pl.multiple_of((i - CH_O) * 512, 512)
        case((i >= CH_O) & (i < CH_GU), [("o", 0, ROWS, jo, 512)])
        jg = pl.multiple_of((i - CH_GU) * 512, 512)
        case((i >= CH_GU) & (i < CH_GL), [("g", 0, ROWS, jg, 512), ("u", 0, ROWS, jg, 512)])
        case(i == CH_GL, [("g", 0, ROWS, N_GU * 512, 256), ("u", 0, ROWS, N_GU * 512, 256)])
        jd = core * TAIL + (i - CH_D) * 256
        case((i >= CH_D) & (i < CH_DR), [("d", jd, 256, 0, D)])
        last = [("d", (1 - core) * 2560, TAIL, 0, D)]
        case((i == CH_DR) & (k < CHUNKS - 1), last)
        case((i == CH_DR) & (k == CHUNKS - 1), last, True)

    def view(bufs, name, layer, r0, nr, c0, nc, half):
        if half:
            nr = nr // 2
            r0 = r0 + y * nr
        r0 = pl.multiple_of(r0, 32)
        return bufs[name].at[layer, pl.ds(r0, nr), pl.ds(c0, nc)]

    def remote(src, dst, ss, rs, dev, half):
        def make(direct, name, layer, r0, nr, c0, nc, slot, n):
            part = half and not direct
            return pltpu.make_async_remote_copy(
                src_ref=view(src, name, layer, r0, nr, c0, nc, part),
                dst_ref=view(dst, name, layer, r0, nr, c0, nc, part),
                send_sem=ss.at[slot, n], recv_sem=rs.at[slot, n], device_id=dev, device_id_type=MESH)
        return make

    copy0 = remote(own, b1, s0s, s0r, c_dev, False)
    copy1 = remote(own, b2, s1s, s1r, x_dev, True)
    copy2 = remote(b2, b2, s2s, s2r, y_dev, True)
    copy3 = remote(b2, b3, s3s, s3r, c_dev, False)

    def start0(*a):
        copy0(*a).start()

    def start1(*a):
        copy1(*a).start()

    def wait0(*a):
        copy0(*a).wait_recv()

    def relay2(*a):
        copy1(*a).wait_recv()
        if not a[0]:
            copy2(*a).start()

    def relay3(*a):
        if not a[0]:
            copy2(*a).wait_recv()
        copy3(*a).start()

    def finish(*a):
        copy3(*a).wait_recv()
        copy0(*a).wait_send()
        copy1(*a).wait_send()
        if not a[0]:
            copy2(*a).wait_send()
        copy3(*a).wait_send()

    def targets(s):
        i = lax.rem(s, STEPS)
        lead = jnp.where(i < ST_A, 5 + i,
               jnp.where(i < ST_D, jnp.maximum(11 + (i - ST_A) // 3, i // 2 + 1),
               jnp.where(i < ST_D + 4 * N_D, 17 + i // 4, 46)))
        lead = jnp.minimum(lead + s // STEPS * PER_LAYER, CHUNKS - 1)
        nxt = jnp.minimum(s + 1, ALL_STEPS - 1)
        i = lax.rem(nxt, STEPS)
        base = nxt // STEPS * PER_LAYER
        early = jnp.where(i < ST_A, 1 + i,
                jnp.where(i < ST_O, ST_A,
                jnp.where(i < ST_G, 1 + CH_O + i - ST_O, 1 + CH_GU + (i - ST_G) // 2)))
        j = i - ST_D
        t = CH_D + j // 4
        p = lax.rem(j + 4 * STEPS, 4)
        late = i >= ST_D
        body = i < ST_T
        need2 = base + jnp.where(late, jnp.where(body, t + jnp.minimum(p, 1), jnp.where(j < 4 * N_D + 1, CH_DR, CH_DR + 1)), early)
        need3 = base + jnp.where(late, jnp.where(body, t + p // 2, CH_DR - 1 + (j - 4 * N_D + 2 + 1) // 2), early)
        needf = base + jnp.where(late, jnp.where(body, t + p // 3, CH_DR - 1 + (j - 4 * N_D + 2) // 2 + (j - 4 * N_D + 2) // 3), early)
        tf = jnp.maximum(lead - LAGF, needf)
        t3 = jnp.maximum(jnp.maximum(lead - LAG3, need3), tf)
        t2 = jnp.maximum(jnp.maximum(lead, need2), t3)
        return t2, t3, tf

    def relays(old, new):
        @pl.loop(old[0], new[0])
        def _(k):
            for_chunk(k, relay2)
            for_chunk(k + AHEAD, start1, AHEAD)
            for_chunk(k + AHEAD0, start0, AHEAD0)
            for_chunk(k + 1, wait0)

        @pl.loop(old[1], new[1])
        def _(k):
            for_chunk(k, relay3)

        @pl.loop(old[2], new[2])
        def _(k):
            for_chunk(k, finish)

    def down_step(i):
        j = i - ST_D
        own_rest = i == ST_T
        other_rest = i == STEPS - 1
        n = jnp.where(i > ST_T, j - 1, j)
        in_d = (i >= ST_D) & (n < 4 * N_D) & (i != ST_T)
        return n // 4, lax.rem(n + 4 * STEPS, 4), in_d, own_rest, other_rest

    def rest_col(side_no):
        return pl.multiple_of(side_no * (2 * FF_ROWS) + 2560, HEAD)

    def tile_col(side_no, core_no, tile):
        return pl.multiple_of(side_no * (2 * FF_ROWS) + core_no * (FF_ROWS + TAIL) + tile * 256, HEAD)

    def load_tile(s):
        layer = s // STEPS
        i = lax.rem(s, STEPS)
        slot = lax.rem(s, 2)

        def cols(name, c0, nc, w0):
            for r, src in enumerate(sources):
                pltpu.make_async_copy(src[name].at[layer, :, pl.ds(c0, nc)],
                                      wbuf.at[slot, pl.ds(r * ROWS, ROWS), pl.ds(w0, nc)], wsem.at[slot]).start()

        @pl.when(i == 0)
        def _():
            cols("k", 0, 256, 0)
            cols("v", 0, 256, 256)

        @pl.when((i >= ST_Q) & (i < ST_A))
        def _():
            cols("q", pl.multiple_of((i - ST_Q) * 512, 512), 512, 0)

        @pl.when((i >= ST_O) & (i < ST_G))
        def _():
            cols("o", pl.multiple_of((i - ST_O) * 512, 512), 512, 0)

        @pl.when((i >= ST_G) & (i < ST_D))
        def _():
            c0 = pl.multiple_of((i - ST_G) * 256, 256)
            cols("g", c0, 256, 0)
            cols("u", c0, 256, 256)

        tile, part, in_d, own_rest, other_rest = down_step(i)
        for r, src in enumerate(sources):
            src_core = core if r % 2 == 0 else 1 - core

            @pl.when(in_d & (part == r))
            def _():
                r0 = pl.multiple_of(src_core * TAIL + tile * 256, 64)
                pltpu.make_async_copy(src["d"].at[layer, pl.ds(r0, 256), :], dbuf.at[slot, pl.ds(0, 256), :], dsem.at[slot]).start()

            @pl.when(own_rest if r < 2 else other_rest)
            def _():
                r0 = pl.multiple_of((1 - src_core) * 2560, 512)
                w0 = pl.multiple_of(src_core * TAIL, TAIL)
                pltpu.make_async_copy(src["d"].at[layer, pl.ds(r0, TAIL), :], dbuf.at[slot, pl.ds(w0, TAIL), :],
                                      dsem.at[slot]).start()

    def norm(layer, which):
        @pl.loop(0, TOK // NB)
        def _(m):
            rows = pl.ds(pl.multiple_of(m * NB, NB), NB)
            total = jnp.zeros((NB, 1), F32)
            for b in range(4):
                blk = x_ref[rows, pl.ds(b * ROWS, ROWS)]
                total = total + jnp.sum(blk * blk, axis=1, keepdims=True)
            inv = lax.rsqrt(total * (1.0 / D) + EPS)
            for b in range(4):
                blk = x_ref[rows, pl.ds(b * ROWS, ROWS)]
                gain = gain_ref[which * LAYERS + layer, :, pl.ds(b * ROWS, ROWS)]
                c0 = pl.multiple_of(rel(b) * ROWS, ROWS)
                h_ref[rows, pl.ds(c0, ROWS)] = (blk * inv * gain).astype(BF16)

    def rotate(vals, rows):
        vals = vals.astype(BF16).astype(F32)
        turned = pltpu.roll(vals, HEAD // 2, 1)
        return (vals * cos_ref[rows, :] + turned * sin_ref[rows, :]).astype(BF16)

    def tile_product(slot, finish_rows):
        @pl.loop(0, TOK // MB)
        def _(m):
            rows = pl.ds(pl.multiple_of(m * MB, MB), MB)
            finish_rows(rows, jnp.dot(h_ref[rows, :], wbuf[slot], preferred_element_type=F32))

    def kv_step(slot):
        def fin(rows, acc):
            for b in range(2):
                kv_ref[rows, pl.ds(b * HEAD, HEAD)] = rotate(acc[:, b * HEAD:(b + 1) * HEAD], rows)
            kv_ref[rows, pl.ds(256, 256)] = acc[:, 256:].astype(BF16)
        tile_product(slot, fin)

    def q_step(slot, j):
        def fin(rows, acc):
            for b in range(4):
                c0 = pl.multiple_of(j * 512 + b * HEAD, HEAD)
                q_ref[rows, pl.ds(c0, HEAD)] = rotate(acc[:, b * HEAD:(b + 1) * HEAD], rows)
        tile_product(slot, fin)

    def o_step(slot, j):
        def fin(rows, acc):
            c0 = pl.ds(pl.multiple_of(j * 512, 512), 512)
            x_ref[rows, c0] = x_ref[rows, c0] + acc
        tile_product(slot, fin)

    def g_step(slot, j):
        def fin(rows, acc):
            gate = acc[:, :256]
            up = acc[:, 256:]
            c0 = pl.multiple_of(j * 256, 256)
            a_ref[rows, pl.ds(c0, 256)] = (gate * jax.nn.sigmoid(gate) * up).astype(BF16)
        tile_product(slot, fin)

    def attend(head):
        kv = head // 8
        q0 = pl.multiple_of(head * HEAD, HEAD)
        k0 = pl.multiple_of(kv * HEAD, HEAD)
        v0 = pl.multiple_of(256 + kv * HEAD, HEAD)
        o0 = pl.multiple_of(rel(head // 4) * ROWS + lax.rem(head, 4) * HEAD, HEAD)
        scale = HEAD ** -0.5
        for b in range(TOK // QB):
            keys = (b + 1) * QB
            rows = pl.ds(b * QB, QB)
            scores = lax.dot_general(q_ref[rows, pl.ds(q0, HEAD)], kv_ref[pl.ds(0, keys), pl.ds(k0, HEAD)],
                                     (((1,), (1,)), ((), ())), preferred_element_type=F32)
            key_idx = lax.broadcasted_iota(jnp.int32, (QB, keys), 1)
            row_idx = lax.broadcasted_iota(jnp.int32, (QB, keys), 0) + b * QB
            first = jnp.concatenate([first_ref[rows, :]] * (keys // HEAD), axis=1)
            ok = (key_idx >= first) & (key_idx <= row_idx)
            scores = jnp.where(ok, scores, -1e30)
            top = jnp.max(scores, axis=1, keepdims=True)
            probs = jnp.exp((scores - top) * scale)
            inv = 1.0 / jnp.sum(probs, axis=1, keepdims=True)
            probs = (probs * inv).astype(BF16)
            mixed = jnp.dot(probs, kv_ref[pl.ds(0, keys), pl.ds(v0, HEAD)], preferred_element_type=F32)
            h_ref[rows, pl.ds(o0, HEAD)] = mixed.astype(BF16)

    def add_product(slot, c0, depth, final):
        @pl.loop(0, TOK // MB)
        def _(m):
            rows = pl.ds(pl.multiple_of(m * MB, MB), MB)
            x_ref[rows, :] = x_ref[rows, :] + jnp.dot(a_ref[rows, pl.ds(c0, depth)], dbuf[slot, pl.ds(0, depth), :],
                                                      preferred_element_type=F32)

            @pl.when(final)
            def _():
                pltpu.make_async_copy(x_ref.at[rows, :], out.at[rows, :], outsem.at[m]).start()

    def d_step(slot, tile, part):
        src_side = lax.rem(side + part // 2, 2)
        src_core = lax.rem(core + part, 2)
        add_product(slot, tile_col(src_side, src_core, tile), 256, False)

    def t_step(slot, other, final):
        add_product(slot, rest_col(lax.rem(side + other, 2)), 2 * TAIL, final)

    def last_columns():
        far = 1 - side
        pieces = ((tile_col(far, core, N_D - 1), 256), (tile_col(far, 1 - core, N_D - 1), 256), (rest_col(far), 2 * TAIL))
        c0 = 0
        copies = []
        for n, (col, width) in enumerate(pieces):
            copies.append(pltpu.make_async_copy(a_ref.at[:, pl.ds(col, width)], last_out.at[:, pl.ds(c0, width)], lastsem.at[n]))
            c0 += width
        return copies

    def wait_w(slot):
        pltpu.make_async_copy(wbuf.at[slot], wbuf.at[slot], wsem.at[slot]).wait()

    def step(s):
        before = [jnp.where(s == 0, one, two) for one, two in zip(FIRST, targets(s - 1))]
        relays(before, targets(s))

        @pl.when(s + 1 < ALL_STEPS)
        def _():
            load_tile(s + 1)

        layer = s // STEPS
        i = lax.rem(s, STEPS)
        slot = lax.rem(s, 2)

        @pl.when((i == 0) | (i == ST_G))
        def _():
            norm(layer, jnp.where(i == 0, 0, 1))

        @pl.when((i < ST_A) | ((i >= ST_O) & (i < ST_D)))
        def _():
            wait_w(slot)

        @pl.when(i == 0)
        def _():
            kv_step(slot)

        @pl.when((i >= ST_Q) & (i < ST_A))
        def _():
            q_step(slot, i - ST_Q)

        @pl.when((i >= ST_A) & (i < ST_O))
        def _():
            attend(i - ST_A)

        @pl.when((i >= ST_O) & (i < ST_G))
        def _():
            o_step(slot, i - ST_O)

        @pl.when((i >= ST_G) & (i < ST_D))
        def _():
            g_step(slot, i - ST_G)

        tile, part, in_d, own_rest, other_rest = down_step(i)

        @pl.when(in_d)
        def _():
            whole = dbuf.at[slot, pl.ds(0, 256), :]
            pltpu.make_async_copy(whole, whole, dsem.at[slot]).wait()
            d_step(slot, tile, part)

        @pl.when(own_rest | other_rest)
        def _():
            whole = dbuf.at[slot, pl.ds(0, 2 * TAIL), :]
            pltpu.make_async_copy(whole, whole, dsem.at[slot]).wait()
            t_step(slot, jnp.where(own_rest, 0, 1), s == ALL_STEPS - 1)

        @pl.when(s == (LAYERS - 1) * STEPS + ST_D)
        def _():
            for copy in last_columns():
                copy.start()

    @pl.loop(0, AHEAD)
    def _(k):
        for_chunk(k, start1)

    @pl.loop(0, AHEAD0)
    def _(k):
        for_chunk(k, start0)

    for copy in inputs:
        copy.wait()

    for n, ref in enumerate((ga_ref, gm_ref)):
        for layer in range(LAYERS):
            gain_ref[n * LAYERS + layer] = ref[pl.ds(layer, 1), :].astype(F32)
    ids = seg_ref[...].astype(F32)
    lane = lax.broadcasted_iota(jnp.int32, (128, HEAD), 1)
    for b in range(TOK // 128):
        rows = pl.ds(b * 128, 128)
        mine = jnp.transpose(jnp.broadcast_to(ids[b:b + 1, :], (128, 128)))
        before = jnp.zeros((128, 128), F32)
        for c in range(TOK // 128):
            before = before + jnp.where(ids[c:c + 1, :] < mine, 1.0, 0.0)
        first = jnp.sum(before, axis=1, keepdims=True)
        pos = lax.broadcasted_iota(jnp.int32, (128, 128), 0).astype(F32) + (b * 128.0) - first
        angles = pos * freq_ref[...]
        cos_ref[rows, :] = jnp.cos(angles)
        sin = jnp.sin(angles)
        sin_ref[rows, :] = jnp.where(lane < HEAD // 2, -sin, sin)
        first_ref[rows, :] = jnp.broadcast_to(first, (128, 128)).astype(jnp.int32)

    @pl.loop(0, TOK // NB)
    def _(m):
        rows = pl.ds(pl.multiple_of(m * NB, NB), NB)
        x_ref[rows, :] = q_ref[rows, :].astype(F32)

    for_chunk(0, wait0)
    relays((0, 0, 0), FIRST)
    load_tile(0)

    @pl.loop(0, ALL_STEPS)
    def _(s):
        step(s)

    relays(targets(ALL_STEPS - 1), (CHUNKS, CHUNKS, CHUNKS))
    for copy in last_columns():
        copy.wait()
    for m in range(TOK // MB):
        rows = pl.ds(m * MB, MB)
        pltpu.make_async_copy(x_ref.at[rows, :], out.at[rows, :], outsem.at[m]).wait()


def result_kernel(x_hbm, a_hbm, w2_hbm, w3_hbm, out, x_ref, a_ref, w_ref, wsem, asem, xsem, osem):
    core = lax.rem(lax.axis_index("fsdp"), 2)
    w0 = 0
    for src, src_core in ((w2_hbm, core), (w3_hbm, 1 - core)):
        r0 = pl.multiple_of(src_core * TAIL + (N_D - 1) * 256, 64)
        pltpu.make_async_copy(src.at[LAYERS - 1, pl.ds(r0, 256), :], w_ref.at[pl.ds(w0, 256), :], wsem).start()
        r0 = pl.multiple_of((1 - src_core) * 2560, 512)
        d0 = pl.multiple_of(512 + src_core * TAIL, 64)
        pltpu.make_async_copy(src.at[LAYERS - 1, pl.ds(r0, TAIL), :], w_ref.at[pl.ds(d0, TAIL), :], wsem).start()
        w0 += 256

    def block(src, dst, sem, m):
        rows = pl.ds(pl.multiple_of(m * MB, MB), MB)
        return pltpu.make_async_copy(src.at[rows, :], dst.at[rows, :], sem.at[m])

    pltpu.make_async_copy(a_hbm, a_ref, asem).start()
    for m in range(TOK // MB):
        block(x_hbm, x_ref, xsem, m).start()
    pltpu.make_async_copy(w_ref, w_ref, wsem).wait()
    pltpu.make_async_copy(a_hbm, a_ref, asem).wait()

    @pl.loop(0, TOK // MB)
    def _(m):
        rows = pl.ds(pl.multiple_of(m * MB, MB), MB)
        block(x_hbm, x_ref, xsem, m).wait()
        x_ref[rows, :] = x_ref[rows, :] + jnp.dot(a_ref[rows, :], w_ref[...], preferred_element_type=F32)
        block(x_ref, out, osem, m).start()

    for m in range(TOK // MB):
        block(x_ref, out, osem, m).wait()


def run_layers(tokens, seg_ids, g_attn, g_mlp, weights):
    shapes = [jax.ShapeDtypeStruct(w.shape, w.dtype) for w in weights]
    half_dim = HEAD // 2
    freq = np.float32(ROPE_BASE) ** (-np.arange(half_dim, dtype=np.float32) / np.float32(half_dim))
    freq = jnp.asarray(np.concatenate([freq, freq]).reshape(1, HEAD))
    sem = pltpu.SemaphoreType.DMA((SLOTS, 2))
    any_spec = pl.BlockSpec(memory_space=pl.ANY)
    outs = pl.pallas_call(
        layer_kernel,
        out_shape=[jax.ShapeDtypeStruct((TOK, D), F32), jax.ShapeDtypeStruct((TOK, FINAL_K), BF16)] + shapes * 3,
        in_specs=[any_spec] * 12,
        out_specs=[any_spec] * 23,
        scratch_shapes=[
            pltpu.VMEM((TOK, D), F32),
            pltpu.VMEM((TOK, D), BF16),
            pltpu.VMEM((TOK, D), BF16),
            pltpu.VMEM((TOK, 512), BF16),
            pltpu.VMEM((TOK, FF), BF16),
            pltpu.VMEM((2, D, 512), BF16),
            pltpu.VMEM((2, 2 * TAIL, D), BF16),
            pltpu.VMEM((TOK, HEAD), F32),
            pltpu.VMEM((TOK, HEAD), F32),
            pltpu.VMEM((TOK, HEAD), jnp.int32),
            pltpu.VMEM((2 * LAYERS, 1, D), F32),
            pltpu.VMEM((TOK // 128, 128), jnp.int32),
            pltpu.VMEM((1, HEAD), F32),
            pltpu.VMEM((LAYERS, D), BF16),
            pltpu.VMEM((LAYERS, D), BF16),
            pltpu.SemaphoreType.DMA((2,)),
            pltpu.SemaphoreType.DMA((2,)),
            pltpu.SemaphoreType.DMA((5,)),
            pltpu.SemaphoreType.DMA((TOK // MB,)),
            pltpu.SemaphoreType.DMA((3,)),
        ] + [sem] * 8,
        compiler_params=pltpu.CompilerParams(collective_id=0, has_side_effects=True, vmem_limit_bytes=66 * 1000 * 1000),
        name="two_layers",
    )(tokens, seg_ids.reshape(TOK // 128, 128), freq, g_attn, g_mlp, *weights)
    return pl.pallas_call(
        result_kernel,
        out_shape=jax.ShapeDtypeStruct((TOK, D), F32),
        in_specs=[any_spec] * 4,
        out_specs=any_spec,
        scratch_shapes=[
            pltpu.VMEM((TOK, D), F32),
            pltpu.VMEM((TOK, FINAL_K), BF16),
            pltpu.VMEM((FINAL_K, D), BF16),
            pltpu.SemaphoreType.DMA,
            pltpu.SemaphoreType.DMA,
            pltpu.SemaphoreType.DMA((TOK // MB,)),
            pltpu.SemaphoreType.DMA((TOK // MB,)),
        ],
        compiler_params=pltpu.CompilerParams(vmem_limit_bytes=60 * 1000 * 1000),
        name="result",
    )(outs[0], outs[1], outs[15], outs[22])


def solution(mesh):
    tok_spec = P(("rep", "fsdp"), None)
    seg_spec = P(("rep", "fsdp"))
    mat_spec = P(None, "fsdp", None)
    gain_spec = P(None, None)

    def per_device(tokens, seg_ids, w_q, w_k, w_v, w_o, w_gate, w_up, w_down, g_attn, g_mlp):
        return run_layers(tokens, seg_ids, g_attn, g_mlp, (w_q, w_k, w_v, w_o, w_gate, w_up, w_down))

    return jax.shard_map(per_device, mesh=mesh, in_specs=(tok_spec, seg_spec, mat_spec, mat_spec, mat_spec, mat_spec, mat_spec, mat_spec, mat_spec, gain_spec, gain_spec), out_specs=tok_spec, check_vma=False)
```

```python
import functools

import jax
import jax.numpy as jnp
import numpy as np
from jax import lax
from jax.experimental import pallas as pl
from jax.experimental.pallas import tpu as pltpu
from jax.sharding import PartitionSpec as P

D = 2048
FF = 11008
HEADS = 16
HEAD = 128
TOK = 1024
EPS = 1e-5
ROPE_BASE = 10000.0
MESH = pl.DeviceIdType.MESH
F32 = jnp.float32
BF16 = jnp.bfloat16

LAYERS = 2
SLOTS = 16
AHEAD = 8
AHEAD0 = 2
ROWS = D // 4
FF_ROWS = FF // 4
TAIL = 192
NAMES = ("q", "k", "v", "o", "g", "u", "d")
DIRECT = (0, 1)

N_Q = 4
N_GU = 21
N_D = 10
CH_Q = 1
CH_O = CH_Q + N_Q
CH_GU = CH_O + N_Q
CH_GL = CH_GU + N_GU
CH_D = CH_GL + 1
CH_DR = CH_D + N_D
PER_LAYER = CH_DR + 1
CHUNKS = LAYERS * PER_LAYER

N_GT = FF // 256
ST_Q = 1
ST_A = ST_Q + N_Q
ST_O = ST_A + HEADS
ST_G = ST_O + 4
ST_D = ST_G + N_GT
ST_NEAR = ST_D + 2 * (N_D - 2)
ST_FAR = ST_NEAR + 4
STEPS = ST_FAR + 2
ALL_STEPS = LAYERS * STEPS - 2
FIRST = (4, 2, 1)
SIDE_K = 512 + 2 * TAIL

MB = 512
NB = 128
QB = 256


def layer_kernel(*refs):
    tok, seg, freq, g_attn, g_mlp = refs[:5]
    own = dict(zip(NAMES, refs[5:12]))
    x_ref, a_ref = refs[12:14]
    b1 = dict(zip(NAMES, refs[14:21]))
    b2 = dict(zip(NAMES, refs[21:28]))
    b3 = dict(zip(NAMES, refs[28:35]))
    (h_ref, q_ref, kv_ref, wbuf, dbuf, cos_ref, sin_ref, first_ref, gain_ref,
     seg_ref, freq_ref, ga_ref, gm_ref, wsem, dsem, iosem) = refs[35:51]
    s0s, s0r, s1s, s1r, s2s, s2r, s3s, s3r = refs[51:]
    sources = (own, b1, b2, b3)
    y = lax.axis_index("rep")
    d = lax.axis_index("fsdp")
    side = d // 2
    core = lax.rem(d, 2)
    x_dev = (y, lax.rem(d + 2, 4))
    y_dev = (1 - y, d)
    c_dev = (y, d + 1 - 2 * core)

    def rel(block):
        return 2 * lax.rem(block // 2 + side, 2) + lax.rem(block + core, 2)

    inputs = [pltpu.make_async_copy(src, dst, iosem.at[n]) for n, (src, dst) in enumerate(
        ((tok, q_ref), (seg, seg_ref), (freq, freq_ref), (g_attn, ga_ref), (g_mlp, gm_ref)))]
    for copy in inputs:
        copy.start()

    with jax.named_scope("barrier"):
        barrier = pltpu.get_barrier_semaphore()
        for dev in (x_dev, y_dev, c_dev):
            pl.semaphore_signal(barrier, inc=1, device_id=dev, device_id_type=MESH)
        pl.semaphore_wait(barrier, 3)

    def for_chunk(k, fn, lo=0):
        layer = k // PER_LAYER
        i = lax.rem(k, PER_LAYER)
        slot = lax.rem(k, SLOTS)
        ok = (k >= lo) & (k < CHUNKS)

        def case(cond, items, direct=()):
            @pl.when(ok & cond)
            def _():
                for n, (name, r0, nr, c0, nc) in enumerate(items):
                    fn(n in direct, name, layer, r0, nr, c0, nc, slot, n)

        case(i == 0, [("k", 0, ROWS, 0, 256), ("v", 0, ROWS, 0, 256)])
        jq = pl.multiple_of((i - CH_Q) * 512, 512)
        case((i >= CH_Q) & (i < CH_O), [("q", 0, ROWS, jq, 512)])
        jo = pl.multiple_of((i - CH_O) * 512, 512)
        case((i >= CH_O) & (i < CH_GU), [("o", 0, ROWS, jo, 512)])
        jg = pl.multiple_of((i - CH_GU) * 512, 512)
        case((i >= CH_GU) & (i < CH_GL), [("g", 0, ROWS, jg, 512), ("u", 0, ROWS, jg, 512)])
        case(i == CH_GL, [("g", 0, ROWS, N_GU * 512, 256), ("u", 0, ROWS, N_GU * 512, 256)])
        jd = core * TAIL + (i - CH_D) * 256
        case((i >= CH_D) & (i < CH_DR), [("d", jd, 128, 0, D), ("d", jd + 128, 128, 0, D)])
        jr = (1 - core) * 2560
        last = [("d", jr, TAIL // 2, 0, D), ("d", jr + TAIL // 2, TAIL // 2, 0, D)]
        case((i == CH_DR) & (k < CHUNKS - 1), last)
        case((i == CH_DR) & (k == CHUNKS - 1), last, DIRECT)

    def view(bufs, name, layer, r0, nr, c0, nc, half):
        if half:
            nr = nr // 2
            r0 = r0 + y * nr
        r0 = pl.multiple_of(r0, 16)
        return bufs[name].at[layer, pl.ds(r0, nr), pl.ds(c0, nc)]

    def remote(src, dst, ss, rs, dev, half):
        def make(direct, name, layer, r0, nr, c0, nc, slot, n):
            part = half and not direct
            return pltpu.make_async_remote_copy(
                src_ref=view(src, name, layer, r0, nr, c0, nc, part),
                dst_ref=view(dst, name, layer, r0, nr, c0, nc, part),
                send_sem=ss.at[slot, n], recv_sem=rs.at[slot, n], device_id=dev, device_id_type=MESH)
        return make

    copy0 = remote(own, b1, s0s, s0r, c_dev, False)
    copy1 = remote(own, b2, s1s, s1r, x_dev, True)
    copy2 = remote(b2, b2, s2s, s2r, y_dev, True)
    copy3 = remote(b2, b3, s3s, s3r, c_dev, False)

    def start0(*a):
        copy0(*a).start()

    def start1(*a):
        copy1(*a).start()

    def wait0(*a):
        copy0(*a).wait_recv()

    def relay2(*a):
        copy1(*a).wait_recv()
        if not a[0]:
            copy2(*a).start()

    def relay3(*a):
        if not a[0]:
            copy2(*a).wait_recv()
        copy3(*a).start()

    def finish(*a):
        copy3(*a).wait_recv()
        copy0(*a).wait_send()
        copy1(*a).wait_send()
        if not a[0]:
            copy2(*a).wait_send()
        copy3(*a).wait_send()

    def targets(s):
        i = lax.rem(s, STEPS)
        base = s // STEPS * PER_LAYER
        third = (i - ST_A) // 3
        t2 = jnp.where(i < ST_A, 5 + i,
             jnp.where(i < ST_D, jnp.maximum(11 + third, (i + 2) // 2),
             jnp.where(i < ST_FAR, (i + 1) // 2, 46)))
        t3 = jnp.where(i < ST_A, 3 + i,
             jnp.where(i < ST_D, jnp.maximum(9 + third, (i - 1) // 2),
             jnp.where(i < ST_NEAR, (i - 2) // 2,
             jnp.where(i < ST_FAR, (i - 4) // 2, 44))))
        t2 = jnp.minimum(t2 + base, CHUNKS - 1)
        t3 = jnp.minimum(t3 + base, CHUNKS - 1)
        nxt = jnp.minimum(s + 1, ALL_STEPS - 1)
        i = lax.rem(nxt, STEPS)
        base = nxt // STEPS * PER_LAYER
        done = jnp.where(i < ST_A, 1 + i,
               jnp.where(i < ST_O, ST_A,
               jnp.where(i < ST_G, 1 + CH_O + i - ST_O,
               jnp.where(i < ST_D, 1 + CH_GU + (i - ST_G) // 2,
               jnp.where(i < ST_NEAR, 1 + CH_D + (i - ST_D) // 2,
               jnp.where(i < ST_FAR, CH_D + N_D - 2 + (i - ST_NEAR) // 2, PER_LAYER))))))
        near = (i >= ST_NEAR) & (i < ST_FAR)
        tf = jnp.maximum(t3 - 2, base + done)
        t3 = jnp.maximum(t3, tf)
        t2 = jnp.maximum(jnp.maximum(t2, t3), base + jnp.where(near, CH_DR, 0))
        return t2, t3, tf

    def relays(old, new):
        @pl.loop(old[0], new[0])
        def _(k):
            with jax.named_scope("r2"):
                for_chunk(k, relay2)
                for_chunk(k + AHEAD, start1, AHEAD)
                for_chunk(k + AHEAD0, start0, AHEAD0)
                for_chunk(k + 1, wait0)

        @pl.loop(old[1], new[1])
        def _(k):
            with jax.named_scope("r3"):
                for_chunk(k, relay3)

        @pl.loop(old[2], new[2])
        def _(k):
            with jax.named_scope("fin"):
                for_chunk(k, finish)

    def down_step(i):
        j = (i - ST_D) // 2
        near = (i >= ST_NEAR) & (i < ST_NEAR + 2)
        far = i >= ST_FAR
        whole = (i >= ST_D) & ~near & ~far
        return j, jnp.where(i > ST_NEAR, j - 1, j), lax.rem(i - ST_D + STEPS, 2), whole, near, far

    def rest_col(side_no):
        return pl.multiple_of(side_no * (2 * FF_ROWS) + 2560, HEAD)

    def tile_col(side_no, core_no, tile):
        return pl.multiple_of(side_no * (2 * FF_ROWS) + core_no * (FF_ROWS + TAIL) + tile * 256, HEAD)

    def load_tile(s):
        layer = s // STEPS
        i = lax.rem(s, STEPS)
        slot = lax.rem(s, 2)

        def cols(name, c0, nc, w0):
            for r, src in enumerate(sources):
                pltpu.make_async_copy(src[name].at[layer, :, pl.ds(c0, nc)],
                                      wbuf.at[slot, pl.ds(r * ROWS, ROWS), pl.ds(w0, nc)], wsem.at[slot]).start()

        @pl.when(i == 0)
        def _():
            cols("k", 0, 256, 0)
            cols("v", 0, 256, 256)

        @pl.when((i >= ST_Q) & (i < ST_A))
        def _():
            cols("q", pl.multiple_of((i - ST_Q) * 512, 512), 512, 0)

        @pl.when((i >= ST_O) & (i < ST_G))
        def _():
            cols("o", pl.multiple_of((i - ST_O) * 512, 512), 512, 0)

        @pl.when((i >= ST_G) & (i < ST_D))
        def _():
            c0 = pl.multiple_of((i - ST_G) * 256, 256)
            cols("g", c0, 256, 0)
            cols("u", c0, 256, 256)

        j, tile, half, whole, near, far = down_step(i)
        dslot = lax.rem(j + STEPS, 2)

        def rows_in(src, r0, nr, w0):
            pltpu.make_async_copy(src["d"].at[layer, pl.ds(r0, nr), :], dbuf.at[dslot, pl.ds(w0, nr), :], dsem.at[dslot]).start()

        @pl.when(whole & (half == 0))
        def _():
            for r, src in enumerate(sources):
                src_core = core if r % 2 == 0 else 1 - core
                rows_in(src, pl.multiple_of(src_core * TAIL + tile * 256, 64), 256, r * 256)

        for cond, first_r in ((near, 0), (far, 2)):
            @pl.when(cond & (half == 0))
            def _():
                for r, src in enumerate(sources[first_r:first_r + 2]):
                    src_core = core if r % 2 == 0 else 1 - core
                    rows_in(src, pl.multiple_of(src_core * TAIL + (N_D - 1) * 256, 64), 256, r * 256)
                    rows_in(src, pl.multiple_of((1 - src_core) * 2560, 512), TAIL, pl.multiple_of(512 + src_core * TAIL, 64))

    def norm(layer, which):
        @pl.loop(0, TOK // NB)
        def _(m):
            rows = pl.ds(pl.multiple_of(m * NB, NB), NB)
            total = jnp.zeros((NB, 1), F32)
            for b in range(4):
                blk = x_ref[rows, pl.ds(b * ROWS, ROWS)]
                total = total + jnp.sum(blk * blk, axis=1, keepdims=True)
            inv = lax.rsqrt(total * (1.0 / D) + EPS)
            for b in range(4):
                blk = x_ref[rows, pl.ds(b * ROWS, ROWS)]
                gain = gain_ref[which * LAYERS + layer, :, pl.ds(b * ROWS, ROWS)]
                c0 = pl.multiple_of(rel(b) * ROWS, ROWS)
                h_ref[rows, pl.ds(c0, ROWS)] = (blk * inv * gain).astype(BF16)

    def rotate(vals, rows):
        vals = vals.astype(BF16).astype(F32)
        turned = pltpu.roll(vals, HEAD // 2, 1)
        return (vals * cos_ref[rows, :] + turned * sin_ref[rows, :]).astype(BF16)

    def tile_product(slot, finish_rows):
        @pl.loop(0, TOK // MB)
        def _(m):
            rows = pl.ds(pl.multiple_of(m * MB, MB), MB)
            finish_rows(rows, jnp.dot(h_ref[rows, :], wbuf[slot], preferred_element_type=F32))

    def kv_step(slot):
        def fin(rows, acc):
            for b in range(2):
                kv_ref[rows, pl.ds(b * HEAD, HEAD)] = rotate(acc[:, b * HEAD:(b + 1) * HEAD], rows)
            kv_ref[rows, pl.ds(256, 256)] = acc[:, 256:].astype(BF16)
        tile_product(slot, fin)

    def q_step(slot, j):
        def fin(rows, acc):
            for b in range(4):
                c0 = pl.multiple_of(j * 512 + b * HEAD, HEAD)
                q_ref[rows, pl.ds(c0, HEAD)] = rotate(acc[:, b * HEAD:(b + 1) * HEAD], rows)
        tile_product(slot, fin)

    def o_step(slot, j):
        def fin(rows, acc):
            c0 = pl.ds(pl.multiple_of(j * 512, 512), 512)
            x_ref[rows, c0] = x_ref[rows, c0] + acc
        tile_product(slot, fin)

    def g_step(slot, j):
        def fin(rows, acc):
            gate = acc[:, :256]
            up = acc[:, 256:]
            c0 = pl.multiple_of(j * 256, 256)
            a_ref[rows, pl.ds(c0, 256)] = (gate * jax.nn.sigmoid(gate) * up).astype(BF16)
        tile_product(slot, fin)

    def attend(head):
        kv = head // 8
        q0 = pl.multiple_of(head * HEAD, HEAD)
        k0 = pl.multiple_of(kv * HEAD, HEAD)
        v0 = pl.multiple_of(256 + kv * HEAD, HEAD)
        o0 = pl.multiple_of(rel(head // 4) * ROWS + lax.rem(head, 4) * HEAD, HEAD)
        scale = HEAD ** -0.5
        for b in range(TOK // QB):
            keys = (b + 1) * QB
            rows = pl.ds(b * QB, QB)
            scores = lax.dot_general(q_ref[rows, pl.ds(q0, HEAD)], kv_ref[pl.ds(0, keys), pl.ds(k0, HEAD)],
                                     (((1,), (1,)), ((), ())), preferred_element_type=F32)
            key_idx = lax.broadcasted_iota(jnp.int32, (QB, keys), 1)
            row_idx = lax.broadcasted_iota(jnp.int32, (QB, keys), 0) + b * QB
            first = jnp.concatenate([first_ref[rows, :]] * (keys // HEAD), axis=1)
            ok = (key_idx >= first) & (key_idx <= row_idx)
            scores = jnp.where(ok, scores, -1e30)
            top = jnp.max(scores, axis=1, keepdims=True)
            probs = jnp.exp((scores - top) * scale)
            inv = 1.0 / jnp.sum(probs, axis=1, keepdims=True)
            probs = (probs * inv).astype(BF16)
            mixed = jnp.dot(probs, kv_ref[pl.ds(0, keys), pl.ds(v0, HEAD)], preferred_element_type=F32)
            h_ref[rows, pl.ds(o0, HEAD)] = mixed.astype(BF16)

    def add_product(dslot, half, cols):
        rows = pl.ds(pl.multiple_of(half * MB, MB), MB)
        depth = sum(width for _, width in cols)
        lhs = jnp.concatenate([a_ref[rows, pl.ds(c0, width)] for c0, width in cols], axis=1)
        x_ref[rows, :] = x_ref[rows, :] + jnp.dot(lhs, dbuf[dslot, pl.ds(0, depth), :], preferred_element_type=F32)

    def wait_d(dslot, half, depth):
        @pl.when(half == 0)
        def _():
            part = dbuf.at[dslot, pl.ds(0, depth), :]
            pltpu.make_async_copy(part, part, dsem.at[dslot]).wait()

    def side_cols(side_no):
        return ((tile_col(side_no, core, N_D - 1), 256), (tile_col(side_no, 1 - core, N_D - 1), 256), (rest_col(side_no), 2 * TAIL))

    def wait_w(slot):
        pltpu.make_async_copy(wbuf.at[slot], wbuf.at[slot], wsem.at[slot]).wait()

    def step(s):
        before = [jnp.where(s == 0, one, two) for one, two in zip(FIRST, targets(s - 1))]
        relays(before, targets(s))

        @pl.when(s + 1 < ALL_STEPS)
        def _():
            load_tile(s + 1)

        with jax.named_scope("comp"):
            compute(s)

    def compute(s):
        layer = s // STEPS
        i = lax.rem(s, STEPS)
        slot = lax.rem(s, 2)

        @pl.when((i == 0) | (i == ST_G))
        def _():
            norm(layer, jnp.where(i == 0, 0, 1))

        @pl.when((i < ST_A) | ((i >= ST_O) & (i < ST_D)))
        def _():
            wait_w(slot)

        @pl.when(i == 0)
        def _():
            kv_step(slot)

        @pl.when((i >= ST_Q) & (i < ST_A))
        def _():
            q_step(slot, i - ST_Q)

        @pl.when((i >= ST_A) & (i < ST_O))
        def _():
            attend(i - ST_A)

        @pl.when((i >= ST_O) & (i < ST_G))
        def _():
            o_step(slot, i - ST_O)

        @pl.when((i >= ST_G) & (i < ST_D))
        def _():
            g_step(slot, i - ST_G)

        j, tile, half, whole, near, far = down_step(i)
        dslot = lax.rem(j + STEPS, 2)

        @pl.when(whole)
        def _():
            wait_d(dslot, half, 1024)
            add_product(dslot, half, [(tile_col(lax.rem(side + r // 2, 2), lax.rem(core + r, 2), tile), 256) for r in range(4)])

        @pl.when(near | far)
        def _():
            wait_d(dslot, half, SIDE_K)
            add_product(dslot, half, side_cols(lax.rem(side + jnp.where(far, 1, 0), 2)))

    @pl.loop(0, AHEAD)
    def _(k):
        for_chunk(k, start1)

    @pl.loop(0, AHEAD0)
    def _(k):
        for_chunk(k, start0)

    for copy in inputs:
        copy.wait()

    for n, ref in enumerate((ga_ref, gm_ref)):
        for layer in range(LAYERS):
            gain_ref[n * LAYERS + layer] = ref[pl.ds(layer, 1), :].astype(F32)
    ids = seg_ref[...].astype(F32)
    lane = lax.broadcasted_iota(jnp.int32, (128, HEAD), 1)
    for b in range(TOK // 128):
        rows = pl.ds(b * 128, 128)
        mine = jnp.transpose(jnp.broadcast_to(ids[b:b + 1, :], (128, 128)))
        before = jnp.zeros((128, 128), F32)
        for c in range(TOK // 128):
            before = before + jnp.where(ids[c:c + 1, :] < mine, 1.0, 0.0)
        first = jnp.sum(before, axis=1, keepdims=True)
        pos = lax.broadcasted_iota(jnp.int32, (128, 128), 0).astype(F32) + (b * 128.0) - first
        angles = pos * freq_ref[...]
        cos_ref[rows, :] = jnp.cos(angles)
        sin = jnp.sin(angles)
        sin_ref[rows, :] = jnp.where(lane < HEAD // 2, -sin, sin)
        first_ref[rows, :] = jnp.broadcast_to(first, (128, 128)).astype(jnp.int32)

    @pl.loop(0, TOK // NB)
    def _(m):
        rows = pl.ds(pl.multiple_of(m * NB, NB), NB)
        x_ref[rows, :] = q_ref[rows, :].astype(F32)

    for_chunk(0, wait0)
    relays((0, 0, 0), FIRST)
    load_tile(0)

    @pl.loop(0, ALL_STEPS)
    def _(s):
        with jax.named_scope("step"):
            step(s)

    relays(targets(ALL_STEPS - 1), (CHUNKS, CHUNKS, CHUNKS))


def result_kernel(x_ref, a_ref, w2_hbm, w3_hbm, out, y_ref, w_ref, wsem, osem):
    d = lax.axis_index("fsdp")
    far = 1 - d // 2
    core = lax.rem(d, 2)
    for n in range(4):
        cols = pl.ds(n * 512, 512)
        for r, (src, src_core) in enumerate(((w2_hbm, core), (w3_hbm, 1 - core))):
            r0 = pl.multiple_of(src_core * TAIL + (N_D - 1) * 256, 64)
            pltpu.make_async_copy(src.at[LAYERS - 1, pl.ds(r0, 256), cols], w_ref.at[n, pl.ds(r * 256, 256), :], wsem.at[n]).start()
            r0 = pl.multiple_of((1 - src_core) * 2560, 512)
            d0 = pl.multiple_of(512 + src_core * TAIL, 64)
            pltpu.make_async_copy(src.at[LAYERS - 1, pl.ds(r0, TAIL), cols], w_ref.at[n, pl.ds(d0, TAIL), :], wsem.at[n]).start()

    c0 = far * (2 * FF_ROWS) + (N_D - 1) * 256
    pieces = ((c0 + core * (FF_ROWS + TAIL), 256), (c0 + (1 - core) * (FF_ROWS + TAIL), 256), (far * (2 * FF_ROWS) + 2560, 2 * TAIL))
    for n in range(4):
        cols = pl.ds(n * 512, 512)
        pltpu.make_async_copy(w_ref.at[n], w_ref.at[n], wsem.at[n]).wait()
        for m in range(2):
            rows = pl.ds(m * 512, 512)
            part = jnp.concatenate([a_ref[rows, pl.ds(pl.multiple_of(col, HEAD), width)] for col, width in pieces], axis=1)
            y_ref[rows, cols] = x_ref[rows, cols] + jnp.dot(part, w_ref[n], preferred_element_type=F32)
            pltpu.make_async_copy(y_ref.at[rows, cols], out.at[rows, cols], osem.at[n, m]).start()
    for n in range(4):
        for m in range(2):
            rows, cols = pl.ds(m * 512, 512), pl.ds(n * 512, 512)
            pltpu.make_async_copy(y_ref.at[rows, cols], out.at[rows, cols], osem.at[n, m]).wait()


def run_layers(tokens, seg_ids, g_attn, g_mlp, weights):
    shapes = [jax.ShapeDtypeStruct(w.shape, w.dtype) for w in weights]
    half_dim = HEAD // 2
    freq = np.float32(ROPE_BASE) ** (-np.arange(half_dim, dtype=np.float32) / np.float32(half_dim))
    freq = jnp.asarray(np.concatenate([freq, freq]).reshape(1, HEAD))
    sem = pltpu.SemaphoreType.DMA((SLOTS, 2))
    any_spec = pl.BlockSpec(memory_space=pl.ANY)
    vmem_spec = pl.BlockSpec(memory_space=pltpu.VMEM)
    outs = pl.pallas_call(
        layer_kernel,
        out_shape=[pltpu.VMEM((TOK, D), F32), pltpu.VMEM((TOK, FF), BF16)] + shapes * 3,
        in_specs=[any_spec] * 12,
        out_specs=[vmem_spec] * 2 + [any_spec] * 21,
        scratch_shapes=[
            pltpu.VMEM((TOK, D), BF16),
            pltpu.VMEM((TOK, D), BF16),
            pltpu.VMEM((TOK, 512), BF16),
            pltpu.VMEM((2, D, 512), BF16),
            pltpu.VMEM((2, 1024, D), BF16),
            pltpu.VMEM((TOK, HEAD), F32),
            pltpu.VMEM((TOK, HEAD), F32),
            pltpu.VMEM((TOK, HEAD), jnp.int32),
            pltpu.VMEM((2 * LAYERS, 1, D), F32),
            pltpu.VMEM((TOK // 128, 128), jnp.int32),
            pltpu.VMEM((1, HEAD), F32),
            pltpu.VMEM((LAYERS, D), BF16),
            pltpu.VMEM((LAYERS, D), BF16),
            pltpu.SemaphoreType.DMA((2,)),
            pltpu.SemaphoreType.DMA((2,)),
            pltpu.SemaphoreType.DMA((5,)),
        ] + [sem] * 8,
        compiler_params=pltpu.CompilerParams(collective_id=0, has_side_effects=True, vmem_limit_bytes=34 * 1000 * 1000),
        name="two_layers",
    )(tokens, seg_ids.reshape(TOK // 128, 128), freq, g_attn, g_mlp, *weights)
    hidden = pltpu.with_memory_space_constraint(outs[0], pltpu.VMEM)
    act = pltpu.with_memory_space_constraint(outs[1], pltpu.VMEM)
    return pl.pallas_call(
        result_kernel,
        out_shape=jax.ShapeDtypeStruct((TOK, D), F32),
        in_specs=[vmem_spec] * 2 + [any_spec] * 2,
        out_specs=any_spec,
        scratch_shapes=[
            pltpu.VMEM((TOK, D), F32),
            pltpu.VMEM((4, SIDE_K, 512), BF16),
            pltpu.SemaphoreType.DMA((4,)),
            pltpu.SemaphoreType.DMA((4, 2)),
        ],
        compiler_params=pltpu.CompilerParams(vmem_limit_bytes=24 * 1000 * 1000),
        name="result",
    )(hidden, act, outs[15], outs[22])


def solution(mesh):
    tok_spec = P(("rep", "fsdp"), None)
    seg_spec = P(("rep", "fsdp"))
    mat_spec = P(None, "fsdp", None)
    gain_spec = P(None, None)

    def per_device(tokens, seg_ids, w_q, w_k, w_v, w_o, w_gate, w_up, w_down, g_attn, g_mlp):
        return run_layers(tokens, seg_ids, g_attn, g_mlp, (w_q, w_k, w_v, w_o, w_gate, w_up, w_down))

    return jax.shard_map(per_device, mesh=mesh, in_specs=(tok_spec, seg_spec, mat_spec, mat_spec, mat_spec, mat_spec, mat_spec, mat_spec, mat_spec, gain_spec, gain_spec), out_specs=tok_spec, check_vma=False)
```

```python
import functools

import jax
import jax.numpy as jnp
import numpy as np
from jax import lax
from jax.experimental import pallas as pl
from jax.experimental.pallas import tpu as pltpu
from jax.sharding import PartitionSpec as P

D = 2048
FF = 11008
HEADS = 16
HEAD = 128
TOK = 1024
EPS = 1e-5
ROPE_BASE = 10000.0
MESH = pl.DeviceIdType.MESH
F32 = jnp.float32
BF16 = jnp.bfloat16

LAYERS = 2
SLOTS = 8
AHEAD = 4
AHEAD0 = 3
ROWS = D // 4
FF_ROWS = FF // 4
TAIL = 192
NAMES = ("q", "k", "v", "o", "g", "u", "d")
DIRECT = (1,)

N_Q = 4
N_GU = 21
N_D = 10
CH_Q = 1
CH_O = CH_Q + N_Q
CH_GU = CH_O + N_Q
CH_GL = CH_GU + N_GU
CH_D = CH_GL + 1
CH_DR = CH_D + N_D
PER_LAYER = CH_DR + 1
CHUNKS = LAYERS * PER_LAYER

N_GT = FF // 256
ST_Q = 1
ST_A = ST_Q + N_Q
ST_O = ST_A + HEADS
ST_G = ST_O + 4
ST_D = ST_G + N_GT
ST_NEAR = ST_D + 2 * (N_D - 2)
ST_IDLE = ST_NEAR + 4
ST_FAR = ST_IDLE + 1
ST_REST = ST_FAR + 2
STEPS = ST_REST + 2
ALL_STEPS = LAYERS * STEPS - 2
FIRST = (4, 2, 1)
REST_K = 2 * TAIL
NEAR_K = 512 + REST_K

MB = 512
NB = 128
QB = 256


def layer_kernel(*refs):
    tok, seg, freq, g_attn, g_mlp = refs[:5]
    own = dict(zip(NAMES, refs[5:12]))
    x_ref, a_ref = refs[12:14]
    b1 = dict(zip(NAMES, refs[14:21]))
    b2 = dict(zip(NAMES, refs[21:28]))
    b3 = dict(zip(NAMES, refs[28:35]))
    (h_ref, q_ref, kv_ref, wbuf, dbuf, cos_ref, sin_ref, first_ref, gain_ref,
     seg_ref, freq_ref, ga_ref, gm_ref, wsem, dsem, iosem) = refs[35:51]
    s0s, s0r, s1s, s1r, s2s, s2r, s3s, s3r = refs[51:]
    sources = (own, b1, b2, b3)
    y = lax.axis_index("rep")
    d = lax.axis_index("fsdp")
    side = d // 2
    core = lax.rem(d, 2)
    x_dev = (y, lax.rem(d + 2, 4))
    y_dev = (1 - y, d)
    c_dev = (y, d + 1 - 2 * core)

    def rel(block):
        return 2 * lax.rem(block // 2 + side, 2) + lax.rem(block + core, 2)

    inputs = [pltpu.make_async_copy(src, dst, iosem.at[n]) for n, (src, dst) in enumerate(
        ((tok, q_ref), (seg, seg_ref), (freq, freq_ref), (g_attn, ga_ref), (g_mlp, gm_ref)))]
    for copy in inputs:
        copy.start()

    with jax.named_scope("barrier"):
        barrier = pltpu.get_barrier_semaphore()
        for dev in (x_dev, y_dev, c_dev):
            pl.semaphore_signal(barrier, inc=1, device_id=dev, device_id_type=MESH)
        pl.semaphore_wait(barrier, 3)

    def for_chunk(k, fn, lo=0):
        layer = k // PER_LAYER
        i = lax.rem(k, PER_LAYER)
        slot = lax.rem(k, SLOTS)
        ok = (k >= lo) & (k < CHUNKS)

        def case(cond, items, direct=()):
            @pl.when(ok & cond)
            def _():
                for n, (name, r0, nr, c0, nc) in enumerate(items):
                    fn(n in direct, name, layer, r0, nr, c0, nc, slot, n)

        case(i == 0, [("k", 0, ROWS, 0, 256), ("v", 0, ROWS, 0, 256)])
        jq = pl.multiple_of((i - CH_Q) * 512, 512)
        case((i >= CH_Q) & (i < CH_O), [("q", 0, ROWS, jq, 512)])
        jo = pl.multiple_of((i - CH_O) * 512, 512)
        case((i >= CH_O) & (i < CH_GU), [("o", 0, ROWS, jo, 512)])
        jg = pl.multiple_of((i - CH_GU) * 512, 512)
        case((i >= CH_GU) & (i < CH_GL), [("g", 0, ROWS, jg, 512), ("u", 0, ROWS, jg, 512)])
        case(i == CH_GL, [("g", 0, ROWS, N_GU * 512, 256), ("u", 0, ROWS, N_GU * 512, 256)])
        jd = core * TAIL + (i - CH_D) * 256
        case((i >= CH_D) & (i < CH_DR), [("d", jd, 128, 0, D), ("d", jd + 128, 128, 0, D)])
        jr = (1 - core) * 2560
        last = [("d", jr, TAIL // 2, 0, D), ("d", jr + TAIL // 2, TAIL // 2, 0, D)]
        case((i == CH_DR) & (k < CHUNKS - 1), last)
        case((i == CH_DR) & (k == CHUNKS - 1), last, DIRECT)

    def view(bufs, name, layer, r0, nr, c0, nc, half):
        if half:
            nr = nr // 2
            r0 = r0 + y * nr
        r0 = pl.multiple_of(r0, 16)
        return bufs[name].at[layer, pl.ds(r0, nr), pl.ds(c0, nc)]

    def remote(src, dst, ss, rs, dev, half):
        def make(direct, name, layer, r0, nr, c0, nc, slot, n):
            part = half and not direct
            return pltpu.make_async_remote_copy(
                src_ref=view(src, name, layer, r0, nr, c0, nc, part),
                dst_ref=view(dst, name, layer, r0, nr, c0, nc, part),
                send_sem=ss.at[slot, n], recv_sem=rs.at[slot, n], device_id=dev, device_id_type=MESH)
        return make

    copy0 = remote(own, b1, s0s, s0r, c_dev, False)
    copy1 = remote(own, b2, s1s, s1r, x_dev, True)
    copy2 = remote(b2, b2, s2s, s2r, y_dev, True)
    copy3 = remote(b2, b3, s3s, s3r, c_dev, False)

    def start0(*a):
        copy0(*a).start()

    def start1(*a):
        copy1(*a).start()

    def wait0(*a):
        copy0(*a).wait_recv()

    def relay2(*a):
        copy1(*a).wait_recv()
        if not a[0]:
            copy2(*a).start()

    def relay3(*a):
        if not a[0]:
            copy2(*a).wait_recv()
        copy3(*a).start()
        copy0(*a).wait_send()
        copy1(*a).wait_send()

    def finish(*a):
        copy3(*a).wait_recv()
        if not a[0]:
            copy2(*a).wait_send()
        copy3(*a).wait_send()

    def targets(s):
        i = lax.rem(s, STEPS)
        base = s // STEPS * PER_LAYER
        third = (i - ST_A) // 3
        t2 = jnp.where(i < ST_A, 5 + i,
             jnp.where(i < ST_D, jnp.maximum(10 + third, (i + 2) // 2),
             jnp.where(i < ST_NEAR, jnp.minimum(i // 2, 40),
             jnp.where(i < ST_IDLE, 42 + (i - ST_NEAR + 1) // 2, 44 + (i - ST_IDLE + 1) // 2))))
        t3 = jnp.where(i < ST_A, 3 + i,
             jnp.where(i < ST_D, jnp.maximum(8 + third, (i - 1) // 2),
             jnp.where(i < ST_NEAR, jnp.minimum((i - 2) // 2, 39),
             jnp.where(i < ST_IDLE, 40, jnp.where(i < ST_FAR, 41, 42 + (i - ST_FAR) // 2)))))
        t2 = jnp.minimum(t2 + base, jnp.where(s < ALL_STEPS - 2, CHUNKS - 1, CHUNKS))
        t3 = jnp.minimum(t3 + base, jnp.where(s < ALL_STEPS - 2, CHUNKS - 1, CHUNKS))
        nxt = jnp.minimum(s + 1, ALL_STEPS - 1)
        i = lax.rem(nxt, STEPS)
        base = nxt // STEPS * PER_LAYER
        done = jnp.where(i < ST_A, 1 + i,
               jnp.where(i < ST_O, ST_A,
               jnp.where(i < ST_G, 1 + CH_O + i - ST_O,
               jnp.where(i < ST_D, 1 + CH_GU + (i - ST_G) // 2,
               jnp.where(i < ST_NEAR, 1 + CH_D + (i - ST_D) // 2,
               jnp.where(i < ST_IDLE, CH_DR - 2 + (i - ST_NEAR) // 2,
               jnp.where(i < ST_FAR, CH_DR - 1,
               jnp.where(i < ST_REST, CH_DR, PER_LAYER))))))))
        tf = jnp.maximum(t3 - 2, base + done)
        t3 = jnp.maximum(t3, tf)
        t2 = jnp.maximum(jnp.maximum(t2, t3), base + jnp.where((i >= ST_NEAR) & (i < ST_IDLE), CH_DR - 1, 0))
        return t2, t3, tf

    def relays(old, new):
        @pl.loop(old[0], new[0])
        def _(k):
            with jax.named_scope("r2"):
                for_chunk(k, relay2)
                for_chunk(k + AHEAD, start1, AHEAD)
                for_chunk(k + AHEAD0, start0, AHEAD0)
                for_chunk(k + AHEAD0 - 1, wait0)

        @pl.loop(old[1], new[1])
        def _(k):
            with jax.named_scope("r3"):
                for_chunk(k, relay3)

        @pl.loop(old[2], new[2])
        def _(k):
            with jax.named_scope("fin"):
                for_chunk(k, finish)

    def down_step(i):
        late = i >= ST_FAR
        n = jnp.where(late, i - ST_D - 1, i - ST_D)
        j = n // 2
        near = (i >= ST_NEAR) & (i < ST_NEAR + 2)
        far = late & (i < ST_REST)
        rest = i >= ST_REST
        whole = (i >= ST_D) & (i < ST_IDLE) & ~near
        return j, jnp.where(i > ST_NEAR, j - 1, j), lax.rem(n + 2 * STEPS, 2), whole, near, far, rest

    def rest_col(side_no):
        return pl.multiple_of(side_no * (2 * FF_ROWS) + 2560, HEAD)

    def tile_col(side_no, core_no, tile):
        return pl.multiple_of(side_no * (2 * FF_ROWS) + core_no * (FF_ROWS + TAIL) + tile * 256, HEAD)

    def load_tile(s):
        layer = s // STEPS
        i = lax.rem(s, STEPS)
        slot = lax.rem(s, 2)

        def cols(name, c0, nc, w0):
            for r, src in enumerate(sources):
                pltpu.make_async_copy(src[name].at[layer, :, pl.ds(c0, nc)],
                                      wbuf.at[slot, pl.ds(r * ROWS, ROWS), pl.ds(w0, nc)], wsem.at[slot]).start()

        @pl.when(i == 0)
        def _():
            cols("k", 0, 256, 0)
            cols("v", 0, 256, 256)

        @pl.when((i >= ST_Q) & (i < ST_A))
        def _():
            cols("q", pl.multiple_of((i - ST_Q) * 512, 512), 512, 0)

        @pl.when((i >= ST_O) & (i < ST_G))
        def _():
            cols("o", pl.multiple_of((i - ST_O) * 512, 512), 512, 0)

        @pl.when((i >= ST_G) & (i < ST_D))
        def _():
            c0 = pl.multiple_of((i - ST_G) * 256, 256)
            cols("g", c0, 256, 0)
            cols("u", c0, 256, 256)

        j, tile, half, whole, near, far, rest = down_step(i)
        dslot = lax.rem(j + 2 * STEPS, 2)

        def rows_in(src, r0, nr, w0):
            pltpu.make_async_copy(src["d"].at[layer, pl.ds(r0, nr), :], dbuf.at[dslot, pl.ds(w0, nr), :], dsem.at[dslot]).start()

        def chunk_rows(r, tile_no, w0):
            src_core = core if r % 2 == 0 else 1 - core
            rows_in(sources[r], pl.multiple_of(src_core * TAIL + tile_no * 256, 64), 256, w0)

        def rest_rows(r, w0):
            src_core = core if r % 2 == 0 else 1 - core
            rows_in(sources[r], pl.multiple_of((1 - src_core) * 2560, 512), TAIL, pl.multiple_of(w0 + src_core * TAIL, 64))

        @pl.when(whole & (half == 0))
        def _():
            for r in range(4):
                chunk_rows(r, tile, r * 256)

        @pl.when(near & (half == 0))
        def _():
            for r in range(2):
                chunk_rows(r, N_D - 1, r * 256)
                rest_rows(r, 512)

        @pl.when(far & (half == 0))
        def _():
            for r in range(2):
                chunk_rows(2 + r, N_D - 1, r * 256)

        @pl.when(rest & (half == 0))
        def _():
            for r in range(2):
                rest_rows(2 + r, 0)

    def norm(layer, which):
        @pl.loop(0, TOK // NB)
        def _(m):
            rows = pl.ds(pl.multiple_of(m * NB, NB), NB)
            total = jnp.zeros((NB, 1), F32)
            for b in range(4):
                blk = x_ref[rows, pl.ds(b * ROWS, ROWS)]
                total = total + jnp.sum(blk * blk, axis=1, keepdims=True)
            inv = lax.rsqrt(total * (1.0 / D) + EPS)
            for b in range(4):
                blk = x_ref[rows, pl.ds(b * ROWS, ROWS)]
                gain = gain_ref[which * LAYERS + layer, :, pl.ds(b * ROWS, ROWS)]
                c0 = pl.multiple_of(rel(b) * ROWS, ROWS)
                h_ref[rows, pl.ds(c0, ROWS)] = (blk * inv * gain).astype(BF16)

    def rotate(vals, rows):
        vals = vals.astype(BF16).astype(F32)
        turned = pltpu.roll(vals, HEAD // 2, 1)
        return (vals * cos_ref[rows, :] + turned * sin_ref[rows, :]).astype(BF16)

    def tile_product(slot, finish_rows):
        @pl.loop(0, TOK // MB)
        def _(m):
            rows = pl.ds(pl.multiple_of(m * MB, MB), MB)
            finish_rows(rows, jnp.dot(h_ref[rows, :], wbuf[slot], preferred_element_type=F32))

    def kv_step(slot):
        def fin(rows, acc):
            for b in range(2):
                kv_ref[rows, pl.ds(b * HEAD, HEAD)] = rotate(acc[:, b * HEAD:(b + 1) * HEAD], rows)
            kv_ref[rows, pl.ds(256, 256)] = acc[:, 256:].astype(BF16)
        tile_product(slot, fin)

    def q_step(slot, j):
        def fin(rows, acc):
            for b in range(4):
                c0 = pl.multiple_of(j * 512 + b * HEAD, HEAD)
                q_ref[rows, pl.ds(c0, HEAD)] = rotate(acc[:, b * HEAD:(b + 1) * HEAD], rows)
        tile_product(slot, fin)

    def o_step(slot, j):
        def fin(rows, acc):
            c0 = pl.ds(pl.multiple_of(j * 512, 512), 512)
            x_ref[rows, c0] = x_ref[rows, c0] + acc
        tile_product(slot, fin)

    def g_step(slot, j):
        def fin(rows, acc):
            gate = acc[:, :256]
            up = acc[:, 256:]
            c0 = pl.multiple_of(j * 256, 256)
            a_ref[rows, pl.ds(c0, 256)] = (gate * jax.nn.sigmoid(gate) * up).astype(BF16)
        tile_product(slot, fin)

    def attend(head):
        kv = head // 8
        q0 = pl.multiple_of(head * HEAD, HEAD)
        k0 = pl.multiple_of(kv * HEAD, HEAD)
        v0 = pl.multiple_of(256 + kv * HEAD, HEAD)
        o0 = pl.multiple_of(rel(head // 4) * ROWS + lax.rem(head, 4) * HEAD, HEAD)
        scale = HEAD ** -0.5
        for b in range(TOK // QB):
            keys = (b + 1) * QB
            rows = pl.ds(b * QB, QB)
            scores = lax.dot_general(q_ref[rows, pl.ds(q0, HEAD)], kv_ref[pl.ds(0, keys), pl.ds(k0, HEAD)],
                                     (((1,), (1,)), ((), ())), preferred_element_type=F32)
            key_idx = lax.broadcasted_iota(jnp.int32, (QB, keys), 1)
            row_idx = lax.broadcasted_iota(jnp.int32, (QB, keys), 0) + b * QB
            first = jnp.concatenate([first_ref[rows, :]] * (keys // HEAD), axis=1)
            ok = (key_idx >= first) & (key_idx <= row_idx)
            scores = jnp.where(ok, scores, -1e30)
            top = jnp.max(scores, axis=1, keepdims=True)
            probs = jnp.exp((scores - top) * scale)
            inv = 1.0 / jnp.sum(probs, axis=1, keepdims=True)
            probs = (probs * inv).astype(BF16)
            mixed = jnp.dot(probs, kv_ref[pl.ds(0, keys), pl.ds(v0, HEAD)], preferred_element_type=F32)
            h_ref[rows, pl.ds(o0, HEAD)] = mixed.astype(BF16)

    def add_product(dslot, half, cols):
        rows = pl.ds(pl.multiple_of(half * MB, MB), MB)
        depth = sum(width for _, width in cols)
        lhs = jnp.concatenate([a_ref[rows, pl.ds(c0, width)] for c0, width in cols], axis=1)
        x_ref[rows, :] = x_ref[rows, :] + jnp.dot(lhs, dbuf[dslot, pl.ds(0, depth), :], preferred_element_type=F32)

    def wait_d(dslot, half, depth):
        @pl.when(half == 0)
        def _():
            part = dbuf.at[dslot, pl.ds(0, depth), :]
            pltpu.make_async_copy(part, part, dsem.at[dslot]).wait()

    def last_cols(side_no):
        return [(tile_col(side_no, core, N_D - 1), 256), (tile_col(side_no, 1 - core, N_D - 1), 256)]

    def wait_w(slot):
        pltpu.make_async_copy(wbuf.at[slot], wbuf.at[slot], wsem.at[slot]).wait()

    def step(s):
        before = [jnp.where(s == 0, one, two) for one, two in zip(FIRST, targets(s - 1))]
        relays(before, targets(s))

        @pl.when(s + 1 < ALL_STEPS)
        def _():
            load_tile(s + 1)

        with jax.named_scope("comp"):
            compute(s)

    def compute(s):
        layer = s // STEPS
        i = lax.rem(s, STEPS)
        slot = lax.rem(s, 2)

        @pl.when((i == 0) | (i == ST_G))
        def _():
            norm(layer, jnp.where(i == 0, 0, 1))

        @pl.when((i < ST_A) | ((i >= ST_O) & (i < ST_D)))
        def _():
            wait_w(slot)

        @pl.when(i == 0)
        def _():
            kv_step(slot)

        @pl.when((i >= ST_Q) & (i < ST_A))
        def _():
            q_step(slot, i - ST_Q)

        @pl.when((i >= ST_A) & (i < ST_O))
        def _():
            attend(i - ST_A)

        @pl.when((i >= ST_O) & (i < ST_G))
        def _():
            o_step(slot, i - ST_O)

        @pl.when((i >= ST_G) & (i < ST_D))
        def _():
            g_step(slot, i - ST_G)

        j, tile, half, whole, near, far, rest = down_step(i)
        dslot = lax.rem(j + 2 * STEPS, 2)

        @pl.when(whole)
        def _():
            wait_d(dslot, half, 1024)
            add_product(dslot, half, [(tile_col(lax.rem(side + r // 2, 2), lax.rem(core + r, 2), tile), 256) for r in range(4)])

        @pl.when(near)
        def _():
            wait_d(dslot, half, NEAR_K)
            add_product(dslot, half, last_cols(side) + [(rest_col(side), REST_K)])

        @pl.when(far)
        def _():
            wait_d(dslot, half, 512)
            add_product(dslot, half, last_cols(1 - side))

        @pl.when(rest)
        def _():
            wait_d(dslot, half, REST_K)
            add_product(dslot, half, [(rest_col(1 - side), REST_K)])

    @pl.loop(0, AHEAD)
    def _(k):
        for_chunk(k, start1)

    @pl.loop(0, AHEAD0)
    def _(k):
        for_chunk(k, start0)

    for copy in inputs:
        copy.wait()

    for n, ref in enumerate((ga_ref, gm_ref)):
        for layer in range(LAYERS):
            gain_ref[n * LAYERS + layer] = ref[pl.ds(layer, 1), :].astype(F32)
    ids = seg_ref[...].astype(F32)
    lane = lax.broadcasted_iota(jnp.int32, (128, HEAD), 1)
    for b in range(TOK // 128):
        rows = pl.ds(b * 128, 128)
        mine = jnp.transpose(jnp.broadcast_to(ids[b:b + 1, :], (128, 128)))
        before = jnp.zeros((128, 128), F32)
        for c in range(TOK // 128):
            before = before + jnp.where(ids[c:c + 1, :] < mine, 1.0, 0.0)
        first = jnp.sum(before, axis=1, keepdims=True)
        pos = lax.broadcasted_iota(jnp.int32, (128, 128), 0).astype(F32) + (b * 128.0) - first
        angles = pos * freq_ref[...]
        cos_ref[rows, :] = jnp.cos(angles)
        sin = jnp.sin(angles)
        sin_ref[rows, :] = jnp.where(lane < HEAD // 2, -sin, sin)
        first_ref[rows, :] = jnp.broadcast_to(first, (128, 128)).astype(jnp.int32)

    @pl.loop(0, TOK // NB)
    def _(m):
        rows = pl.ds(pl.multiple_of(m * NB, NB), NB)
        x_ref[rows, :] = q_ref[rows, :].astype(F32)

    for k in range(AHEAD0 - 1):
        for_chunk(k, wait0)
    relays((0, 0, 0), FIRST)
    load_tile(0)

    @pl.loop(0, ALL_STEPS)
    def _(s):
        with jax.named_scope("step"):
            step(s)

    relays(targets(ALL_STEPS - 1), (CHUNKS, CHUNKS, CHUNKS))


def result_kernel(x_ref, a_ref, w2_hbm, w3_hbm, out, y_ref, w_ref, wsem, osem):
    d = lax.axis_index("fsdp")
    core = lax.rem(d, 2)
    c0 = pl.multiple_of((1 - d // 2) * (2 * FF_ROWS) + 2560, HEAD)
    for n in range(4):
        cols = pl.ds(n * 512, 512)
        for src, src_core in ((w2_hbm, core), (w3_hbm, 1 - core)):
            r0 = pl.multiple_of((1 - src_core) * 2560, 512)
            d0 = pl.multiple_of(src_core * TAIL, 64)
            pltpu.make_async_copy(src.at[LAYERS - 1, pl.ds(r0, TAIL), cols], w_ref.at[n, pl.ds(d0, TAIL), :], wsem.at[n]).start()

    def store(n, m):
        rows, cols = pl.ds(m * 512, 512), pl.ds(n * 512, 512)
        return pltpu.make_async_copy(y_ref.at[rows, cols], out.at[rows, cols], osem.at[n, m])

    for n in range(4):
        cols = pl.ds(n * 512, 512)
        pltpu.make_async_copy(w_ref.at[n], w_ref.at[n], wsem.at[n]).wait()
        for m in range(2):
            rows = pl.ds(m * 512, 512)
            y_ref[rows, cols] = x_ref[rows, cols] + jnp.dot(a_ref[rows, pl.ds(c0, REST_K)], w_ref[n], preferred_element_type=F32)
            store(n, m).start()
    for n in range(4):
        for m in range(2):
            store(n, m).wait()


def run_layers(tokens, seg_ids, g_attn, g_mlp, weights):
    shapes = [jax.ShapeDtypeStruct(w.shape, w.dtype) for w in weights]
    half_dim = HEAD // 2
    freq = np.float32(ROPE_BASE) ** (-np.arange(half_dim, dtype=np.float32) / np.float32(half_dim))
    freq = jnp.asarray(np.concatenate([freq, freq]).reshape(1, HEAD))
    sem = pltpu.SemaphoreType.DMA((SLOTS, 2))
    any_spec = pl.BlockSpec(memory_space=pl.ANY)
    vmem_spec = pl.BlockSpec(memory_space=pltpu.VMEM)
    outs = pl.pallas_call(
        layer_kernel,
        out_shape=[pltpu.VMEM((TOK, D), F32), pltpu.VMEM((TOK, FF), BF16)] + shapes * 3,
        in_specs=[any_spec] * 12,
        out_specs=[vmem_spec] * 2 + [any_spec] * 21,
        scratch_shapes=[
            pltpu.VMEM((TOK, D), BF16),
            pltpu.VMEM((TOK, D), BF16),
            pltpu.VMEM((TOK, 512), BF16),
            pltpu.VMEM((2, D, 512), BF16),
            pltpu.VMEM((2, 1024, D), BF16),
            pltpu.VMEM((TOK, HEAD), F32),
            pltpu.VMEM((TOK, HEAD), F32),
            pltpu.VMEM((TOK, HEAD), jnp.int32),
            pltpu.VMEM((2 * LAYERS, 1, D), F32),
            pltpu.VMEM((TOK // 128, 128), jnp.int32),
            pltpu.VMEM((1, HEAD), F32),
            pltpu.VMEM((LAYERS, D), BF16),
            pltpu.VMEM((LAYERS, D), BF16),
            pltpu.SemaphoreType.DMA((2,)),
            pltpu.SemaphoreType.DMA((2,)),
            pltpu.SemaphoreType.DMA((5,)),
        ] + [sem] * 8,
        compiler_params=pltpu.CompilerParams(collective_id=0, has_side_effects=True, vmem_limit_bytes=34 * 1000 * 1000),
        name="two_layers",
    )(tokens, seg_ids.reshape(TOK // 128, 128), freq, g_attn, g_mlp, *weights)
    hidden = pltpu.with_memory_space_constraint(outs[0], pltpu.VMEM)
    act = pltpu.with_memory_space_constraint(outs[1], pltpu.VMEM)
    return pl.pallas_call(
        result_kernel,
        out_shape=jax.ShapeDtypeStruct((TOK, D), F32),
        in_specs=[vmem_spec] * 2 + [any_spec] * 2,
        out_specs=any_spec,
        scratch_shapes=[
            pltpu.VMEM((TOK, D), F32),
            pltpu.VMEM((4, REST_K, 512), BF16),
            pltpu.SemaphoreType.DMA((4,)),
            pltpu.SemaphoreType.DMA((4, 2)),
        ],
        compiler_params=pltpu.CompilerParams(vmem_limit_bytes=24 * 1000 * 1000),
        name="result",
    )(hidden, act, outs[15], outs[22])


def solution(mesh):
    tok_spec = P(("rep", "fsdp"), None)
    seg_spec = P(("rep", "fsdp"))
    mat_spec = P(None, "fsdp", None)
    gain_spec = P(None, None)

    def per_device(tokens, seg_ids, w_q, w_k, w_v, w_o, w_gate, w_up, w_down, g_attn, g_mlp):
        return run_layers(tokens, seg_ids, g_attn, g_mlp, (w_q, w_k, w_v, w_o, w_gate, w_up, w_down))

    return jax.shard_map(per_device, mesh=mesh, in_specs=(tok_spec, seg_spec, mat_spec, mat_spec, mat_spec, mat_spec, mat_spec, mat_spec, mat_spec, gain_spec, gain_spec), out_specs=tok_spec, check_vma=False)
```

```python
import functools

import jax
import jax.numpy as jnp
import numpy as np
from jax import lax
from jax.experimental import pallas as pl
from jax.experimental.pallas import tpu as pltpu
from jax.sharding import PartitionSpec as P

D = 2048
FF = 11008
HEADS = 16
HEAD = 128
TOK = 1024
EPS = 1e-5
ROPE_BASE = 10000.0
MESH = pl.DeviceIdType.MESH
F32 = jnp.float32
BF16 = jnp.bfloat16

LAYERS = 2
SLOTS = 8
AHEAD = 4
AHEAD0 = 3
ROWS = D // 4
FF_ROWS = FF // 4
TAIL = 192
NAMES = ("q", "k", "v", "o", "g", "u", "d")
DIRECT = (0, 1)

N_Q = 4
N_GU = 21
N_D = 10
CH_Q = 1
CH_O = CH_Q + N_Q
CH_GU = CH_O + N_Q
CH_GL = CH_GU + N_GU
CH_D = CH_GL + 1
CH_DR = CH_D + N_D
PER_LAYER = CH_DR + 1
CHUNKS = LAYERS * PER_LAYER

N_GT = FF // 256
ST_Q = 1
ST_A = ST_Q + N_Q
ST_O = ST_A + HEADS
ST_G = ST_O + 4
ST_D = ST_G + N_GT
ST_NEAR = ST_D + 2 * (N_D - 2)
ST_IDLE = ST_NEAR + 4
ST_FAR = ST_IDLE + 1
ST_REST = ST_FAR + 2
STEPS = ST_REST + 2
ALL_STEPS = LAYERS * STEPS - 2
FIRST = (4, 2, 1)
REST_K = 2 * TAIL
NEAR_K = 512 + REST_K

MB = 512
NB = 128
QB = 256


def layer_kernel(*refs):
    tok, seg, freq, g_attn, g_mlp = refs[:5]
    own = dict(zip(NAMES, refs[5:12]))
    x_ref, a_ref = refs[12:14]
    b1 = dict(zip(NAMES, refs[14:21]))
    b2 = dict(zip(NAMES, refs[21:28]))
    b3 = dict(zip(NAMES, refs[28:35]))
    (h_ref, q_ref, kv_ref, wbuf, dbuf, cos_ref, sin_ref, first_ref, gain_ref,
     seg_ref, freq_ref, ga_ref, gm_ref, wsem, dsem, iosem) = refs[35:51]
    s0s, s0r, s1s, s1r, s2s, s2r, s3s, s3r = refs[51:]
    sources = (own, b1, b2, b3)
    y = lax.axis_index("rep")
    d = lax.axis_index("fsdp")
    side = d // 2
    core = lax.rem(d, 2)
    x_dev = (y, lax.rem(d + 2, 4))
    y_dev = (1 - y, d)
    c_dev = (y, d + 1 - 2 * core)

    def rel(block):
        return 2 * lax.rem(block // 2 + side, 2) + lax.rem(block + core, 2)

    inputs = [pltpu.make_async_copy(src, dst, iosem.at[n]) for n, (src, dst) in enumerate(
        ((tok, q_ref), (seg, seg_ref), (freq, freq_ref), (g_attn, ga_ref), (g_mlp, gm_ref)))]
    for copy in inputs:
        copy.start()

    with jax.named_scope("barrier"):
        barrier = pltpu.get_barrier_semaphore()
        for dev in (x_dev, y_dev, c_dev):
            pl.semaphore_signal(barrier, inc=1, device_id=dev, device_id_type=MESH)
        pl.semaphore_wait(barrier, 3)

    def for_chunk(k, fn, lo=0):
        layer = k // PER_LAYER
        i = lax.rem(k, PER_LAYER)
        slot = lax.rem(k, SLOTS)
        ok = (k >= lo) & (k < CHUNKS)

        def case(cond, items, direct=()):
            @pl.when(ok & cond)
            def _():
                for n, (name, r0, nr, c0, nc) in enumerate(items):
                    fn(n in direct, name, layer, r0, nr, c0, nc, slot, n)

        case(i == 0, [("k", 0, ROWS, 0, 256), ("v", 0, ROWS, 0, 256)])
        jq = pl.multiple_of((i - CH_Q) * 512, 512)
        case((i >= CH_Q) & (i < CH_O), [("q", 0, ROWS, jq, 512)])
        jo = pl.multiple_of((i - CH_O) * 512, 512)
        case((i >= CH_O) & (i < CH_GU), [("o", 0, ROWS, jo, 512)])
        jg = pl.multiple_of((i - CH_GU) * 512, 512)
        case((i >= CH_GU) & (i < CH_GL), [("g", 0, ROWS, jg, 512), ("u", 0, ROWS, jg, 512)])
        case(i == CH_GL, [("g", 0, ROWS, N_GU * 512, 256), ("u", 0, ROWS, N_GU * 512, 256)])
        jd = core * TAIL + (i - CH_D) * 256
        case((i >= CH_D) & (i < CH_DR), [("d", jd, 128, 0, D), ("d", jd + 128, 128, 0, D)])
        jr = (1 - core) * 2560
        last = [("d", jr, TAIL // 2, 0, D), ("d", jr + TAIL // 2, TAIL // 2, 0, D)]
        case((i == CH_DR) & (k < CHUNKS - 1), last)
        case((i == CH_DR) & (k == CHUNKS - 1), last, DIRECT)

    def view(bufs, name, layer, r0, nr, c0, nc, half):
        if half:
            nr = nr // 2
            r0 = r0 + y * nr
        r0 = pl.multiple_of(r0, 16)
        return bufs[name].at[layer, pl.ds(r0, nr), pl.ds(c0, nc)]

    def remote(src, dst, ss, rs, dev, half):
        def make(direct, name, layer, r0, nr, c0, nc, slot, n):
            part = half and not direct
            return pltpu.make_async_remote_copy(
                src_ref=view(src, name, layer, r0, nr, c0, nc, part),
                dst_ref=view(dst, name, layer, r0, nr, c0, nc, part),
                send_sem=ss.at[slot, n], recv_sem=rs.at[slot, n], device_id=dev, device_id_type=MESH)
        return make

    copy0 = remote(own, b1, s0s, s0r, c_dev, False)
    copy1 = remote(own, b2, s1s, s1r, x_dev, True)
    copy2 = remote(b2, b2, s2s, s2r, y_dev, True)
    copy3 = remote(b2, b3, s3s, s3r, c_dev, False)

    def start0(*a):
        copy0(*a).start()

    def start1(*a):
        copy1(*a).start()

    def wait0(*a):
        copy0(*a).wait_recv()

    def relay2(*a):
        copy1(*a).wait_recv()
        if not a[0]:
            copy2(*a).start()

    def relay3(*a):
        if not a[0]:
            copy2(*a).wait_recv()
        copy3(*a).start()
        copy0(*a).wait_send()
        copy1(*a).wait_send()

    def finish(*a):
        copy3(*a).wait_recv()
        if not a[0]:
            copy2(*a).wait_send()
        copy3(*a).wait_send()

    def targets(s):
        i = lax.rem(s, STEPS)
        base = s // STEPS * PER_LAYER
        third = (i - ST_A) // 3
        t2 = jnp.where(i < ST_A, 5 + i,
             jnp.where(i < ST_D, jnp.maximum(10 + third, (i + 2) // 2),
             jnp.where(i < ST_NEAR - 3, (i + 1) // 2,
             jnp.where(i < ST_NEAR + 1, jnp.minimum(i // 2, CH_DR), CH_DR + 1 + jnp.maximum(i - ST_NEAR - 2, 0) // 2))))
        t3 = jnp.where(i < ST_A, 3 + i,
             jnp.where(i < ST_D, jnp.maximum(8 + third, (i - 1) // 2),
             jnp.where(i < ST_NEAR, (i - 2) // 2,
             jnp.where(i < ST_NEAR + 2, CH_DR - 1, jnp.where(i < ST_FAR, CH_DR, CH_DR + 1 + (i - ST_FAR) // 2)))))
        t2 = jnp.minimum(t2 + base, jnp.where(s < ALL_STEPS - 2, CHUNKS - 1, CHUNKS))
        t3 = jnp.minimum(t3 + base, jnp.where(s < ALL_STEPS - 2, CHUNKS - 1, CHUNKS))
        nxt = jnp.minimum(s + 1, ALL_STEPS - 1)
        i = lax.rem(nxt, STEPS)
        base = nxt // STEPS * PER_LAYER
        done = jnp.where(i < ST_A, 1 + i,
               jnp.where(i < ST_O, ST_A,
               jnp.where(i < ST_G, 1 + CH_O + i - ST_O,
               jnp.where(i < ST_D, 1 + CH_GU + (i - ST_G) // 2,
               jnp.where(i < ST_NEAR, 1 + CH_D + (i - ST_D) // 2,
               jnp.where(i < ST_IDLE, CH_DR - 2 + (i - ST_NEAR) // 2,
               jnp.where(i < ST_FAR, CH_DR - 1,
               jnp.where(i < ST_REST, CH_DR, PER_LAYER))))))))
        tf = jnp.maximum(t3 - 2, base + done)
        t3 = jnp.maximum(t3, tf)
        t2 = jnp.maximum(jnp.maximum(t2, t3), base + jnp.where((i >= ST_NEAR) & (i < ST_IDLE), CH_DR - 1, 0))
        return t2, t3, tf

    def relays(old, new):
        @pl.loop(old[0], new[0])
        def _(k):
            with jax.named_scope("r2"):
                for_chunk(k, relay2)
                for_chunk(k + AHEAD, start1, AHEAD)
                for_chunk(k + AHEAD0, start0, AHEAD0)
                for_chunk(k + AHEAD0 - 1, wait0)

        @pl.loop(old[1], new[1])
        def _(k):
            with jax.named_scope("r3"):
                for_chunk(k, relay3)

        @pl.loop(old[2], new[2])
        def _(k):
            with jax.named_scope("fin"):
                for_chunk(k, finish)

    def down_step(i):
        late = i >= ST_FAR
        n = jnp.where(late, i - ST_D - 1, i - ST_D)
        j = n // 2
        near = (i >= ST_NEAR) & (i < ST_NEAR + 2)
        far = late & (i < ST_REST)
        rest = i >= ST_REST
        whole = (i >= ST_D) & (i < ST_IDLE) & ~near
        return j, jnp.where(i > ST_NEAR, j - 1, j), lax.rem(n + 2 * STEPS, 2), whole, near, far, rest

    def rest_col(side_no):
        return pl.multiple_of(side_no * (2 * FF_ROWS) + 2560, HEAD)

    def tile_col(side_no, core_no, tile):
        return pl.multiple_of(side_no * (2 * FF_ROWS) + core_no * (FF_ROWS + TAIL) + tile * 256, HEAD)

    def load_tile(s):
        layer = s // STEPS
        i = lax.rem(s, STEPS)
        slot = lax.rem(s, 2)

        def cols(name, c0, nc, w0):
            for r, src in enumerate(sources):
                pltpu.make_async_copy(src[name].at[layer, :, pl.ds(c0, nc)],
                                      wbuf.at[slot, pl.ds(r * ROWS, ROWS), pl.ds(w0, nc)], wsem.at[slot]).start()

        @pl.when(i == 0)
        def _():
            cols("k", 0, 256, 0)
            cols("v", 0, 256, 256)

        @pl.when((i >= ST_Q) & (i < ST_A))
        def _():
            cols("q", pl.multiple_of((i - ST_Q) * 512, 512), 512, 0)

        @pl.when((i >= ST_O) & (i < ST_G))
        def _():
            cols("o", pl.multiple_of((i - ST_O) * 512, 512), 512, 0)

        @pl.when((i >= ST_G) & (i < ST_D))
        def _():
            c0 = pl.multiple_of((i - ST_G) * 256, 256)
            cols("g", c0, 256, 0)
            cols("u", c0, 256, 256)

        j, tile, half, whole, near, far, rest = down_step(i)
        dslot = lax.rem(j + 2 * STEPS, 2)

        def rows_in(src, r0, nr, w0):
            pltpu.make_async_copy(src["d"].at[layer, pl.ds(r0, nr), :], dbuf.at[dslot, pl.ds(w0, nr), :], dsem.at[dslot]).start()

        def chunk_rows(r, tile_no, w0):
            src_core = core if r % 2 == 0 else 1 - core
            rows_in(sources[r], pl.multiple_of(src_core * TAIL + tile_no * 256, 64), 256, w0)

        def rest_rows(r, w0):
            src_core = core if r % 2 == 0 else 1 - core
            rows_in(sources[r], pl.multiple_of((1 - src_core) * 2560, 512), TAIL, pl.multiple_of(w0 + src_core * TAIL, 64))

        @pl.when(whole & (half == 0))
        def _():
            for r in range(4):
                chunk_rows(r, tile, r * 256)

        @pl.when(near & (half == 0))
        def _():
            for r in range(2):
                chunk_rows(r, N_D - 1, r * 256)
                rest_rows(r, 512)

        @pl.when(far & (half == 0))
        def _():
            for r in range(2):
                chunk_rows(2 + r, N_D - 1, r * 256)

        @pl.when(rest & (half == 0))
        def _():
            for r in range(2):
                rest_rows(2 + r, 0)

    def norm(layer, which):
        @pl.loop(0, TOK // NB)
        def _(m):
            rows = pl.ds(pl.multiple_of(m * NB, NB), NB)
            total = jnp.zeros((NB, 1), F32)
            for b in range(4):
                blk = x_ref[rows, pl.ds(b * ROWS, ROWS)]
                total = total + jnp.sum(blk * blk, axis=1, keepdims=True)
            inv = lax.rsqrt(total * (1.0 / D) + EPS)
            for b in range(4):
                blk = x_ref[rows, pl.ds(b * ROWS, ROWS)]
                gain = gain_ref[which * LAYERS + layer, :, pl.ds(b * ROWS, ROWS)]
                c0 = pl.multiple_of(rel(b) * ROWS, ROWS)
                h_ref[rows, pl.ds(c0, ROWS)] = (blk * inv * gain).astype(BF16)

    def rotate(vals, rows):
        vals = vals.astype(BF16).astype(F32)
        turned = pltpu.roll(vals, HEAD // 2, 1)
        return (vals * cos_ref[rows, :] + turned * sin_ref[rows, :]).astype(BF16)

    def tile_product(slot, finish_rows):
        @pl.loop(0, TOK // MB)
        def _(m):
            rows = pl.ds(pl.multiple_of(m * MB, MB), MB)
            finish_rows(rows, jnp.dot(h_ref[rows, :], wbuf[slot], preferred_element_type=F32))

    def kv_step(slot):
        def fin(rows, acc):
            for b in range(2):
                kv_ref[rows, pl.ds(b * HEAD, HEAD)] = rotate(acc[:, b * HEAD:(b + 1) * HEAD], rows)
            kv_ref[rows, pl.ds(256, 256)] = acc[:, 256:].astype(BF16)
        tile_product(slot, fin)

    def q_step(slot, j):
        def fin(rows, acc):
            for b in range(4):
                c0 = pl.multiple_of(j * 512 + b * HEAD, HEAD)
                q_ref[rows, pl.ds(c0, HEAD)] = rotate(acc[:, b * HEAD:(b + 1) * HEAD], rows)
        tile_product(slot, fin)

    def o_step(slot, j):
        def fin(rows, acc):
            c0 = pl.ds(pl.multiple_of(j * 512, 512), 512)
            x_ref[rows, c0] = x_ref[rows, c0] + acc
        tile_product(slot, fin)

    def g_step(slot, j):
        def fin(rows, acc):
            gate = acc[:, :256]
            up = acc[:, 256:]
            c0 = pl.multiple_of(j * 256, 256)
            a_ref[rows, pl.ds(c0, 256)] = (gate * jax.nn.sigmoid(gate) * up).astype(BF16)
        tile_product(slot, fin)

    def attend(head):
        kv = head // 8
        q0 = pl.multiple_of(head * HEAD, HEAD)
        k0 = pl.multiple_of(kv * HEAD, HEAD)
        v0 = pl.multiple_of(256 + kv * HEAD, HEAD)
        o0 = pl.multiple_of(rel(head // 4) * ROWS + lax.rem(head, 4) * HEAD, HEAD)
        scale = HEAD ** -0.5
        for b in range(TOK // QB):
            keys = (b + 1) * QB
            rows = pl.ds(b * QB, QB)
            scores = lax.dot_general(q_ref[rows, pl.ds(q0, HEAD)], kv_ref[pl.ds(0, keys), pl.ds(k0, HEAD)],
                                     (((1,), (1,)), ((), ())), preferred_element_type=F32)
            key_idx = lax.broadcasted_iota(jnp.int32, (QB, keys), 1)
            row_idx = lax.broadcasted_iota(jnp.int32, (QB, keys), 0) + b * QB
            first = jnp.concatenate([first_ref[rows, :]] * (keys // HEAD), axis=1)
            ok = (key_idx >= first) & (key_idx <= row_idx)
            scores = jnp.where(ok, scores, -1e30)
            top = jnp.max(scores, axis=1, keepdims=True)
            probs = jnp.exp((scores - top) * scale)
            inv = 1.0 / jnp.sum(probs, axis=1, keepdims=True)
            probs = (probs * inv).astype(BF16)
            mixed = jnp.dot(probs, kv_ref[pl.ds(0, keys), pl.ds(v0, HEAD)], preferred_element_type=F32)
            h_ref[rows, pl.ds(o0, HEAD)] = mixed.astype(BF16)

    def add_product(dslot, half, cols):
        rows = pl.ds(pl.multiple_of(half * MB, MB), MB)
        depth = sum(width for _, width in cols)
        lhs = jnp.concatenate([a_ref[rows, pl.ds(c0, width)] for c0, width in cols], axis=1)
        x_ref[rows, :] = x_ref[rows, :] + jnp.dot(lhs, dbuf[dslot, pl.ds(0, depth), :], preferred_element_type=F32)

    def wait_d(dslot, half, depth):
        @pl.when(half == 0)
        def _():
            part = dbuf.at[dslot, pl.ds(0, depth), :]
            pltpu.make_async_copy(part, part, dsem.at[dslot]).wait()

    def last_cols(side_no):
        return [(tile_col(side_no, core, N_D - 1), 256), (tile_col(side_no, 1 - core, N_D - 1), 256)]

    def wait_w(slot):
        pltpu.make_async_copy(wbuf.at[slot], wbuf.at[slot], wsem.at[slot]).wait()

    def step(s):
        before = [jnp.where(s == 0, one, two) for one, two in zip(FIRST, targets(s - 1))]
        relays(before, targets(s))

        @pl.when(s + 1 < ALL_STEPS)
        def _():
            load_tile(s + 1)

        with jax.named_scope("comp"):
            compute(s)

    def compute(s):
        layer = s // STEPS
        i = lax.rem(s, STEPS)
        slot = lax.rem(s, 2)

        @pl.when((i == 0) | (i == ST_G))
        def _():
            norm(layer, jnp.where(i == 0, 0, 1))

        @pl.when((i < ST_A) | ((i >= ST_O) & (i < ST_D)))
        def _():
            wait_w(slot)

        @pl.when(i == 0)
        def _():
            kv_step(slot)

        @pl.when((i >= ST_Q) & (i < ST_A))
        def _():
            q_step(slot, i - ST_Q)

        @pl.when((i >= ST_A) & (i < ST_O))
        def _():
            attend(i - ST_A)

        @pl.when((i >= ST_O) & (i < ST_G))
        def _():
            o_step(slot, i - ST_O)

        @pl.when((i >= ST_G) & (i < ST_D))
        def _():
            g_step(slot, i - ST_G)

        j, tile, half, whole, near, far, rest = down_step(i)
        dslot = lax.rem(j + 2 * STEPS, 2)

        @pl.when(whole)
        def _():
            wait_d(dslot, half, 1024)
            add_product(dslot, half, [(tile_col(lax.rem(side + r // 2, 2), lax.rem(core + r, 2), tile), 256) for r in range(4)])

        @pl.when(near)
        def _():
            wait_d(dslot, half, NEAR_K)
            add_product(dslot, half, last_cols(side) + [(rest_col(side), REST_K)])

        @pl.when(far)
        def _():
            wait_d(dslot, half, 512)
            add_product(dslot, half, last_cols(1 - side))

        @pl.when(rest)
        def _():
            wait_d(dslot, half, REST_K)
            add_product(dslot, half, [(rest_col(1 - side), REST_K)])

    @pl.loop(0, AHEAD)
    def _(k):
        for_chunk(k, start1)

    @pl.loop(0, AHEAD0)
    def _(k):
        for_chunk(k, start0)

    for copy in inputs:
        copy.wait()

    for n, ref in enumerate((ga_ref, gm_ref)):
        for layer in range(LAYERS):
            gain_ref[n * LAYERS + layer] = ref[pl.ds(layer, 1), :].astype(F32)
    ids = seg_ref[...].astype(F32)
    lane = lax.broadcasted_iota(jnp.int32, (128, HEAD), 1)
    for b in range(TOK // 128):
        rows = pl.ds(b * 128, 128)
        mine = jnp.transpose(jnp.broadcast_to(ids[b:b + 1, :], (128, 128)))
        before = jnp.zeros((128, 128), F32)
        for c in range(TOK // 128):
            before = before + jnp.where(ids[c:c + 1, :] < mine, 1.0, 0.0)
        first = jnp.sum(before, axis=1, keepdims=True)
        pos = lax.broadcasted_iota(jnp.int32, (128, 128), 0).astype(F32) + (b * 128.0) - first
        angles = pos * freq_ref[...]
        cos_ref[rows, :] = jnp.cos(angles)
        sin = jnp.sin(angles)
        sin_ref[rows, :] = jnp.where(lane < HEAD // 2, -sin, sin)
        first_ref[rows, :] = jnp.broadcast_to(first, (128, 128)).astype(jnp.int32)

    @pl.loop(0, TOK // NB)
    def _(m):
        rows = pl.ds(pl.multiple_of(m * NB, NB), NB)
        x_ref[rows, :] = q_ref[rows, :].astype(F32)

    for k in range(AHEAD0 - 1):
        for_chunk(k, wait0)
    relays((0, 0, 0), FIRST)
    load_tile(0)

    @pl.loop(0, ALL_STEPS)
    def _(s):
        with jax.named_scope("step"):
            step(s)

    relays(targets(ALL_STEPS - 1), (CHUNKS, CHUNKS, CHUNKS))


def result_kernel(x_ref, a_ref, w2_hbm, w3_hbm, out, y_ref, w_ref, wsem, osem):
    d = lax.axis_index("fsdp")
    core = lax.rem(d, 2)
    c0 = pl.multiple_of((1 - d // 2) * (2 * FF_ROWS) + 2560, HEAD)
    for n in range(4):
        cols = pl.ds(n * 512, 512)
        for src, src_core in ((w2_hbm, core), (w3_hbm, 1 - core)):
            r0 = pl.multiple_of((1 - src_core) * 2560, 512)
            d0 = pl.multiple_of(src_core * TAIL, 64)
            pltpu.make_async_copy(src.at[LAYERS - 1, pl.ds(r0, TAIL), cols], w_ref.at[n, pl.ds(d0, TAIL), :], wsem.at[n]).start()

    def store(n, m):
        rows, cols = pl.ds(m * 512, 512), pl.ds(n * 512, 512)
        return pltpu.make_async_copy(y_ref.at[rows, cols], out.at[rows, cols], osem.at[n, m])

    for n in range(4):
        cols = pl.ds(n * 512, 512)
        pltpu.make_async_copy(w_ref.at[n], w_ref.at[n], wsem.at[n]).wait()
        for m in range(2):
            rows = pl.ds(m * 512, 512)
            y_ref[rows, cols] = x_ref[rows, cols] + jnp.dot(a_ref[rows, pl.ds(c0, REST_K)], w_ref[n], preferred_element_type=F32)
            store(n, m).start()
    for n in range(4):
        for m in range(2):
            store(n, m).wait()


def run_layers(tokens, seg_ids, g_attn, g_mlp, weights):
    shapes = [jax.ShapeDtypeStruct(w.shape, w.dtype) for w in weights]
    half_dim = HEAD // 2
    freq = np.float32(ROPE_BASE) ** (-np.arange(half_dim, dtype=np.float32) / np.float32(half_dim))
    freq = jnp.asarray(np.concatenate([freq, freq]).reshape(1, HEAD))
    sem = pltpu.SemaphoreType.DMA((SLOTS, 2))
    any_spec = pl.BlockSpec(memory_space=pl.ANY)
    vmem_spec = pl.BlockSpec(memory_space=pltpu.VMEM)
    outs = pl.pallas_call(
        layer_kernel,
        out_shape=[pltpu.VMEM((TOK, D), F32), pltpu.VMEM((TOK, FF), BF16)] + shapes * 3,
        in_specs=[any_spec] * 12,
        out_specs=[vmem_spec] * 2 + [any_spec] * 21,
        scratch_shapes=[
            pltpu.VMEM((TOK, D), BF16),
            pltpu.VMEM((TOK, D), BF16),
            pltpu.VMEM((TOK, 512), BF16),
            pltpu.VMEM((2, D, 512), BF16),
            pltpu.VMEM((2, 1024, D), BF16),
            pltpu.VMEM((TOK, HEAD), F32),
            pltpu.VMEM((TOK, HEAD), F32),
            pltpu.VMEM((TOK, HEAD), jnp.int32),
            pltpu.VMEM((2 * LAYERS, 1, D), F32),
            pltpu.VMEM((TOK // 128, 128), jnp.int32),
            pltpu.VMEM((1, HEAD), F32),
            pltpu.VMEM((LAYERS, D), BF16),
            pltpu.VMEM((LAYERS, D), BF16),
            pltpu.SemaphoreType.DMA((2,)),
            pltpu.SemaphoreType.DMA((2,)),
            pltpu.SemaphoreType.DMA((5,)),
        ] + [sem] * 8,
        compiler_params=pltpu.CompilerParams(collective_id=0, has_side_effects=True, vmem_limit_bytes=34 * 1000 * 1000),
        name="two_layers",
    )(tokens, seg_ids.reshape(TOK // 128, 128), freq, g_attn, g_mlp, *weights)
    hidden = pltpu.with_memory_space_constraint(outs[0], pltpu.VMEM)
    act = pltpu.with_memory_space_constraint(outs[1], pltpu.VMEM)
    return pl.pallas_call(
        result_kernel,
        out_shape=jax.ShapeDtypeStruct((TOK, D), F32),
        in_specs=[vmem_spec] * 2 + [any_spec] * 2,
        out_specs=any_spec,
        scratch_shapes=[
            pltpu.VMEM((TOK, D), F32),
            pltpu.VMEM((4, REST_K, 512), BF16),
            pltpu.SemaphoreType.DMA((4,)),
            pltpu.SemaphoreType.DMA((4, 2)),
        ],
        compiler_params=pltpu.CompilerParams(vmem_limit_bytes=24 * 1000 * 1000),
        name="result",
    )(hidden, act, outs[15], outs[22])


def solution(mesh):
    tok_spec = P(("rep", "fsdp"), None)
    seg_spec = P(("rep", "fsdp"))
    mat_spec = P(None, "fsdp", None)
    gain_spec = P(None, None)

    def per_device(tokens, seg_ids, w_q, w_k, w_v, w_o, w_gate, w_up, w_down, g_attn, g_mlp):
        return run_layers(tokens, seg_ids, g_attn, g_mlp, (w_q, w_k, w_v, w_o, w_gate, w_up, w_down))

    return jax.shard_map(per_device, mesh=mesh, in_specs=(tok_spec, seg_spec, mat_spec, mat_spec, mat_spec, mat_spec, mat_spec, mat_spec, mat_spec, gain_spec, gain_spec), out_specs=tok_spec, check_vma=False)
```

```python
import functools

import jax
import jax.numpy as jnp
import numpy as np
from jax import lax
from jax.experimental import pallas as pl
from jax.experimental.pallas import tpu as pltpu
from jax.sharding import PartitionSpec as P

D = 2048
FF = 11008
HEADS = 16
HEAD = 128
TOK = 1024
EPS = 1e-5
ROPE_BASE = 10000.0
MESH = pl.DeviceIdType.MESH
F32 = jnp.float32
BF16 = jnp.bfloat16

LAYERS = 2
SLOTS = 8
ITEM_SLOTS = 2 * SLOTS
AHEAD = 8
AHEAD0 = 5
ROWS = D // 4
FF_ROWS = FF // 4
TAIL = 192
NAMES = ("q", "k", "v", "o", "g", "u", "d")

N_Q = 4
N_GU = 21
N_D = 10
CH_Q = 1
CH_O = CH_Q + N_Q
CH_GU = CH_O + N_Q
CH_GL = CH_GU + N_GU
CH_D = CH_GL + 1
CH_DR = CH_D + N_D
PER_LAYER = CH_DR + 1
CHUNKS = LAYERS * PER_LAYER
ITEMS = 2 * CHUNKS

NEAR_AT = 6

N_GT = FF // 256
ST_Q = 1
ST_A = ST_Q + N_Q
ST_O = ST_A + HEADS
ST_G = ST_O + 4
ST_D = ST_G + N_GT
ST_NEAR = ST_D + 2 * NEAR_AT
ST_IDLE = ST_D + 2 * N_D
ST_FAR = ST_IDLE + 1
ST_REST = ST_FAR + 2
STEPS = ST_REST + 2
ALL_STEPS = LAYERS * STEPS - 2
START = (4, 1, 0)
FIRST = (8, 3, 1)
REST_K = 2 * TAIL
NEAR_K = 512 + REST_K

MB = 512
NB = 128
QB = 256


def layer_kernel(*refs):
    tok, seg, freq, g_attn, g_mlp = refs[:5]
    own = dict(zip(NAMES, refs[5:12]))
    x_ref, a_ref = refs[12:14]
    b1 = dict(zip(NAMES, refs[14:21]))
    b2 = dict(zip(NAMES, refs[21:28]))
    b3 = dict(zip(NAMES, refs[28:35]))
    (h_ref, q_ref, kv_ref, wbuf, dbuf, cos_ref, sin_ref, first_ref, gain_ref,
     seg_ref, freq_ref, ga_ref, gm_ref, wsem, dsem, iosem) = refs[35:51]
    s0s, s0r, s1s, s1r, s2s, s2r, s3s, s3r = refs[51:]
    sources = (own, b1, b2, b3)
    y = lax.axis_index("rep")
    d = lax.axis_index("fsdp")
    side = d // 2
    core = lax.rem(d, 2)
    x_dev = (y, lax.rem(d + 2, 4))
    y_dev = (1 - y, d)
    c_dev = (y, d + 1 - 2 * core)

    def rel(block):
        return 2 * lax.rem(block // 2 + side, 2) + lax.rem(block + core, 2)

    inputs = [pltpu.make_async_copy(src, dst, iosem.at[n]) for n, (src, dst) in enumerate(
        ((tok, q_ref), (seg, seg_ref), (freq, freq_ref), (g_attn, ga_ref), (g_mlp, gm_ref)))]
    for copy in inputs:
        copy.start()

    with jax.named_scope("barrier"):
        barrier = pltpu.get_barrier_semaphore()
        for dev in (x_dev, y_dev, c_dev):
            pl.semaphore_signal(barrier, inc=1, device_id=dev, device_id_type=MESH)
        pl.semaphore_wait(barrier, 3)

    def kinds(k):
        i = lax.rem(k, PER_LAYER)
        jq = pl.multiple_of((i - CH_Q) * 512, 512)
        jo = pl.multiple_of((i - CH_O) * 512, 512)
        jg = pl.multiple_of((i - CH_GU) * 512, 512)
        jd = core * TAIL + (i - CH_D) * 256
        jr = (1 - core) * 2560
        last = N_GU * 512
        kv = [("k", 0, ROWS, 0, 256), ("v", 0, ROWS, 0, 256)]
        gu = [("g", 0, ROWS, jg, 512), ("u", 0, ROWS, jg, 512)]
        gl = [("g", 0, ROWS, last, 256), ("u", 0, ROWS, last, 256)]

        def split_cols(name, c0):
            return [(name, 0, ROWS, c0, 256), (name, 0, ROWS, c0 + 256, 256)], [(name, 0, ROWS, c0, 512)]

        def split_rows(r0, nr):
            return [("d", r0, nr // 2, 0, D), ("d", r0 + nr // 2, nr // 2, 0, D)], [("d", r0, nr, 0, D)]

        return [
            (i == 0, kv, kv),
            ((i >= CH_Q) & (i < CH_O), *split_cols("q", jq)),
            ((i >= CH_O) & (i < CH_GU), *split_cols("o", jo)),
            ((i >= CH_GU) & (i < CH_GL), gu, gu),
            (i == CH_GL, gl, gl),
            ((i >= CH_D) & (i < CH_DR), *split_rows(jd, 256)),
            (i == CH_DR, *split_rows(jr, TAIL)),
        ]

    def for_chunk(k, fn):
        layer = k // PER_LAYER
        slot = lax.rem(k, SLOTS)
        for cond, _, whole in kinds(k):
            @pl.when((k < CHUNKS) & cond)
            def _():
                for n, piece in enumerate(whole):
                    fn(False, layer, piece, (slot, n))

    def for_pair(k, fn):
        layer = k // PER_LAYER
        table = kinds(k)
        for c, (cond, pieces, _) in enumerate(table):
            for end in ((False, True) if c == len(table) - 1 else (None,)):
                here = cond if end is None else cond & ((k == CHUNKS - 1) if end else (k < CHUNKS - 1))

                @pl.when((k < CHUNKS) & here)
                def _():
                    for n, piece in enumerate(pieces):
                        fn(bool(end) and n == 1, layer, piece, (lax.rem(2 * k + n, ITEM_SLOTS),))

    def for_item(m, fn):
        k = m // 2
        n = lax.rem(m, 2)
        layer = k // PER_LAYER
        slot = (lax.rem(m, ITEM_SLOTS),)
        for cond, (one, two), _ in kinds(k):
            if one[0] == two[0]:
                name, r0, nr, c0, nc = one
                r0 = r0 + n * (nr if nc == D else 0)
                c0 = c0 + n * (0 if nc == D else nc) if nc == D else pl.multiple_of(c0 + n * nc, 256)
                piece = (name, r0, nr, c0 if nc != D else 0, nc)

                @pl.when((m < ITEMS - 1) & cond)
                def _():
                    fn(False, layer, piece, slot)
                if nc == D and nr == TAIL // 2:
                    @pl.when((m == ITEMS - 1) & cond)
                    def _():
                        fn(True, layer, piece, slot)
            else:
                for which, piece in enumerate((one, two)):
                    @pl.when((m < ITEMS) & cond & (n == which))
                    def _():
                        fn(False, layer, piece, slot)

    def view(bufs, name, layer, r0, nr, c0, nc, half):
        if half:
            nr = nr // 2
            r0 = r0 + y * nr
        r0 = pl.multiple_of(r0, 16)
        return bufs[name].at[layer, pl.ds(r0, nr), pl.ds(c0, nc)]

    def remote(src, dst, ss, rs, dev, half):
        def make(whole, layer, piece, slot):
            part = half and not whole
            return pltpu.make_async_remote_copy(
                src_ref=view(src, piece[0], layer, *piece[1:], part),
                dst_ref=view(dst, piece[0], layer, *piece[1:], part),
                send_sem=ss.at[slot], recv_sem=rs.at[slot], device_id=dev, device_id_type=MESH)
        return make

    copy0 = remote(own, b1, s0s, s0r, c_dev, False)
    copy1 = remote(own, b2, s1s, s1r, x_dev, True)
    copy2 = remote(b2, b2, s2s, s2r, y_dev, True)
    copy3 = remote(b2, b3, s3s, s3r, c_dev, False)

    def start0(*a):
        copy0(*a).start()

    def start1(*a):
        copy1(*a).start()

    def wait0(*a):
        copy0(*a).wait_recv()

    def relay2(*a):
        copy1(*a).wait_recv()
        if not a[0]:
            copy2(*a).start()

    def arrived(*a):
        if not a[0]:
            copy2(*a).wait_recv()
        copy1(*a).wait_send()

    def relay3(*a):
        copy3(*a).start()
        copy0(*a).wait_send()

    def finish(*a):
        copy3(*a).wait_recv()
        copy3(*a).wait_send()

    def sent(*a):
        if not a[0]:
            copy2(*a).wait_send()

    def targets(s):
        i = lax.rem(s, STEPS)
        layer = s // STEPS
        heads = (i - ST_A) // 2
        t2 = jnp.where(i < ST_A, 8 + 2 * i - 4 * layer,
             jnp.where(i < ST_D, jnp.maximum(i, jnp.where(layer == 0, 18 + heads, jnp.minimum(14 + 2 * heads, 16 + heads))),
             jnp.where(i < ST_NEAR, i,
             jnp.where(i < ST_IDLE, ST_NEAR - 1 + (i - ST_NEAR + 1) // 2, i - 4))))
        t3 = jnp.where(i < ST_NEAR + 3, (t2 - 2) // 2, jnp.where(i < ST_IDLE - 1, CH_DR - 1, CH_DR + (i - ST_IDLE + 1) // 2))
        end = s >= ALL_STEPS - 2
        t2 = jnp.minimum(t2 + layer * 2 * PER_LAYER, jnp.where(end, ITEMS, ITEMS - 1))
        t3 = jnp.minimum(t3 + layer * PER_LAYER, jnp.where(end, CHUNKS, CHUNKS - 1))
        nxt = jnp.minimum(s + 1, ALL_STEPS - 1)
        i = lax.rem(nxt, STEPS)
        done = jnp.where(i < ST_A, 1 + i,
               jnp.where(i < ST_O, ST_A,
               jnp.where(i < ST_G, 1 + CH_O + i - ST_O,
               jnp.where(i < ST_D, 1 + CH_GU + (i - ST_G) // 2,
               jnp.where(i < ST_NEAR, 1 + CH_D + (i - ST_D) // 2,
               jnp.where(i < ST_IDLE, CH_D + (i - ST_D) // 2,
               jnp.where(i < ST_FAR, CH_DR - 1,
               jnp.where(i < ST_REST, CH_DR, PER_LAYER))))))))
        tf = jnp.maximum(t3 - 2, done + nxt // STEPS * PER_LAYER)
        t3 = jnp.maximum(t3, tf)
        return jnp.maximum(t2, 2 * t3), t3, tf

    def relays(old, new):
        @pl.loop(old[0], new[0])
        def _(m):
            with jax.named_scope("r2"):
                for_item(m, relay2)
                for_item(m + AHEAD, start1)
                n = lax.rem(m, 2)
                for_chunk(m // 2 + jnp.where(n == 0, AHEAD0, CHUNKS), start0)
                for_chunk(m // 2 + jnp.where(n == 0, CHUNKS, AHEAD0 - 1), wait0)

        @pl.loop(old[1], new[1])
        def _(k):
            with jax.named_scope("r3"):
                for_pair(k, arrived)
                for_chunk(k, relay3)

        @pl.loop(old[2], new[2])
        def _(k):
            with jax.named_scope("fin"):
                for_chunk(k, finish)
                for_pair(k, sent)

    def down_step(i):
        late = i >= ST_FAR
        n = jnp.where(late, i - ST_D - 1, i - ST_D)
        j = n // 2
        near = (i >= ST_NEAR) & (i < ST_NEAR + 2)
        far = late & (i < ST_REST)
        rest = i >= ST_REST
        whole = (i >= ST_D) & (i < ST_IDLE) & ~near
        return j, jnp.where(i > ST_NEAR, j - 1, j), lax.rem(n + 2 * STEPS, 2), whole, near, far, rest

    def rest_col(side_no):
        return pl.multiple_of(side_no * (2 * FF_ROWS) + 2560, HEAD)

    def tile_col(side_no, core_no, tile):
        return pl.multiple_of(side_no * (2 * FF_ROWS) + core_no * (FF_ROWS + TAIL) + tile * 256, HEAD)

    def load_tile(s):
        layer = s // STEPS
        i = lax.rem(s, STEPS)
        slot = lax.rem(s, 2)

        def cols(name, c0, nc, w0):
            for r, src in enumerate(sources):
                pltpu.make_async_copy(src[name].at[layer, :, pl.ds(c0, nc)],
                                      wbuf.at[slot, pl.ds(r * ROWS, ROWS), pl.ds(w0, nc)], wsem.at[slot]).start()

        @pl.when(i == 0)
        def _():
            cols("k", 0, 256, 0)
            cols("v", 0, 256, 256)

        @pl.when((i >= ST_Q) & (i < ST_A))
        def _():
            cols("q", pl.multiple_of((i - ST_Q) * 512, 512), 512, 0)

        @pl.when((i >= ST_O) & (i < ST_G))
        def _():
            cols("o", pl.multiple_of((i - ST_O) * 512, 512), 512, 0)

        @pl.when((i >= ST_G) & (i < ST_D))
        def _():
            c0 = pl.multiple_of((i - ST_G) * 256, 256)
            cols("g", c0, 256, 0)
            cols("u", c0, 256, 256)

        j, tile, half, whole, near, far, rest = down_step(i)
        dslot = lax.rem(j + 2 * STEPS, 2)

        def rows_in(src, r0, nr, w0):
            pltpu.make_async_copy(src["d"].at[layer, pl.ds(r0, nr), :], dbuf.at[dslot, pl.ds(w0, nr), :], dsem.at[dslot]).start()

        def chunk_rows(r, tile_no, w0):
            src_core = core if r % 2 == 0 else 1 - core
            rows_in(sources[r], pl.multiple_of(src_core * TAIL + tile_no * 256, 64), 256, w0)

        def rest_rows(r, w0):
            src_core = core if r % 2 == 0 else 1 - core
            rows_in(sources[r], pl.multiple_of((1 - src_core) * 2560, 512), TAIL, pl.multiple_of(w0 + src_core * TAIL, 64))

        @pl.when(whole & (half == 0))
        def _():
            for r in range(4):
                chunk_rows(r, tile, r * 256)

        @pl.when(near & (half == 0))
        def _():
            for r in range(2):
                chunk_rows(r, N_D - 1, r * 256)
                rest_rows(r, 512)

        @pl.when(far & (half == 0))
        def _():
            for r in range(2):
                chunk_rows(2 + r, N_D - 1, r * 256)

        @pl.when(rest & (half == 0))
        def _():
            for r in range(2):
                rest_rows(2 + r, 0)

    def norm(layer, which):
        @pl.loop(0, TOK // NB)
        def _(m):
            rows = pl.ds(pl.multiple_of(m * NB, NB), NB)
            total = jnp.zeros((NB, 1), F32)
            for b in range(4):
                blk = x_ref[rows, pl.ds(b * ROWS, ROWS)]
                total = total + jnp.sum(blk * blk, axis=1, keepdims=True)
            inv = lax.rsqrt(total * (1.0 / D) + EPS)
            for b in range(4):
                blk = x_ref[rows, pl.ds(b * ROWS, ROWS)]
                gain = gain_ref[which * LAYERS + layer, :, pl.ds(b * ROWS, ROWS)]
                c0 = pl.multiple_of(rel(b) * ROWS, ROWS)
                h_ref[rows, pl.ds(c0, ROWS)] = (blk * inv * gain).astype(BF16)

    def rotate(vals, rows):
        vals = vals.astype(BF16).astype(F32)
        turned = pltpu.roll(vals, HEAD // 2, 1)
        return (vals * cos_ref[rows, :] + turned * sin_ref[rows, :]).astype(BF16)

    def tile_product(slot, finish_rows):
        @pl.loop(0, TOK // MB)
        def _(m):
            rows = pl.ds(pl.multiple_of(m * MB, MB), MB)
            finish_rows(rows, jnp.dot(h_ref[rows, :], wbuf[slot], preferred_element_type=F32))

    def kv_step(slot):
        def fin(rows, acc):
            for b in range(2):
                kv_ref[rows, pl.ds(b * HEAD, HEAD)] = rotate(acc[:, b * HEAD:(b + 1) * HEAD], rows)
            kv_ref[rows, pl.ds(256, 256)] = acc[:, 256:].astype(BF16)
        tile_product(slot, fin)

    def q_step(slot, j):
        def fin(rows, acc):
            for b in range(4):
                c0 = pl.multiple_of(j * 512 + b * HEAD, HEAD)
                q_ref[rows, pl.ds(c0, HEAD)] = rotate(acc[:, b * HEAD:(b + 1) * HEAD], rows)
        tile_product(slot, fin)

    def o_step(slot, j):
        def fin(rows, acc):
            c0 = pl.ds(pl.multiple_of(j * 512, 512), 512)
            x_ref[rows, c0] = x_ref[rows, c0] + acc
        tile_product(slot, fin)

    def g_step(slot, j):
        def fin(rows, acc):
            gate = acc[:, :256]
            up = acc[:, 256:]
            c0 = pl.multiple_of(j * 256, 256)
            a_ref[rows, pl.ds(c0, 256)] = (gate * jax.nn.sigmoid(gate) * up).astype(BF16)
        tile_product(slot, fin)

    def attend(head):
        kv = head // 8
        q0 = pl.multiple_of(head * HEAD, HEAD)
        k0 = pl.multiple_of(kv * HEAD, HEAD)
        v0 = pl.multiple_of(256 + kv * HEAD, HEAD)
        o0 = pl.multiple_of(rel(head // 4) * ROWS + lax.rem(head, 4) * HEAD, HEAD)
        scale = HEAD ** -0.5
        for b in range(TOK // QB):
            keys = (b + 1) * QB
            rows = pl.ds(b * QB, QB)
            scores = lax.dot_general(q_ref[rows, pl.ds(q0, HEAD)], kv_ref[pl.ds(0, keys), pl.ds(k0, HEAD)],
                                     (((1,), (1,)), ((), ())), preferred_element_type=F32)
            key_idx = lax.broadcasted_iota(jnp.int32, (QB, keys), 1)
            row_idx = lax.broadcasted_iota(jnp.int32, (QB, keys), 0) + b * QB
            first = jnp.concatenate([first_ref[rows, :]] * (keys // HEAD), axis=1)
            ok = (key_idx >= first) & (key_idx <= row_idx)
            scores = jnp.where(ok, scores, -1e30)
            top = jnp.max(scores, axis=1, keepdims=True)
            probs = jnp.exp((scores - top) * scale)
            inv = 1.0 / jnp.sum(probs, axis=1, keepdims=True)
            probs = (probs * inv).astype(BF16)
            mixed = jnp.dot(probs, kv_ref[pl.ds(0, keys), pl.ds(v0, HEAD)], preferred_element_type=F32)
            h_ref[rows, pl.ds(o0, HEAD)] = mixed.astype(BF16)

    def add_product(dslot, half, cols):
        rows = pl.ds(pl.multiple_of(half * MB, MB), MB)
        depth = sum(width for _, width in cols)
        lhs = jnp.concatenate([a_ref[rows, pl.ds(c0, width)] for c0, width in cols], axis=1)
        x_ref[rows, :] = x_ref[rows, :] + jnp.dot(lhs, dbuf[dslot, pl.ds(0, depth), :], preferred_element_type=F32)

    def wait_d(dslot, half, depth):
        @pl.when(half == 0)
        def _():
            part = dbuf.at[dslot, pl.ds(0, depth), :]
            pltpu.make_async_copy(part, part, dsem.at[dslot]).wait()

    def last_cols(side_no):
        return [(tile_col(side_no, core, N_D - 1), 256), (tile_col(side_no, 1 - core, N_D - 1), 256)]

    def wait_w(slot):
        pltpu.make_async_copy(wbuf.at[slot], wbuf.at[slot], wsem.at[slot]).wait()

    def step(s):
        before = [jnp.where(s == 0, one, two) for one, two in zip(FIRST, targets(s - 1))]
        relays(before, targets(s))

        @pl.when(s + 1 < ALL_STEPS)
        def _():
            load_tile(s + 1)

        with jax.named_scope("comp"):
            compute(s)

    def compute(s):
        layer = s // STEPS
        i = lax.rem(s, STEPS)
        slot = lax.rem(s, 2)

        @pl.when((i == 0) | (i == ST_G))
        def _():
            norm(layer, jnp.where(i == 0, 0, 1))

        @pl.when((i < ST_A) | ((i >= ST_O) & (i < ST_D)))
        def _():
            wait_w(slot)

        @pl.when(i == 0)
        def _():
            kv_step(slot)

        @pl.when((i >= ST_Q) & (i < ST_A))
        def _():
            q_step(slot, i - ST_Q)

        @pl.when((i >= ST_A) & (i < ST_O))
        def _():
            attend(i - ST_A)

        @pl.when((i >= ST_O) & (i < ST_G))
        def _():
            o_step(slot, i - ST_O)

        @pl.when((i >= ST_G) & (i < ST_D))
        def _():
            g_step(slot, i - ST_G)

        j, tile, half, whole, near, far, rest = down_step(i)
        dslot = lax.rem(j + 2 * STEPS, 2)

        @pl.when(whole)
        def _():
            wait_d(dslot, half, 1024)
            add_product(dslot, half, [(tile_col(lax.rem(side + r // 2, 2), lax.rem(core + r, 2), tile), 256) for r in range(4)])

        @pl.when(near)
        def _():
            wait_d(dslot, half, NEAR_K)
            add_product(dslot, half, last_cols(side) + [(rest_col(side), REST_K)])

        @pl.when(far)
        def _():
            wait_d(dslot, half, 512)
            add_product(dslot, half, last_cols(1 - side))

        @pl.when(rest)
        def _():
            wait_d(dslot, half, REST_K)
            add_product(dslot, half, [(rest_col(1 - side), REST_K)])

    @pl.loop(0, AHEAD)
    def _(m):
        for_item(m, start1)

    @pl.loop(0, AHEAD0)
    def _(k):
        for_chunk(k, start0)

    for copy in inputs:
        copy.wait()

    for n, ref in enumerate((ga_ref, gm_ref)):
        for layer in range(LAYERS):
            gain_ref[n * LAYERS + layer] = ref[pl.ds(layer, 1), :].astype(F32)
    ids = seg_ref[...].astype(F32)
    lane = lax.broadcasted_iota(jnp.int32, (128, HEAD), 1)
    for b in range(TOK // 128):
        rows = pl.ds(b * 128, 128)
        mine = jnp.transpose(jnp.broadcast_to(ids[b:b + 1, :], (128, 128)))
        before = jnp.zeros((128, 128), F32)
        for c in range(TOK // 128):
            before = before + jnp.where(ids[c:c + 1, :] < mine, 1.0, 0.0)
        first = jnp.sum(before, axis=1, keepdims=True)
        pos = lax.broadcasted_iota(jnp.int32, (128, 128), 0).astype(F32) + (b * 128.0) - first
        angles = pos * freq_ref[...]
        cos_ref[rows, :] = jnp.cos(angles)
        sin = jnp.sin(angles)
        sin_ref[rows, :] = jnp.where(lane < HEAD // 2, -sin, sin)
        first_ref[rows, :] = jnp.broadcast_to(first, (128, 128)).astype(jnp.int32)

    @pl.loop(0, TOK // NB)
    def _(m):
        rows = pl.ds(pl.multiple_of(m * NB, NB), NB)
        x_ref[rows, :] = q_ref[rows, :].astype(F32)

    @pl.loop(0, AHEAD0 - 1)
    def _(k):
        for_chunk(k, wait0)

    relays((0, 0, 0), START)
    relays(START, FIRST)
    load_tile(0)

    @pl.loop(0, ALL_STEPS)
    def _(s):
        with jax.named_scope("step"):
            step(s)

    relays(targets(ALL_STEPS - 1), (ITEMS, CHUNKS, CHUNKS))


def result_kernel(x_ref, a_ref, w2_hbm, w3_hbm, out, y_ref, w_ref, wsem, osem):
    d = lax.axis_index("fsdp")
    core = lax.rem(d, 2)
    c0 = pl.multiple_of((1 - d // 2) * (2 * FF_ROWS) + 2560, HEAD)
    for n in range(4):
        cols = pl.ds(n * 512, 512)
        for src, src_core in ((w2_hbm, core), (w3_hbm, 1 - core)):
            r0 = pl.multiple_of((1 - src_core) * 2560, 512)
            d0 = pl.multiple_of(src_core * TAIL, 64)
            pltpu.make_async_copy(src.at[LAYERS - 1, pl.ds(r0, TAIL), cols], w_ref.at[n, pl.ds(d0, TAIL), :], wsem.at[n]).start()

    def store(n, m):
        rows, cols = pl.ds(m * 512, 512), pl.ds(n * 512, 512)
        return pltpu.make_async_copy(y_ref.at[rows, cols], out.at[rows, cols], osem.at[n, m])

    for n in range(4):
        cols = pl.ds(n * 512, 512)
        pltpu.make_async_copy(w_ref.at[n], w_ref.at[n], wsem.at[n]).wait()
        for m in range(2):
            rows = pl.ds(m * 512, 512)
            y_ref[rows, cols] = x_ref[rows, cols] + jnp.dot(a_ref[rows, pl.ds(c0, REST_K)], w_ref[n], preferred_element_type=F32)
            store(n, m).start()
    for n in range(4):
        for m in range(2):
            store(n, m).wait()


def run_layers(tokens, seg_ids, g_attn, g_mlp, weights):
    shapes = [jax.ShapeDtypeStruct(w.shape, w.dtype) for w in weights]
    half_dim = HEAD // 2
    freq = np.float32(ROPE_BASE) ** (-np.arange(half_dim, dtype=np.float32) / np.float32(half_dim))
    freq = jnp.asarray(np.concatenate([freq, freq]).reshape(1, HEAD))
    sem = pltpu.SemaphoreType.DMA((SLOTS, 2))
    item_sem = pltpu.SemaphoreType.DMA((ITEM_SLOTS,))
    any_spec = pl.BlockSpec(memory_space=pl.ANY)
    vmem_spec = pl.BlockSpec(memory_space=pltpu.VMEM)
    outs = pl.pallas_call(
        layer_kernel,
        out_shape=[pltpu.VMEM((TOK, D), F32), pltpu.VMEM((TOK, FF), BF16)] + shapes * 3,
        in_specs=[any_spec] * 12,
        out_specs=[vmem_spec] * 2 + [any_spec] * 21,
        scratch_shapes=[
            pltpu.VMEM((TOK, D), BF16),
            pltpu.VMEM((TOK, D), BF16),
            pltpu.VMEM((TOK, 512), BF16),
            pltpu.VMEM((2, D, 512), BF16),
            pltpu.VMEM((2, 1024, D), BF16),
            pltpu.VMEM((TOK, HEAD), F32),
            pltpu.VMEM((TOK, HEAD), F32),
            pltpu.VMEM((TOK, HEAD), jnp.int32),
            pltpu.VMEM((2 * LAYERS, 1, D), F32),
            pltpu.VMEM((TOK // 128, 128), jnp.int32),
            pltpu.VMEM((1, HEAD), F32),
            pltpu.VMEM((LAYERS, D), BF16),
            pltpu.VMEM((LAYERS, D), BF16),
            pltpu.SemaphoreType.DMA((2,)),
            pltpu.SemaphoreType.DMA((2,)),
            pltpu.SemaphoreType.DMA((5,)),
        ] + [sem] * 2 + [item_sem] * 4 + [sem] * 2,
        compiler_params=pltpu.CompilerParams(collective_id=0, has_side_effects=True, vmem_limit_bytes=34 * 1000 * 1000),
        name="two_layers",
    )(tokens, seg_ids.reshape(TOK // 128, 128), freq, g_attn, g_mlp, *weights)
    hidden = pltpu.with_memory_space_constraint(outs[0], pltpu.VMEM)
    act = pltpu.with_memory_space_constraint(outs[1], pltpu.VMEM)
    return pl.pallas_call(
        result_kernel,
        out_shape=jax.ShapeDtypeStruct((TOK, D), F32),
        in_specs=[vmem_spec] * 2 + [any_spec] * 2,
        out_specs=any_spec,
        scratch_shapes=[
            pltpu.VMEM((TOK, D), F32),
            pltpu.VMEM((4, REST_K, 512), BF16),
            pltpu.SemaphoreType.DMA((4,)),
            pltpu.SemaphoreType.DMA((4, 2)),
        ],
        compiler_params=pltpu.CompilerParams(vmem_limit_bytes=24 * 1000 * 1000),
        name="result",
    )(hidden, act, outs[15], outs[22])


def solution(mesh):
    tok_spec = P(("rep", "fsdp"), None)
    seg_spec = P(("rep", "fsdp"))
    mat_spec = P(None, "fsdp", None)
    gain_spec = P(None, None)

    def per_device(tokens, seg_ids, w_q, w_k, w_v, w_o, w_gate, w_up, w_down, g_attn, g_mlp):
        return run_layers(tokens, seg_ids, g_attn, g_mlp, (w_q, w_k, w_v, w_o, w_gate, w_up, w_down))

    return jax.shard_map(per_device, mesh=mesh, in_specs=(tok_spec, seg_spec, mat_spec, mat_spec, mat_spec, mat_spec, mat_spec, mat_spec, mat_spec, gain_spec, gain_spec), out_specs=tok_spec, check_vma=False)
```

```python
import functools

import jax
import jax.numpy as jnp
import numpy as np
from jax import lax
from jax.experimental import pallas as pl
from jax.experimental.pallas import tpu as pltpu
from jax.sharding import PartitionSpec as P

D = 2048
FF = 11008
HEADS = 16
HEAD = 128
TOK = 1024
EPS = 1e-5
ROPE_BASE = 10000.0
MESH = pl.DeviceIdType.MESH
F32 = jnp.float32
BF16 = jnp.bfloat16

LAYERS = 2
SLOTS = 8
ITEM_SLOTS = 2 * SLOTS
AHEAD = 8
AHEAD0 = 5
ROWS = D // 4
FF_ROWS = FF // 4
TAIL = 192
NAMES = ("q", "k", "v", "o", "g", "u", "d")

N_Q = 4
N_GU = 21
N_D = 10
CH_Q = 1
CH_O = CH_Q + N_Q
CH_GU = CH_O + N_Q
CH_GL = CH_GU + N_GU
CH_D = CH_GL + 1
CH_DR = CH_D + N_D
PER_LAYER = CH_DR + 1
CHUNKS = LAYERS * PER_LAYER
ITEMS = 2 * CHUNKS

NEAR_AT = 6

N_GT = FF // 256
ST_Q = 1
ST_A = ST_Q + N_Q
ST_O = ST_A + HEADS
ST_G = ST_O + 4
ST_D = ST_G + N_GT
ST_NEAR = ST_D + 2 * NEAR_AT
ST_IDLE = ST_D + 2 * N_D
ST_FAR = ST_IDLE + 1
ST_REST = ST_FAR + 2
STEPS = ST_REST + 2
ALL_STEPS = LAYERS * STEPS - 2
START = (4, 1, 0)
FIRST = (8, 3, 1)
REST_K = 2 * TAIL
NEAR_K = 512 + REST_K

MB = 512
NB = 128
QB = 256


def layer_kernel(*refs):
    tok, seg, freq, g_attn, g_mlp = refs[:5]
    own = dict(zip(NAMES, refs[5:12]))
    x_ref, a_ref = refs[12:14]
    b1 = dict(zip(NAMES, refs[14:21]))
    b2 = dict(zip(NAMES, refs[21:28]))
    b3 = dict(zip(NAMES, refs[28:35]))
    (h_ref, q_ref, kv_ref, wbuf, dbuf, cos_ref, sin_ref, first_ref, gain_ref,
     seg_ref, freq_ref, ga_ref, gm_ref, wsem, dsem, iosem) = refs[35:51]
    s0s, s0r, s1s, s1r, s2s, s2r, s3s, s3r = refs[51:]
    sources = (own, b1, b2, b3)
    y = lax.axis_index("rep")
    d = lax.axis_index("fsdp")
    side = d // 2
    core = lax.rem(d, 2)
    x_dev = (y, lax.rem(d + 2, 4))
    y_dev = (1 - y, d)
    c_dev = (y, d + 1 - 2 * core)

    def rel(block):
        return 2 * lax.rem(block // 2 + side, 2) + lax.rem(block + core, 2)

    inputs = [pltpu.make_async_copy(src, dst, iosem.at[n]) for n, (src, dst) in enumerate(
        ((tok, q_ref), (seg, seg_ref), (freq, freq_ref), (g_attn, ga_ref), (g_mlp, gm_ref)))]
    for copy in inputs:
        copy.start()

    with jax.named_scope("barrier"):
        barrier = pltpu.get_barrier_semaphore()
        for dev in (x_dev, y_dev, c_dev):
            pl.semaphore_signal(barrier, inc=1, device_id=dev, device_id_type=MESH)
        pl.semaphore_wait(barrier, 3)

    def kinds(k):
        i = lax.rem(k, PER_LAYER)
        jq = pl.multiple_of((i - CH_Q) * 512, 512)
        jo = pl.multiple_of((i - CH_O) * 512, 512)
        jg = pl.multiple_of((i - CH_GU) * 512, 512)
        jd = core * TAIL + (i - CH_D) * 256
        jr = (1 - core) * 2560
        last = N_GU * 512
        kv = [("k", 0, ROWS, 0, 256), ("v", 0, ROWS, 0, 256)]
        gu = [("g", 0, ROWS, jg, 512), ("u", 0, ROWS, jg, 512)]
        gl = [("g", 0, ROWS, last, 256), ("u", 0, ROWS, last, 256)]

        def split_cols(name, c0):
            return [(name, 0, ROWS, c0, 256), (name, 0, ROWS, c0 + 256, 256)], [(name, 0, ROWS, c0, 512)]

        def split_rows(r0, nr):
            return [("d", r0, nr // 2, 0, D), ("d", r0 + nr // 2, nr // 2, 0, D)], [("d", r0, nr, 0, D)]

        return [
            (i == 0, kv, kv),
            ((i >= CH_Q) & (i < CH_O), *split_cols("q", jq)),
            ((i >= CH_O) & (i < CH_GU), *split_cols("o", jo)),
            ((i >= CH_GU) & (i < CH_GL), gu, gu),
            (i == CH_GL, gl, gl),
            ((i >= CH_D) & (i < CH_DR), *split_rows(jd, 256)),
            (i == CH_DR, *split_rows(jr, TAIL)),
        ]

    def for_chunk(k, fn):
        layer = k // PER_LAYER
        slot = lax.rem(k, SLOTS)
        for cond, _, whole in kinds(k):
            @pl.when((k < CHUNKS) & cond)
            def _():
                for n, piece in enumerate(whole):
                    fn(False, layer, piece, (slot, n))

    def for_pair(k, fn):
        layer = k // PER_LAYER
        table = kinds(k)
        for c, (cond, pieces, _) in enumerate(table):
            for end in ((False, True) if c == len(table) - 1 else (None,)):
                here = cond if end is None else cond & ((k == CHUNKS - 1) if end else (k < CHUNKS - 1))

                @pl.when((k < CHUNKS) & here)
                def _():
                    for n, piece in enumerate(pieces):
                        fn(bool(end) and n == 1, layer, piece, (lax.rem(2 * k + n, ITEM_SLOTS),))

    def for_item(m, fn):
        k = m // 2
        n = lax.rem(m, 2)
        layer = k // PER_LAYER
        slot = (lax.rem(m, ITEM_SLOTS),)
        for cond, (one, two), _ in kinds(k):
            if one[0] == two[0]:
                name, r0, nr, c0, nc = one
                r0 = r0 + n * (nr if nc == D else 0)
                c0 = c0 + n * (0 if nc == D else nc) if nc == D else pl.multiple_of(c0 + n * nc, 256)
                piece = (name, r0, nr, c0 if nc != D else 0, nc)

                @pl.when((m < ITEMS - 1) & cond)
                def _():
                    fn(False, layer, piece, slot)
                if nc == D and nr == TAIL // 2:
                    @pl.when((m == ITEMS - 1) & cond)
                    def _():
                        fn(True, layer, piece, slot)
            else:
                for which, piece in enumerate((one, two)):
                    @pl.when((m < ITEMS) & cond & (n == which))
                    def _():
                        fn(False, layer, piece, slot)

    def view(bufs, name, layer, r0, nr, c0, nc, half):
        if half:
            nr = nr // 2
            r0 = r0 + y * nr
        r0 = pl.multiple_of(r0, 16)
        return bufs[name].at[layer, pl.ds(r0, nr), pl.ds(c0, nc)]

    def remote(src, dst, ss, rs, dev, half):
        def make(whole, layer, piece, slot):
            part = half and not whole
            return pltpu.make_async_remote_copy(
                src_ref=view(src, piece[0], layer, *piece[1:], part),
                dst_ref=view(dst, piece[0], layer, *piece[1:], part),
                send_sem=ss.at[slot], recv_sem=rs.at[slot], device_id=dev, device_id_type=MESH)
        return make

    copy0 = remote(own, b1, s0s, s0r, c_dev, False)
    copy1 = remote(own, b2, s1s, s1r, x_dev, True)
    copy2 = remote(b2, b2, s2s, s2r, y_dev, True)
    copy3 = remote(b2, b3, s3s, s3r, c_dev, False)

    def start0(*a):
        copy0(*a).start()

    def start1(*a):
        copy1(*a).start()

    def wait0(*a):
        copy0(*a).wait_recv()

    def relay2(*a):
        copy1(*a).wait_recv()
        if not a[0]:
            copy2(*a).start()

    def arrived(*a):
        if not a[0]:
            copy2(*a).wait_recv()
        copy1(*a).wait_send()

    def relay3(*a):
        copy3(*a).start()
        copy0(*a).wait_send()

    def finish(*a):
        copy3(*a).wait_recv()
        copy3(*a).wait_send()

    def sent(*a):
        if not a[0]:
            copy2(*a).wait_send()

    def targets(s):
        i = lax.rem(s, STEPS)
        layer = s // STEPS
        first = layer == 0
        heads = jnp.where(first, 19 + 3 * (i - ST_A) // 5, jnp.minimum(11 + i, 18 + 3 * (i - ST_A - 2) // 5))
        t2 = jnp.where(i < ST_A, jnp.where(first, 10, 6) + 2 * i,
             jnp.where(i < ST_D, jnp.maximum(i + 2, heads),
             jnp.where(i < ST_NEAR, jnp.maximum(i, ST_D + 1),
             jnp.where(i < ST_IDLE, ST_NEAR - 1 + (i - ST_NEAR + 1) // 2, i - 4))))
        t3 = jnp.where(i < ST_D, (t2 - 3) // 2,
             jnp.where(i < ST_NEAR + 3, (t2 - 2) // 2, jnp.where(i < ST_IDLE - 1, CH_DR - 1, CH_DR + (i - ST_IDLE + 1) // 2)))
        end = s >= ALL_STEPS - 2
        t2 = jnp.minimum(t2 + layer * 2 * PER_LAYER, jnp.where(end, ITEMS, ITEMS - 1))
        t3 = jnp.minimum(t3 + layer * PER_LAYER, jnp.where(end, CHUNKS, CHUNKS - 1))
        nxt = jnp.minimum(s + 1, ALL_STEPS - 1)
        i = lax.rem(nxt, STEPS)
        done = jnp.where(i < ST_A, 1 + i,
               jnp.where(i < ST_O, ST_A,
               jnp.where(i < ST_G, 1 + CH_O + i - ST_O,
               jnp.where(i < ST_D, 1 + CH_GU + (i - ST_G) // 2,
               jnp.where(i < ST_NEAR, 1 + CH_D + (i - ST_D) // 2,
               jnp.where(i < ST_IDLE, CH_D + (i - ST_D) // 2,
               jnp.where(i < ST_FAR, CH_DR - 1,
               jnp.where(i < ST_REST, CH_DR, PER_LAYER))))))))
        tf = jnp.maximum(t3 - 2, done + nxt // STEPS * PER_LAYER)
        t3 = jnp.maximum(t3, tf)
        return jnp.maximum(t2, 2 * t3), t3, tf

    def relays(old, new):
        @pl.loop(old[0], new[0])
        def _(m):
            with jax.named_scope("r2"):
                for_item(m, relay2)
                for_item(m + AHEAD, start1)
                n = lax.rem(m, 2)
                for_chunk(m // 2 + jnp.where(n == 0, AHEAD0, CHUNKS), start0)
                for_chunk(m // 2 + jnp.where(n == 0, CHUNKS, AHEAD0 - 1), wait0)

        @pl.loop(old[1], new[1])
        def _(k):
            with jax.named_scope("r3"):
                for_pair(k, arrived)
                for_chunk(k, relay3)

        @pl.loop(old[2], new[2])
        def _(k):
            with jax.named_scope("fin"):
                for_chunk(k, finish)
                for_pair(k, sent)

    def down_step(i):
        late = i >= ST_FAR
        n = jnp.where(late, i - ST_D - 1, i - ST_D)
        j = n // 2
        near = (i >= ST_NEAR) & (i < ST_NEAR + 2)
        far = late & (i < ST_REST)
        rest = i >= ST_REST
        whole = (i >= ST_D) & (i < ST_IDLE) & ~near
        return j, jnp.where(i > ST_NEAR, j - 1, j), lax.rem(n + 2 * STEPS, 2), whole, near, far, rest

    def rest_col(side_no):
        return pl.multiple_of(side_no * (2 * FF_ROWS) + 2560, HEAD)

    def tile_col(side_no, core_no, tile):
        return pl.multiple_of(side_no * (2 * FF_ROWS) + core_no * (FF_ROWS + TAIL) + tile * 256, HEAD)

    def load_tile(s):
        layer = s // STEPS
        i = lax.rem(s, STEPS)
        slot = lax.rem(s, 2)

        def cols(name, c0, nc, w0):
            for r, src in enumerate(sources):
                pltpu.make_async_copy(src[name].at[layer, :, pl.ds(c0, nc)],
                                      wbuf.at[slot, pl.ds(r * ROWS, ROWS), pl.ds(w0, nc)], wsem.at[slot]).start()

        @pl.when(i == 0)
        def _():
            cols("k", 0, 256, 0)
            cols("v", 0, 256, 256)

        @pl.when((i >= ST_Q) & (i < ST_A))
        def _():
            cols("q", pl.multiple_of((i - ST_Q) * 512, 512), 512, 0)

        @pl.when((i >= ST_O) & (i < ST_G))
        def _():
            cols("o", pl.multiple_of((i - ST_O) * 512, 512), 512, 0)

        @pl.when((i >= ST_G) & (i < ST_D))
        def _():
            c0 = pl.multiple_of((i - ST_G) * 256, 256)
            cols("g", c0, 256, 0)
            cols("u", c0, 256, 256)

        j, tile, half, whole, near, far, rest = down_step(i)
        dslot = lax.rem(j + 2 * STEPS, 2)

        def rows_in(src, r0, nr, w0):
            pltpu.make_async_copy(src["d"].at[layer, pl.ds(r0, nr), :], dbuf.at[dslot, pl.ds(w0, nr), :], dsem.at[dslot]).start()

        def chunk_rows(r, tile_no, w0):
            src_core = core if r % 2 == 0 else 1 - core
            rows_in(sources[r], pl.multiple_of(src_core * TAIL + tile_no * 256, 64), 256, w0)

        def rest_rows(r, w0):
            src_core = core if r % 2 == 0 else 1 - core
            rows_in(sources[r], pl.multiple_of((1 - src_core) * 2560, 512), TAIL, pl.multiple_of(w0 + src_core * TAIL, 64))

        @pl.when(whole & (half == 0))
        def _():
            for r in range(4):
                chunk_rows(r, tile, r * 256)

        @pl.when(near & (half == 0))
        def _():
            for r in range(2):
                chunk_rows(r, N_D - 1, r * 256)
                rest_rows(r, 512)

        @pl.when(far & (half == 0))
        def _():
            for r in range(2):
                chunk_rows(2 + r, N_D - 1, r * 256)

        @pl.when(rest & (half == 0))
        def _():
            for r in range(2):
                rest_rows(2 + r, 0)

    def norm(layer, which):
        @pl.loop(0, TOK // NB)
        def _(m):
            rows = pl.ds(pl.multiple_of(m * NB, NB), NB)
            total = jnp.zeros((NB, 1), F32)
            for b in range(4):
                blk = x_ref[rows, pl.ds(b * ROWS, ROWS)]
                total = total + jnp.sum(blk * blk, axis=1, keepdims=True)
            inv = lax.rsqrt(total * (1.0 / D) + EPS)
            for b in range(4):
                blk = x_ref[rows, pl.ds(b * ROWS, ROWS)]
                gain = gain_ref[which * LAYERS + layer, :, pl.ds(b * ROWS, ROWS)]
                c0 = pl.multiple_of(rel(b) * ROWS, ROWS)
                h_ref[rows, pl.ds(c0, ROWS)] = (blk * inv * gain).astype(BF16)

    def rotate(vals, rows):
        vals = vals.astype(BF16).astype(F32)
        turned = pltpu.roll(vals, HEAD // 2, 1)
        return (vals * cos_ref[rows, :] + turned * sin_ref[rows, :]).astype(BF16)

    def tile_product(slot, finish_rows):
        @pl.loop(0, TOK // MB)
        def _(m):
            rows = pl.ds(pl.multiple_of(m * MB, MB), MB)
            finish_rows(rows, jnp.dot(h_ref[rows, :], wbuf[slot], preferred_element_type=F32))

    def kv_step(slot):
        def fin(rows, acc):
            for b in range(2):
                kv_ref[rows, pl.ds(b * HEAD, HEAD)] = rotate(acc[:, b * HEAD:(b + 1) * HEAD], rows)
            kv_ref[rows, pl.ds(256, 256)] = acc[:, 256:].astype(BF16)
        tile_product(slot, fin)

    def q_step(slot, j):
        def fin(rows, acc):
            for b in range(4):
                c0 = pl.multiple_of(j * 512 + b * HEAD, HEAD)
                q_ref[rows, pl.ds(c0, HEAD)] = rotate(acc[:, b * HEAD:(b + 1) * HEAD], rows)
        tile_product(slot, fin)

    def o_step(slot, j):
        def fin(rows, acc):
            c0 = pl.ds(pl.multiple_of(j * 512, 512), 512)
            x_ref[rows, c0] = x_ref[rows, c0] + acc
        tile_product(slot, fin)

    def g_step(slot, j):
        def fin(rows, acc):
            gate = acc[:, :256]
            up = acc[:, 256:]
            c0 = pl.multiple_of(j * 256, 256)
            a_ref[rows, pl.ds(c0, 256)] = (gate * jax.nn.sigmoid(gate) * up).astype(BF16)
        tile_product(slot, fin)

    def attend(head):
        kv = head // 8
        q0 = pl.multiple_of(head * HEAD, HEAD)
        k0 = pl.multiple_of(kv * HEAD, HEAD)
        v0 = pl.multiple_of(256 + kv * HEAD, HEAD)
        o0 = pl.multiple_of(rel(head // 4) * ROWS + lax.rem(head, 4) * HEAD, HEAD)
        scale = HEAD ** -0.5
        for b in range(TOK // QB):
            keys = (b + 1) * QB
            rows = pl.ds(b * QB, QB)
            scores = lax.dot_general(q_ref[rows, pl.ds(q0, HEAD)], kv_ref[pl.ds(0, keys), pl.ds(k0, HEAD)],
                                     (((1,), (1,)), ((), ())), preferred_element_type=F32)
            key_idx = lax.broadcasted_iota(jnp.int32, (QB, keys), 1)
            row_idx = lax.broadcasted_iota(jnp.int32, (QB, keys), 0) + b * QB
            first = jnp.concatenate([first_ref[rows, :]] * (keys // HEAD), axis=1)
            ok = (key_idx >= first) & (key_idx <= row_idx)
            scores = jnp.where(ok, scores, -1e30)
            top = jnp.max(scores, axis=1, keepdims=True)
            probs = jnp.exp((scores - top) * scale)
            inv = 1.0 / jnp.sum(probs, axis=1, keepdims=True)
            probs = (probs * inv).astype(BF16)
            mixed = jnp.dot(probs, kv_ref[pl.ds(0, keys), pl.ds(v0, HEAD)], preferred_element_type=F32)
            h_ref[rows, pl.ds(o0, HEAD)] = mixed.astype(BF16)

    def add_product(dslot, half, cols):
        rows = pl.ds(pl.multiple_of(half * MB, MB), MB)
        depth = sum(width for _, width in cols)
        lhs = jnp.concatenate([a_ref[rows, pl.ds(c0, width)] for c0, width in cols], axis=1)
        x_ref[rows, :] = x_ref[rows, :] + jnp.dot(lhs, dbuf[dslot, pl.ds(0, depth), :], preferred_element_type=F32)

    def wait_d(dslot, half, depth):
        @pl.when(half == 0)
        def _():
            part = dbuf.at[dslot, pl.ds(0, depth), :]
            pltpu.make_async_copy(part, part, dsem.at[dslot]).wait()

    def last_cols(side_no):
        return [(tile_col(side_no, core, N_D - 1), 256), (tile_col(side_no, 1 - core, N_D - 1), 256)]

    def wait_w(slot):
        pltpu.make_async_copy(wbuf.at[slot], wbuf.at[slot], wsem.at[slot]).wait()

    def step(s):
        before = [jnp.where(s == 0, one, two) for one, two in zip(FIRST, targets(s - 1))]
        relays(before, targets(s))

        @pl.when(s + 1 < ALL_STEPS)
        def _():
            load_tile(s + 1)

        with jax.named_scope("comp"):
            compute(s)

    def compute(s):
        layer = s // STEPS
        i = lax.rem(s, STEPS)
        slot = lax.rem(s, 2)

        @pl.when((i == 0) | (i == ST_G))
        def _():
            norm(layer, jnp.where(i == 0, 0, 1))

        @pl.when((i < ST_A) | ((i >= ST_O) & (i < ST_D)))
        def _():
            wait_w(slot)

        @pl.when(i == 0)
        def _():
            kv_step(slot)

        @pl.when((i >= ST_Q) & (i < ST_A))
        def _():
            q_step(slot, i - ST_Q)

        @pl.when((i >= ST_A) & (i < ST_O))
        def _():
            attend(i - ST_A)

        @pl.when((i >= ST_O) & (i < ST_G))
        def _():
            o_step(slot, i - ST_O)

        @pl.when((i >= ST_G) & (i < ST_D))
        def _():
            g_step(slot, i - ST_G)

        j, tile, half, whole, near, far, rest = down_step(i)
        dslot = lax.rem(j + 2 * STEPS, 2)

        @pl.when(whole)
        def _():
            wait_d(dslot, half, 1024)
            add_product(dslot, half, [(tile_col(lax.rem(side + r // 2, 2), lax.rem(core + r, 2), tile), 256) for r in range(4)])

        @pl.when(near)
        def _():
            wait_d(dslot, half, NEAR_K)
            add_product(dslot, half, last_cols(side) + [(rest_col(side), REST_K)])

        @pl.when(far)
        def _():
            wait_d(dslot, half, 512)
            add_product(dslot, half, last_cols(1 - side))

        @pl.when(rest)
        def _():
            wait_d(dslot, half, REST_K)
            add_product(dslot, half, [(rest_col(1 - side), REST_K)])

    @pl.loop(0, AHEAD)
    def _(m):
        for_item(m, start1)

    @pl.loop(0, AHEAD0)
    def _(k):
        for_chunk(k, start0)

    for copy in inputs:
        copy.wait()

    for n, ref in enumerate((ga_ref, gm_ref)):
        for layer in range(LAYERS):
            gain_ref[n * LAYERS + layer] = ref[pl.ds(layer, 1), :].astype(F32)
    ids = seg_ref[...].astype(F32)
    lane = lax.broadcasted_iota(jnp.int32, (128, HEAD), 1)
    for b in range(TOK // 128):
        rows = pl.ds(b * 128, 128)
        mine = jnp.transpose(jnp.broadcast_to(ids[b:b + 1, :], (128, 128)))
        before = jnp.zeros((128, 128), F32)
        for c in range(TOK // 128):
            before = before + jnp.where(ids[c:c + 1, :] < mine, 1.0, 0.0)
        first = jnp.sum(before, axis=1, keepdims=True)
        pos = lax.broadcasted_iota(jnp.int32, (128, 128), 0).astype(F32) + (b * 128.0) - first
        angles = pos * freq_ref[...]
        cos_ref[rows, :] = jnp.cos(angles)
        sin = jnp.sin(angles)
        sin_ref[rows, :] = jnp.where(lane < HEAD // 2, -sin, sin)
        first_ref[rows, :] = jnp.broadcast_to(first, (128, 128)).astype(jnp.int32)

    @pl.loop(0, TOK // NB)
    def _(m):
        rows = pl.ds(pl.multiple_of(m * NB, NB), NB)
        x_ref[rows, :] = q_ref[rows, :].astype(F32)

    @pl.loop(0, AHEAD0 - 1)
    def _(k):
        for_chunk(k, wait0)

    relays((0, 0, 0), START)
    relays(START, FIRST)
    load_tile(0)

    @pl.loop(0, ALL_STEPS)
    def _(s):
        with jax.named_scope("step"):
            step(s)

    relays(targets(ALL_STEPS - 1), (ITEMS, CHUNKS, CHUNKS))


def result_kernel(x_ref, a_ref, w2_hbm, w3_hbm, out, y_ref, w_ref, wsem, osem):
    d = lax.axis_index("fsdp")
    core = lax.rem(d, 2)
    c0 = pl.multiple_of((1 - d // 2) * (2 * FF_ROWS) + 2560, HEAD)
    for n in range(4):
        cols = pl.ds(n * 512, 512)
        for src, src_core in ((w2_hbm, core), (w3_hbm, 1 - core)):
            r0 = pl.multiple_of((1 - src_core) * 2560, 512)
            d0 = pl.multiple_of(src_core * TAIL, 64)
            pltpu.make_async_copy(src.at[LAYERS - 1, pl.ds(r0, TAIL), cols], w_ref.at[n, pl.ds(d0, TAIL), :], wsem.at[n]).start()

    def store(n, m):
        rows, cols = pl.ds(m * 512, 512), pl.ds(n * 512, 512)
        return pltpu.make_async_copy(y_ref.at[rows, cols], out.at[rows, cols], osem.at[n, m])

    for n in range(4):
        cols = pl.ds(n * 512, 512)
        pltpu.make_async_copy(w_ref.at[n], w_ref.at[n], wsem.at[n]).wait()
        for m in range(2):
            rows = pl.ds(m * 512, 512)
            y_ref[rows, cols] = x_ref[rows, cols] + jnp.dot(a_ref[rows, pl.ds(c0, REST_K)], w_ref[n], preferred_element_type=F32)
            store(n, m).start()
    for n in range(4):
        for m in range(2):
            store(n, m).wait()


def run_layers(tokens, seg_ids, g_attn, g_mlp, weights):
    shapes = [jax.ShapeDtypeStruct(w.shape, w.dtype) for w in weights]
    half_dim = HEAD // 2
    freq = np.float32(ROPE_BASE) ** (-np.arange(half_dim, dtype=np.float32) / np.float32(half_dim))
    freq = jnp.asarray(np.concatenate([freq, freq]).reshape(1, HEAD))
    sem = pltpu.SemaphoreType.DMA((SLOTS, 2))
    item_sem = pltpu.SemaphoreType.DMA((ITEM_SLOTS,))
    any_spec = pl.BlockSpec(memory_space=pl.ANY)
    vmem_spec = pl.BlockSpec(memory_space=pltpu.VMEM)
    outs = pl.pallas_call(
        layer_kernel,
        out_shape=[pltpu.VMEM((TOK, D), F32), pltpu.VMEM((TOK, FF), BF16)] + shapes * 3,
        in_specs=[any_spec] * 12,
        out_specs=[vmem_spec] * 2 + [any_spec] * 21,
        scratch_shapes=[
            pltpu.VMEM((TOK, D), BF16),
            pltpu.VMEM((TOK, D), BF16),
            pltpu.VMEM((TOK, 512), BF16),
            pltpu.VMEM((2, D, 512), BF16),
            pltpu.VMEM((2, 1024, D), BF16),
            pltpu.VMEM((TOK, HEAD), F32),
            pltpu.VMEM((TOK, HEAD), F32),
            pltpu.VMEM((TOK, HEAD), jnp.int32),
            pltpu.VMEM((2 * LAYERS, 1, D), F32),
            pltpu.VMEM((TOK // 128, 128), jnp.int32),
            pltpu.VMEM((1, HEAD), F32),
            pltpu.VMEM((LAYERS, D), BF16),
            pltpu.VMEM((LAYERS, D), BF16),
            pltpu.SemaphoreType.DMA((2,)),
            pltpu.SemaphoreType.DMA((2,)),
            pltpu.SemaphoreType.DMA((5,)),
        ] + [sem] * 2 + [item_sem] * 4 + [sem] * 2,
        compiler_params=pltpu.CompilerParams(collective_id=0, has_side_effects=True, vmem_limit_bytes=34 * 1000 * 1000),
        name="two_layers",
    )(tokens, seg_ids.reshape(TOK // 128, 128), freq, g_attn, g_mlp, *weights)
    hidden = pltpu.with_memory_space_constraint(outs[0], pltpu.VMEM)
    act = pltpu.with_memory_space_constraint(outs[1], pltpu.VMEM)
    return pl.pallas_call(
        result_kernel,
        out_shape=jax.ShapeDtypeStruct((TOK, D), F32),
        in_specs=[vmem_spec] * 2 + [any_spec] * 2,
        out_specs=any_spec,
        scratch_shapes=[
            pltpu.VMEM((TOK, D), F32),
            pltpu.VMEM((4, REST_K, 512), BF16),
            pltpu.SemaphoreType.DMA((4,)),
            pltpu.SemaphoreType.DMA((4, 2)),
        ],
        compiler_params=pltpu.CompilerParams(vmem_limit_bytes=24 * 1000 * 1000),
        name="result",
    )(hidden, act, outs[15], outs[22])


def solution(mesh):
    tok_spec = P(("rep", "fsdp"), None)
    seg_spec = P(("rep", "fsdp"))
    mat_spec = P(None, "fsdp", None)
    gain_spec = P(None, None)

    def per_device(tokens, seg_ids, w_q, w_k, w_v, w_o, w_gate, w_up, w_down, g_attn, g_mlp):
        return run_layers(tokens, seg_ids, g_attn, g_mlp, (w_q, w_k, w_v, w_o, w_gate, w_up, w_down))

    return jax.shard_map(per_device, mesh=mesh, in_specs=(tok_spec, seg_spec, mat_spec, mat_spec, mat_spec, mat_spec, mat_spec, mat_spec, mat_spec, gain_spec, gain_spec), out_specs=tok_spec, check_vma=False)
```

```python
import functools

import jax
import jax.numpy as jnp
import numpy as np
from jax import lax
from jax.experimental import pallas as pl
from jax.experimental.pallas import tpu as pltpu
from jax.sharding import PartitionSpec as P

D = 2048
FF = 11008
HEADS = 16
HEAD = 128
TOK = 1024
EPS = 1e-5
ROPE_BASE = 10000.0
MESH = pl.DeviceIdType.MESH
F32 = jnp.float32
BF16 = jnp.bfloat16

LAYERS = 2
SLOTS = 8
ITEM_SLOTS = 2 * SLOTS
AHEAD = 8
AHEAD0 = 5
ROWS = D // 4
FF_ROWS = FF // 4
TAIL = 192
NAMES = ("q", "k", "v", "o", "g", "u", "d")

N_Q = 4
N_GU = 21
N_D = 10
CH_Q = 1
CH_O = CH_Q + N_Q
CH_GU = CH_O + N_Q
CH_GL = CH_GU + N_GU
CH_D = CH_GL + 1
CH_DR = CH_D + N_D
PER_LAYER = CH_DR + 1
CHUNKS = LAYERS * PER_LAYER
ITEMS = 2 * CHUNKS

NEAR_AT = 6

N_GT = FF // 256
ST_Q = 1
ST_A = ST_Q + N_Q
ST_O = ST_A + HEADS
ST_G = ST_O + 4
ST_D = ST_G + N_GT
ST_NEAR = ST_D + 2 * NEAR_AT
ST_IDLE = ST_D + 2 * N_D
ST_FAR = ST_IDLE + 1
ST_REST = ST_FAR + 2
STEPS = ST_REST + 2
ALL_STEPS = LAYERS * STEPS - 2
START = (4, 1, 0)
FIRST = (8, 3, 1)
REST_K = 2 * TAIL
NEAR_K = 512 + REST_K

MB = 512
NB = 128
QB = 256


def layer_kernel(*refs):
    tok, seg, freq, g_attn, g_mlp = refs[:5]
    own = dict(zip(NAMES, refs[5:12]))
    x_ref, a_ref = refs[12:14]
    b1 = dict(zip(NAMES, refs[14:21]))
    b2 = dict(zip(NAMES, refs[21:28]))
    b3 = dict(zip(NAMES, refs[28:35]))
    (h_ref, q_ref, kv_ref, wbuf, dbuf, cos_ref, sin_ref, first_ref, gain_ref,
     seg_ref, freq_ref, ga_ref, gm_ref, wsem, dsem, iosem) = refs[35:51]
    s0s, s0r, s1s, s1r, s2s, s2r, s3s, s3r = refs[51:]
    sources = (own, b1, b2, b3)
    y = lax.axis_index("rep")
    d = lax.axis_index("fsdp")
    side = d // 2
    core = lax.rem(d, 2)
    x_dev = (y, lax.rem(d + 2, 4))
    y_dev = (1 - y, d)
    c_dev = (y, d + 1 - 2 * core)

    def rel(block):
        return 2 * lax.rem(block // 2 + side, 2) + lax.rem(block + core, 2)

    inputs = [pltpu.make_async_copy(src, dst, iosem.at[n]) for n, (src, dst) in enumerate(
        ((tok, q_ref), (seg, seg_ref), (freq, freq_ref), (g_attn, ga_ref), (g_mlp, gm_ref)))]
    for copy in inputs:
        copy.start()

    with jax.named_scope("barrier"):
        barrier = pltpu.get_barrier_semaphore()
        for dev in (x_dev, y_dev, c_dev):
            pl.semaphore_signal(barrier, inc=1, device_id=dev, device_id_type=MESH)
        pl.semaphore_wait(barrier, 3)

    def kinds(k):
        i = lax.rem(k, PER_LAYER)
        jq = pl.multiple_of((i - CH_Q) * 512, 512)
        jo = pl.multiple_of((i - CH_O) * 512, 512)
        jg = pl.multiple_of((i - CH_GU) * 512, 512)
        jd = core * TAIL + (i - CH_D) * 256
        jr = (1 - core) * 2560
        last = N_GU * 512
        kv = [("k", 0, ROWS, 0, 256), ("v", 0, ROWS, 0, 256)]
        gu = [("g", 0, ROWS, jg, 512), ("u", 0, ROWS, jg, 512)]
        gl = [("g", 0, ROWS, last, 256), ("u", 0, ROWS, last, 256)]

        def split_cols(name, c0):
            return [(name, 0, ROWS, c0, 256), (name, 0, ROWS, c0 + 256, 256)], [(name, 0, ROWS, c0, 512)]

        def split_rows(r0, nr):
            return [("d", r0, nr // 2, 0, D), ("d", r0 + nr // 2, nr // 2, 0, D)], [("d", r0, nr, 0, D)]

        return [
            (i == 0, kv, kv),
            ((i >= CH_Q) & (i < CH_O), *split_cols("q", jq)),
            ((i >= CH_O) & (i < CH_GU), *split_cols("o", jo)),
            ((i >= CH_GU) & (i < CH_GL), gu, gu),
            (i == CH_GL, gl, gl),
            ((i >= CH_D) & (i < CH_DR), *split_rows(jd, 256)),
            (i == CH_DR, *split_rows(jr, TAIL)),
        ]

    def for_chunk(k, fn):
        layer = k // PER_LAYER
        slot = lax.rem(k, SLOTS)
        for cond, _, whole in kinds(k):
            @pl.when((k < CHUNKS) & cond)
            def _():
                for n, piece in enumerate(whole):
                    fn(False, layer, piece, (slot, n))

    def for_pair(k, fn):
        layer = k // PER_LAYER
        table = kinds(k)
        for c, (cond, pieces, _) in enumerate(table):
            for end in ((False, True) if c == len(table) - 1 else (None,)):
                here = cond if end is None else cond & ((k == CHUNKS - 1) if end else (k < CHUNKS - 1))

                @pl.when((k < CHUNKS) & here)
                def _():
                    for n, piece in enumerate(pieces):
                        fn(bool(end) and n == 1, layer, piece, (lax.rem(2 * k + n, ITEM_SLOTS),))

    def for_item(m, fn):
        k = m // 2
        n = lax.rem(m, 2)
        layer = k // PER_LAYER
        slot = (lax.rem(m, ITEM_SLOTS),)
        for cond, (one, two), _ in kinds(k):
            if one[0] == two[0]:
                name, r0, nr, c0, nc = one
                r0 = r0 + n * (nr if nc == D else 0)
                c0 = c0 + n * (0 if nc == D else nc) if nc == D else pl.multiple_of(c0 + n * nc, 256)
                piece = (name, r0, nr, c0 if nc != D else 0, nc)

                @pl.when((m < ITEMS - 1) & cond)
                def _():
                    fn(False, layer, piece, slot)
                if nc == D and nr == TAIL // 2:
                    @pl.when((m == ITEMS - 1) & cond)
                    def _():
                        fn(True, layer, piece, slot)
            else:
                for which, piece in enumerate((one, two)):
                    @pl.when((m < ITEMS) & cond & (n == which))
                    def _():
                        fn(False, layer, piece, slot)

    def view(bufs, name, layer, r0, nr, c0, nc, half):
        if half:
            nr = nr // 2
            r0 = r0 + y * nr
        r0 = pl.multiple_of(r0, 16)
        return bufs[name].at[layer, pl.ds(r0, nr), pl.ds(c0, nc)]

    def remote(src, dst, ss, rs, dev, half):
        def make(whole, layer, piece, slot):
            part = half and not whole
            return pltpu.make_async_remote_copy(
                src_ref=view(src, piece[0], layer, *piece[1:], part),
                dst_ref=view(dst, piece[0], layer, *piece[1:], part),
                send_sem=ss.at[slot], recv_sem=rs.at[slot], device_id=dev, device_id_type=MESH)
        return make

    copy0 = remote(own, b1, s0s, s0r, c_dev, False)
    copy1 = remote(own, b2, s1s, s1r, x_dev, True)
    copy2 = remote(b2, b2, s2s, s2r, y_dev, True)
    copy3 = remote(b2, b3, s3s, s3r, c_dev, False)

    def start0(*a):
        copy0(*a).start()

    def start1(*a):
        copy1(*a).start()

    def wait0(*a):
        copy0(*a).wait_recv()

    def relay2(*a):
        copy1(*a).wait_recv()
        if not a[0]:
            copy2(*a).start()

    def arrived(*a):
        if not a[0]:
            copy2(*a).wait_recv()
        copy1(*a).wait_send()

    def relay3(*a):
        copy3(*a).start()
        copy0(*a).wait_send()

    def finish(*a):
        copy3(*a).wait_recv()
        copy3(*a).wait_send()

    def sent(*a):
        if not a[0]:
            copy2(*a).wait_send()

    def targets(s):
        i = lax.rem(s, STEPS)
        layer = s // STEPS
        first = layer == 0
        tail = i - ST_NEAR
        t2 = jnp.where(i < ST_A, 10 + 2 * i,
             jnp.where(i < ST_D, jnp.maximum(i + 2, 19 + 3 * (i - ST_A) // 5),
             jnp.where(i < ST_NEAR, jnp.maximum(i, ST_D + 1),
             jnp.where(first, ST_NEAR + jnp.where(tail < 4, tail // 2, tail - 2),
             ST_NEAR + jnp.where(i < ST_IDLE, (tail + 1) // 2 - 1, tail - 4)))))
        t3 = jnp.where(i < ST_D, (t2 - 3) // 2,
             jnp.where(i < ST_NEAR + jnp.where(first, 6, 3), (t2 - 2) // 2,
             jnp.where(i < ST_IDLE - 1, CH_DR - 1, CH_DR + (i - ST_IDLE + 1) // 2)))
        end = s >= ALL_STEPS - 2
        t2 = jnp.minimum(t2 + layer * 2 * PER_LAYER, jnp.where(end, ITEMS, ITEMS - 1))
        t3 = jnp.minimum(t3 + layer * PER_LAYER, jnp.where(end, CHUNKS, CHUNKS - 1))
        nxt = jnp.minimum(s + 1, ALL_STEPS - 1)
        i = lax.rem(nxt, STEPS)
        done = jnp.where(i < ST_A, 1 + i,
               jnp.where(i < ST_O, ST_A,
               jnp.where(i < ST_G, 1 + CH_O + i - ST_O,
               jnp.where(i < ST_D, 1 + CH_GU + (i - ST_G) // 2,
               jnp.where(i < ST_NEAR, 1 + CH_D + (i - ST_D) // 2,
               jnp.where(i < ST_IDLE, CH_D + (i - ST_D) // 2,
               jnp.where(i < ST_FAR, CH_DR - 1,
               jnp.where(i < ST_REST, CH_DR, PER_LAYER))))))))
        tf = jnp.maximum(t3 - 2, done + nxt // STEPS * PER_LAYER)
        t3 = jnp.maximum(t3, tf)
        return jnp.maximum(t2, 2 * t3), t3, tf

    def relays(old, new):
        @pl.loop(old[0], new[0])
        def _(m):
            with jax.named_scope("r2"):
                for_item(m, relay2)
                for_item(m + AHEAD, start1)
                n = lax.rem(m, 2)
                for_chunk(m // 2 + jnp.where(n == 0, AHEAD0, CHUNKS), start0)
                for_chunk(m // 2 + jnp.where(n == 0, CHUNKS, AHEAD0 - 1), wait0)

        @pl.loop(old[1], new[1])
        def _(k):
            with jax.named_scope("r3"):
                for_pair(k, arrived)
                for_chunk(k, relay3)

        @pl.loop(old[2], new[2])
        def _(k):
            with jax.named_scope("fin"):
                for_chunk(k, finish)
                for_pair(k, sent)

    def down_step(i):
        late = i >= ST_FAR
        n = jnp.where(late, i - ST_D - 1, i - ST_D)
        j = n // 2
        near = (i >= ST_NEAR) & (i < ST_NEAR + 2)
        far = late & (i < ST_REST)
        rest = i >= ST_REST
        whole = (i >= ST_D) & (i < ST_IDLE) & ~near
        return j, jnp.where(i > ST_NEAR, j - 1, j), lax.rem(n + 2 * STEPS, 2), whole, near, far, rest

    def rest_col(side_no):
        return pl.multiple_of(side_no * (2 * FF_ROWS) + 2560, HEAD)

    def tile_col(side_no, core_no, tile):
        return pl.multiple_of(side_no * (2 * FF_ROWS) + core_no * (FF_ROWS + TAIL) + tile * 256, HEAD)

    def load_tile(s):
        layer = s // STEPS
        i = lax.rem(s, STEPS)
        slot = lax.rem(s, 2)

        def cols(name, c0, nc, w0):
            for r, src in enumerate(sources):
                pltpu.make_async_copy(src[name].at[layer, :, pl.ds(c0, nc)],
                                      wbuf.at[slot, pl.ds(r * ROWS, ROWS), pl.ds(w0, nc)], wsem.at[slot]).start()

        @pl.when(i == 0)
        def _():
            cols("k", 0, 256, 0)
            cols("v", 0, 256, 256)

        @pl.when((i >= ST_Q) & (i < ST_A))
        def _():
            cols("q", pl.multiple_of((i - ST_Q) * 512, 512), 512, 0)

        @pl.when((i >= ST_O) & (i < ST_G))
        def _():
            cols("o", pl.multiple_of((i - ST_O) * 512, 512), 512, 0)

        @pl.when((i >= ST_G) & (i < ST_D))
        def _():
            c0 = pl.multiple_of((i - ST_G) * 256, 256)
            cols("g", c0, 256, 0)
            cols("u", c0, 256, 256)

        j, tile, half, whole, near, far, rest = down_step(i)
        dslot = lax.rem(j + 2 * STEPS, 2)

        def rows_in(src, r0, nr, w0):
            pltpu.make_async_copy(src["d"].at[layer, pl.ds(r0, nr), :], dbuf.at[dslot, pl.ds(w0, nr), :], dsem.at[dslot]).start()

        def chunk_rows(r, tile_no, w0):
            src_core = core if r % 2 == 0 else 1 - core
            rows_in(sources[r], pl.multiple_of(src_core * TAIL + tile_no * 256, 64), 256, w0)

        def rest_rows(r, w0):
            src_core = core if r % 2 == 0 else 1 - core
            rows_in(sources[r], pl.multiple_of((1 - src_core) * 2560, 512), TAIL, pl.multiple_of(w0 + src_core * TAIL, 64))

        @pl.when(whole & (half == 0))
        def _():
            for r in range(4):
                chunk_rows(r, tile, r * 256)

        @pl.when(near & (half == 0))
        def _():
            for r in range(2):
                chunk_rows(r, N_D - 1, r * 256)
                rest_rows(r, 512)

        @pl.when(far & (half == 0))
        def _():
            for r in range(2):
                chunk_rows(2 + r, N_D - 1, r * 256)

        @pl.when(rest & (half == 0))
        def _():
            for r in range(2):
                rest_rows(2 + r, 0)

    def norm(layer, which):
        @pl.loop(0, TOK // NB)
        def _(m):
            rows = pl.ds(pl.multiple_of(m * NB, NB), NB)
            total = jnp.zeros((NB, 1), F32)
            for b in range(4):
                blk = x_ref[rows, pl.ds(b * ROWS, ROWS)]
                total = total + jnp.sum(blk * blk, axis=1, keepdims=True)
            inv = lax.rsqrt(total * (1.0 / D) + EPS)
            for b in range(4):
                blk = x_ref[rows, pl.ds(b * ROWS, ROWS)]
                gain = gain_ref[which * LAYERS + layer, :, pl.ds(b * ROWS, ROWS)]
                c0 = pl.multiple_of(rel(b) * ROWS, ROWS)
                h_ref[rows, pl.ds(c0, ROWS)] = (blk * inv * gain).astype(BF16)

    def rotate(vals, rows):
        vals = vals.astype(BF16).astype(F32)
        turned = pltpu.roll(vals, HEAD // 2, 1)
        return (vals * cos_ref[rows, :] + turned * sin_ref[rows, :]).astype(BF16)

    def tile_product(slot, finish_rows):
        @pl.loop(0, TOK // MB)
        def _(m):
            rows = pl.ds(pl.multiple_of(m * MB, MB), MB)
            finish_rows(rows, jnp.dot(h_ref[rows, :], wbuf[slot], preferred_element_type=F32))

    def kv_step(slot):
        def fin(rows, acc):
            for b in range(2):
                kv_ref[rows, pl.ds(b * HEAD, HEAD)] = rotate(acc[:, b * HEAD:(b + 1) * HEAD], rows)
            kv_ref[rows, pl.ds(256, 256)] = acc[:, 256:].astype(BF16)
        tile_product(slot, fin)

    def q_step(slot, j):
        def fin(rows, acc):
            for b in range(4):
                c0 = pl.multiple_of(j * 512 + b * HEAD, HEAD)
                q_ref[rows, pl.ds(c0, HEAD)] = rotate(acc[:, b * HEAD:(b + 1) * HEAD], rows)
        tile_product(slot, fin)

    def o_step(slot, j):
        def fin(rows, acc):
            c0 = pl.ds(pl.multiple_of(j * 512, 512), 512)
            x_ref[rows, c0] = x_ref[rows, c0] + acc
        tile_product(slot, fin)

    def g_step(slot, j):
        def fin(rows, acc):
            gate = acc[:, :256]
            up = acc[:, 256:]
            c0 = pl.multiple_of(j * 256, 256)
            a_ref[rows, pl.ds(c0, 256)] = (gate * jax.nn.sigmoid(gate) * up).astype(BF16)
        tile_product(slot, fin)

    def attend(head):
        kv = head // 8
        q0 = pl.multiple_of(head * HEAD, HEAD)
        k0 = pl.multiple_of(kv * HEAD, HEAD)
        v0 = pl.multiple_of(256 + kv * HEAD, HEAD)
        o0 = pl.multiple_of(rel(head // 4) * ROWS + lax.rem(head, 4) * HEAD, HEAD)
        scale = HEAD ** -0.5
        for b in range(TOK // QB):
            keys = (b + 1) * QB
            rows = pl.ds(b * QB, QB)
            scores = lax.dot_general(q_ref[rows, pl.ds(q0, HEAD)], kv_ref[pl.ds(0, keys), pl.ds(k0, HEAD)],
                                     (((1,), (1,)), ((), ())), preferred_element_type=F32)
            key_idx = lax.broadcasted_iota(jnp.int32, (QB, keys), 1)
            row_idx = lax.broadcasted_iota(jnp.int32, (QB, keys), 0) + b * QB
            first = jnp.concatenate([first_ref[rows, :]] * (keys // HEAD), axis=1)
            ok = (key_idx >= first) & (key_idx <= row_idx)
            scores = jnp.where(ok, scores, -1e30)
            top = jnp.max(scores, axis=1, keepdims=True)
            probs = jnp.exp((scores - top) * scale)
            inv = 1.0 / jnp.sum(probs, axis=1, keepdims=True)
            probs = (probs * inv).astype(BF16)
            mixed = jnp.dot(probs, kv_ref[pl.ds(0, keys), pl.ds(v0, HEAD)], preferred_element_type=F32)
            h_ref[rows, pl.ds(o0, HEAD)] = mixed.astype(BF16)

    def add_product(dslot, half, cols):
        rows = pl.ds(pl.multiple_of(half * MB, MB), MB)
        depth = sum(width for _, width in cols)
        lhs = jnp.concatenate([a_ref[rows, pl.ds(c0, width)] for c0, width in cols], axis=1)
        x_ref[rows, :] = x_ref[rows, :] + jnp.dot(lhs, dbuf[dslot, pl.ds(0, depth), :], preferred_element_type=F32)

    def wait_d(dslot, half, depth):
        @pl.when(half == 0)
        def _():
            part = dbuf.at[dslot, pl.ds(0, depth), :]
            pltpu.make_async_copy(part, part, dsem.at[dslot]).wait()

    def last_cols(side_no):
        return [(tile_col(side_no, core, N_D - 1), 256), (tile_col(side_no, 1 - core, N_D - 1), 256)]

    def wait_w(slot):
        pltpu.make_async_copy(wbuf.at[slot], wbuf.at[slot], wsem.at[slot]).wait()

    def step(s):
        before = [jnp.where(s == 0, one, two) for one, two in zip(FIRST, targets(s - 1))]
        relays(before, targets(s))

        @pl.when(s + 1 < ALL_STEPS)
        def _():
            load_tile(s + 1)

        with jax.named_scope("comp"):
            compute(s)

    def compute(s):
        layer = s // STEPS
        i = lax.rem(s, STEPS)
        slot = lax.rem(s, 2)

        @pl.when((i == 0) | (i == ST_G))
        def _():
            norm(layer, jnp.where(i == 0, 0, 1))

        @pl.when((i < ST_A) | ((i >= ST_O) & (i < ST_D)))
        def _():
            wait_w(slot)

        @pl.when(i == 0)
        def _():
            kv_step(slot)

        @pl.when((i >= ST_Q) & (i < ST_A))
        def _():
            q_step(slot, i - ST_Q)

        @pl.when((i >= ST_A) & (i < ST_O))
        def _():
            attend(i - ST_A)

        @pl.when((i >= ST_O) & (i < ST_G))
        def _():
            o_step(slot, i - ST_O)

        @pl.when((i >= ST_G) & (i < ST_D))
        def _():
            g_step(slot, i - ST_G)

        j, tile, half, whole, near, far, rest = down_step(i)
        dslot = lax.rem(j + 2 * STEPS, 2)

        @pl.when(whole)
        def _():
            wait_d(dslot, half, 1024)
            add_product(dslot, half, [(tile_col(lax.rem(side + r // 2, 2), lax.rem(core + r, 2), tile), 256) for r in range(4)])

        @pl.when(near)
        def _():
            wait_d(dslot, half, NEAR_K)
            add_product(dslot, half, last_cols(side) + [(rest_col(side), REST_K)])

        @pl.when(far)
        def _():
            wait_d(dslot, half, 512)
            add_product(dslot, half, last_cols(1 - side))

        @pl.when(rest)
        def _():
            wait_d(dslot, half, REST_K)
            add_product(dslot, half, [(rest_col(1 - side), REST_K)])

    @pl.loop(0, AHEAD)
    def _(m):
        for_item(m, start1)

    @pl.loop(0, AHEAD0)
    def _(k):
        for_chunk(k, start0)

    for copy in inputs:
        copy.wait()

    for n, ref in enumerate((ga_ref, gm_ref)):
        for layer in range(LAYERS):
            gain_ref[n * LAYERS + layer] = ref[pl.ds(layer, 1), :].astype(F32)
    ids = seg_ref[...].astype(F32)
    lane = lax.broadcasted_iota(jnp.int32, (128, HEAD), 1)
    for b in range(TOK // 128):
        rows = pl.ds(b * 128, 128)
        mine = jnp.transpose(jnp.broadcast_to(ids[b:b + 1, :], (128, 128)))
        before = jnp.zeros((128, 128), F32)
        for c in range(TOK // 128):
            before = before + jnp.where(ids[c:c + 1, :] < mine, 1.0, 0.0)
        first = jnp.sum(before, axis=1, keepdims=True)
        pos = lax.broadcasted_iota(jnp.int32, (128, 128), 0).astype(F32) + (b * 128.0) - first
        angles = pos * freq_ref[...]
        cos_ref[rows, :] = jnp.cos(angles)
        sin = jnp.sin(angles)
        sin_ref[rows, :] = jnp.where(lane < HEAD // 2, -sin, sin)
        first_ref[rows, :] = jnp.broadcast_to(first, (128, 128)).astype(jnp.int32)

    @pl.loop(0, TOK // NB)
    def _(m):
        rows = pl.ds(pl.multiple_of(m * NB, NB), NB)
        x_ref[rows, :] = q_ref[rows, :].astype(F32)

    @pl.loop(0, AHEAD0 - 1)
    def _(k):
        for_chunk(k, wait0)

    relays((0, 0, 0), START)
    relays(START, FIRST)
    load_tile(0)

    @pl.loop(0, ALL_STEPS)
    def _(s):
        with jax.named_scope("step"):
            step(s)

    relays(targets(ALL_STEPS - 1), (ITEMS, CHUNKS, CHUNKS))


def result_kernel(x_ref, a_ref, w2_hbm, w3_hbm, out, y_ref, w_ref, wsem, osem):
    d = lax.axis_index("fsdp")
    core = lax.rem(d, 2)
    c0 = pl.multiple_of((1 - d // 2) * (2 * FF_ROWS) + 2560, HEAD)
    for n in range(4):
        cols = pl.ds(n * 512, 512)
        for src, src_core in ((w2_hbm, core), (w3_hbm, 1 - core)):
            r0 = pl.multiple_of((1 - src_core) * 2560, 512)
            d0 = pl.multiple_of(src_core * TAIL, 64)
            pltpu.make_async_copy(src.at[LAYERS - 1, pl.ds(r0, TAIL), cols], w_ref.at[n, pl.ds(d0, TAIL), :], wsem.at[n]).start()

    def store(n, m):
        rows, cols = pl.ds(m * 512, 512), pl.ds(n * 512, 512)
        return pltpu.make_async_copy(y_ref.at[rows, cols], out.at[rows, cols], osem.at[n, m])

    for n in range(4):
        cols = pl.ds(n * 512, 512)
        pltpu.make_async_copy(w_ref.at[n], w_ref.at[n], wsem.at[n]).wait()
        for m in range(2):
            rows = pl.ds(m * 512, 512)
            y_ref[rows, cols] = x_ref[rows, cols] + jnp.dot(a_ref[rows, pl.ds(c0, REST_K)], w_ref[n], preferred_element_type=F32)
            store(n, m).start()
    for n in range(4):
        for m in range(2):
            store(n, m).wait()


def run_layers(tokens, seg_ids, g_attn, g_mlp, weights):
    shapes = [jax.ShapeDtypeStruct(w.shape, w.dtype) for w in weights]
    half_dim = HEAD // 2
    freq = np.float32(ROPE_BASE) ** (-np.arange(half_dim, dtype=np.float32) / np.float32(half_dim))
    freq = jnp.asarray(np.concatenate([freq, freq]).reshape(1, HEAD))
    sem = pltpu.SemaphoreType.DMA((SLOTS, 2))
    item_sem = pltpu.SemaphoreType.DMA((ITEM_SLOTS,))
    any_spec = pl.BlockSpec(memory_space=pl.ANY)
    vmem_spec = pl.BlockSpec(memory_space=pltpu.VMEM)
    outs = pl.pallas_call(
        layer_kernel,
        out_shape=[pltpu.VMEM((TOK, D), F32), pltpu.VMEM((TOK, FF), BF16)] + shapes * 3,
        in_specs=[any_spec] * 12,
        out_specs=[vmem_spec] * 2 + [any_spec] * 21,
        scratch_shapes=[
            pltpu.VMEM((TOK, D), BF16),
            pltpu.VMEM((TOK, D), BF16),
            pltpu.VMEM((TOK, 512), BF16),
            pltpu.VMEM((2, D, 512), BF16),
            pltpu.VMEM((2, 1024, D), BF16),
            pltpu.VMEM((TOK, HEAD), F32),
            pltpu.VMEM((TOK, HEAD), F32),
            pltpu.VMEM((TOK, HEAD), jnp.int32),
            pltpu.VMEM((2 * LAYERS, 1, D), F32),
            pltpu.VMEM((TOK // 128, 128), jnp.int32),
            pltpu.VMEM((1, HEAD), F32),
            pltpu.VMEM((LAYERS, D), BF16),
            pltpu.VMEM((LAYERS, D), BF16),
            pltpu.SemaphoreType.DMA((2,)),
            pltpu.SemaphoreType.DMA((2,)),
            pltpu.SemaphoreType.DMA((5,)),
        ] + [sem] * 2 + [item_sem] * 4 + [sem] * 2,
        compiler_params=pltpu.CompilerParams(collective_id=0, has_side_effects=True, vmem_limit_bytes=34 * 1000 * 1000),
        name="two_layers",
    )(tokens, seg_ids.reshape(TOK // 128, 128), freq, g_attn, g_mlp, *weights)
    hidden = pltpu.with_memory_space_constraint(outs[0], pltpu.VMEM)
    act = pltpu.with_memory_space_constraint(outs[1], pltpu.VMEM)
    return pl.pallas_call(
        result_kernel,
        out_shape=jax.ShapeDtypeStruct((TOK, D), F32),
        in_specs=[vmem_spec] * 2 + [any_spec] * 2,
        out_specs=any_spec,
        scratch_shapes=[
            pltpu.VMEM((TOK, D), F32),
            pltpu.VMEM((4, REST_K, 512), BF16),
            pltpu.SemaphoreType.DMA((4,)),
            pltpu.SemaphoreType.DMA((4, 2)),
        ],
        compiler_params=pltpu.CompilerParams(vmem_limit_bytes=24 * 1000 * 1000),
        name="result",
    )(hidden, act, outs[15], outs[22])


def solution(mesh):
    tok_spec = P(("rep", "fsdp"), None)
    seg_spec = P(("rep", "fsdp"))
    mat_spec = P(None, "fsdp", None)
    gain_spec = P(None, None)

    def per_device(tokens, seg_ids, w_q, w_k, w_v, w_o, w_gate, w_up, w_down, g_attn, g_mlp):
        return run_layers(tokens, seg_ids, g_attn, g_mlp, (w_q, w_k, w_v, w_o, w_gate, w_up, w_down))

    return jax.shard_map(per_device, mesh=mesh, in_specs=(tok_spec, seg_spec, mat_spec, mat_spec, mat_spec, mat_spec, mat_spec, mat_spec, mat_spec, gain_spec, gain_spec), out_specs=tok_spec, check_vma=False)
```

```python
import functools

import jax
import jax.numpy as jnp
import numpy as np
from jax import lax
from jax.experimental import pallas as pl
from jax.experimental.pallas import tpu as pltpu
from jax.sharding import PartitionSpec as P

D = 2048
FF = 11008
HEADS = 16
HEAD = 128
TOK = 1024
EPS = 1e-5
ROPE_BASE = 10000.0
MESH = pl.DeviceIdType.MESH
F32 = jnp.float32
BF16 = jnp.bfloat16

LAYERS = 2
SLOTS = 8
ITEM_SLOTS = 2 * SLOTS
AHEAD = 8
AHEAD0 = 5
ROWS = D // 4
FF_ROWS = FF // 4
TAIL = 192
NAMES = ("q", "k", "v", "o", "g", "u", "d")

N_Q = 4
N_GU = 21
N_D = 10
CH_Q = 1
CH_O = CH_Q + N_Q
CH_GU = CH_O + N_Q
CH_GL = CH_GU + N_GU
CH_D = CH_GL + 1
CH_DR = CH_D + N_D
PER_LAYER = CH_DR + 1
CHUNKS = LAYERS * PER_LAYER
ITEMS = 2 * CHUNKS

NEAR_AT = 5

N_GT = FF // 256
ST_Q = 1
ST_A = ST_Q + N_Q
ST_O = ST_A + HEADS
ST_G = ST_O + 4
ST_D = ST_G + N_GT
ST_NEAR = ST_D + 2 * NEAR_AT
ST_READY = ST_D + 2 * (N_D - 1)
ST_IDLE = ST_READY + 3
ST_FAR = ST_IDLE + 1
ST_REST = ST_FAR + 2
STEPS = ST_REST + 2
ALL_STEPS = LAYERS * STEPS - 2
START = (4, 1, 0)
FIRST = (8, 3, 1)
REST_K = 2 * TAIL
NEAR_K = 512 + REST_K

MB = 512
NB = 128
QB = 256


def layer_kernel(*refs):
    tok, seg, freq, g_attn, g_mlp = refs[:5]
    own = dict(zip(NAMES, refs[5:12]))
    x_ref, a_ref = refs[12:14]
    b1 = dict(zip(NAMES, refs[14:21]))
    b2 = dict(zip(NAMES, refs[21:28]))
    b3 = dict(zip(NAMES, refs[28:35]))
    (h_ref, q_ref, kv_ref, wbuf, dbuf, cos_ref, sin_ref, first_ref, gain_ref,
     seg_ref, freq_ref, ga_ref, gm_ref, wsem, dsem, iosem) = refs[35:51]
    s0s, s0r, s1s, s1r, s2s, s2r, s3s, s3r = refs[51:]
    sources = (own, b1, b2, b3)
    y = lax.axis_index("rep")
    d = lax.axis_index("fsdp")
    side = d // 2
    core = lax.rem(d, 2)
    x_dev = (y, lax.rem(d + 2, 4))
    y_dev = (1 - y, d)
    c_dev = (y, d + 1 - 2 * core)

    def rel(block):
        return 2 * lax.rem(block // 2 + side, 2) + lax.rem(block + core, 2)

    inputs = [pltpu.make_async_copy(src, dst, iosem.at[n]) for n, (src, dst) in enumerate(
        ((tok, q_ref), (seg, seg_ref), (freq, freq_ref), (g_attn, ga_ref), (g_mlp, gm_ref)))]
    for copy in inputs:
        copy.start()

    with jax.named_scope("barrier"):
        barrier = pltpu.get_barrier_semaphore()
        for dev in (x_dev, y_dev, c_dev):
            pl.semaphore_signal(barrier, inc=1, device_id=dev, device_id_type=MESH)
        pl.semaphore_wait(barrier, 3)

    def kinds(k):
        i = lax.rem(k, PER_LAYER)
        jq = pl.multiple_of((i - CH_Q) * 512, 512)
        jo = pl.multiple_of((i - CH_O) * 512, 512)
        jg = pl.multiple_of((i - CH_GU) * 512, 512)
        jd = core * TAIL + (i - CH_D) * 256
        jr = (1 - core) * 2560
        last = N_GU * 512
        kv = [("k", 0, ROWS, 0, 256), ("v", 0, ROWS, 0, 256)]
        gu = [("g", 0, ROWS, jg, 512), ("u", 0, ROWS, jg, 512)]
        gl = [("g", 0, ROWS, last, 256), ("u", 0, ROWS, last, 256)]

        def split_cols(name, c0):
            return [(name, 0, ROWS, c0, 256), (name, 0, ROWS, c0 + 256, 256)], [(name, 0, ROWS, c0, 512)]

        def split_rows(r0, nr):
            return [("d", r0, nr // 2, 0, D), ("d", r0 + nr // 2, nr // 2, 0, D)], [("d", r0, nr, 0, D)]

        return [
            (i == 0, kv, kv),
            ((i >= CH_Q) & (i < CH_O), *split_cols("q", jq)),
            ((i >= CH_O) & (i < CH_GU), *split_cols("o", jo)),
            ((i >= CH_GU) & (i < CH_GL), gu, gu),
            (i == CH_GL, gl, gl),
            ((i >= CH_D) & (i < CH_DR), *split_rows(jd, 256)),
            (i == CH_DR, *split_rows(jr, TAIL)),
        ]

    def for_chunk(k, fn):
        layer = k // PER_LAYER
        slot = lax.rem(k, SLOTS)
        for cond, _, whole in kinds(k):
            @pl.when((k < CHUNKS) & cond)
            def _():
                for n, piece in enumerate(whole):
                    fn(False, layer, piece, (slot, n))

    def for_pair(k, fn):
        layer = k // PER_LAYER
        table = kinds(k)
        for c, (cond, pieces, _) in enumerate(table):
            for end in ((False, True) if c == len(table) - 1 else (None,)):
                here = cond if end is None else cond & ((k == CHUNKS - 1) if end else (k < CHUNKS - 1))

                @pl.when((k < CHUNKS) & here)
                def _():
                    for n, piece in enumerate(pieces):
                        fn(bool(end) and n == 1, layer, piece, (lax.rem(2 * k + n, ITEM_SLOTS),))

    def for_item(m, fn):
        k = m // 2
        n = lax.rem(m, 2)
        layer = k // PER_LAYER
        slot = (lax.rem(m, ITEM_SLOTS),)
        for cond, (one, two), _ in kinds(k):
            if one[0] == two[0]:
                name, r0, nr, c0, nc = one
                r0 = r0 + n * (nr if nc == D else 0)
                c0 = c0 + n * (0 if nc == D else nc) if nc == D else pl.multiple_of(c0 + n * nc, 256)
                piece = (name, r0, nr, c0 if nc != D else 0, nc)

                @pl.when((m < ITEMS - 1) & cond)
                def _():
                    fn(False, layer, piece, slot)
                if nc == D and nr == TAIL // 2:
                    @pl.when((m == ITEMS - 1) & cond)
                    def _():
                        fn(True, layer, piece, slot)
            else:
                for which, piece in enumerate((one, two)):
                    @pl.when((m < ITEMS) & cond & (n == which))
                    def _():
                        fn(False, layer, piece, slot)

    def view(bufs, name, layer, r0, nr, c0, nc, half):
        if half:
            nr = nr // 2
            r0 = r0 + y * nr
        r0 = pl.multiple_of(r0, 16)
        return bufs[name].at[layer, pl.ds(r0, nr), pl.ds(c0, nc)]

    def remote(src, dst, ss, rs, dev, half):
        def make(whole, layer, piece, slot):
            part = half and not whole
            return pltpu.make_async_remote_copy(
                src_ref=view(src, piece[0], layer, *piece[1:], part),
                dst_ref=view(dst, piece[0], layer, *piece[1:], part),
                send_sem=ss.at[slot], recv_sem=rs.at[slot], device_id=dev, device_id_type=MESH)
        return make

    copy0 = remote(own, b1, s0s, s0r, c_dev, False)
    copy1 = remote(own, b2, s1s, s1r, x_dev, True)
    copy2 = remote(b2, b2, s2s, s2r, y_dev, True)
    copy3 = remote(b2, b3, s3s, s3r, c_dev, False)

    def start0(*a):
        copy0(*a).start()

    def start1(*a):
        copy1(*a).start()

    def wait0(*a):
        copy0(*a).wait_recv()

    def relay2(*a):
        copy1(*a).wait_recv()
        if not a[0]:
            copy2(*a).start()

    def arrived(*a):
        if not a[0]:
            copy2(*a).wait_recv()
        copy1(*a).wait_send()

    def relay3(*a):
        copy3(*a).start()
        copy0(*a).wait_send()

    def finish(*a):
        copy3(*a).wait_recv()
        copy3(*a).wait_send()

    def sent(*a):
        if not a[0]:
            copy2(*a).wait_send()

    def targets(s):
        i = lax.rem(s, STEPS)
        layer = s // STEPS
        first = layer == 0
        late = 1 - jnp.minimum(layer, 1)
        t2 = jnp.where(i < ST_A, 8 + 2 * i + 2 * late,
             jnp.where(i < ST_G + 1, 18 + late + 3 * (i - ST_A) // 5,
             jnp.where(i < ST_D, jnp.maximum(i + 2, 31 + late + (i - ST_G - 1) // 2),
             jnp.where(i < ST_NEAR, jnp.maximum(i, jnp.minimum(i + 1, ST_D + 2)),
             jnp.where(first, jnp.where(i < ST_NEAR + 2, i, jnp.where(i < ST_READY - 2, 40 + i // 2, jnp.where(i < ST_READY, i - 2, i - 3))),
             jnp.where(i < ST_READY - 2, 38 + (i + 1) // 2, 39 + i // 2))))))
        final = i == STEPS - 1
        t3 = jnp.where(i < ST_D, (t2 - 3) // 2,
             jnp.where(first, jnp.where(i < ST_IDLE, (t2 - 2) // 2, CH_DR + (i - ST_IDLE + 1) // 2 + jnp.where(final, 1, 0)),
             jnp.where(i < ST_READY - 4, (t2 - 2) // 2, 39 + (i - ST_READY + 4) // 3 + jnp.where(i == ST_FAR, 1, 0))))
        end = s >= ALL_STEPS - 2
        t2 = jnp.minimum(t2 + layer * 2 * PER_LAYER, jnp.where(end, ITEMS, ITEMS - 1))
        t3 = jnp.minimum(t3 + layer * PER_LAYER, jnp.where(end, CHUNKS, CHUNKS - 1))
        nxt = jnp.minimum(s + 1, ALL_STEPS - 1)
        i = lax.rem(nxt, STEPS)
        done = jnp.where(i < ST_A, 1 + i,
               jnp.where(i < ST_O, ST_A,
               jnp.where(i < ST_G, 1 + CH_O + i - ST_O,
               jnp.where(i < ST_D, 1 + CH_GU + (i - ST_G) // 2,
               jnp.where(i < ST_NEAR, 1 + CH_D + (i - ST_D) // 2,
               jnp.where(i < ST_READY, CH_D + (i - ST_D) // 2,
               jnp.where(i < ST_READY + 1, CH_DR - 2,
               jnp.where(i < ST_FAR, CH_DR - 1,
               jnp.where(i < ST_REST, CH_DR, PER_LAYER)))))))))
        tf = jnp.maximum(t3 - 2, done + nxt // STEPS * PER_LAYER)
        t3 = jnp.maximum(t3, tf)
        return jnp.maximum(t2, 2 * t3), t3, tf

    def relays(old, new):
        @pl.loop(old[0], new[0])
        def _(m):
            with jax.named_scope("r2"):
                for_item(m, relay2)
                for_item(m + AHEAD, start1)
                n = lax.rem(m, 2)
                for_chunk(m // 2 + jnp.where(n == 0, AHEAD0, CHUNKS), start0)
                for_chunk(m // 2 + jnp.where(n == 0, CHUNKS, AHEAD0 - 1), wait0)

        @pl.loop(old[1], new[1])
        def _(k):
            with jax.named_scope("r3"):
                for_pair(k, arrived)
                for_chunk(k, relay3)

        @pl.loop(old[2], new[2])
        def _(k):
            with jax.named_scope("fin"):
                for_chunk(k, finish)
                for_pair(k, sent)

    def down_step(i):
        n = i - ST_D - jnp.where(i > ST_READY, 1, 0) - jnp.where(i > ST_IDLE, 1, 0)
        j = n // 2
        near = (i >= ST_NEAR) & (i < ST_NEAR + 2)
        far = (i >= ST_FAR) & (i < ST_REST)
        rest = i >= ST_REST
        whole = (i >= ST_D) & (i < ST_IDLE) & ~near & (i != ST_READY)
        return j, jnp.where(i > ST_NEAR, j - 1, j), lax.rem(n + 2 * STEPS, 2), whole, near, far, rest

    def rest_col(side_no):
        return pl.multiple_of(side_no * (2 * FF_ROWS) + 2560, HEAD)

    def tile_col(side_no, core_no, tile):
        return pl.multiple_of(side_no * (2 * FF_ROWS) + core_no * (FF_ROWS + TAIL) + tile * 256, HEAD)

    def load_tile(s):
        layer = s // STEPS
        i = lax.rem(s, STEPS)
        slot = lax.rem(s, 2)

        def cols(name, c0, nc, w0):
            for r, src in enumerate(sources):
                pltpu.make_async_copy(src[name].at[layer, :, pl.ds(c0, nc)],
                                      wbuf.at[slot, pl.ds(r * ROWS, ROWS), pl.ds(w0, nc)], wsem.at[slot]).start()

        @pl.when(i == 0)
        def _():
            cols("k", 0, 256, 0)
            cols("v", 0, 256, 256)

        @pl.when((i >= ST_Q) & (i < ST_A))
        def _():
            cols("q", pl.multiple_of((i - ST_Q) * 512, 512), 512, 0)

        @pl.when((i >= ST_O) & (i < ST_G))
        def _():
            cols("o", pl.multiple_of((i - ST_O) * 512, 512), 512, 0)

        @pl.when((i >= ST_G) & (i < ST_D))
        def _():
            c0 = pl.multiple_of((i - ST_G) * 256, 256)
            cols("g", c0, 256, 0)
            cols("u", c0, 256, 256)

        j, tile, half, whole, near, far, rest = down_step(i)
        dslot = lax.rem(j + 2 * STEPS, 2)

        def rows_in(src, r0, nr, w0):
            pltpu.make_async_copy(src["d"].at[layer, pl.ds(r0, nr), :], dbuf.at[dslot, pl.ds(w0, nr), :], dsem.at[dslot]).start()

        def chunk_rows(r, tile_no, w0):
            src_core = core if r % 2 == 0 else 1 - core
            rows_in(sources[r], pl.multiple_of(src_core * TAIL + tile_no * 256, 64), 256, w0)

        def rest_rows(r, w0):
            src_core = core if r % 2 == 0 else 1 - core
            rows_in(sources[r], pl.multiple_of((1 - src_core) * 2560, 512), TAIL, pl.multiple_of(w0 + src_core * TAIL, 64))

        @pl.when(whole & (half == 0))
        def _():
            for r in range(4):
                chunk_rows(r, tile, r * 256)

        @pl.when(near & (half == 0))
        def _():
            for r in range(2):
                chunk_rows(r, N_D - 1, r * 256)
                rest_rows(r, 512)

        @pl.when(far & (half == 0))
        def _():
            for r in range(2):
                chunk_rows(2 + r, N_D - 1, r * 256)

        @pl.when(rest & (half == 0))
        def _():
            for r in range(2):
                rest_rows(2 + r, 0)

    def norm(layer, which):
        @pl.loop(0, TOK // NB)
        def _(m):
            rows = pl.ds(pl.multiple_of(m * NB, NB), NB)
            total = jnp.zeros((NB, 1), F32)
            for b in range(4):
                blk = x_ref[rows, pl.ds(b * ROWS, ROWS)]
                total = total + jnp.sum(blk * blk, axis=1, keepdims=True)
            inv = lax.rsqrt(total * (1.0 / D) + EPS)
            for b in range(4):
                blk = x_ref[rows, pl.ds(b * ROWS, ROWS)]
                gain = gain_ref[which * LAYERS + layer, :, pl.ds(b * ROWS, ROWS)]
                c0 = pl.multiple_of(rel(b) * ROWS, ROWS)
                h_ref[rows, pl.ds(c0, ROWS)] = (blk * inv * gain).astype(BF16)

    def rotate(vals, rows):
        vals = vals.astype(BF16).astype(F32)
        turned = pltpu.roll(vals, HEAD // 2, 1)
        return (vals * cos_ref[rows, :] + turned * sin_ref[rows, :]).astype(BF16)

    def tile_product(slot, finish_rows):
        @pl.loop(0, TOK // MB)
        def _(m):
            rows = pl.ds(pl.multiple_of(m * MB, MB), MB)
            finish_rows(rows, jnp.dot(h_ref[rows, :], wbuf[slot], preferred_element_type=F32))

    def kv_step(slot):
        def fin(rows, acc):
            for b in range(2):
                kv_ref[rows, pl.ds(b * HEAD, HEAD)] = rotate(acc[:, b * HEAD:(b + 1) * HEAD], rows)
            kv_ref[rows, pl.ds(256, 256)] = acc[:, 256:].astype(BF16)
        tile_product(slot, fin)

    def q_step(slot, j):
        def fin(rows, acc):
            for b in range(4):
                c0 = pl.multiple_of(j * 512 + b * HEAD, HEAD)
                q_ref[rows, pl.ds(c0, HEAD)] = rotate(acc[:, b * HEAD:(b + 1) * HEAD], rows)
        tile_product(slot, fin)

    def o_step(slot, j):
        def fin(rows, acc):
            c0 = pl.ds(pl.multiple_of(j * 512, 512), 512)
            x_ref[rows, c0] = x_ref[rows, c0] + acc
        tile_product(slot, fin)

    def g_step(slot, j):
        def fin(rows, acc):
            gate = acc[:, :256]
            up = acc[:, 256:]
            c0 = pl.multiple_of(j * 256, 256)
            a_ref[rows, pl.ds(c0, 256)] = (gate * jax.nn.sigmoid(gate) * up).astype(BF16)
        tile_product(slot, fin)

    def attend(head):
        kv = head // 8
        q0 = pl.multiple_of(head * HEAD, HEAD)
        k0 = pl.multiple_of(kv * HEAD, HEAD)
        v0 = pl.multiple_of(256 + kv * HEAD, HEAD)
        o0 = pl.multiple_of(rel(head // 4) * ROWS + lax.rem(head, 4) * HEAD, HEAD)
        scale = HEAD ** -0.5
        for b in range(TOK // QB):
            keys = (b + 1) * QB
            rows = pl.ds(b * QB, QB)
            scores = lax.dot_general(q_ref[rows, pl.ds(q0, HEAD)], kv_ref[pl.ds(0, keys), pl.ds(k0, HEAD)],
                                     (((1,), (1,)), ((), ())), preferred_element_type=F32)
            key_idx = lax.broadcasted_iota(jnp.int32, (QB, keys), 1)
            row_idx = lax.broadcasted_iota(jnp.int32, (QB, keys), 0) + b * QB
            first = jnp.concatenate([first_ref[rows, :]] * (keys // HEAD), axis=1)
            ok = (key_idx >= first) & (key_idx <= row_idx)
            scores = jnp.where(ok, scores, -1e30)
            top = jnp.max(scores, axis=1, keepdims=True)
            probs = jnp.exp((scores - top) * scale)
            inv = 1.0 / jnp.sum(probs, axis=1, keepdims=True)
            probs = (probs * inv).astype(BF16)
            mixed = jnp.dot(probs, kv_ref[pl.ds(0, keys), pl.ds(v0, HEAD)], preferred_element_type=F32)
            h_ref[rows, pl.ds(o0, HEAD)] = mixed.astype(BF16)

    def add_product(dslot, half, cols):
        rows = pl.ds(pl.multiple_of(half * MB, MB), MB)
        depth = sum(width for _, width in cols)
        lhs = jnp.concatenate([a_ref[rows, pl.ds(c0, width)] for c0, width in cols], axis=1)
        x_ref[rows, :] = x_ref[rows, :] + jnp.dot(lhs, dbuf[dslot, pl.ds(0, depth), :], preferred_element_type=F32)

    def wait_d(dslot, half, depth):
        @pl.when(half == 0)
        def _():
            part = dbuf.at[dslot, pl.ds(0, depth), :]
            pltpu.make_async_copy(part, part, dsem.at[dslot]).wait()

    def last_cols(side_no):
        return [(tile_col(side_no, core, N_D - 1), 256), (tile_col(side_no, 1 - core, N_D - 1), 256)]

    def wait_w(slot):
        pltpu.make_async_copy(wbuf.at[slot], wbuf.at[slot], wsem.at[slot]).wait()

    def step(s):
        before = [jnp.where(s == 0, one, two) for one, two in zip(FIRST, targets(s - 1))]
        relays(before, targets(s))

        @pl.when(s + 1 < ALL_STEPS)
        def _():
            load_tile(s + 1)

        with jax.named_scope("comp"):
            compute(s)

    def compute(s):
        layer = s // STEPS
        i = lax.rem(s, STEPS)
        slot = lax.rem(s, 2)

        @pl.when(((i == 0) & (layer > 0)) | (i == ST_G))
        def _():
            norm(layer, jnp.where(i == 0, 0, 1))

        @pl.when((i < ST_A) | ((i >= ST_O) & (i < ST_D)))
        def _():
            wait_w(slot)

        @pl.when(i == 0)
        def _():
            kv_step(slot)

        @pl.when((i >= ST_Q) & (i < ST_A))
        def _():
            q_step(slot, i - ST_Q)

        @pl.when((i >= ST_A) & (i < ST_O))
        def _():
            attend(i - ST_A)

        @pl.when((i >= ST_O) & (i < ST_G))
        def _():
            o_step(slot, i - ST_O)

        @pl.when((i >= ST_G) & (i < ST_D))
        def _():
            g_step(slot, i - ST_G)

        j, tile, half, whole, near, far, rest = down_step(i)
        dslot = lax.rem(j + 2 * STEPS, 2)

        @pl.when(whole)
        def _():
            wait_d(dslot, half, 1024)
            add_product(dslot, half, [(tile_col(lax.rem(side + r // 2, 2), lax.rem(core + r, 2), tile), 256) for r in range(4)])

        @pl.when(near)
        def _():
            wait_d(dslot, half, NEAR_K)
            add_product(dslot, half, last_cols(side) + [(rest_col(side), REST_K)])

        @pl.when(far)
        def _():
            wait_d(dslot, half, 512)
            add_product(dslot, half, last_cols(1 - side))

        @pl.when(rest)
        def _():
            wait_d(dslot, half, REST_K)
            add_product(dslot, half, [(rest_col(1 - side), REST_K)])

    @pl.loop(0, AHEAD)
    def _(m):
        for_item(m, start1)

    @pl.loop(0, AHEAD0)
    def _(k):
        for_chunk(k, start0)

    for copy in inputs:
        copy.wait()

    for n, ref in enumerate((ga_ref, gm_ref)):
        for layer in range(LAYERS):
            gain_ref[n * LAYERS + layer] = ref[pl.ds(layer, 1), :].astype(F32)
    ids = seg_ref[...].astype(F32)
    lane = lax.broadcasted_iota(jnp.int32, (128, HEAD), 1)
    for b in range(TOK // 128):
        rows = pl.ds(b * 128, 128)
        mine = jnp.transpose(jnp.broadcast_to(ids[b:b + 1, :], (128, 128)))
        before = jnp.zeros((128, 128), F32)
        for c in range(TOK // 128):
            before = before + jnp.where(ids[c:c + 1, :] < mine, 1.0, 0.0)
        first = jnp.sum(before, axis=1, keepdims=True)
        pos = lax.broadcasted_iota(jnp.int32, (128, 128), 0).astype(F32) + (b * 128.0) - first
        angles = pos * freq_ref[...]
        cos_ref[rows, :] = jnp.cos(angles)
        sin = jnp.sin(angles)
        sin_ref[rows, :] = jnp.where(lane < HEAD // 2, -sin, sin)
        first_ref[rows, :] = jnp.broadcast_to(first, (128, 128)).astype(jnp.int32)

    @pl.loop(0, TOK // NB)
    def _(m):
        rows = pl.ds(pl.multiple_of(m * NB, NB), NB)
        x_ref[rows, :] = q_ref[rows, :].astype(F32)

    relays((0, 0, 0), (2, 0, 0))
    norm(0, 0)

    @pl.loop(0, AHEAD0 - 1)
    def _(k):
        for_chunk(k, wait0)

    relays((2, 0, 0), START)
    relays(START, FIRST)
    load_tile(0)

    @pl.loop(0, ALL_STEPS)
    def _(s):
        with jax.named_scope("step"):
            step(s)

    relays(targets(ALL_STEPS - 1), (ITEMS, CHUNKS, CHUNKS))


def result_kernel(x_ref, a_ref, w2_hbm, w3_hbm, out, y_ref, w_ref, wsem, osem):
    d = lax.axis_index("fsdp")
    core = lax.rem(d, 2)
    c0 = pl.multiple_of((1 - d // 2) * (2 * FF_ROWS) + 2560, HEAD)
    for n in range(4):
        cols = pl.ds(n * 512, 512)
        for src, src_core in ((w2_hbm, core), (w3_hbm, 1 - core)):
            r0 = pl.multiple_of((1 - src_core) * 2560, 512)
            d0 = pl.multiple_of(src_core * TAIL, 64)
            pltpu.make_async_copy(src.at[LAYERS - 1, pl.ds(r0, TAIL), cols], w_ref.at[n, pl.ds(d0, TAIL), :], wsem.at[n]).start()

    def store(n, m):
        rows, cols = pl.ds(m * 512, 512), pl.ds(n * 512, 512)
        return pltpu.make_async_copy(y_ref.at[rows, cols], out.at[rows, cols], osem.at[n, m])

    for n in range(4):
        cols = pl.ds(n * 512, 512)
        pltpu.make_async_copy(w_ref.at[n], w_ref.at[n], wsem.at[n]).wait()
        for m in range(2):
            rows = pl.ds(m * 512, 512)
            y_ref[rows, cols] = x_ref[rows, cols] + jnp.dot(a_ref[rows, pl.ds(c0, REST_K)], w_ref[n], preferred_element_type=F32)
            store(n, m).start()
    for n in range(4):
        for m in range(2):
            store(n, m).wait()


def run_layers(tokens, seg_ids, g_attn, g_mlp, weights):
    shapes = [jax.ShapeDtypeStruct(w.shape, w.dtype) for w in weights]
    half_dim = HEAD // 2
    freq = np.float32(ROPE_BASE) ** (-np.arange(half_dim, dtype=np.float32) / np.float32(half_dim))
    freq = jnp.asarray(np.concatenate([freq, freq]).reshape(1, HEAD))
    sem = pltpu.SemaphoreType.DMA((SLOTS, 2))
    item_sem = pltpu.SemaphoreType.DMA((ITEM_SLOTS,))
    any_spec = pl.BlockSpec(memory_space=pl.ANY)
    vmem_spec = pl.BlockSpec(memory_space=pltpu.VMEM)
    outs = pl.pallas_call(
        layer_kernel,
        out_shape=[pltpu.VMEM((TOK, D), F32), pltpu.VMEM((TOK, FF), BF16)] + shapes * 3,
        in_specs=[any_spec] * 12,
        out_specs=[vmem_spec] * 2 + [any_spec] * 21,
        scratch_shapes=[
            pltpu.VMEM((TOK, D), BF16),
            pltpu.VMEM((TOK, D), BF16),
            pltpu.VMEM((TOK, 512), BF16),
            pltpu.VMEM((2, D, 512), BF16),
            pltpu.VMEM((2, 1024, D), BF16),
            pltpu.VMEM((TOK, HEAD), F32),
            pltpu.VMEM((TOK, HEAD), F32),
            pltpu.VMEM((TOK, HEAD), jnp.int32),
            pltpu.VMEM((2 * LAYERS, 1, D), F32),
            pltpu.VMEM((TOK // 128, 128), jnp.int32),
            pltpu.VMEM((1, HEAD), F32),
            pltpu.VMEM((LAYERS, D), BF16),
            pltpu.VMEM((LAYERS, D), BF16),
            pltpu.SemaphoreType.DMA((2,)),
            pltpu.SemaphoreType.DMA((2,)),
            pltpu.SemaphoreType.DMA((5,)),
        ] + [sem] * 2 + [item_sem] * 4 + [sem] * 2,
        compiler_params=pltpu.CompilerParams(collective_id=0, has_side_effects=True, vmem_limit_bytes=34 * 1000 * 1000),
        name="two_layers",
    )(tokens, seg_ids.reshape(TOK // 128, 128), freq, g_attn, g_mlp, *weights)
    hidden = pltpu.with_memory_space_constraint(outs[0], pltpu.VMEM)
    act = pltpu.with_memory_space_constraint(outs[1], pltpu.VMEM)
    return pl.pallas_call(
        result_kernel,
        out_shape=jax.ShapeDtypeStruct((TOK, D), F32),
        in_specs=[vmem_spec] * 2 + [any_spec] * 2,
        out_specs=any_spec,
        scratch_shapes=[
            pltpu.VMEM((TOK, D), F32),
            pltpu.VMEM((4, REST_K, 512), BF16),
            pltpu.SemaphoreType.DMA((4,)),
            pltpu.SemaphoreType.DMA((4, 2)),
        ],
        compiler_params=pltpu.CompilerParams(vmem_limit_bytes=24 * 1000 * 1000),
        name="result",
    )(hidden, act, outs[15], outs[22])


def solution(mesh):
    tok_spec = P(("rep", "fsdp"), None)
    seg_spec = P(("rep", "fsdp"))
    mat_spec = P(None, "fsdp", None)
    gain_spec = P(None, None)

    def per_device(tokens, seg_ids, w_q, w_k, w_v, w_o, w_gate, w_up, w_down, g_attn, g_mlp):
        return run_layers(tokens, seg_ids, g_attn, g_mlp, (w_q, w_k, w_v, w_o, w_gate, w_up, w_down))

    return jax.shard_map(per_device, mesh=mesh, in_specs=(tok_spec, seg_spec, mat_spec, mat_spec, mat_spec, mat_spec, mat_spec, mat_spec, mat_spec, gain_spec, gain_spec), out_specs=tok_spec, check_vma=False)
```

```python
import functools

import jax
import jax.numpy as jnp
import numpy as np
from jax import lax
from jax.experimental import pallas as pl
from jax.experimental.pallas import tpu as pltpu
from jax.sharding import PartitionSpec as P

D = 2048
FF = 11008
HEADS = 16
HEAD = 128
TOK = 1024
EPS = 1e-5
ROPE_BASE = 10000.0
MESH = pl.DeviceIdType.MESH
F32 = jnp.float32
BF16 = jnp.bfloat16

LAYERS = 2
SLOTS = 8
ITEM_SLOTS = 2 * SLOTS
AHEAD = 8
AHEAD0 = 5
ROWS = D // 4
FF_ROWS = FF // 4
TAIL = 192
NAMES = ("q", "k", "v", "o", "g", "u", "d")

N_Q = 4
N_GU = 21
N_D = 10
CH_Q = 1
CH_O = CH_Q + N_Q
CH_GU = CH_O + N_Q
CH_GL = CH_GU + N_GU
CH_D = CH_GL + 1
CH_DR = CH_D + N_D
PER_LAYER = CH_DR + 1
CHUNKS = LAYERS * PER_LAYER
ITEMS = 2 * CHUNKS

NEAR_AT = 5

N_GT = FF // 256
ST_Q = 1
ST_A = ST_Q + N_Q
ST_O = ST_A + HEADS
ST_G = ST_O + 4
ST_D = ST_G + N_GT
ST_NEAR = ST_D + 2 * NEAR_AT
ST_READY = ST_D + 2 * (N_D - 1)
ST_IDLE = ST_READY + 3
ST_FAR = ST_IDLE + 1
ST_REST = ST_FAR + 2
STEPS = ST_REST + 2
ALL_STEPS = LAYERS * STEPS - 2
START = (4, 1, 0)
FIRST = (8, 3, 1)
REST_K = 2 * TAIL
NEAR_K = 512 + REST_K

MB = 512
NB = 128
QB = 256


def layer_kernel(*refs):
    tok, seg, freq, g_attn, g_mlp = refs[:5]
    own = dict(zip(NAMES, refs[5:12]))
    x_ref, a_ref = refs[12:14]
    b1 = dict(zip(NAMES, refs[14:21]))
    b2 = dict(zip(NAMES, refs[21:28]))
    b3 = dict(zip(NAMES, refs[28:35]))
    (h_ref, q_ref, kv_ref, wbuf, dbuf, cos_ref, sin_ref, first_ref, gain_ref,
     seg_ref, freq_ref, ga_ref, gm_ref, wsem, dsem, iosem) = refs[35:51]
    s0s, s0r, s1s, s1r, s2s, s2r, s3s, s3r = refs[51:]
    sources = (own, b1, b2, b3)
    y = lax.axis_index("rep")
    d = lax.axis_index("fsdp")
    side = d // 2
    core = lax.rem(d, 2)
    x_dev = (y, lax.rem(d + 2, 4))
    y_dev = (1 - y, d)
    c_dev = (y, d + 1 - 2 * core)

    def rel(block):
        return 2 * lax.rem(block // 2 + side, 2) + lax.rem(block + core, 2)

    inputs = [pltpu.make_async_copy(src, dst, iosem.at[n]) for n, (src, dst) in enumerate(
        ((tok, q_ref), (seg, seg_ref), (freq, freq_ref), (g_attn, ga_ref), (g_mlp, gm_ref)))]
    for copy in inputs:
        copy.start()

    with jax.named_scope("barrier"):
        barrier = pltpu.get_barrier_semaphore()
        for dev in (x_dev, y_dev, c_dev):
            pl.semaphore_signal(barrier, inc=1, device_id=dev, device_id_type=MESH)
        pl.semaphore_wait(barrier, 3)

    def kinds(k):
        i = lax.rem(k, PER_LAYER)
        jq = pl.multiple_of((i - CH_Q) * 512, 512)
        jo = pl.multiple_of((i - CH_O) * 512, 512)
        jg = pl.multiple_of((i - CH_GU) * 512, 512)
        jd = core * TAIL + (i - CH_D) * 256
        jr = (1 - core) * 2560
        last = N_GU * 512
        kv = [("k", 0, ROWS, 0, 256), ("v", 0, ROWS, 0, 256)]
        gu = [("g", 0, ROWS, jg, 512), ("u", 0, ROWS, jg, 512)]
        gl = [("g", 0, ROWS, last, 256), ("u", 0, ROWS, last, 256)]

        def split_cols(name, c0):
            return [(name, 0, ROWS, c0, 256), (name, 0, ROWS, c0 + 256, 256)], [(name, 0, ROWS, c0, 512)]

        def split_rows(r0, nr):
            return [("d", r0, nr // 2, 0, D), ("d", r0 + nr // 2, nr // 2, 0, D)], [("d", r0, nr, 0, D)]

        return [
            (i == 0, kv, kv),
            ((i >= CH_Q) & (i < CH_O), *split_cols("q", jq)),
            ((i >= CH_O) & (i < CH_GU), *split_cols("o", jo)),
            ((i >= CH_GU) & (i < CH_GL), gu, gu),
            (i == CH_GL, gl, gl),
            ((i >= CH_D) & (i < CH_DR), *split_rows(jd, 256)),
            (i == CH_DR, *split_rows(jr, TAIL)),
        ]

    def for_chunk(k, fn):
        layer = k // PER_LAYER
        slot = lax.rem(k, SLOTS)
        for cond, _, whole in kinds(k):
            @pl.when((k < CHUNKS) & cond)
            def _():
                for n, piece in enumerate(whole):
                    fn(False, layer, piece, (slot, n))

    def for_pair(k, fn):
        layer = k // PER_LAYER
        table = kinds(k)
        for c, (cond, pieces, _) in enumerate(table):
            for end in ((False, True) if c == len(table) - 1 else (None,)):
                here = cond if end is None else cond & ((k == CHUNKS - 1) if end else (k < CHUNKS - 1))

                @pl.when((k < CHUNKS) & here)
                def _():
                    for n, piece in enumerate(pieces):
                        fn(bool(end) and n == 1, layer, piece, (lax.rem(2 * k + n, ITEM_SLOTS),))

    def for_item(m, fn):
        k = m // 2
        n = lax.rem(m, 2)
        layer = k // PER_LAYER
        slot = (lax.rem(m, ITEM_SLOTS),)
        for cond, (one, two), _ in kinds(k):
            if one[0] == two[0]:
                name, r0, nr, c0, nc = one
                r0 = r0 + n * (nr if nc == D else 0)
                c0 = c0 + n * (0 if nc == D else nc) if nc == D else pl.multiple_of(c0 + n * nc, 256)
                piece = (name, r0, nr, c0 if nc != D else 0, nc)

                @pl.when((m < ITEMS - 1) & cond)
                def _():
                    fn(False, layer, piece, slot)
                if nc == D and nr == TAIL // 2:
                    @pl.when((m == ITEMS - 1) & cond)
                    def _():
                        fn(True, layer, piece, slot)
            else:
                for which, piece in enumerate((one, two)):
                    @pl.when((m < ITEMS) & cond & (n == which))
                    def _():
                        fn(False, layer, piece, slot)

    def view(bufs, name, layer, r0, nr, c0, nc, half):
        if half:
            nr = nr // 2
            r0 = r0 + y * nr
        r0 = pl.multiple_of(r0, 16)
        return bufs[name].at[layer, pl.ds(r0, nr), pl.ds(c0, nc)]

    def remote(src, dst, ss, rs, dev, half):
        def make(whole, layer, piece, slot):
            part = half and not whole
            return pltpu.make_async_remote_copy(
                src_ref=view(src, piece[0], layer, *piece[1:], part),
                dst_ref=view(dst, piece[0], layer, *piece[1:], part),
                send_sem=ss.at[slot], recv_sem=rs.at[slot], device_id=dev, device_id_type=MESH)
        return make

    copy0 = remote(own, b1, s0s, s0r, c_dev, False)
    copy1 = remote(own, b2, s1s, s1r, x_dev, True)
    copy2 = remote(b2, b2, s2s, s2r, y_dev, True)
    copy3 = remote(b2, b3, s3s, s3r, c_dev, False)

    def start0(*a):
        copy0(*a).start()

    def start1(*a):
        copy1(*a).start()

    def wait0(*a):
        copy0(*a).wait_recv()

    def relay2(*a):
        copy1(*a).wait_recv()
        if not a[0]:
            copy2(*a).start()

    def arrived(*a):
        if not a[0]:
            copy2(*a).wait_recv()
        copy1(*a).wait_send()

    def relay3(*a):
        copy3(*a).start()
        copy0(*a).wait_send()

    def finish(*a):
        copy3(*a).wait_recv()
        copy3(*a).wait_send()

    def sent(*a):
        if not a[0]:
            copy2(*a).wait_send()

    def targets(s):
        i = lax.rem(s, STEPS)
        layer = s // STEPS
        first = layer == 0
        late = 1 - jnp.minimum(layer, 1)
        t2 = jnp.where(i < ST_A, 9 + 2 * i + late,
             jnp.where(i < ST_G + 1, 18 + late + 3 * (i - ST_A) // 5,
             jnp.where(i < ST_D, jnp.maximum(i + 3, 31 + late + (i - ST_G - 1) // 2),
             jnp.where(i < ST_NEAR, jnp.maximum(i, jnp.minimum(ST_D + 2 + (i - ST_D + 1) // 2, ST_D + 4)),
             jnp.where(first, jnp.where(i < ST_NEAR + 2, i, jnp.where(i < ST_READY - 2, 40 + i // 2, jnp.where(i < ST_READY, i - 2, i - 3))),
             jnp.where(i < ST_READY - 2, 38 + (i + 1) // 2, 39 + i // 2))))))
        final = i == STEPS - 1
        t3 = jnp.where(i < ST_D, jnp.where(i < ST_A, 3 + i, (t2 - 3) // 2),
             jnp.where(first, jnp.where(i < ST_IDLE, (t2 - 2) // 2, CH_DR + (i - ST_IDLE + 1) // 2 + jnp.where(final, 1, 0)),
             jnp.where(i < ST_READY - 4, (t2 - 2) // 2, 39 + (i - ST_READY + 4) // 3 + jnp.where(i == ST_FAR, 1, 0))))
        end = s >= ALL_STEPS - 2
        t2 = jnp.minimum(t2 + layer * 2 * PER_LAYER, jnp.where(end, ITEMS, ITEMS - 1))
        t3 = jnp.minimum(t3 + layer * PER_LAYER, jnp.where(end, CHUNKS, CHUNKS - 1))
        nxt = jnp.minimum(s + 1, ALL_STEPS - 1)
        i = lax.rem(nxt, STEPS)
        done = jnp.where(i < ST_A, 1 + i,
               jnp.where(i < ST_O, ST_A,
               jnp.where(i < ST_G, 1 + CH_O + i - ST_O,
               jnp.where(i < ST_D, 1 + CH_GU + (i - ST_G) // 2,
               jnp.where(i < ST_NEAR, 1 + CH_D + (i - ST_D) // 2,
               jnp.where(i < ST_READY, CH_D + (i - ST_D) // 2,
               jnp.where(i < ST_READY + 1, CH_DR - 2,
               jnp.where(i < ST_FAR, CH_DR - 1,
               jnp.where(i < ST_REST, CH_DR, PER_LAYER)))))))))
        tf = jnp.maximum(t3 - 2, done + nxt // STEPS * PER_LAYER)
        t3 = jnp.maximum(t3, tf)
        return jnp.maximum(t2, 2 * t3), t3, tf

    def relays(old, new):
        @pl.loop(old[0], new[0])
        def _(m):
            with jax.named_scope("r2"):
                for_item(m, relay2)
                for_item(m + AHEAD, start1)
                n = lax.rem(m, 2)
                for_chunk(m // 2 + jnp.where(n == 0, AHEAD0, CHUNKS), start0)
                for_chunk(m // 2 + jnp.where(n == 0, CHUNKS, AHEAD0 - 1), wait0)

        @pl.loop(old[1], new[1])
        def _(k):
            with jax.named_scope("r3"):
                for_pair(k, arrived)
                for_chunk(k, relay3)

        @pl.loop(old[2], new[2])
        def _(k):
            with jax.named_scope("fin"):
                for_chunk(k, finish)
                for_pair(k, sent)

    def down_step(i):
        n = i - ST_D - jnp.where(i > ST_READY, 1, 0) - jnp.where(i > ST_IDLE, 1, 0)
        j = n // 2
        near = (i >= ST_NEAR) & (i < ST_NEAR + 2)
        far = (i >= ST_FAR) & (i < ST_REST)
        rest = i >= ST_REST
        whole = (i >= ST_D) & (i < ST_IDLE) & ~near & (i != ST_READY)
        return j, jnp.where(i > ST_NEAR, j - 1, j), lax.rem(n + 2 * STEPS, 2), whole, near, far, rest

    def rest_col(side_no):
        return pl.multiple_of(side_no * (2 * FF_ROWS) + 2560, HEAD)

    def tile_col(side_no, core_no, tile):
        return pl.multiple_of(side_no * (2 * FF_ROWS) + core_no * (FF_ROWS + TAIL) + tile * 256, HEAD)

    def load_tile(s):
        layer = s // STEPS
        i = lax.rem(s, STEPS)
        slot = lax.rem(s, 2)

        def cols(name, c0, nc, w0):
            for r, src in enumerate(sources):
                pltpu.make_async_copy(src[name].at[layer, :, pl.ds(c0, nc)],
                                      wbuf.at[slot, pl.ds(r * ROWS, ROWS), pl.ds(w0, nc)], wsem.at[slot]).start()

        @pl.when(i == 0)
        def _():
            cols("k", 0, 256, 0)
            cols("v", 0, 256, 256)

        @pl.when((i >= ST_Q) & (i < ST_A))
        def _():
            cols("q", pl.multiple_of((i - ST_Q) * 512, 512), 512, 0)

        @pl.when((i >= ST_O) & (i < ST_G))
        def _():
            cols("o", pl.multiple_of((i - ST_O) * 512, 512), 512, 0)

        @pl.when((i >= ST_G) & (i < ST_D))
        def _():
            c0 = pl.multiple_of((i - ST_G) * 256, 256)
            cols("g", c0, 256, 0)
            cols("u", c0, 256, 256)

        j, tile, half, whole, near, far, rest = down_step(i)
        dslot = lax.rem(j + 2 * STEPS, 2)

        def rows_in(src, r0, nr, w0):
            pltpu.make_async_copy(src["d"].at[layer, pl.ds(r0, nr), :], dbuf.at[dslot, pl.ds(w0, nr), :], dsem.at[dslot]).start()

        def chunk_rows(r, tile_no, w0):
            src_core = core if r % 2 == 0 else 1 - core
            rows_in(sources[r], pl.multiple_of(src_core * TAIL + tile_no * 256, 64), 256, w0)

        def rest_rows(r, w0):
            src_core = core if r % 2 == 0 else 1 - core
            rows_in(sources[r], pl.multiple_of((1 - src_core) * 2560, 512), TAIL, pl.multiple_of(w0 + src_core * TAIL, 64))

        @pl.when(whole & (half == 0))
        def _():
            for r in range(4):
                chunk_rows(r, tile, r * 256)

        @pl.when(near & (half == 0))
        def _():
            for r in range(2):
                chunk_rows(r, N_D - 1, r * 256)
                rest_rows(r, 512)

        @pl.when(far & (half == 0))
        def _():
            for r in range(2):
                chunk_rows(2 + r, N_D - 1, r * 256)

        @pl.when(rest & (half == 0))
        def _():
            for r in range(2):
                rest_rows(2 + r, 0)

    def norm(layer, which):
        @pl.loop(0, TOK // NB)
        def _(m):
            rows = pl.ds(pl.multiple_of(m * NB, NB), NB)
            total = jnp.zeros((NB, 1), F32)
            for b in range(4):
                blk = x_ref[rows, pl.ds(b * ROWS, ROWS)]
                total = total + jnp.sum(blk * blk, axis=1, keepdims=True)
            inv = lax.rsqrt(total * (1.0 / D) + EPS)
            for b in range(4):
                blk = x_ref[rows, pl.ds(b * ROWS, ROWS)]
                gain = gain_ref[which * LAYERS + layer, :, pl.ds(b * ROWS, ROWS)]
                c0 = pl.multiple_of(rel(b) * ROWS, ROWS)
                h_ref[rows, pl.ds(c0, ROWS)] = (blk * inv * gain).astype(BF16)

    def rotate(vals, rows):
        vals = vals.astype(BF16).astype(F32)
        turned = pltpu.roll(vals, HEAD // 2, 1)
        return (vals * cos_ref[rows, :] + turned * sin_ref[rows, :]).astype(BF16)

    def tile_product(slot, finish_rows):
        @pl.loop(0, TOK // MB)
        def _(m):
            rows = pl.ds(pl.multiple_of(m * MB, MB), MB)
            finish_rows(rows, jnp.dot(h_ref[rows, :], wbuf[slot], preferred_element_type=F32))

    def kv_step(slot):
        def fin(rows, acc):
            for b in range(2):
                kv_ref[rows, pl.ds(b * HEAD, HEAD)] = rotate(acc[:, b * HEAD:(b + 1) * HEAD], rows)
            kv_ref[rows, pl.ds(256, 256)] = acc[:, 256:].astype(BF16)
        tile_product(slot, fin)

    def q_step(slot, j):
        def fin(rows, acc):
            for b in range(4):
                c0 = pl.multiple_of(j * 512 + b * HEAD, HEAD)
                q_ref[rows, pl.ds(c0, HEAD)] = rotate(acc[:, b * HEAD:(b + 1) * HEAD], rows)
        tile_product(slot, fin)

    def o_step(slot, j):
        def fin(rows, acc):
            c0 = pl.ds(pl.multiple_of(j * 512, 512), 512)
            x_ref[rows, c0] = x_ref[rows, c0] + acc
        tile_product(slot, fin)

    def g_step(slot, j):
        def fin(rows, acc):
            gate = acc[:, :256]
            up = acc[:, 256:]
            c0 = pl.multiple_of(j * 256, 256)
            a_ref[rows, pl.ds(c0, 256)] = (gate * jax.nn.sigmoid(gate) * up).astype(BF16)
        tile_product(slot, fin)

    def attend(head):
        kv = head // 8
        q0 = pl.multiple_of(head * HEAD, HEAD)
        k0 = pl.multiple_of(kv * HEAD, HEAD)
        v0 = pl.multiple_of(256 + kv * HEAD, HEAD)
        o0 = pl.multiple_of(rel(head // 4) * ROWS + lax.rem(head, 4) * HEAD, HEAD)
        scale = HEAD ** -0.5
        for b in range(TOK // QB):
            keys = (b + 1) * QB
            rows = pl.ds(b * QB, QB)
            scores = lax.dot_general(q_ref[rows, pl.ds(q0, HEAD)], kv_ref[pl.ds(0, keys), pl.ds(k0, HEAD)],
                                     (((1,), (1,)), ((), ())), preferred_element_type=F32)
            key_idx = lax.broadcasted_iota(jnp.int32, (QB, keys), 1)
            row_idx = lax.broadcasted_iota(jnp.int32, (QB, keys), 0) + b * QB
            first = jnp.concatenate([first_ref[rows, :]] * (keys // HEAD), axis=1)
            ok = (key_idx >= first) & (key_idx <= row_idx)
            scores = jnp.where(ok, scores, -1e30)
            top = jnp.max(scores, axis=1, keepdims=True)
            probs = jnp.exp((scores - top) * scale)
            inv = 1.0 / jnp.sum(probs, axis=1, keepdims=True)
            probs = (probs * inv).astype(BF16)
            mixed = jnp.dot(probs, kv_ref[pl.ds(0, keys), pl.ds(v0, HEAD)], preferred_element_type=F32)
            h_ref[rows, pl.ds(o0, HEAD)] = mixed.astype(BF16)

    def add_product(dslot, half, cols):
        rows = pl.ds(pl.multiple_of(half * MB, MB), MB)
        depth = sum(width for _, width in cols)
        lhs = jnp.concatenate([a_ref[rows, pl.ds(c0, width)] for c0, width in cols], axis=1)
        x_ref[rows, :] = x_ref[rows, :] + jnp.dot(lhs, dbuf[dslot, pl.ds(0, depth), :], preferred_element_type=F32)

    def wait_d(dslot, half, depth):
        @pl.when(half == 0)
        def _():
            part = dbuf.at[dslot, pl.ds(0, depth), :]
            pltpu.make_async_copy(part, part, dsem.at[dslot]).wait()

    def last_cols(side_no):
        return [(tile_col(side_no, core, N_D - 1), 256), (tile_col(side_no, 1 - core, N_D - 1), 256)]

    def wait_w(slot):
        pltpu.make_async_copy(wbuf.at[slot], wbuf.at[slot], wsem.at[slot]).wait()

    def step(s):
        before = [jnp.where(s == 0, one, two) for one, two in zip(FIRST, targets(s - 1))]
        relays(before, targets(s))

        @pl.when(s + 1 < ALL_STEPS)
        def _():
            load_tile(s + 1)

        with jax.named_scope("comp"):
            compute(s)

    def compute(s):
        layer = s // STEPS
        i = lax.rem(s, STEPS)
        slot = lax.rem(s, 2)

        @pl.when(((i == 0) & (layer > 0)) | (i == ST_G))
        def _():
            norm(layer, jnp.where(i == 0, 0, 1))

        @pl.when((i < ST_A) | ((i >= ST_O) & (i < ST_D)))
        def _():
            wait_w(slot)

        @pl.when(i == 0)
        def _():
            kv_step(slot)

        @pl.when((i >= ST_Q) & (i < ST_A))
        def _():
            q_step(slot, i - ST_Q)

        @pl.when((i >= ST_A) & (i < ST_O))
        def _():
            attend(i - ST_A)

        @pl.when((i >= ST_O) & (i < ST_G))
        def _():
            o_step(slot, i - ST_O)

        @pl.when((i >= ST_G) & (i < ST_D))
        def _():
            g_step(slot, i - ST_G)

        j, tile, half, whole, near, far, rest = down_step(i)
        dslot = lax.rem(j + 2 * STEPS, 2)

        @pl.when(whole)
        def _():
            wait_d(dslot, half, 1024)
            add_product(dslot, half, [(tile_col(lax.rem(side + r // 2, 2), lax.rem(core + r, 2), tile), 256) for r in range(4)])

        @pl.when(near)
        def _():
            wait_d(dslot, half, NEAR_K)
            add_product(dslot, half, last_cols(side) + [(rest_col(side), REST_K)])

        @pl.when(far)
        def _():
            wait_d(dslot, half, 512)
            add_product(dslot, half, last_cols(1 - side))

        @pl.when(rest)
        def _():
            wait_d(dslot, half, REST_K)
            add_product(dslot, half, [(rest_col(1 - side), REST_K)])

    @pl.loop(0, AHEAD)
    def _(m):
        for_item(m, start1)

    @pl.loop(0, AHEAD0)
    def _(k):
        for_chunk(k, start0)

    for copy in inputs:
        copy.wait()

    for n, ref in enumerate((ga_ref, gm_ref)):
        for layer in range(LAYERS):
            gain_ref[n * LAYERS + layer] = ref[pl.ds(layer, 1), :].astype(F32)
    ids = seg_ref[...].astype(F32)
    lane = lax.broadcasted_iota(jnp.int32, (128, HEAD), 1)
    for b in range(TOK // 128):
        rows = pl.ds(b * 128, 128)
        mine = jnp.transpose(jnp.broadcast_to(ids[b:b + 1, :], (128, 128)))
        before = jnp.zeros((128, 128), F32)
        for c in range(TOK // 128):
            before = before + jnp.where(ids[c:c + 1, :] < mine, 1.0, 0.0)
        first = jnp.sum(before, axis=1, keepdims=True)
        pos = lax.broadcasted_iota(jnp.int32, (128, 128), 0).astype(F32) + (b * 128.0) - first
        angles = pos * freq_ref[...]
        cos_ref[rows, :] = jnp.cos(angles)
        sin = jnp.sin(angles)
        sin_ref[rows, :] = jnp.where(lane < HEAD // 2, -sin, sin)
        first_ref[rows, :] = jnp.broadcast_to(first, (128, 128)).astype(jnp.int32)

    @pl.loop(0, TOK // NB)
    def _(m):
        rows = pl.ds(pl.multiple_of(m * NB, NB), NB)
        x_ref[rows, :] = q_ref[rows, :].astype(F32)

    relays((0, 0, 0), (2, 0, 0))
    norm(0, 0)

    @pl.loop(0, AHEAD0 - 1)
    def _(k):
        for_chunk(k, wait0)

    relays((2, 0, 0), START)
    relays(START, FIRST)
    load_tile(0)

    @pl.loop(0, ALL_STEPS)
    def _(s):
        with jax.named_scope("step"):
            step(s)

    relays(targets(ALL_STEPS - 1), (ITEMS, CHUNKS, CHUNKS))


def result_kernel(x_ref, a_ref, w2_hbm, w3_hbm, out, y_ref, w_ref, wsem, osem):
    d = lax.axis_index("fsdp")
    core = lax.rem(d, 2)
    c0 = pl.multiple_of((1 - d // 2) * (2 * FF_ROWS) + 2560, HEAD)
    for n in range(4):
        cols = pl.ds(n * 512, 512)
        for src, src_core in ((w2_hbm, core), (w3_hbm, 1 - core)):
            r0 = pl.multiple_of((1 - src_core) * 2560, 512)
            d0 = pl.multiple_of(src_core * TAIL, 64)
            pltpu.make_async_copy(src.at[LAYERS - 1, pl.ds(r0, TAIL), cols], w_ref.at[n, pl.ds(d0, TAIL), :], wsem.at[n]).start()

    def store(n, m):
        rows, cols = pl.ds(m * 512, 512), pl.ds(n * 512, 512)
        return pltpu.make_async_copy(y_ref.at[rows, cols], out.at[rows, cols], osem.at[n, m])

    for n in range(4):
        cols = pl.ds(n * 512, 512)
        pltpu.make_async_copy(w_ref.at[n], w_ref.at[n], wsem.at[n]).wait()
        for m in range(2):
            rows = pl.ds(m * 512, 512)
            y_ref[rows, cols] = x_ref[rows, cols] + jnp.dot(a_ref[rows, pl.ds(c0, REST_K)], w_ref[n], preferred_element_type=F32)
            store(n, m).start()
    for n in range(4):
        for m in range(2):
            store(n, m).wait()


def run_layers(tokens, seg_ids, g_attn, g_mlp, weights):
    shapes = [jax.ShapeDtypeStruct(w.shape, w.dtype) for w in weights]
    half_dim = HEAD // 2
    freq = np.float32(ROPE_BASE) ** (-np.arange(half_dim, dtype=np.float32) / np.float32(half_dim))
    freq = jnp.asarray(np.concatenate([freq, freq]).reshape(1, HEAD))
    sem = pltpu.SemaphoreType.DMA((SLOTS, 2))
    item_sem = pltpu.SemaphoreType.DMA((ITEM_SLOTS,))
    any_spec = pl.BlockSpec(memory_space=pl.ANY)
    vmem_spec = pl.BlockSpec(memory_space=pltpu.VMEM)
    outs = pl.pallas_call(
        layer_kernel,
        out_shape=[pltpu.VMEM((TOK, D), F32), pltpu.VMEM((TOK, FF), BF16)] + shapes * 3,
        in_specs=[any_spec] * 12,
        out_specs=[vmem_spec] * 2 + [any_spec] * 21,
        scratch_shapes=[
            pltpu.VMEM((TOK, D), BF16),
            pltpu.VMEM((TOK, D), BF16),
            pltpu.VMEM((TOK, 512), BF16),
            pltpu.VMEM((2, D, 512), BF16),
            pltpu.VMEM((2, 1024, D), BF16),
            pltpu.VMEM((TOK, HEAD), F32),
            pltpu.VMEM((TOK, HEAD), F32),
            pltpu.VMEM((TOK, HEAD), jnp.int32),
            pltpu.VMEM((2 * LAYERS, 1, D), F32),
            pltpu.VMEM((TOK // 128, 128), jnp.int32),
            pltpu.VMEM((1, HEAD), F32),
            pltpu.VMEM((LAYERS, D), BF16),
            pltpu.VMEM((LAYERS, D), BF16),
            pltpu.SemaphoreType.DMA((2,)),
            pltpu.SemaphoreType.DMA((2,)),
            pltpu.SemaphoreType.DMA((5,)),
        ] + [sem] * 2 + [item_sem] * 4 + [sem] * 2,
        compiler_params=pltpu.CompilerParams(collective_id=0, has_side_effects=True, vmem_limit_bytes=34 * 1000 * 1000),
        name="two_layers",
    )(tokens, seg_ids.reshape(TOK // 128, 128), freq, g_attn, g_mlp, *weights)
    hidden = pltpu.with_memory_space_constraint(outs[0], pltpu.VMEM)
    act = pltpu.with_memory_space_constraint(outs[1], pltpu.VMEM)
    return pl.pallas_call(
        result_kernel,
        out_shape=jax.ShapeDtypeStruct((TOK, D), F32),
        in_specs=[vmem_spec] * 2 + [any_spec] * 2,
        out_specs=any_spec,
        scratch_shapes=[
            pltpu.VMEM((TOK, D), F32),
            pltpu.VMEM((4, REST_K, 512), BF16),
            pltpu.SemaphoreType.DMA((4,)),
            pltpu.SemaphoreType.DMA((4, 2)),
        ],
        compiler_params=pltpu.CompilerParams(vmem_limit_bytes=24 * 1000 * 1000),
        name="result",
    )(hidden, act, outs[15], outs[22])


def solution(mesh):
    tok_spec = P(("rep", "fsdp"), None)
    seg_spec = P(("rep", "fsdp"))
    mat_spec = P(None, "fsdp", None)
    gain_spec = P(None, None)

    def per_device(tokens, seg_ids, w_q, w_k, w_v, w_o, w_gate, w_up, w_down, g_attn, g_mlp):
        return run_layers(tokens, seg_ids, g_attn, g_mlp, (w_q, w_k, w_v, w_o, w_gate, w_up, w_down))

    return jax.shard_map(per_device, mesh=mesh, in_specs=(tok_spec, seg_spec, mat_spec, mat_spec, mat_spec, mat_spec, mat_spec, mat_spec, mat_spec, gain_spec, gain_spec), out_specs=tok_spec, check_vma=False)
```

```python
import functools

import jax
import jax.numpy as jnp
import numpy as np
from jax import lax
from jax.experimental import pallas as pl
from jax.experimental.pallas import tpu as pltpu
from jax.sharding import PartitionSpec as P

D = 2048
FF = 11008
HEADS = 16
HEAD = 128
TOK = 1024
EPS = 1e-5
ROPE_BASE = 10000.0
MESH = pl.DeviceIdType.MESH
F32 = jnp.float32
BF16 = jnp.bfloat16

LAYERS = 2
SLOTS = 8
ITEM_SLOTS = 2 * SLOTS
AHEAD = 8
AHEAD0 = 5
ROWS = D // 4
FF_ROWS = FF // 4
TAIL = 192
NAMES = ("q", "k", "v", "o", "g", "u", "d")

N_Q = 4
N_GU = 21
N_D = 10
CH_Q = 1
CH_O = CH_Q + N_Q
CH_GU = CH_O + N_Q
CH_GL = CH_GU + N_GU
CH_D = CH_GL + 1
CH_DR = CH_D + N_D
PER_LAYER = CH_DR + 1
CHUNKS = LAYERS * PER_LAYER
ITEMS = 2 * CHUNKS

NEAR_AT = 5

N_GT = FF // 256
ST_Q = 1
ST_A = ST_Q + N_Q
ST_O = ST_A + HEADS
ST_G = ST_O + 4
ST_D = ST_G + N_GT
ST_NEAR = ST_D + 2 * NEAR_AT
ST_READY = ST_D + 2 * (N_D - 1)
ST_CROSS = ST_READY + 3
ST_IDLE = ST_CROSS + 2
ST_FAR = ST_IDLE + 1
ST_REST = ST_FAR + 2
STEPS = ST_REST + 2
ALL_STEPS = LAYERS * STEPS - 2
START = (4, 1, 0)
FIRST = (8, 3, 1)
REST_K = 2 * TAIL
NEAR_K = 512 + REST_K

MB = 512
NB = 128
QB = 256


def layer_kernel(*refs):
    tok, seg, freq, g_attn, g_mlp = refs[:5]
    own = dict(zip(NAMES, refs[5:12]))
    x_ref, a_ref = refs[12:14]
    b1 = dict(zip(NAMES, refs[14:21]))
    b2 = dict(zip(NAMES, refs[21:28]))
    b3 = dict(zip(NAMES, refs[28:35]))
    (h_ref, q_ref, kv_ref, wbuf, dbuf, cos_ref, sin_ref, first_ref, gain_ref,
     seg_ref, freq_ref, ga_ref, gm_ref, wsem, dsem, iosem) = refs[35:51]
    s0s, s0r, s1s, s1r, s2s, s2r, s3s, s3r = refs[51:]
    sources = (own, b1, b2, b3)
    y = lax.axis_index("rep")
    d = lax.axis_index("fsdp")
    side = d // 2
    core = lax.rem(d, 2)
    x_dev = (y, lax.rem(d + 2, 4))
    y_dev = (1 - y, d)
    c_dev = (y, d + 1 - 2 * core)

    def rel(block):
        return 2 * lax.rem(block // 2 + side, 2) + lax.rem(block + core, 2)

    inputs = [pltpu.make_async_copy(src, dst, iosem.at[n]) for n, (src, dst) in enumerate(
        ((tok, q_ref), (seg, seg_ref), (freq, freq_ref), (g_attn, ga_ref), (g_mlp, gm_ref)))]
    for copy in inputs:
        copy.start()

    with jax.named_scope("barrier"):
        barrier = pltpu.get_barrier_semaphore()
        for dev in (x_dev, y_dev, c_dev):
            pl.semaphore_signal(barrier, inc=1, device_id=dev, device_id_type=MESH)
        pl.semaphore_wait(barrier, 3)

    def kinds(k):
        i = lax.rem(k, PER_LAYER)
        jq = pl.multiple_of((i - CH_Q) * 512, 512)
        jo = pl.multiple_of((i - CH_O) * 512, 512)
        jg = pl.multiple_of((i - CH_GU) * 512, 512)
        jd = core * TAIL + (i - CH_D) * 256
        jr = (1 - core) * 2560
        last = N_GU * 512
        kv = [("k", 0, ROWS, 0, 256), ("v", 0, ROWS, 0, 256)]
        gu = [("g", 0, ROWS, jg, 512), ("u", 0, ROWS, jg, 512)]
        gl = [("g", 0, ROWS, last, 256), ("u", 0, ROWS, last, 256)]

        def split_cols(name, c0):
            whole = [(name, 0, ROWS, c0, 512)]
            return [(name, 0, ROWS, c0, 256), (name, 0, ROWS, c0 + 256, 256)], whole, whole

        def split_rows(r0, nr):
            halves = [("d", r0, nr // 2, 0, D), ("d", r0 + nr // 2, nr // 2, 0, D)]
            return halves, [("d", r0, nr, 0, D)], halves

        return [
            (i == 0, kv, kv, kv),
            ((i >= CH_Q) & (i < CH_O), *split_cols("q", jq)),
            ((i >= CH_O) & (i < CH_GU), *split_cols("o", jo)),
            ((i >= CH_GU) & (i < CH_GL), gu, gu, gu),
            (i == CH_GL, gl, gl, gl),
            ((i >= CH_D) & (i < CH_DR), *split_rows(jd, 256)),
            (i == CH_DR, *split_rows(jr, TAIL)),
        ]

    def for_chunk(k, fn, form=2):
        layer = k // PER_LAYER
        slot = lax.rem(k, SLOTS)
        for kind in kinds(k):
            @pl.when((k < CHUNKS) & kind[0])
            def _():
                for n, piece in enumerate(kind[form]):
                    fn(False, layer, piece, (slot, n))

    def for_pair(k, fn):
        layer = k // PER_LAYER
        table = kinds(k)
        for c, (cond, pieces, _, _) in enumerate(table):
            for end in ((False, True) if c == len(table) - 1 else (None,)):
                here = cond if end is None else cond & ((k == CHUNKS - 1) if end else (k < CHUNKS - 1))

                @pl.when((k < CHUNKS) & here)
                def _():
                    for n, piece in enumerate(pieces):
                        fn(bool(end) and n == 1, layer, piece, (lax.rem(2 * k + n, ITEM_SLOTS),))

    def for_item(m, fn):
        k = m // 2
        n = lax.rem(m, 2)
        layer = k // PER_LAYER
        slot = (lax.rem(m, ITEM_SLOTS),)
        for cond, (one, two), _, _ in kinds(k):
            if one[0] == two[0]:
                name, r0, nr, c0, nc = one
                r0 = r0 + n * (nr if nc == D else 0)
                c0 = c0 + n * (0 if nc == D else nc) if nc == D else pl.multiple_of(c0 + n * nc, 256)
                piece = (name, r0, nr, c0 if nc != D else 0, nc)

                @pl.when((m < ITEMS - 1) & cond)
                def _():
                    fn(False, layer, piece, slot)
                if nc == D and nr == TAIL // 2:
                    @pl.when((m == ITEMS - 1) & cond)
                    def _():
                        fn(True, layer, piece, slot)
            else:
                for which, piece in enumerate((one, two)):
                    @pl.when((m < ITEMS) & cond & (n == which))
                    def _():
                        fn(False, layer, piece, slot)

    def view(bufs, name, layer, r0, nr, c0, nc, half):
        if half:
            nr = nr // 2
            r0 = r0 + y * nr
        r0 = pl.multiple_of(r0, 16)
        return bufs[name].at[layer, pl.ds(r0, nr), pl.ds(c0, nc)]

    def remote(src, dst, ss, rs, dev, half):
        def make(whole, layer, piece, slot):
            part = half and not whole
            return pltpu.make_async_remote_copy(
                src_ref=view(src, piece[0], layer, *piece[1:], part),
                dst_ref=view(dst, piece[0], layer, *piece[1:], part),
                send_sem=ss.at[slot], recv_sem=rs.at[slot], device_id=dev, device_id_type=MESH)
        return make

    copy0 = remote(own, b1, s0s, s0r, c_dev, False)
    copy1 = remote(own, b2, s1s, s1r, x_dev, True)
    copy2 = remote(b2, b2, s2s, s2r, y_dev, True)
    copy3 = remote(b2, b3, s3s, s3r, c_dev, False)

    def start0(*a):
        copy0(*a).start()

    def start1(*a):
        copy1(*a).start()

    def wait0(*a):
        copy0(*a).wait_recv()

    def relay2(*a):
        copy1(*a).wait_recv()
        if not a[0]:
            copy2(*a).start()

    def arrived(*a):
        if not a[0]:
            copy2(*a).wait_recv()
        copy1(*a).wait_send()

    def relay3(*a):
        copy3(*a).start()

    def pushed(*a):
        copy0(*a).wait_send()

    def finish(*a):
        copy3(*a).wait_recv()
        copy3(*a).wait_send()

    def sent(*a):
        if not a[0]:
            copy2(*a).wait_send()

    def targets(s):
        i = lax.rem(s, STEPS)
        layer = s // STEPS
        first = layer == 0
        late = 1 - jnp.minimum(layer, 1)
        t2 = jnp.where(i < ST_A, 9 + 2 * i + late,
             jnp.where(i < ST_G + 1, 18 + late + 3 * (i - ST_A) // 5,
             jnp.where(i < ST_D, jnp.maximum(i + 3, 31 + late + (i - ST_G - 1) // 2),
             jnp.where(i < ST_NEAR, jnp.maximum(i, jnp.minimum(ST_D + 2 + (i - ST_D + 1) // 2, ST_D + 4)),
             jnp.where(first, jnp.where(i < ST_NEAR + 2, i, jnp.where(i < ST_READY - 2, 40 + i // 2, jnp.where(i < ST_READY, i - 2,
             jnp.where(i < ST_CROSS, i - 3, jnp.where(i < ST_REST, ST_CROSS - 3 + (i - ST_CROSS) // 2, i - 5))))),
             jnp.where(i < ST_READY - 2, 38 + (i + 1) // 2, 39 + i // 2))))))
        after = jnp.where(i >= ST_FAR, 1, 0) + jnp.where(i >= ST_REST, 1, 0) + jnp.where(i >= ST_REST + 1, 1, 0)
        t3 = jnp.where(i < ST_D, jnp.where(i < ST_A, 3 + i, (t2 - 3) // 2),
             jnp.where(first, jnp.where(i < ST_CROSS, (t2 - 2) // 2, CH_DR + after),
             jnp.where(i < ST_READY - 4, (t2 - 2) // 2, jnp.where(i <= ST_CROSS, 39 + (i - ST_READY + 4) // 3, CH_DR + 1))))
        end = s >= ALL_STEPS - (ST_REST - ST_CROSS - 1)
        t2 = jnp.minimum(t2 + layer * 2 * PER_LAYER, jnp.where(end, ITEMS, ITEMS - 1))
        t3 = jnp.minimum(t3 + layer * PER_LAYER, jnp.where(end, CHUNKS, CHUNKS - 1))
        nxt = jnp.minimum(s + 1, ALL_STEPS - 1)
        i = lax.rem(nxt, STEPS)
        done = jnp.where(i < ST_A, 1 + i,
               jnp.where(i < ST_O, ST_A,
               jnp.where(i < ST_G, 1 + CH_O + i - ST_O,
               jnp.where(i < ST_D, 1 + CH_GU + (i - ST_G) // 2,
               jnp.where(i < ST_NEAR, 1 + CH_D + (i - ST_D) // 2,
               jnp.where(i < ST_READY, CH_D + (i - ST_D) // 2,
               jnp.where(i < ST_READY + 1, CH_DR - 2,
               jnp.where(i < ST_FAR, CH_DR - 1,
               jnp.where(i < ST_REST, CH_DR, PER_LAYER)))))))))
        base = nxt // STEPS * PER_LAYER
        tf = jnp.maximum(t3 - 2, done + base)
        cross = jnp.where(i < ST_READY, 0, jnp.where(i < ST_CROSS, CH_DR - 1, CH_DR))
        t3 = jnp.maximum(jnp.maximum(t3, tf), base + cross)
        return jnp.maximum(t2, 2 * t3), t3, tf

    def relays(old, new):
        @pl.loop(old[0], new[0])
        def _(m):
            with jax.named_scope("r2"):
                for_item(m, relay2)
                for_item(m + AHEAD, start1)
                n = lax.rem(m, 2)
                for_chunk(m // 2 + jnp.where(n == 0, AHEAD0, CHUNKS), start0)
                for_chunk(m // 2 + jnp.where(n == 0, CHUNKS, AHEAD0 - 1), wait0)

        @pl.loop(old[1], new[1])
        def _(k):
            with jax.named_scope("r3"):
                for_pair(k, arrived)
                for_chunk(k, relay3, 3)
                for_chunk(k, pushed)

        @pl.loop(old[2], new[2])
        def _(k):
            with jax.named_scope("fin"):
                for_chunk(k, finish, 3)
                for_pair(k, sent)

    def down_step(i):
        n = i - ST_D - jnp.where(i > ST_READY, 1, 0) - jnp.where(i > ST_IDLE, 1, 0)
        j = n // 2
        near = (i >= ST_NEAR) & (i < ST_NEAR + 2)
        cross = (i >= ST_CROSS) & (i < ST_IDLE)
        far = (i >= ST_FAR) & (i < ST_REST)
        rest = i >= ST_REST
        whole = (i >= ST_D) & (i < ST_CROSS) & ~near & (i != ST_READY)
        return j, jnp.where(i > ST_NEAR, j - 1, j), lax.rem(n + 2 * STEPS, 2), whole, near, cross, far, rest

    def rest_col(side_no):
        return pl.multiple_of(side_no * (2 * FF_ROWS) + 2560, HEAD)

    def tile_col(side_no, core_no, tile):
        return pl.multiple_of(side_no * (2 * FF_ROWS) + core_no * (FF_ROWS + TAIL) + tile * 256, HEAD)

    def load_tile(s):
        layer = s // STEPS
        i = lax.rem(s, STEPS)
        slot = lax.rem(s, 2)

        def cols(name, c0, nc, w0):
            for r, src in enumerate(sources):
                pltpu.make_async_copy(src[name].at[layer, :, pl.ds(c0, nc)],
                                      wbuf.at[slot, pl.ds(r * ROWS, ROWS), pl.ds(w0, nc)], wsem.at[slot]).start()

        @pl.when(i == 0)
        def _():
            cols("k", 0, 256, 0)
            cols("v", 0, 256, 256)

        @pl.when((i >= ST_Q) & (i < ST_A))
        def _():
            cols("q", pl.multiple_of((i - ST_Q) * 512, 512), 512, 0)

        @pl.when((i >= ST_O) & (i < ST_G))
        def _():
            cols("o", pl.multiple_of((i - ST_O) * 512, 512), 512, 0)

        @pl.when((i >= ST_G) & (i < ST_D))
        def _():
            c0 = pl.multiple_of((i - ST_G) * 256, 256)
            cols("g", c0, 256, 0)
            cols("u", c0, 256, 256)

        j, tile, half, whole, near, cross, far, rest = down_step(i)
        dslot = lax.rem(j + 2 * STEPS, 2)

        def rows_in(src, r0, nr, w0):
            pltpu.make_async_copy(src["d"].at[layer, pl.ds(r0, nr), :], dbuf.at[dslot, pl.ds(w0, nr), :], dsem.at[dslot]).start()

        def chunk_rows(r, tile_no, w0):
            src_core = core if r % 2 == 0 else 1 - core
            rows_in(sources[r], pl.multiple_of(src_core * TAIL + tile_no * 256, 64), 256, w0)

        def rest_rows(r, w0):
            src_core = core if r % 2 == 0 else 1 - core
            rows_in(sources[r], pl.multiple_of((1 - src_core) * 2560, 512), TAIL, pl.multiple_of(w0 + src_core * TAIL, 64))

        @pl.when((whole & (half == 0) & (i != ST_READY + 1)) | (i == ST_READY))
        def _():
            for r in range(3):
                chunk_rows(r, jnp.where(i == ST_READY, N_D - 2, tile), r * 256)

        @pl.when(whole & (half == 0))
        def _():
            chunk_rows(3, tile, 768)

        @pl.when(near & (half == 0))
        def _():
            for r in range(2):
                chunk_rows(r, N_D - 1, r * 256)
                rest_rows(r, 512)

        @pl.when(cross & (half == 0))
        def _():
            chunk_rows(2, N_D - 1, 0)

        @pl.when(far & (half == 0))
        def _():
            chunk_rows(3, N_D - 1, 0)

        @pl.when(rest & (half == 0))
        def _():
            for r in range(2):
                rest_rows(2 + r, 0)

    def norm(layer, which):
        @pl.loop(0, TOK // NB)
        def _(m):
            rows = pl.ds(pl.multiple_of(m * NB, NB), NB)
            total = jnp.zeros((NB, 1), F32)
            for b in range(4):
                blk = x_ref[rows, pl.ds(b * ROWS, ROWS)]
                total = total + jnp.sum(blk * blk, axis=1, keepdims=True)
            inv = lax.rsqrt(total * (1.0 / D) + EPS)
            for b in range(4):
                blk = x_ref[rows, pl.ds(b * ROWS, ROWS)]
                gain = gain_ref[which * LAYERS + layer, :, pl.ds(b * ROWS, ROWS)]
                c0 = pl.multiple_of(rel(b) * ROWS, ROWS)
                h_ref[rows, pl.ds(c0, ROWS)] = (blk * inv * gain).astype(BF16)

    def rotate(vals, rows):
        vals = vals.astype(BF16).astype(F32)
        turned = pltpu.roll(vals, HEAD // 2, 1)
        return (vals * cos_ref[rows, :] + turned * sin_ref[rows, :]).astype(BF16)

    def tile_product(slot, finish_rows):
        @pl.loop(0, TOK // MB)
        def _(m):
            rows = pl.ds(pl.multiple_of(m * MB, MB), MB)
            finish_rows(rows, jnp.dot(h_ref[rows, :], wbuf[slot], preferred_element_type=F32))

    def kv_step(slot):
        def fin(rows, acc):
            for b in range(2):
                kv_ref[rows, pl.ds(b * HEAD, HEAD)] = rotate(acc[:, b * HEAD:(b + 1) * HEAD], rows)
            kv_ref[rows, pl.ds(256, 256)] = acc[:, 256:].astype(BF16)
        tile_product(slot, fin)

    def q_step(slot, j):
        def fin(rows, acc):
            for b in range(4):
                c0 = pl.multiple_of(j * 512 + b * HEAD, HEAD)
                q_ref[rows, pl.ds(c0, HEAD)] = rotate(acc[:, b * HEAD:(b + 1) * HEAD], rows)
        tile_product(slot, fin)

    def o_step(slot, j):
        def fin(rows, acc):
            c0 = pl.ds(pl.multiple_of(j * 512, 512), 512)
            x_ref[rows, c0] = x_ref[rows, c0] + acc
        tile_product(slot, fin)

    def g_step(slot, j):
        def fin(rows, acc):
            gate = acc[:, :256]
            up = acc[:, 256:]
            c0 = pl.multiple_of(j * 256, 256)
            a_ref[rows, pl.ds(c0, 256)] = (gate * jax.nn.sigmoid(gate) * up).astype(BF16)
        tile_product(slot, fin)

    def attend(head):
        kv = head // 8
        q0 = pl.multiple_of(head * HEAD, HEAD)
        k0 = pl.multiple_of(kv * HEAD, HEAD)
        v0 = pl.multiple_of(256 + kv * HEAD, HEAD)
        o0 = pl.multiple_of(rel(head // 4) * ROWS + lax.rem(head, 4) * HEAD, HEAD)
        scale = HEAD ** -0.5
        for b in range(TOK // QB):
            keys = (b + 1) * QB
            rows = pl.ds(b * QB, QB)
            scores = lax.dot_general(q_ref[rows, pl.ds(q0, HEAD)], kv_ref[pl.ds(0, keys), pl.ds(k0, HEAD)],
                                     (((1,), (1,)), ((), ())), preferred_element_type=F32)
            key_idx = lax.broadcasted_iota(jnp.int32, (QB, keys), 1)
            row_idx = lax.broadcasted_iota(jnp.int32, (QB, keys), 0) + b * QB
            first = jnp.concatenate([first_ref[rows, :]] * (keys // HEAD), axis=1)
            ok = (key_idx >= first) & (key_idx <= row_idx)
            scores = jnp.where(ok, scores, -1e30)
            top = jnp.max(scores, axis=1, keepdims=True)
            probs = jnp.exp((scores - top) * scale)
            inv = 1.0 / jnp.sum(probs, axis=1, keepdims=True)
            probs = (probs * inv).astype(BF16)
            mixed = jnp.dot(probs, kv_ref[pl.ds(0, keys), pl.ds(v0, HEAD)], preferred_element_type=F32)
            h_ref[rows, pl.ds(o0, HEAD)] = mixed.astype(BF16)

    def add_product(dslot, half, cols):
        rows = pl.ds(pl.multiple_of(half * MB, MB), MB)
        depth = sum(width for _, width in cols)
        lhs = jnp.concatenate([a_ref[rows, pl.ds(c0, width)] for c0, width in cols], axis=1)
        x_ref[rows, :] = x_ref[rows, :] + jnp.dot(lhs, dbuf[dslot, pl.ds(0, depth), :], preferred_element_type=F32)

    def wait_d(dslot, half, depth):
        @pl.when(half == 0)
        def _():
            part = dbuf.at[dslot, pl.ds(0, depth), :]
            pltpu.make_async_copy(part, part, dsem.at[dslot]).wait()

    def last_cols(side_no):
        return [(tile_col(side_no, core, N_D - 1), 256), (tile_col(side_no, 1 - core, N_D - 1), 256)]

    def wait_w(slot):
        pltpu.make_async_copy(wbuf.at[slot], wbuf.at[slot], wsem.at[slot]).wait()

    def step(s):
        before = [jnp.where(s == 0, one, two) for one, two in zip(FIRST, targets(s - 1))]
        relays(before, targets(s))

        @pl.when(s + 1 < ALL_STEPS)
        def _():
            load_tile(s + 1)

        with jax.named_scope("comp"):
            compute(s)

    def compute(s):
        layer = s // STEPS
        i = lax.rem(s, STEPS)
        slot = lax.rem(s, 2)

        @pl.when(((i == 0) & (layer > 0)) | (i == ST_G))
        def _():
            norm(layer, jnp.where(i == 0, 0, 1))

        @pl.when((i < ST_A) | ((i >= ST_O) & (i < ST_D)))
        def _():
            wait_w(slot)

        @pl.when(i == 0)
        def _():
            kv_step(slot)

        @pl.when((i >= ST_Q) & (i < ST_A))
        def _():
            q_step(slot, i - ST_Q)

        @pl.when((i >= ST_A) & (i < ST_O))
        def _():
            attend(i - ST_A)

        @pl.when((i >= ST_O) & (i < ST_G))
        def _():
            o_step(slot, i - ST_O)

        @pl.when((i >= ST_G) & (i < ST_D))
        def _():
            g_step(slot, i - ST_G)

        j, tile, half, whole, near, cross, far, rest = down_step(i)
        dslot = lax.rem(j + 2 * STEPS, 2)

        @pl.when(whole)
        def _():
            wait_d(dslot, half, 1024)
            add_product(dslot, half, [(tile_col(lax.rem(side + r // 2, 2), lax.rem(core + r, 2), tile), 256) for r in range(4)])

        @pl.when(near)
        def _():
            wait_d(dslot, half, NEAR_K)
            add_product(dslot, half, last_cols(side) + [(rest_col(side), REST_K)])

        @pl.when(cross | far)
        def _():
            wait_d(dslot, half, 256)
            add_product(dslot, half, [(tile_col(1 - side, jnp.where(cross, core, 1 - core), N_D - 1), 256)])

        @pl.when(rest)
        def _():
            wait_d(dslot, half, REST_K)
            add_product(dslot, half, [(rest_col(1 - side), REST_K)])

    @pl.loop(0, AHEAD)
    def _(m):
        for_item(m, start1)

    @pl.loop(0, AHEAD0)
    def _(k):
        for_chunk(k, start0)

    for copy in inputs:
        copy.wait()

    for n, ref in enumerate((ga_ref, gm_ref)):
        for layer in range(LAYERS):
            gain_ref[n * LAYERS + layer] = ref[pl.ds(layer, 1), :].astype(F32)
    ids = seg_ref[...].astype(F32)
    lane = lax.broadcasted_iota(jnp.int32, (128, HEAD), 1)
    for b in range(TOK // 128):
        rows = pl.ds(b * 128, 128)
        mine = jnp.transpose(jnp.broadcast_to(ids[b:b + 1, :], (128, 128)))
        before = jnp.zeros((128, 128), F32)
        for c in range(TOK // 128):
            before = before + jnp.where(ids[c:c + 1, :] < mine, 1.0, 0.0)
        first = jnp.sum(before, axis=1, keepdims=True)
        pos = lax.broadcasted_iota(jnp.int32, (128, 128), 0).astype(F32) + (b * 128.0) - first
        angles = pos * freq_ref[...]
        cos_ref[rows, :] = jnp.cos(angles)
        sin = jnp.sin(angles)
        sin_ref[rows, :] = jnp.where(lane < HEAD // 2, -sin, sin)
        first_ref[rows, :] = jnp.broadcast_to(first, (128, 128)).astype(jnp.int32)

    @pl.loop(0, TOK // NB)
    def _(m):
        rows = pl.ds(pl.multiple_of(m * NB, NB), NB)
        x_ref[rows, :] = q_ref[rows, :].astype(F32)

    relays((0, 0, 0), (2, 0, 0))
    norm(0, 0)

    @pl.loop(0, AHEAD0 - 1)
    def _(k):
        for_chunk(k, wait0)

    relays((2, 0, 0), START)
    relays(START, FIRST)
    load_tile(0)

    @pl.loop(0, ALL_STEPS)
    def _(s):
        with jax.named_scope("step"):
            step(s)

    relays(targets(ALL_STEPS - 1), (ITEMS, CHUNKS, CHUNKS))


RESULT_TILES = ((0, 256), (256, 256), (512, 512), (1024, 512), (1536, 512))


def result_kernel(x_ref, a_ref, w2_hbm, w3_hbm, out, y_ref, w_ref, wsem, osem):
    d = lax.axis_index("fsdp")
    core = lax.rem(d, 2)
    c0 = pl.multiple_of((1 - d // 2) * (2 * FF_ROWS) + 2560, HEAD)
    for n, (start, width) in enumerate(RESULT_TILES):
        cols = pl.ds(start, width)
        for src, src_core in ((w2_hbm, core), (w3_hbm, 1 - core)):
            r0 = pl.multiple_of((1 - src_core) * 2560, 512)
            d0 = pl.multiple_of(src_core * TAIL, 64)
            pltpu.make_async_copy(src.at[LAYERS - 1, pl.ds(r0, TAIL), cols], w_ref.at[pl.ds(d0, TAIL), cols], wsem.at[n]).start()

    def store(n, m):
        rows, cols = pl.ds(m * 512, 512), pl.ds(*RESULT_TILES[n])
        return pltpu.make_async_copy(y_ref.at[rows, cols], out.at[rows, cols], osem.at[n, m])

    for n, (start, width) in enumerate(RESULT_TILES):
        cols = pl.ds(start, width)
        pltpu.make_async_copy(w_ref.at[:, cols], w_ref.at[:, cols], wsem.at[n]).wait()
        for m in range(2):
            rows = pl.ds(m * 512, 512)
            y_ref[rows, cols] = x_ref[rows, cols] + jnp.dot(a_ref[rows, pl.ds(c0, REST_K)], w_ref[:, cols], preferred_element_type=F32)
            store(n, m).start()
    for n in range(len(RESULT_TILES)):
        for m in range(2):
            store(n, m).wait()


def run_layers(tokens, seg_ids, g_attn, g_mlp, weights):
    shapes = [jax.ShapeDtypeStruct(w.shape, w.dtype) for w in weights]
    half_dim = HEAD // 2
    freq = np.float32(ROPE_BASE) ** (-np.arange(half_dim, dtype=np.float32) / np.float32(half_dim))
    freq = jnp.asarray(np.concatenate([freq, freq]).reshape(1, HEAD))
    sem = pltpu.SemaphoreType.DMA((SLOTS, 2))
    item_sem = pltpu.SemaphoreType.DMA((ITEM_SLOTS,))
    any_spec = pl.BlockSpec(memory_space=pl.ANY)
    vmem_spec = pl.BlockSpec(memory_space=pltpu.VMEM)
    outs = pl.pallas_call(
        layer_kernel,
        out_shape=[pltpu.VMEM((TOK, D), F32), pltpu.VMEM((TOK, FF), BF16)] + shapes * 3,
        in_specs=[any_spec] * 12,
        out_specs=[vmem_spec] * 2 + [any_spec] * 21,
        scratch_shapes=[
            pltpu.VMEM((TOK, D), BF16),
            pltpu.VMEM((TOK, D), BF16),
            pltpu.VMEM((TOK, 512), BF16),
            pltpu.VMEM((2, D, 512), BF16),
            pltpu.VMEM((2, 1024, D), BF16),
            pltpu.VMEM((TOK, HEAD), F32),
            pltpu.VMEM((TOK, HEAD), F32),
            pltpu.VMEM((TOK, HEAD), jnp.int32),
            pltpu.VMEM((2 * LAYERS, 1, D), F32),
            pltpu.VMEM((TOK // 128, 128), jnp.int32),
            pltpu.VMEM((1, HEAD), F32),
            pltpu.VMEM((LAYERS, D), BF16),
            pltpu.VMEM((LAYERS, D), BF16),
            pltpu.SemaphoreType.DMA((2,)),
            pltpu.SemaphoreType.DMA((2,)),
            pltpu.SemaphoreType.DMA((5,)),
        ] + [sem] * 2 + [item_sem] * 4 + [sem] * 2,
        compiler_params=pltpu.CompilerParams(collective_id=0, has_side_effects=True, vmem_limit_bytes=34 * 1000 * 1000),
        name="two_layers",
    )(tokens, seg_ids.reshape(TOK // 128, 128), freq, g_attn, g_mlp, *weights)
    hidden = pltpu.with_memory_space_constraint(outs[0], pltpu.VMEM)
    act = pltpu.with_memory_space_constraint(outs[1], pltpu.VMEM)
    return pl.pallas_call(
        result_kernel,
        out_shape=jax.ShapeDtypeStruct((TOK, D), F32),
        in_specs=[vmem_spec] * 2 + [any_spec] * 2,
        out_specs=any_spec,
        scratch_shapes=[
            pltpu.VMEM((TOK, D), F32),
            pltpu.VMEM((REST_K, D), BF16),
            pltpu.SemaphoreType.DMA((len(RESULT_TILES),)),
            pltpu.SemaphoreType.DMA((len(RESULT_TILES), 2)),
        ],
        compiler_params=pltpu.CompilerParams(vmem_limit_bytes=24 * 1000 * 1000),
        name="result",
    )(hidden, act, outs[15], outs[22])


def solution(mesh):
    tok_spec = P(("rep", "fsdp"), None)
    seg_spec = P(("rep", "fsdp"))
    mat_spec = P(None, "fsdp", None)
    gain_spec = P(None, None)

    def per_device(tokens, seg_ids, w_q, w_k, w_v, w_o, w_gate, w_up, w_down, g_attn, g_mlp):
        return run_layers(tokens, seg_ids, g_attn, g_mlp, (w_q, w_k, w_v, w_o, w_gate, w_up, w_down))

    return jax.shard_map(per_device, mesh=mesh, in_specs=(tok_spec, seg_spec, mat_spec, mat_spec, mat_spec, mat_spec, mat_spec, mat_spec, mat_spec, gain_spec, gain_spec), out_specs=tok_spec, check_vma=False)
```

```python
import functools

import jax
import jax.numpy as jnp
import numpy as np
from jax import lax
from jax.experimental import pallas as pl
from jax.experimental.pallas import tpu as pltpu
from jax.sharding import PartitionSpec as P

D = 2048
FF = 11008
HEADS = 16
HEAD = 128
TOK = 1024
EPS = 1e-5
ROPE_BASE = 10000.0
MESH = pl.DeviceIdType.MESH
F32 = jnp.float32
BF16 = jnp.bfloat16

LAYERS = 2
SLOTS = 8
ITEM_SLOTS = 2 * SLOTS
AHEAD = 8
AHEAD0 = 5
ROWS = D // 4
FF_ROWS = FF // 4
TAIL = 192
NAMES = ("q", "k", "v", "o", "g", "u", "d")

N_Q = 4
N_GU = 21
N_D = 10
CH_Q = 1
CH_O = CH_Q + N_Q
CH_GU = CH_O + N_Q
CH_GL = CH_GU + N_GU
CH_D = CH_GL + 1
CH_DR = CH_D + N_D
PER_LAYER = CH_DR + 1
CHUNKS = LAYERS * PER_LAYER
ITEMS = 2 * CHUNKS
PUSHES = CHUNKS + 2

NEAR_AT = 5

N_GT = FF // 256
ST_Q = 1
ST_A = ST_Q + N_Q
ST_O = ST_A + HEADS
ST_G = ST_O + 4
ST_D = ST_G + N_GT
ST_NEAR = ST_D + 2 * NEAR_AT
ST_READY = ST_D + 2 * (N_D - 1)
ST_IDLE = ST_READY + 3
ST_FAR = ST_IDLE + 1
ST_REST = ST_FAR + 2
STEPS = ST_REST + 2
ALL_STEPS = LAYERS * STEPS - 2
START = (4, 1, 0)
FIRST = (8, 3, 1)
REST_K = 2 * TAIL
NEAR_K = 512 + REST_K

MB = 512
NB = 128
QB = 256


def layer_kernel(*refs):
    tok, seg, freq, g_attn, g_mlp = refs[:5]
    own = dict(zip(NAMES, refs[5:12]))
    x_ref, a_ref = refs[12:14]
    b1 = dict(zip(NAMES, refs[14:21]))
    b2 = dict(zip(NAMES, refs[21:28]))
    b3 = dict(zip(NAMES, refs[28:35]))
    (h_ref, q_ref, kv_ref, wbuf, dbuf, cos_ref, sin_ref, first_ref, gain_ref,
     seg_ref, freq_ref, ga_ref, gm_ref, wsem, dsem, iosem) = refs[35:51]
    s0s, s0r, s1s, s1r, s2s, s2r, s3s, s3r = refs[51:]
    sources = (own, b1, b2, b3)
    y = lax.axis_index("rep")
    d = lax.axis_index("fsdp")
    side = d // 2
    core = lax.rem(d, 2)
    x_dev = (y, lax.rem(d + 2, 4))
    y_dev = (1 - y, d)
    c_dev = (y, d + 1 - 2 * core)

    def rel(block):
        return 2 * lax.rem(block // 2 + side, 2) + lax.rem(block + core, 2)

    inputs = [pltpu.make_async_copy(src, dst, iosem.at[n]) for n, (src, dst) in enumerate(
        ((tok, q_ref), (seg, seg_ref), (freq, freq_ref), (g_attn, ga_ref), (g_mlp, gm_ref)))]
    for copy in inputs:
        copy.start()

    with jax.named_scope("barrier"):
        barrier = pltpu.get_barrier_semaphore()
        for dev in (x_dev, y_dev, c_dev):
            pl.semaphore_signal(barrier, inc=1, device_id=dev, device_id_type=MESH)
        pl.semaphore_wait(barrier, 3)

    def kinds(k):
        i = lax.rem(k, PER_LAYER)
        jq = pl.multiple_of((i - CH_Q) * 512, 512)
        jo = pl.multiple_of((i - CH_O) * 512, 512)
        jg = pl.multiple_of((i - CH_GU) * 512, 512)
        jd = core * TAIL + (i - CH_D) * 256
        jr = (1 - core) * 2560
        last = N_GU * 512
        kv = [("k", 0, ROWS, 0, 256), ("v", 0, ROWS, 0, 256)]
        gu = [("g", 0, ROWS, jg, 512), ("u", 0, ROWS, jg, 512)]
        gl = [("g", 0, ROWS, last, 256), ("u", 0, ROWS, last, 256)]

        def split_cols(name, c0):
            whole = [(name, 0, ROWS, c0, 512)]
            return [(name, 0, ROWS, c0, 256), (name, 0, ROWS, c0 + 256, 256)], whole, whole

        def split_rows(r0, nr):
            halves = [("d", r0, nr // 2, 0, D), ("d", r0 + nr // 2, nr // 2, 0, D)]
            return halves, [("d", r0, nr, 0, D)], halves

        return [
            (i == 0, kv, kv, kv),
            ((i >= CH_Q) & (i < CH_O), *split_cols("q", jq)),
            ((i >= CH_O) & (i < CH_GU), *split_cols("o", jo)),
            ((i >= CH_GU) & (i < CH_GL), gu, gu, gu),
            (i == CH_GL, gl, gl, gl),
            ((i >= CH_D) & (i < CH_DR), *split_rows(jd, 256)),
            (i == CH_DR, *split_rows(jr, TAIL)),
        ]

    def for_chunk(k, fn, form=2, part=None):
        layer = k // PER_LAYER
        slot = lax.rem(k, SLOTS)
        for kind in kinds(k):
            @pl.when((k < CHUNKS) & kind[0])
            def _():
                for n, piece in enumerate(kind[form]):
                    if part is None:
                        fn(False, layer, piece, (slot, n))
                    else:
                        @pl.when(part != 1 - n)
                        def _():
                            fn(False, layer, piece, (slot, n))

    def for_pair(k, fn, part=None):
        layer = k // PER_LAYER
        table = kinds(k)
        for c, (cond, pieces, _, _) in enumerate(table):
            for end in ((False, True) if c == len(table) - 1 else (None,)):
                here = cond if end is None else cond & ((k == CHUNKS - 1) if end else (k < CHUNKS - 1))

                @pl.when((k < CHUNKS) & here)
                def _():
                    for n, piece in enumerate(pieces):
                        args = (bool(end) and n == 1, layer, piece, (lax.rem(2 * k + n, ITEM_SLOTS),))
                        if part is None:
                            fn(*args)
                        else:
                            @pl.when(part != 1 - n)
                            def _():
                                fn(*args)

    def for_item(m, fn):
        k = m // 2
        n = lax.rem(m, 2)
        layer = k // PER_LAYER
        slot = (lax.rem(m, ITEM_SLOTS),)
        for cond, (one, two), _, _ in kinds(k):
            if one[0] == two[0]:
                name, r0, nr, c0, nc = one
                r0 = r0 + n * (nr if nc == D else 0)
                c0 = c0 + n * (0 if nc == D else nc) if nc == D else pl.multiple_of(c0 + n * nc, 256)
                piece = (name, r0, nr, c0 if nc != D else 0, nc)

                @pl.when((m < ITEMS - 1) & cond)
                def _():
                    fn(False, layer, piece, slot)
                if nc == D and nr == TAIL // 2:
                    @pl.when((m == ITEMS - 1) & cond)
                    def _():
                        fn(True, layer, piece, slot)
            else:
                for which, piece in enumerate((one, two)):
                    @pl.when((m < ITEMS) & cond & (n == which))
                    def _():
                        fn(False, layer, piece, slot)

    def view(bufs, name, layer, r0, nr, c0, nc, half):
        if half:
            nr = nr // 2
            r0 = r0 + y * nr
        r0 = pl.multiple_of(r0, 16)
        return bufs[name].at[layer, pl.ds(r0, nr), pl.ds(c0, nc)]

    def remote(src, dst, ss, rs, dev, half):
        def make(whole, layer, piece, slot):
            part = half and not whole
            return pltpu.make_async_remote_copy(
                src_ref=view(src, piece[0], layer, *piece[1:], part),
                dst_ref=view(dst, piece[0], layer, *piece[1:], part),
                send_sem=ss.at[slot], recv_sem=rs.at[slot], device_id=dev, device_id_type=MESH)
        return make

    copy0 = remote(own, b1, s0s, s0r, c_dev, False)
    copy1 = remote(own, b2, s1s, s1r, x_dev, True)
    copy2 = remote(b2, b2, s2s, s2r, y_dev, True)
    copy3 = remote(b2, b3, s3s, s3r, c_dev, False)

    def start0(*a):
        copy0(*a).start()

    def start1(*a):
        copy1(*a).start()

    def wait0(*a):
        copy0(*a).wait_recv()

    def relay2(*a):
        copy1(*a).wait_recv()
        if not a[0]:
            copy2(*a).start()

    def arrived(*a):
        if not a[0]:
            copy2(*a).wait_recv()
        copy1(*a).wait_send()

    def relay3(*a):
        copy3(*a).start()

    def pushed(*a):
        copy0(*a).wait_send()

    def finish(*a):
        copy3(*a).wait_recv()
        copy3(*a).wait_send()

    def sent(*a):
        if not a[0]:
            copy2(*a).wait_send()

    def targets(s):
        i = lax.rem(s, STEPS)
        layer = s // STEPS
        first = layer == 0
        late = 1 - jnp.minimum(layer, 1)
        t2 = jnp.where(i < ST_A, 9 + 2 * i + late,
             jnp.where(i < ST_G + 1, 18 + late + 3 * (i - ST_A) // 5,
             jnp.where(i < ST_D, jnp.maximum(i + 4, 31 + late + (i - ST_G - 1) // 2),
             jnp.where(i < ST_NEAR, jnp.maximum(i, ST_D + 3 + (2 * (i - ST_D) + 1) // 3),
             jnp.where(first, jnp.where(i < ST_NEAR + 2, i, jnp.where(i < ST_READY - 2, 40 + i // 2, jnp.where(i < ST_READY, i - 2, i - 3))),
             jnp.where(i < ST_READY - 2, 38 + (i + 1) // 2, 39 + i // 2))))))
        final = i == STEPS - 1
        t3 = jnp.where(i < ST_D, jnp.where(i < ST_A, 3 + i, (t2 - 3) // 2),
             jnp.where(first, jnp.where(i < ST_IDLE, (t2 - 2) // 2, CH_DR + (i - ST_IDLE + 1) // 2 + jnp.where(final, 1, 0)),
             jnp.where(i < ST_READY - 4, (t2 - 2) // 2, jnp.where(i < ST_READY + 1, 39 + (i - ST_READY + 4) // 3, i - ST_READY + 40))))
        end = s >= ALL_STEPS - 2
        t2 = jnp.minimum(t2 + layer * 2 * PER_LAYER, jnp.where(end, ITEMS, ITEMS - 1))
        t3 = jnp.minimum(t3 + layer * PER_LAYER, PUSHES)
        nxt = jnp.minimum(s + 1, ALL_STEPS - 1)
        i = lax.rem(nxt, STEPS)
        base = nxt // STEPS * PER_LAYER
        done = jnp.where(i < ST_A, 1 + i,
               jnp.where(i < ST_O, ST_A,
               jnp.where(i < ST_G, 1 + CH_O + i - ST_O,
               jnp.where(i < ST_D, 1 + CH_GU + (i - ST_G) // 2,
               jnp.where(i < ST_NEAR, 1 + CH_D + (i - ST_D) // 2,
               jnp.where(i < ST_READY, CH_D + (i - ST_D) // 2,
               jnp.where(i < ST_READY + 1, CH_DR - 2,
               jnp.where(i < ST_FAR, CH_DR - 1,
               jnp.where(i < ST_REST, CH_DR, PER_LAYER)))))))))
        tf = jnp.maximum(jnp.minimum(t3 - 2, CHUNKS - 2), done + base)
        pushes = tf + jnp.where(tf == CHUNKS - 1, 1, 0)
        t3 = jnp.maximum(jnp.maximum(t3, pushes), base + jnp.where((i >= ST_READY) & (i < ST_FAR), CH_DR - 1, 0))
        return jnp.maximum(t2, 2 * jnp.minimum(t3, CHUNKS - 2)), t3, tf

    def relays(old, new):
        @pl.loop(old[0], new[0])
        def _(m):
            with jax.named_scope("r2"):
                for_item(m, relay2)
                for_item(m + AHEAD, start1)
                n = lax.rem(m, 2)
                for_chunk(m // 2 + jnp.where(n == 0, AHEAD0, CHUNKS), start0)
                for_chunk(m // 2 + jnp.where(n == 0, CHUNKS, AHEAD0 - 1), wait0)

        @pl.loop(old[1], new[1])
        def _(p):
            with jax.named_scope("r3"):
                extra = jnp.maximum(p - (CHUNKS - 2), 0)
                k = p - (extra + 1) // 2
                part = jnp.where(p < CHUNKS - 2, 2, lax.rem(extra, 2))
                for_pair(k, arrived, part)
                for_chunk(k, relay3, 3, part)
                for_chunk(jnp.where(part == 1, CHUNKS, k), pushed)

        @pl.loop(old[2], new[2])
        def _(k):
            with jax.named_scope("fin"):
                for_chunk(k, finish, 3)
                for_pair(k, sent)

    def down_step(i):
        n = i - ST_D - jnp.where(i > ST_READY, 1, 0) - jnp.where(i > ST_IDLE, 1, 0)
        j = n // 2
        near = (i >= ST_NEAR) & (i < ST_NEAR + 2)
        far = (i >= ST_FAR) & (i < ST_REST)
        rest = i >= ST_REST
        whole = (i >= ST_D) & (i < ST_IDLE) & ~near & (i != ST_READY)
        return j, jnp.where(i > ST_NEAR, j - 1, j), lax.rem(n + 2 * STEPS, 2), whole, near, far, rest

    def rest_col(side_no):
        return pl.multiple_of(side_no * (2 * FF_ROWS) + 2560, HEAD)

    def tile_col(side_no, core_no, tile):
        return pl.multiple_of(side_no * (2 * FF_ROWS) + core_no * (FF_ROWS + TAIL) + tile * 256, HEAD)

    def load_tile(s):
        layer = s // STEPS
        i = lax.rem(s, STEPS)
        slot = lax.rem(s, 2)

        def cols(name, c0, nc, w0):
            for r, src in enumerate(sources):
                pltpu.make_async_copy(src[name].at[layer, :, pl.ds(c0, nc)],
                                      wbuf.at[slot, pl.ds(r * ROWS, ROWS), pl.ds(w0, nc)], wsem.at[slot]).start()

        @pl.when(i == 0)
        def _():
            cols("k", 0, 256, 0)
            cols("v", 0, 256, 256)

        @pl.when((i >= ST_Q) & (i < ST_A))
        def _():
            cols("q", pl.multiple_of((i - ST_Q) * 512, 512), 512, 0)

        @pl.when((i >= ST_O) & (i < ST_G))
        def _():
            cols("o", pl.multiple_of((i - ST_O) * 512, 512), 512, 0)

        @pl.when((i >= ST_G) & (i < ST_D))
        def _():
            c0 = pl.multiple_of((i - ST_G) * 256, 256)
            cols("g", c0, 256, 0)
            cols("u", c0, 256, 256)

        j, tile, half, whole, near, far, rest = down_step(i)
        dslot = lax.rem(j + 2 * STEPS, 2)

        def rows_in(src, r0, nr, w0):
            pltpu.make_async_copy(src["d"].at[layer, pl.ds(r0, nr), :], dbuf.at[dslot, pl.ds(w0, nr), :], dsem.at[dslot]).start()

        def chunk_rows(r, tile_no, w0):
            src_core = core if r % 2 == 0 else 1 - core
            rows_in(sources[r], pl.multiple_of(src_core * TAIL + tile_no * 256, 64), 256, w0)

        def rest_rows(r, w0):
            src_core = core if r % 2 == 0 else 1 - core
            rows_in(sources[r], pl.multiple_of((1 - src_core) * 2560, 512), TAIL, pl.multiple_of(w0 + src_core * TAIL, 64))

        @pl.when((whole & (half == 0) & (i != ST_READY + 1)) | (i == ST_READY))
        def _():
            for r in range(3):
                chunk_rows(r, jnp.where(i == ST_READY, N_D - 2, tile), r * 256)

        @pl.when(whole & (half == 0))
        def _():
            chunk_rows(3, tile, 768)

        @pl.when(near & (half == 0))
        def _():
            for r in range(2):
                chunk_rows(r, N_D - 1, r * 256)
                rest_rows(r, 512)

        @pl.when(far & (half == 0))
        def _():
            for r in range(2):
                chunk_rows(2 + r, N_D - 1, r * 256)

        @pl.when(rest & (half == 0))
        def _():
            for r in range(2):
                rest_rows(2 + r, 0)

    def norm(layer, which):
        @pl.loop(0, TOK // NB)
        def _(m):
            rows = pl.ds(pl.multiple_of(m * NB, NB), NB)
            total = jnp.zeros((NB, 1), F32)
            for b in range(4):
                blk = x_ref[rows, pl.ds(b * ROWS, ROWS)]
                total = total + jnp.sum(blk * blk, axis=1, keepdims=True)
            inv = lax.rsqrt(total * (1.0 / D) + EPS)
            for b in range(4):
                blk = x_ref[rows, pl.ds(b * ROWS, ROWS)]
                gain = gain_ref[which * LAYERS + layer, :, pl.ds(b * ROWS, ROWS)]
                c0 = pl.multiple_of(rel(b) * ROWS, ROWS)
                h_ref[rows, pl.ds(c0, ROWS)] = (blk * inv * gain).astype(BF16)

    def rotate(vals, rows):
        vals = vals.astype(BF16).astype(F32)
        turned = pltpu.roll(vals, HEAD // 2, 1)
        return (vals * cos_ref[rows, :] + turned * sin_ref[rows, :]).astype(BF16)

    def tile_product(slot, finish_rows):
        @pl.loop(0, TOK // MB)
        def _(m):
            rows = pl.ds(pl.multiple_of(m * MB, MB), MB)
            finish_rows(rows, jnp.dot(h_ref[rows, :], wbuf[slot], preferred_element_type=F32))

    def kv_step(slot):
        def fin(rows, acc):
            for b in range(2):
                kv_ref[rows, pl.ds(b * HEAD, HEAD)] = rotate(acc[:, b * HEAD:(b + 1) * HEAD], rows)
            kv_ref[rows, pl.ds(256, 256)] = acc[:, 256:].astype(BF16)
        tile_product(slot, fin)

    def q_step(slot, j):
        def fin(rows, acc):
            for b in range(4):
                c0 = pl.multiple_of(j * 512 + b * HEAD, HEAD)
                q_ref[rows, pl.ds(c0, HEAD)] = rotate(acc[:, b * HEAD:(b + 1) * HEAD], rows)
        tile_product(slot, fin)

    def o_step(slot, j):
        def fin(rows, acc):
            c0 = pl.ds(pl.multiple_of(j * 512, 512), 512)
            x_ref[rows, c0] = x_ref[rows, c0] + acc
        tile_product(slot, fin)

    def g_step(slot, j):
        def fin(rows, acc):
            gate = acc[:, :256]
            up = acc[:, 256:]
            c0 = pl.multiple_of(j * 256, 256)
            a_ref[rows, pl.ds(c0, 256)] = (gate * jax.nn.sigmoid(gate) * up).astype(BF16)
        tile_product(slot, fin)

    def attend(head):
        kv = head // 8
        q0 = pl.multiple_of(head * HEAD, HEAD)
        k0 = pl.multiple_of(kv * HEAD, HEAD)
        v0 = pl.multiple_of(256 + kv * HEAD, HEAD)
        o0 = pl.multiple_of(rel(head // 4) * ROWS + lax.rem(head, 4) * HEAD, HEAD)
        scale = HEAD ** -0.5
        for b in range(TOK // QB):
            keys = (b + 1) * QB
            rows = pl.ds(b * QB, QB)
            scores = lax.dot_general(q_ref[rows, pl.ds(q0, HEAD)], kv_ref[pl.ds(0, keys), pl.ds(k0, HEAD)],
                                     (((1,), (1,)), ((), ())), preferred_element_type=F32)
            key_idx = lax.broadcasted_iota(jnp.int32, (QB, keys), 1)
            row_idx = lax.broadcasted_iota(jnp.int32, (QB, keys), 0) + b * QB
            first = jnp.concatenate([first_ref[rows, :]] * (keys // HEAD), axis=1)
            ok = (key_idx >= first) & (key_idx <= row_idx)
            scores = jnp.where(ok, scores, -1e30)
            top = jnp.max(scores, axis=1, keepdims=True)
            probs = jnp.exp((scores - top) * scale)
            inv = 1.0 / jnp.sum(probs, axis=1, keepdims=True)
            probs = (probs * inv).astype(BF16)
            mixed = jnp.dot(probs, kv_ref[pl.ds(0, keys), pl.ds(v0, HEAD)], preferred_element_type=F32)
            h_ref[rows, pl.ds(o0, HEAD)] = mixed.astype(BF16)

    def add_product(dslot, half, cols):
        rows = pl.ds(pl.multiple_of(half * MB, MB), MB)
        depth = sum(width for _, width in cols)
        lhs = jnp.concatenate([a_ref[rows, pl.ds(c0, width)] for c0, width in cols], axis=1)
        x_ref[rows, :] = x_ref[rows, :] + jnp.dot(lhs, dbuf[dslot, pl.ds(0, depth), :], preferred_element_type=F32)

    def wait_d(dslot, half, depth):
        @pl.when(half == 0)
        def _():
            part = dbuf.at[dslot, pl.ds(0, depth), :]
            pltpu.make_async_copy(part, part, dsem.at[dslot]).wait()

    def last_cols(side_no):
        return [(tile_col(side_no, core, N_D - 1), 256), (tile_col(side_no, 1 - core, N_D - 1), 256)]

    def wait_w(slot):
        pltpu.make_async_copy(wbuf.at[slot], wbuf.at[slot], wsem.at[slot]).wait()

    def step(s):
        before = [jnp.where(s == 0, one, two) for one, two in zip(FIRST, targets(s - 1))]
        relays(before, targets(s))

        @pl.when(s + 1 < ALL_STEPS)
        def _():
            load_tile(s + 1)

        with jax.named_scope("comp"):
            compute(s)

    def compute(s):
        layer = s // STEPS
        i = lax.rem(s, STEPS)
        slot = lax.rem(s, 2)

        @pl.when(((i == 0) & (layer > 0)) | (i == ST_G))
        def _():
            norm(layer, jnp.where(i == 0, 0, 1))

        @pl.when((i < ST_A) | ((i >= ST_O) & (i < ST_D)))
        def _():
            wait_w(slot)

        @pl.when(i == 0)
        def _():
            kv_step(slot)

        @pl.when((i >= ST_Q) & (i < ST_A))
        def _():
            q_step(slot, i - ST_Q)

        @pl.when((i >= ST_A) & (i < ST_O))
        def _():
            attend(i - ST_A)

        @pl.when((i >= ST_O) & (i < ST_G))
        def _():
            o_step(slot, i - ST_O)

        @pl.when((i >= ST_G) & (i < ST_D))
        def _():
            g_step(slot, i - ST_G)

        j, tile, half, whole, near, far, rest = down_step(i)
        dslot = lax.rem(j + 2 * STEPS, 2)

        @pl.when(whole)
        def _():
            wait_d(dslot, half, 1024)
            add_product(dslot, half, [(tile_col(lax.rem(side + r // 2, 2), lax.rem(core + r, 2), tile), 256) for r in range(4)])

        @pl.when(near)
        def _():
            wait_d(dslot, half, NEAR_K)
            add_product(dslot, half, last_cols(side) + [(rest_col(side), REST_K)])

        @pl.when(far)
        def _():
            wait_d(dslot, half, 512)
            add_product(dslot, half, last_cols(1 - side))

        @pl.when(rest)
        def _():
            wait_d(dslot, half, REST_K)
            add_product(dslot, half, [(rest_col(1 - side), REST_K)])

    @pl.loop(0, AHEAD)
    def _(m):
        for_item(m, start1)

    @pl.loop(0, AHEAD0)
    def _(k):
        for_chunk(k, start0)

    for copy in inputs:
        copy.wait()

    for n, ref in enumerate((ga_ref, gm_ref)):
        for layer in range(LAYERS):
            gain_ref[n * LAYERS + layer] = ref[pl.ds(layer, 1), :].astype(F32)
    ids = seg_ref[...].astype(F32)
    lane = lax.broadcasted_iota(jnp.int32, (128, HEAD), 1)
    for b in range(TOK // 128):
        rows = pl.ds(b * 128, 128)
        mine = jnp.transpose(jnp.broadcast_to(ids[b:b + 1, :], (128, 128)))
        before = jnp.zeros((128, 128), F32)
        for c in range(TOK // 128):
            before = before + jnp.where(ids[c:c + 1, :] < mine, 1.0, 0.0)
        first = jnp.sum(before, axis=1, keepdims=True)
        pos = lax.broadcasted_iota(jnp.int32, (128, 128), 0).astype(F32) + (b * 128.0) - first
        angles = pos * freq_ref[...]
        cos_ref[rows, :] = jnp.cos(angles)
        sin = jnp.sin(angles)
        sin_ref[rows, :] = jnp.where(lane < HEAD // 2, -sin, sin)
        first_ref[rows, :] = jnp.broadcast_to(first, (128, 128)).astype(jnp.int32)

    @pl.loop(0, TOK // NB)
    def _(m):
        rows = pl.ds(pl.multiple_of(m * NB, NB), NB)
        x_ref[rows, :] = q_ref[rows, :].astype(F32)

    relays((0, 0, 0), (2, 0, 0))
    norm(0, 0)

    @pl.loop(0, AHEAD0 - 1)
    def _(k):
        for_chunk(k, wait0)

    relays((2, 0, 0), START)
    relays(START, FIRST)
    load_tile(0)

    @pl.loop(0, ALL_STEPS)
    def _(s):
        with jax.named_scope("step"):
            step(s)

    relays(targets(ALL_STEPS - 1), (ITEMS, PUSHES, CHUNKS))


def result_kernel(x_ref, a_ref, w2_hbm, w3_hbm, out, y_ref, w_ref, wsem, osem):
    d = lax.axis_index("fsdp")
    core = lax.rem(d, 2)
    c0 = pl.multiple_of((1 - d // 2) * (2 * FF_ROWS) + 2560, HEAD)
    for n in range(4):
        cols = pl.ds(n * 512, 512)
        for src, src_core in ((w2_hbm, core), (w3_hbm, 1 - core)):
            r0 = pl.multiple_of((1 - src_core) * 2560, 512)
            d0 = pl.multiple_of(src_core * TAIL, 64)
            pltpu.make_async_copy(src.at[LAYERS - 1, pl.ds(r0, TAIL), cols], w_ref.at[n, pl.ds(d0, TAIL), :], wsem.at[n]).start()

    def store(n, m):
        rows, cols = pl.ds(m * 512, 512), pl.ds(n * 512, 512)
        return pltpu.make_async_copy(y_ref.at[rows, cols], out.at[rows, cols], osem.at[n, m])

    for n in range(4):
        cols = pl.ds(n * 512, 512)
        pltpu.make_async_copy(w_ref.at[n], w_ref.at[n], wsem.at[n]).wait()
        for m in range(2):
            rows = pl.ds(m * 512, 512)
            y_ref[rows, cols] = x_ref[rows, cols] + jnp.dot(a_ref[rows, pl.ds(c0, REST_K)], w_ref[n], preferred_element_type=F32)
            store(n, m).start()
    for n in range(4):
        for m in range(2):
            store(n, m).wait()


def run_layers(tokens, seg_ids, g_attn, g_mlp, weights):
    shapes = [jax.ShapeDtypeStruct(w.shape, w.dtype) for w in weights]
    half_dim = HEAD // 2
    freq = np.float32(ROPE_BASE) ** (-np.arange(half_dim, dtype=np.float32) / np.float32(half_dim))
    freq = jnp.asarray(np.concatenate([freq, freq]).reshape(1, HEAD))
    sem = pltpu.SemaphoreType.DMA((SLOTS, 2))
    item_sem = pltpu.SemaphoreType.DMA((ITEM_SLOTS,))
    any_spec = pl.BlockSpec(memory_space=pl.ANY)
    vmem_spec = pl.BlockSpec(memory_space=pltpu.VMEM)
    outs = pl.pallas_call(
        layer_kernel,
        out_shape=[pltpu.VMEM((TOK, D), F32), pltpu.VMEM((TOK, FF), BF16)] + shapes * 3,
        in_specs=[any_spec] * 12,
        out_specs=[vmem_spec] * 2 + [any_spec] * 21,
        scratch_shapes=[
            pltpu.VMEM((TOK, D), BF16),
            pltpu.VMEM((TOK, D), BF16),
            pltpu.VMEM((TOK, 512), BF16),
            pltpu.VMEM((2, D, 512), BF16),
            pltpu.VMEM((2, 1024, D), BF16),
            pltpu.VMEM((TOK, HEAD), F32),
            pltpu.VMEM((TOK, HEAD), F32),
            pltpu.VMEM((TOK, HEAD), jnp.int32),
            pltpu.VMEM((2 * LAYERS, 1, D), F32),
            pltpu.VMEM((TOK // 128, 128), jnp.int32),
            pltpu.VMEM((1, HEAD), F32),
            pltpu.VMEM((LAYERS, D), BF16),
            pltpu.VMEM((LAYERS, D), BF16),
            pltpu.SemaphoreType.DMA((2,)),
            pltpu.SemaphoreType.DMA((2,)),
            pltpu.SemaphoreType.DMA((5,)),
        ] + [sem] * 2 + [item_sem] * 4 + [sem] * 2,
        compiler_params=pltpu.CompilerParams(collective_id=0, has_side_effects=True, vmem_limit_bytes=34 * 1000 * 1000),
        name="two_layers",
    )(tokens, seg_ids.reshape(TOK // 128, 128), freq, g_attn, g_mlp, *weights)
    hidden = pltpu.with_memory_space_constraint(outs[0], pltpu.VMEM)
    act = pltpu.with_memory_space_constraint(outs[1], pltpu.VMEM)
    return pl.pallas_call(
        result_kernel,
        out_shape=jax.ShapeDtypeStruct((TOK, D), F32),
        in_specs=[vmem_spec] * 2 + [any_spec] * 2,
        out_specs=any_spec,
        scratch_shapes=[
            pltpu.VMEM((TOK, D), F32),
            pltpu.VMEM((4, REST_K, 512), BF16),
            pltpu.SemaphoreType.DMA((4,)),
            pltpu.SemaphoreType.DMA((4, 2)),
        ],
        compiler_params=pltpu.CompilerParams(vmem_limit_bytes=24 * 1000 * 1000),
        name="result",
    )(hidden, act, outs[15], outs[22])


def solution(mesh):
    tok_spec = P(("rep", "fsdp"), None)
    seg_spec = P(("rep", "fsdp"))
    mat_spec = P(None, "fsdp", None)
    gain_spec = P(None, None)

    def per_device(tokens, seg_ids, w_q, w_k, w_v, w_o, w_gate, w_up, w_down, g_attn, g_mlp):
        return run_layers(tokens, seg_ids, g_attn, g_mlp, (w_q, w_k, w_v, w_o, w_gate, w_up, w_down))

    return jax.shard_map(per_device, mesh=mesh, in_specs=(tok_spec, seg_spec, mat_spec, mat_spec, mat_spec, mat_spec, mat_spec, mat_spec, mat_spec, gain_spec, gain_spec), out_specs=tok_spec, check_vma=False)
```

```python
import functools

import jax
import jax.numpy as jnp
import numpy as np
from jax import lax
from jax.experimental import pallas as pl
from jax.experimental.pallas import tpu as pltpu
from jax.sharding import PartitionSpec as P

D = 2048
FF = 11008
HEADS = 16
HEAD = 128
TOK = 1024
EPS = 1e-5
ROPE_BASE = 10000.0
MESH = pl.DeviceIdType.MESH
F32 = jnp.float32
BF16 = jnp.bfloat16

LAYERS = 2
SLOTS = 8
ITEM_SLOTS = 2 * SLOTS
AHEAD = 8
AHEAD0 = 5
ROWS = D // 4
FF_ROWS = FF // 4
TAIL = 192
NAMES = ("q", "k", "v", "o", "g", "u", "d")

N_Q = 4
N_GU = 21
N_D = 10
CH_Q = 1
CH_O = CH_Q + N_Q
CH_GU = CH_O + N_Q
CH_GL = CH_GU + N_GU
CH_D = CH_GL + 1
CH_DR = CH_D + N_D
PER_LAYER = CH_DR + 1
CHUNKS = LAYERS * PER_LAYER
ITEMS = 2 * CHUNKS
PUSHES = CHUNKS + 2

NEAR_AT = 5

N_GT = FF // 256
ST_Q = 1
ST_A = ST_Q + N_Q
ST_O = ST_A + HEADS
ST_G = ST_O + 4
ST_D = ST_G + N_GT
ST_NEAR = ST_D + 2 * NEAR_AT
ST_READY = ST_D + 2 * (N_D - 1)
ST_IDLE = ST_READY + 3
ST_FAR = ST_IDLE + 1
ST_REST = ST_FAR + 2
STEPS = ST_REST + 2
ALL_STEPS = LAYERS * STEPS - 2
START = (4, 1, 0)
FIRST = (8, 3, 1)
REST_K = 2 * TAIL
NEAR_K = 512 + REST_K

MB = 512
NB = 128
QB = 256


def layer_kernel(*refs):
    tok, seg, freq, g_attn, g_mlp = refs[:5]
    own = dict(zip(NAMES, refs[5:12]))
    x_ref, a_ref = refs[12:14]
    b1 = dict(zip(NAMES, refs[14:21]))
    b2 = dict(zip(NAMES, refs[21:28]))
    b3 = dict(zip(NAMES, refs[28:35]))
    (h_ref, q_ref, kv_ref, wbuf, dbuf, cos_ref, sin_ref, first_ref, gain_ref,
     seg_ref, freq_ref, ga_ref, gm_ref, wsem, dsem, iosem) = refs[35:51]
    s0s, s0r, s1s, s1r, s2s, s2r, s3s, s3r = refs[51:]
    sources = (own, b1, b2, b3)
    y = lax.axis_index("rep")
    d = lax.axis_index("fsdp")
    side = d // 2
    core = lax.rem(d, 2)
    x_dev = (y, lax.rem(d + 2, 4))
    y_dev = (1 - y, d)
    c_dev = (y, d + 1 - 2 * core)

    def rel(block):
        return 2 * lax.rem(block // 2 + side, 2) + lax.rem(block + core, 2)

    inputs = [pltpu.make_async_copy(src, dst, iosem.at[n]) for n, (src, dst) in enumerate(
        ((tok, q_ref), (seg, seg_ref), (freq, freq_ref), (g_attn, ga_ref), (g_mlp, gm_ref)))]
    for copy in inputs:
        copy.start()

    with jax.named_scope("barrier"):
        barrier = pltpu.get_barrier_semaphore()
        for dev in (x_dev, y_dev, c_dev):
            pl.semaphore_signal(barrier, inc=1, device_id=dev, device_id_type=MESH)
        pl.semaphore_wait(barrier, 3)

    def kinds(k):
        i = lax.rem(k, PER_LAYER)
        jq = pl.multiple_of((i - CH_Q) * 512, 512)
        jo = pl.multiple_of((i - CH_O) * 512, 512)
        jg = pl.multiple_of((i - CH_GU) * 512, 512)
        jd = core * TAIL + (i - CH_D) * 256
        jr = (1 - core) * 2560
        last = N_GU * 512
        kv = [("k", 0, ROWS, 0, 256), ("v", 0, ROWS, 0, 256)]
        gu = [("g", 0, ROWS, jg, 512), ("u", 0, ROWS, jg, 512)]
        gl = [("g", 0, ROWS, last, 256), ("u", 0, ROWS, last, 256)]

        def split_cols(name, c0):
            whole = [(name, 0, ROWS, c0, 512)]
            return [(name, 0, ROWS, c0, 256), (name, 0, ROWS, c0 + 256, 256)], whole, whole

        def split_rows(r0, nr):
            halves = [("d", r0, nr // 2, 0, D), ("d", r0 + nr // 2, nr // 2, 0, D)]
            return halves, [("d", r0, nr, 0, D)], halves

        return [
            (i == 0, kv, kv, kv),
            ((i >= CH_Q) & (i < CH_O), *split_cols("q", jq)),
            ((i >= CH_O) & (i < CH_GU), *split_cols("o", jo)),
            ((i >= CH_GU) & (i < CH_GL), gu, gu, gu),
            (i == CH_GL, gl, gl, gl),
            ((i >= CH_D) & (i < CH_DR), *split_rows(jd, 256)),
            (i == CH_DR, *split_rows(jr, TAIL)),
        ]

    def for_chunk(k, fn, form=2, part=None):
        layer = k // PER_LAYER
        slot = lax.rem(k, SLOTS)
        for kind in kinds(k):
            @pl.when((k < CHUNKS) & kind[0])
            def _():
                for n, piece in enumerate(kind[form]):
                    if part is None:
                        fn(False, layer, piece, (slot, n))
                    else:
                        @pl.when(part != 1 - n)
                        def _():
                            fn(False, layer, piece, (slot, n))

    def for_pair(k, fn, part=None):
        layer = k // PER_LAYER
        table = kinds(k)
        for c, (cond, pieces, _, _) in enumerate(table):
            for end in ((False, True) if c == len(table) - 1 else (None,)):
                here = cond if end is None else cond & ((k == CHUNKS - 1) if end else (k < CHUNKS - 1))

                @pl.when((k < CHUNKS) & here)
                def _():
                    for n, piece in enumerate(pieces):
                        args = (bool(end) and n == 1, layer, piece, (lax.rem(2 * k + n, ITEM_SLOTS),))
                        if part is None:
                            fn(*args)
                        else:
                            @pl.when(part != 1 - n)
                            def _():
                                fn(*args)

    def for_item(m, fn):
        k = m // 2
        n = lax.rem(m, 2)
        layer = k // PER_LAYER
        slot = (lax.rem(m, ITEM_SLOTS),)
        for cond, (one, two), _, _ in kinds(k):
            if one[0] == two[0]:
                name, r0, nr, c0, nc = one
                r0 = r0 + n * (nr if nc == D else 0)
                c0 = c0 + n * (0 if nc == D else nc) if nc == D else pl.multiple_of(c0 + n * nc, 256)
                piece = (name, r0, nr, c0 if nc != D else 0, nc)

                @pl.when((m < ITEMS - 1) & cond)
                def _():
                    fn(False, layer, piece, slot)
                if nc == D and nr == TAIL // 2:
                    @pl.when((m == ITEMS - 1) & cond)
                    def _():
                        fn(True, layer, piece, slot)
            else:
                for which, piece in enumerate((one, two)):
                    @pl.when((m < ITEMS) & cond & (n == which))
                    def _():
                        fn(False, layer, piece, slot)

    def view(bufs, name, layer, r0, nr, c0, nc, half):
        if half:
            nr = nr // 2
            r0 = r0 + y * nr
        r0 = pl.multiple_of(r0, 16)
        return bufs[name].at[layer, pl.ds(r0, nr), pl.ds(c0, nc)]

    def remote(src, dst, ss, rs, dev, half):
        def make(whole, layer, piece, slot):
            part = half and not whole
            return pltpu.make_async_remote_copy(
                src_ref=view(src, piece[0], layer, *piece[1:], part),
                dst_ref=view(dst, piece[0], layer, *piece[1:], part),
                send_sem=ss.at[slot], recv_sem=rs.at[slot], device_id=dev, device_id_type=MESH)
        return make

    copy0 = remote(own, b1, s0s, s0r, c_dev, False)
    copy1 = remote(own, b2, s1s, s1r, x_dev, True)
    copy2 = remote(b2, b2, s2s, s2r, y_dev, True)
    copy3 = remote(b2, b3, s3s, s3r, c_dev, False)

    def start0(*a):
        copy0(*a).start()

    def start1(*a):
        copy1(*a).start()

    def wait0(*a):
        copy0(*a).wait_recv()

    def relay2(*a):
        copy1(*a).wait_recv()
        if not a[0]:
            copy2(*a).start()

    def arrived(*a):
        if not a[0]:
            copy2(*a).wait_recv()
        copy1(*a).wait_send()

    def relay3(*a):
        copy3(*a).start()

    def pushed(*a):
        copy0(*a).wait_send()

    def finish(*a):
        copy3(*a).wait_recv()
        copy3(*a).wait_send()

    def sent(*a):
        if not a[0]:
            copy2(*a).wait_send()

    def targets(s):
        i = lax.rem(s, STEPS)
        layer = s // STEPS
        first = layer == 0
        late = 1 - jnp.minimum(layer, 1)
        t2 = jnp.where(i < ST_A, 9 + 2 * i + late,
             jnp.where(i < ST_G + 1, 18 + late + 3 * (i - ST_A) // 5,
             jnp.where(i < ST_D, jnp.maximum(i + 4, 31 + late + (i - ST_G - 1) // 2),
             jnp.where(i < ST_NEAR, jnp.maximum(i, ST_D + 3 + (2 * (i - ST_D) + 1) // 3),
             jnp.where(first, jnp.where(i < ST_NEAR + 2, i, jnp.where(i < ST_READY - 2, 40 + i // 2, jnp.where(i < ST_READY, i - 2, i - 3))),
             jnp.where(i < ST_READY - 2, 38 + (i + 1) // 2, 39 + i // 2))))))
        final = i == STEPS - 1
        t3 = jnp.where(i < ST_D, jnp.where(i < ST_A, 3 + i, (t2 - 3) // 2),
             jnp.where(first, jnp.where(i < ST_IDLE, (t2 - 2) // 2, CH_DR + (i - ST_IDLE + 1) // 2 + jnp.where(final, 1, 0)),
             jnp.where(i < ST_READY - 4, (t2 - 2) // 2, jnp.where(i < ST_READY + 2, 39 + (i - ST_READY + 4) // 3, i - ST_READY + 39 + jnp.where(i == ST_FAR, 1, 0)))))
        end = s >= ALL_STEPS - 2
        t2 = jnp.minimum(t2 + layer * 2 * PER_LAYER, jnp.where(end, ITEMS, ITEMS - 1))
        t3 = jnp.minimum(t3 + layer * PER_LAYER, PUSHES)
        nxt = jnp.minimum(s + 1, ALL_STEPS - 1)
        i = lax.rem(nxt, STEPS)
        base = nxt // STEPS * PER_LAYER
        done = jnp.where(i < ST_A, 1 + i,
               jnp.where(i < ST_O, ST_A,
               jnp.where(i < ST_G, 1 + CH_O + i - ST_O,
               jnp.where(i < ST_D, 1 + CH_GU + (i - ST_G) // 2,
               jnp.where(i < ST_NEAR, 1 + CH_D + (i - ST_D) // 2,
               jnp.where(i < ST_READY, CH_D + (i - ST_D) // 2,
               jnp.where(i < ST_READY + 1, CH_DR - 2,
               jnp.where(i < ST_FAR, CH_DR - 1,
               jnp.where(i < ST_REST, CH_DR, PER_LAYER)))))))))
        tf = jnp.maximum(jnp.minimum(t3 - 2, CHUNKS - 2), done + base)
        pushes = tf + jnp.where(tf == CHUNKS - 1, 1, 0)
        t3 = jnp.maximum(jnp.maximum(t3, pushes), base + jnp.where((i >= ST_READY) & (i < ST_FAR), CH_DR - 1, 0))
        return jnp.maximum(t2, 2 * jnp.minimum(t3, CHUNKS - 2)), t3, tf

    def relays(old, new):
        @pl.loop(old[0], new[0])
        def _(m):
            with jax.named_scope("r2"):
                for_item(m, relay2)
                for_item(m + AHEAD, start1)
                n = lax.rem(m, 2)
                for_chunk(m // 2 + jnp.where(n == 0, AHEAD0, CHUNKS), start0)
                for_chunk(m // 2 + jnp.where(n == 0, CHUNKS, AHEAD0 - 1), wait0)

        @pl.loop(old[1], new[1])
        def _(p):
            with jax.named_scope("r3"):
                extra = jnp.maximum(p - (CHUNKS - 2), 0)
                k = p - (extra + 1) // 2
                part = jnp.where(p < CHUNKS - 2, 2, lax.rem(extra, 2))
                for_pair(k, arrived, part)
                for_chunk(k, relay3, 3, part)
                for_chunk(jnp.where(part == 1, CHUNKS, k), pushed)

        @pl.loop(old[2], new[2])
        def _(k):
            with jax.named_scope("fin"):
                for_chunk(k, finish, 3)
                for_pair(k, sent)

    def down_step(i):
        n = i - ST_D - jnp.where(i > ST_READY, 1, 0) - jnp.where(i > ST_IDLE, 1, 0)
        j = n // 2
        near = (i >= ST_NEAR) & (i < ST_NEAR + 2)
        far = (i >= ST_FAR) & (i < ST_REST)
        rest = i >= ST_REST
        whole = (i >= ST_D) & (i < ST_IDLE) & ~near & (i != ST_READY)
        return j, jnp.where(i > ST_NEAR, j - 1, j), lax.rem(n + 2 * STEPS, 2), whole, near, far, rest

    def rest_col(side_no):
        return pl.multiple_of(side_no * (2 * FF_ROWS) + 2560, HEAD)

    def tile_col(side_no, core_no, tile):
        return pl.multiple_of(side_no * (2 * FF_ROWS) + core_no * (FF_ROWS + TAIL) + tile * 256, HEAD)

    def load_tile(s):
        layer = s // STEPS
        i = lax.rem(s, STEPS)
        slot = lax.rem(s, 2)

        def cols(name, c0, nc, w0):
            for r, src in enumerate(sources):
                pltpu.make_async_copy(src[name].at[layer, :, pl.ds(c0, nc)],
                                      wbuf.at[slot, pl.ds(r * ROWS, ROWS), pl.ds(w0, nc)], wsem.at[slot]).start()

        @pl.when(i == 0)
        def _():
            cols("k", 0, 256, 0)
            cols("v", 0, 256, 256)

        @pl.when((i >= ST_Q) & (i < ST_A))
        def _():
            cols("q", pl.multiple_of((i - ST_Q) * 512, 512), 512, 0)

        @pl.when((i >= ST_O) & (i < ST_G))
        def _():
            cols("o", pl.multiple_of((i - ST_O) * 512, 512), 512, 0)

        @pl.when((i >= ST_G) & (i < ST_D))
        def _():
            c0 = pl.multiple_of((i - ST_G) * 256, 256)
            cols("g", c0, 256, 0)
            cols("u", c0, 256, 256)

        j, tile, half, whole, near, far, rest = down_step(i)
        dslot = lax.rem(j + 2 * STEPS, 2)

        def rows_in(src, r0, nr, w0):
            pltpu.make_async_copy(src["d"].at[layer, pl.ds(r0, nr), :], dbuf.at[dslot, pl.ds(w0, nr), :], dsem.at[dslot]).start()

        def chunk_rows(r, tile_no, w0):
            src_core = core if r % 2 == 0 else 1 - core
            rows_in(sources[r], pl.multiple_of(src_core * TAIL + tile_no * 256, 64), 256, w0)

        def rest_rows(r, w0):
            src_core = core if r % 2 == 0 else 1 - core
            rows_in(sources[r], pl.multiple_of((1 - src_core) * 2560, 512), TAIL, pl.multiple_of(w0 + src_core * TAIL, 64))

        @pl.when((whole & (half == 0) & (i != ST_READY + 1)) | (i == ST_READY))
        def _():
            for r in range(3):
                chunk_rows(r, jnp.where(i == ST_READY, N_D - 2, tile), r * 256)

        @pl.when(whole & (half == 0))
        def _():
            chunk_rows(3, tile, 768)

        @pl.when(near & (half == 0))
        def _():
            for r in range(2):
                chunk_rows(r, N_D - 1, r * 256)
                rest_rows(r, 512)

        @pl.when(far & (half == 0))
        def _():
            for r in range(2):
                chunk_rows(2 + r, N_D - 1, r * 256)

        @pl.when(rest & (half == 0))
        def _():
            for r in range(2):
                rest_rows(2 + r, 0)

    def norm(layer, which):
        @pl.loop(0, TOK // NB)
        def _(m):
            rows = pl.ds(pl.multiple_of(m * NB, NB), NB)
            total = jnp.zeros((NB, 1), F32)
            for b in range(4):
                blk = x_ref[rows, pl.ds(b * ROWS, ROWS)]
                total = total + jnp.sum(blk * blk, axis=1, keepdims=True)
            inv = lax.rsqrt(total * (1.0 / D) + EPS)
            for b in range(4):
                blk = x_ref[rows, pl.ds(b * ROWS, ROWS)]
                gain = gain_ref[which * LAYERS + layer, :, pl.ds(b * ROWS, ROWS)]
                c0 = pl.multiple_of(rel(b) * ROWS, ROWS)
                h_ref[rows, pl.ds(c0, ROWS)] = (blk * inv * gain).astype(BF16)

    def rotate(vals, rows):
        vals = vals.astype(BF16).astype(F32)
        turned = pltpu.roll(vals, HEAD // 2, 1)
        return (vals * cos_ref[rows, :] + turned * sin_ref[rows, :]).astype(BF16)

    def tile_product(slot, finish_rows):
        @pl.loop(0, TOK // MB)
        def _(m):
            rows = pl.ds(pl.multiple_of(m * MB, MB), MB)
            finish_rows(rows, jnp.dot(h_ref[rows, :], wbuf[slot], preferred_element_type=F32))

    def kv_step(slot):
        def fin(rows, acc):
            for b in range(2):
                kv_ref[rows, pl.ds(b * HEAD, HEAD)] = rotate(acc[:, b * HEAD:(b + 1) * HEAD], rows)
            kv_ref[rows, pl.ds(256, 256)] = acc[:, 256:].astype(BF16)
        tile_product(slot, fin)

    def q_step(slot, j):
        def fin(rows, acc):
            for b in range(4):
                c0 = pl.multiple_of(j * 512 + b * HEAD, HEAD)
                q_ref[rows, pl.ds(c0, HEAD)] = rotate(acc[:, b * HEAD:(b + 1) * HEAD], rows)
        tile_product(slot, fin)

    def o_step(slot, j):
        def fin(rows, acc):
            c0 = pl.ds(pl.multiple_of(j * 512, 512), 512)
            x_ref[rows, c0] = x_ref[rows, c0] + acc
        tile_product(slot, fin)

    def g_step(slot, j):
        def fin(rows, acc):
            gate = acc[:, :256]
            up = acc[:, 256:]
            c0 = pl.multiple_of(j * 256, 256)
            a_ref[rows, pl.ds(c0, 256)] = (gate * jax.nn.sigmoid(gate) * up).astype(BF16)
        tile_product(slot, fin)

    def attend(head):
        kv = head // 8
        q0 = pl.multiple_of(head * HEAD, HEAD)
        k0 = pl.multiple_of(kv * HEAD, HEAD)
        v0 = pl.multiple_of(256 + kv * HEAD, HEAD)
        o0 = pl.multiple_of(rel(head // 4) * ROWS + lax.rem(head, 4) * HEAD, HEAD)
        scale = HEAD ** -0.5
        for b in range(TOK // QB):
            keys = (b + 1) * QB
            rows = pl.ds(b * QB, QB)
            scores = lax.dot_general(q_ref[rows, pl.ds(q0, HEAD)], kv_ref[pl.ds(0, keys), pl.ds(k0, HEAD)],
                                     (((1,), (1,)), ((), ())), preferred_element_type=F32)
            key_idx = lax.broadcasted_iota(jnp.int32, (QB, keys), 1)
            row_idx = lax.broadcasted_iota(jnp.int32, (QB, keys), 0) + b * QB
            first = jnp.concatenate([first_ref[rows, :]] * (keys // HEAD), axis=1)
            ok = (key_idx >= first) & (key_idx <= row_idx)
            scores = jnp.where(ok, scores, -1e30)
            top = jnp.max(scores, axis=1, keepdims=True)
            probs = jnp.exp((scores - top) * scale)
            inv = 1.0 / jnp.sum(probs, axis=1, keepdims=True)
            probs = (probs * inv).astype(BF16)
            mixed = jnp.dot(probs, kv_ref[pl.ds(0, keys), pl.ds(v0, HEAD)], preferred_element_type=F32)
            h_ref[rows, pl.ds(o0, HEAD)] = mixed.astype(BF16)

    def add_product(dslot, half, cols):
        rows = pl.ds(pl.multiple_of(half * MB, MB), MB)
        depth = sum(width for _, width in cols)
        lhs = jnp.concatenate([a_ref[rows, pl.ds(c0, width)] for c0, width in cols], axis=1)
        x_ref[rows, :] = x_ref[rows, :] + jnp.dot(lhs, dbuf[dslot, pl.ds(0, depth), :], preferred_element_type=F32)

    def wait_d(dslot, half, depth):
        @pl.when(half == 0)
        def _():
            part = dbuf.at[dslot, pl.ds(0, depth), :]
            pltpu.make_async_copy(part, part, dsem.at[dslot]).wait()

    def last_cols(side_no):
        return [(tile_col(side_no, core, N_D - 1), 256), (tile_col(side_no, 1 - core, N_D - 1), 256)]

    def wait_w(slot):
        pltpu.make_async_copy(wbuf.at[slot], wbuf.at[slot], wsem.at[slot]).wait()

    def step(s):
        before = [jnp.where(s == 0, one, two) for one, two in zip(FIRST, targets(s - 1))]
        relays(before, targets(s))

        @pl.when(s + 1 < ALL_STEPS)
        def _():
            load_tile(s + 1)

        with jax.named_scope("comp"):
            compute(s)

    def compute(s):
        layer = s // STEPS
        i = lax.rem(s, STEPS)
        slot = lax.rem(s, 2)

        @pl.when(((i == 0) & (layer > 0)) | (i == ST_G))
        def _():
            norm(layer, jnp.where(i == 0, 0, 1))

        @pl.when((i < ST_A) | ((i >= ST_O) & (i < ST_D)))
        def _():
            wait_w(slot)

        @pl.when(i == 0)
        def _():
            kv_step(slot)

        @pl.when((i >= ST_Q) & (i < ST_A))
        def _():
            q_step(slot, i - ST_Q)

        @pl.when((i >= ST_A) & (i < ST_O))
        def _():
            attend(i - ST_A)

        @pl.when((i >= ST_O) & (i < ST_G))
        def _():
            o_step(slot, i - ST_O)

        @pl.when((i >= ST_G) & (i < ST_D))
        def _():
            g_step(slot, i - ST_G)

        j, tile, half, whole, near, far, rest = down_step(i)
        dslot = lax.rem(j + 2 * STEPS, 2)

        @pl.when(whole)
        def _():
            wait_d(dslot, half, 1024)
            add_product(dslot, half, [(tile_col(lax.rem(side + r // 2, 2), lax.rem(core + r, 2), tile), 256) for r in range(4)])

        @pl.when(near)
        def _():
            wait_d(dslot, half, NEAR_K)
            add_product(dslot, half, last_cols(side) + [(rest_col(side), REST_K)])

        @pl.when(far)
        def _():
            wait_d(dslot, half, 512)
            add_product(dslot, half, last_cols(1 - side))

        @pl.when(rest)
        def _():
            wait_d(dslot, half, REST_K)
            add_product(dslot, half, [(rest_col(1 - side), REST_K)])

    @pl.loop(0, AHEAD)
    def _(m):
        for_item(m, start1)

    @pl.loop(0, AHEAD0)
    def _(k):
        for_chunk(k, start0)

    for copy in inputs:
        copy.wait()

    for n, ref in enumerate((ga_ref, gm_ref)):
        for layer in range(LAYERS):
            gain_ref[n * LAYERS + layer] = ref[pl.ds(layer, 1), :].astype(F32)
    ids = seg_ref[...].astype(F32)
    lane = lax.broadcasted_iota(jnp.int32, (128, HEAD), 1)
    for b in range(TOK // 128):
        rows = pl.ds(b * 128, 128)
        mine = jnp.transpose(jnp.broadcast_to(ids[b:b + 1, :], (128, 128)))
        before = jnp.zeros((128, 128), F32)
        for c in range(TOK // 128):
            before = before + jnp.where(ids[c:c + 1, :] < mine, 1.0, 0.0)
        first = jnp.sum(before, axis=1, keepdims=True)
        pos = lax.broadcasted_iota(jnp.int32, (128, 128), 0).astype(F32) + (b * 128.0) - first
        angles = pos * freq_ref[...]
        cos_ref[rows, :] = jnp.cos(angles)
        sin = jnp.sin(angles)
        sin_ref[rows, :] = jnp.where(lane < HEAD // 2, -sin, sin)
        first_ref[rows, :] = jnp.broadcast_to(first, (128, 128)).astype(jnp.int32)

    @pl.loop(0, TOK // NB)
    def _(m):
        rows = pl.ds(pl.multiple_of(m * NB, NB), NB)
        x_ref[rows, :] = q_ref[rows, :].astype(F32)

    relays((0, 0, 0), (2, 0, 0))
    norm(0, 0)

    @pl.loop(0, AHEAD0 - 1)
    def _(k):
        for_chunk(k, wait0)

    relays((2, 0, 0), START)
    relays(START, FIRST)
    load_tile(0)

    @pl.loop(0, ALL_STEPS)
    def _(s):
        with jax.named_scope("step"):
            step(s)

    relays(targets(ALL_STEPS - 1), (ITEMS, PUSHES, CHUNKS))


def result_kernel(x_ref, a_ref, w2_hbm, w3_hbm, out, y_ref, w_ref, wsem, osem):
    d = lax.axis_index("fsdp")
    core = lax.rem(d, 2)
    c0 = pl.multiple_of((1 - d // 2) * (2 * FF_ROWS) + 2560, HEAD)
    for n in range(4):
        cols = pl.ds(n * 512, 512)
        for src, src_core in ((w2_hbm, core), (w3_hbm, 1 - core)):
            r0 = pl.multiple_of((1 - src_core) * 2560, 512)
            d0 = pl.multiple_of(src_core * TAIL, 64)
            pltpu.make_async_copy(src.at[LAYERS - 1, pl.ds(r0, TAIL), cols], w_ref.at[n, pl.ds(d0, TAIL), :], wsem.at[n]).start()

    def store(n, m):
        rows, cols = pl.ds(m * 512, 512), pl.ds(n * 512, 512)
        return pltpu.make_async_copy(y_ref.at[rows, cols], out.at[rows, cols], osem.at[n, m])

    for n in range(4):
        cols = pl.ds(n * 512, 512)
        pltpu.make_async_copy(w_ref.at[n], w_ref.at[n], wsem.at[n]).wait()
        for m in range(2):
            rows = pl.ds(m * 512, 512)
            y_ref[rows, cols] = x_ref[rows, cols] + jnp.dot(a_ref[rows, pl.ds(c0, REST_K)], w_ref[n], preferred_element_type=F32)
            store(n, m).start()
    for n in range(4):
        for m in range(2):
            store(n, m).wait()


def run_layers(tokens, seg_ids, g_attn, g_mlp, weights):
    shapes = [jax.ShapeDtypeStruct(w.shape, w.dtype) for w in weights]
    half_dim = HEAD // 2
    freq = np.float32(ROPE_BASE) ** (-np.arange(half_dim, dtype=np.float32) / np.float32(half_dim))
    freq = jnp.asarray(np.concatenate([freq, freq]).reshape(1, HEAD))
    sem = pltpu.SemaphoreType.DMA((SLOTS, 2))
    item_sem = pltpu.SemaphoreType.DMA((ITEM_SLOTS,))
    any_spec = pl.BlockSpec(memory_space=pl.ANY)
    vmem_spec = pl.BlockSpec(memory_space=pltpu.VMEM)
    outs = pl.pallas_call(
        layer_kernel,
        out_shape=[pltpu.VMEM((TOK, D), F32), pltpu.VMEM((TOK, FF), BF16)] + shapes * 3,
        in_specs=[any_spec] * 12,
        out_specs=[vmem_spec] * 2 + [any_spec] * 21,
        scratch_shapes=[
            pltpu.VMEM((TOK, D), BF16),
            pltpu.VMEM((TOK, D), BF16),
            pltpu.VMEM((TOK, 512), BF16),
            pltpu.VMEM((2, D, 512), BF16),
            pltpu.VMEM((2, 1024, D), BF16),
            pltpu.VMEM((TOK, HEAD), F32),
            pltpu.VMEM((TOK, HEAD), F32),
            pltpu.VMEM((TOK, HEAD), jnp.int32),
            pltpu.VMEM((2 * LAYERS, 1, D), F32),
            pltpu.VMEM((TOK // 128, 128), jnp.int32),
            pltpu.VMEM((1, HEAD), F32),
            pltpu.VMEM((LAYERS, D), BF16),
            pltpu.VMEM((LAYERS, D), BF16),
            pltpu.SemaphoreType.DMA((2,)),
            pltpu.SemaphoreType.DMA((2,)),
            pltpu.SemaphoreType.DMA((5,)),
        ] + [sem] * 2 + [item_sem] * 4 + [sem] * 2,
        compiler_params=pltpu.CompilerParams(collective_id=0, has_side_effects=True, vmem_limit_bytes=34 * 1000 * 1000),
        name="two_layers",
    )(tokens, seg_ids.reshape(TOK // 128, 128), freq, g_attn, g_mlp, *weights)
    hidden = pltpu.with_memory_space_constraint(outs[0], pltpu.VMEM)
    act = pltpu.with_memory_space_constraint(outs[1], pltpu.VMEM)
    return pl.pallas_call(
        result_kernel,
        out_shape=jax.ShapeDtypeStruct((TOK, D), F32),
        in_specs=[vmem_spec] * 2 + [any_spec] * 2,
        out_specs=any_spec,
        scratch_shapes=[
            pltpu.VMEM((TOK, D), F32),
            pltpu.VMEM((4, REST_K, 512), BF16),
            pltpu.SemaphoreType.DMA((4,)),
            pltpu.SemaphoreType.DMA((4, 2)),
        ],
        compiler_params=pltpu.CompilerParams(vmem_limit_bytes=24 * 1000 * 1000),
        name="result",
    )(hidden, act, outs[15], outs[22])


def solution(mesh):
    tok_spec = P(("rep", "fsdp"), None)
    seg_spec = P(("rep", "fsdp"))
    mat_spec = P(None, "fsdp", None)
    gain_spec = P(None, None)

    def per_device(tokens, seg_ids, w_q, w_k, w_v, w_o, w_gate, w_up, w_down, g_attn, g_mlp):
        return run_layers(tokens, seg_ids, g_attn, g_mlp, (w_q, w_k, w_v, w_o, w_gate, w_up, w_down))

    return jax.shard_map(per_device, mesh=mesh, in_specs=(tok_spec, seg_spec, mat_spec, mat_spec, mat_spec, mat_spec, mat_spec, mat_spec, mat_spec, gain_spec, gain_spec), out_specs=tok_spec, check_vma=False)
```

```python
import functools

import jax
import jax.numpy as jnp
import numpy as np
from jax import lax
from jax.experimental import pallas as pl
from jax.experimental.pallas import tpu as pltpu
from jax.sharding import PartitionSpec as P

D = 2048
FF = 11008
HEADS = 16
HEAD = 128
TOK = 1024
EPS = 1e-5
ROPE_BASE = 10000.0
MESH = pl.DeviceIdType.MESH
F32 = jnp.float32
BF16 = jnp.bfloat16

LAYERS = 2
SLOTS = 8
ITEM_SLOTS = 2 * SLOTS
AHEAD = 8
AHEAD0 = 5
ROWS = D // 4
FF_ROWS = FF // 4
TAIL = 192
NAMES = ("q", "k", "v", "o", "g", "u", "d")

N_Q = 4
N_GU = 21
N_D = 10
CH_Q = 1
CH_O = CH_Q + N_Q
CH_GU = CH_O + N_Q
CH_GL = CH_GU + N_GU
CH_D = CH_GL + 1
CH_DR = CH_D + N_D
PER_LAYER = CH_DR + 1
CHUNKS = LAYERS * PER_LAYER
ITEMS = 2 * CHUNKS
PUSHES = CHUNKS + 2

NEAR_AT = 5

N_GT = FF // 256
ST_Q = 1
ST_A = ST_Q + N_Q
ST_O = ST_A + HEADS
ST_G = ST_O + 4
ST_D = ST_G + N_GT
ST_NEAR = ST_D + 2 * NEAR_AT
ST_READY = ST_D + 2 * (N_D - 1)
ST_IDLE = ST_READY + 3
ST_FAR = ST_IDLE + 1
ST_REST = ST_FAR + 2
STEPS = ST_REST + 2
ALL_STEPS = LAYERS * STEPS - 2
START = (4, 1, 0)
FIRST = (8, 3, 1)
REST_K = 2 * TAIL
NEAR_K = 512 + REST_K

MB = 512
NB = 128
QB = 256


def layer_kernel(*refs):
    tok, seg, freq, g_attn, g_mlp = refs[:5]
    own = dict(zip(NAMES, refs[5:12]))
    x_ref, a_ref, rest_ref = refs[12:15]
    b1 = dict(zip(NAMES, refs[15:22]))
    b2 = dict(zip(NAMES, refs[22:29]))
    b3 = dict(zip(NAMES, refs[29:36]))
    (h_ref, q_ref, kv_ref, wbuf, dbuf, cos_ref, sin_ref, first_ref, gain_ref,
     seg_ref, freq_ref, ga_ref, gm_ref, far_ref, wsem, dsem, iosem, lsem) = refs[36:54]
    s0s, s0r, s1s, s1r, s2s, s2r, s3s, s3r = refs[54:]
    sources = (own, b1, b2, b3)
    y = lax.axis_index("rep")
    d = lax.axis_index("fsdp")
    side = d // 2
    core = lax.rem(d, 2)
    x_dev = (y, lax.rem(d + 2, 4))
    y_dev = (1 - y, d)
    c_dev = (y, d + 1 - 2 * core)

    def rel(block):
        return 2 * lax.rem(block // 2 + side, 2) + lax.rem(block + core, 2)

    inputs = [pltpu.make_async_copy(src, dst, iosem.at[n]) for n, (src, dst) in enumerate(
        ((tok, q_ref), (seg, seg_ref), (freq, freq_ref), (g_attn, ga_ref), (g_mlp, gm_ref)))]
    for copy in inputs:
        copy.start()

    with jax.named_scope("barrier"):
        barrier = pltpu.get_barrier_semaphore()
        for dev in (x_dev, y_dev, c_dev):
            pl.semaphore_signal(barrier, inc=1, device_id=dev, device_id_type=MESH)
        pl.semaphore_wait(barrier, 3)

    def kinds(k):
        i = lax.rem(k, PER_LAYER)
        jq = pl.multiple_of((i - CH_Q) * 512, 512)
        jo = pl.multiple_of((i - CH_O) * 512, 512)
        jg = pl.multiple_of((i - CH_GU) * 512, 512)
        jd = core * TAIL + (i - CH_D) * 256
        jr = (1 - core) * 2560
        last = N_GU * 512
        kv = [("k", 0, ROWS, 0, 256), ("v", 0, ROWS, 0, 256)]
        gu = [("g", 0, ROWS, jg, 512), ("u", 0, ROWS, jg, 512)]
        gl = [("g", 0, ROWS, last, 256), ("u", 0, ROWS, last, 256)]

        def split_cols(name, c0):
            whole = [(name, 0, ROWS, c0, 512)]
            return [(name, 0, ROWS, c0, 256), (name, 0, ROWS, c0 + 256, 256)], whole, whole

        def split_rows(r0, nr):
            halves = [("d", r0, nr // 2, 0, D), ("d", r0 + nr // 2, nr // 2, 0, D)]
            return halves, [("d", r0, nr, 0, D)], halves

        return [
            (i == 0, kv, kv, kv, 0),
            ((i >= CH_Q) & (i < CH_O), *split_cols("q", jq), 0),
            ((i >= CH_O) & (i < CH_GU), *split_cols("o", jo), 0),
            ((i >= CH_GU) & (i < CH_GL), gu, gu, gu, 0),
            (i == CH_GL, gl, gl, gl, 0),
            ((i >= CH_D) & (i < CH_DR) & (k != CHUNKS - 2), *split_rows(jd, 256), 0),
            (k == CHUNKS - 2, *split_rows(jd, 256), 2),
            ((i == CH_DR) & (k != CHUNKS - 1), *split_rows(jr, TAIL), 0),
            (k == CHUNKS - 1, *split_rows(jr, TAIL), 1),
        ]

    def for_chunk(k, fn, form=2, part=None):
        layer = k // PER_LAYER
        slot = lax.rem(k, SLOTS)
        for kind in kinds(k):
            @pl.when((k < CHUNKS) & kind[0])
            def _():
                for n, piece in enumerate(kind[form]):
                    if part is None:
                        fn(kind[4], layer, piece, (slot, n))
                    else:
                        @pl.when(part != 1 - n)
                        def _():
                            fn(kind[4], layer, piece, (slot, n))

    def for_pair(k, fn, part=None):
        layer = k // PER_LAYER
        for cond, pieces, _, _, mark in kinds(k):
            @pl.when((k < CHUNKS) & cond)
            def _():
                for n, piece in enumerate(pieces):
                    args = (mark == 1 and n == 1, layer, piece, (lax.rem(2 * k + n, ITEM_SLOTS),))
                    if part is None:
                        fn(*args)
                    else:
                        @pl.when(part != 1 - n)
                        def _():
                            fn(*args)

    def for_item(m, fn):
        k = m // 2
        n = lax.rem(m, 2)
        layer = k // PER_LAYER
        slot = (lax.rem(m, ITEM_SLOTS),)
        for cond, (one, two), _, _, mark in kinds(k):
            if one[0] == two[0] and mark != 1:
                name, r0, nr, c0, nc = one
                r0, c0 = (r0 + n * nr, c0) if nc == D else (r0, pl.multiple_of(c0 + n * nc, 256))

                @pl.when((m < ITEMS) & cond)
                def _():
                    fn(False, layer, (name, r0, nr, c0, nc), slot)
            else:
                for which, piece in enumerate((one, two)):
                    @pl.when((m < ITEMS) & cond & (n == which))
                    def _():
                        fn(mark == 1 and which == 1, layer, piece, slot)

    def view(bufs, name, layer, r0, nr, c0, nc, half):
        if half:
            nr = nr // 2
            r0 = r0 + y * nr
        r0 = pl.multiple_of(r0, 16)
        return bufs[name].at[layer, pl.ds(r0, nr), pl.ds(c0, nc)]

    def remote(src, dst, ss, rs, dev, half):
        def make(whole, layer, piece, slot):
            part = half and not whole
            return pltpu.make_async_remote_copy(
                src_ref=view(src, piece[0], layer, *piece[1:], part),
                dst_ref=view(dst, piece[0], layer, *piece[1:], part),
                send_sem=ss.at[slot], recv_sem=rs.at[slot], device_id=dev, device_id_type=MESH)
        return make

    copy0 = remote(own, b1, s0s, s0r, c_dev, False)
    copy1 = remote(own, b2, s1s, s1r, x_dev, True)
    copy2 = remote(b2, b2, s2s, s2r, y_dev, True)

    def copy3(mark, layer, piece, slot):
        name, r0, nr, c0, nc = piece
        if mark == 0:
            return remote(b2, b3, s3s, s3r, c_dev, False)(False, layer, piece, slot)
        if mark == 1:
            dst = rest_ref.at[pl.ds(pl.multiple_of(r0 - (1 - core) * 2560 + core * TAIL, 32), nr), :]
        else:
            dst = far_ref.at[pl.ds(pl.multiple_of(r0 - core * TAIL - (N_D - 1) * 256 + 256, 128), nr), :]
        return pltpu.make_async_remote_copy(
            src_ref=view(b2, name, layer, r0, nr, c0, nc, False), dst_ref=dst,
            send_sem=s3s.at[slot], recv_sem=s3r.at[slot], device_id=c_dev, device_id_type=MESH)

    def start0(*a):
        copy0(*a).start()

    def start1(*a):
        copy1(*a).start()

    def wait0(*a):
        copy0(*a).wait_recv()

    def relay2(*a):
        copy1(*a).wait_recv()
        if not a[0]:
            copy2(*a).start()

    def arrived(*a):
        if not a[0]:
            copy2(*a).wait_recv()
        copy1(*a).wait_send()

    def relay3(*a):
        copy3(*a).start()

    def pushed(*a):
        copy0(*a).wait_send()

    def finish(*a):
        copy3(*a).wait_recv()
        copy3(*a).wait_send()

    def sent(*a):
        if not a[0]:
            copy2(*a).wait_send()

    def targets(s):
        i = lax.rem(s, STEPS)
        layer = s // STEPS
        first = layer == 0
        late = 1 - jnp.minimum(layer, 1)
        t2 = jnp.where(i < ST_A, 9 + 2 * i + late,
             jnp.where(i < ST_G + 1, 18 + late + 3 * (i - ST_A) // 5,
             jnp.where(i < ST_D, jnp.maximum(i + 4, 31 + late + (i - ST_G - 1) // 2),
             jnp.where(i < ST_NEAR, jnp.maximum(i, ST_D + 3 + (2 * (i - ST_D) + 1) // 3),
             jnp.where(first, jnp.where(i < ST_NEAR + 2, i, jnp.where(i < ST_READY - 2, 40 + i // 2, jnp.where(i < ST_READY, i - 2, i - 3))),
             jnp.where(i < ST_READY - 2, 38 + (i + 1) // 2, 39 + i // 2))))))
        final = i == STEPS - 1
        t3 = jnp.where(i < ST_D, jnp.where(i < ST_A, 3 + i, (t2 - 3) // 2),
             jnp.where(first, jnp.where(i < ST_IDLE, (t2 - 2) // 2, CH_DR + (i - ST_IDLE + 1) // 2 + jnp.where(final, 1, 0)),
             jnp.where(i < ST_READY - 4, (t2 - 2) // 2, jnp.where(i < ST_READY + 2, 39 + (i - ST_READY + 4) // 3, i - ST_READY + 39 + jnp.where(i == ST_FAR, 1, 0)))))
        end = s >= ALL_STEPS - 2
        t2 = jnp.minimum(t2 + layer * 2 * PER_LAYER, jnp.where(end, ITEMS, ITEMS - 1))
        t3 = jnp.minimum(t3 + layer * PER_LAYER, PUSHES)
        nxt = jnp.minimum(s + 1, ALL_STEPS - 1)
        i = lax.rem(nxt, STEPS)
        base = nxt // STEPS * PER_LAYER
        done = jnp.where(i < ST_A, 1 + i,
               jnp.where(i < ST_O, ST_A,
               jnp.where(i < ST_G, 1 + CH_O + i - ST_O,
               jnp.where(i < ST_D, 1 + CH_GU + (i - ST_G) // 2,
               jnp.where(i < ST_NEAR, 1 + CH_D + (i - ST_D) // 2,
               jnp.where(i < ST_READY, CH_D + (i - ST_D) // 2,
               jnp.where(i < ST_READY + 1, CH_DR - 2,
               jnp.where(i < ST_FAR, CH_DR - 1,
               jnp.where(i < ST_REST, CH_DR, PER_LAYER)))))))))
        tf = jnp.maximum(jnp.minimum(t3 - 2, CHUNKS - 2), done + base)
        pushes = tf + jnp.where(tf == CHUNKS - 1, 1, 0)
        t3 = jnp.maximum(jnp.maximum(t3, pushes), base + jnp.where((i >= ST_READY) & (i < ST_FAR), CH_DR - 1, 0))
        return jnp.maximum(t2, 2 * jnp.minimum(t3, CHUNKS - 2)), t3, tf

    def relays(old, new):
        @pl.loop(old[0], new[0])
        def _(m):
            with jax.named_scope("r2"):
                for_item(m, relay2)
                for_item(m + AHEAD, start1)
                n = lax.rem(m, 2)
                for_chunk(m // 2 + jnp.where(n == 0, AHEAD0, CHUNKS), start0)
                for_chunk(m // 2 + jnp.where(n == 0, CHUNKS, AHEAD0 - 1), wait0)

        @pl.loop(old[1], new[1])
        def _(p):
            with jax.named_scope("r3"):
                extra = jnp.maximum(p - (CHUNKS - 2), 0)
                k = p - (extra + 1) // 2
                part = jnp.where(p < CHUNKS - 2, 2, lax.rem(extra, 2))
                for_pair(k, arrived, part)
                for_chunk(k, relay3, 3, part)
                for_chunk(jnp.where(part == 1, CHUNKS, k), pushed)

        @pl.loop(old[2], new[2])
        def _(k):
            with jax.named_scope("fin"):
                for_chunk(k, finish, 3)
                for_pair(k, sent)

    def down_step(i):
        n = i - ST_D - jnp.where(i > ST_READY, 1, 0) - jnp.where(i > ST_IDLE, 1, 0)
        j = n // 2
        near = (i >= ST_NEAR) & (i < ST_NEAR + 2)
        far = (i >= ST_FAR) & (i < ST_REST)
        rest = i >= ST_REST
        whole = (i >= ST_D) & (i < ST_IDLE) & ~near & (i != ST_READY)
        return j, jnp.where(i > ST_NEAR, j - 1, j), lax.rem(n + 2 * STEPS, 2), whole, near, far, rest

    def rest_col(side_no):
        return pl.multiple_of(side_no * (2 * FF_ROWS) + 2560, HEAD)

    def tile_col(side_no, core_no, tile):
        return pl.multiple_of(side_no * (2 * FF_ROWS) + core_no * (FF_ROWS + TAIL) + tile * 256, HEAD)

    def near_far():
        r0 = pl.multiple_of(core * TAIL + (N_D - 1) * 256, 64)
        return pltpu.make_async_copy(b2["d"].at[LAYERS - 1, pl.ds(r0, 256), :], far_ref.at[pl.ds(0, 256), :], lsem.at[0])

    def near_rest():
        r0 = pl.multiple_of((1 - core) * 2560, 512)
        return pltpu.make_async_copy(b2["d"].at[LAYERS - 1, pl.ds(r0, TAIL), :],
                                     rest_ref.at[pl.ds(pl.multiple_of(core * TAIL, 64), TAIL), :], lsem.at[1])

    def load_tile(s):
        layer = s // STEPS
        i = lax.rem(s, STEPS)
        slot = lax.rem(s, 2)

        def cols(name, c0, nc, w0):
            for r, src in enumerate(sources):
                pltpu.make_async_copy(src[name].at[layer, :, pl.ds(c0, nc)],
                                      wbuf.at[slot, pl.ds(r * ROWS, ROWS), pl.ds(w0, nc)], wsem.at[slot]).start()

        @pl.when(i == 0)
        def _():
            cols("k", 0, 256, 0)
            cols("v", 0, 256, 256)

        @pl.when((i >= ST_Q) & (i < ST_A))
        def _():
            cols("q", pl.multiple_of((i - ST_Q) * 512, 512), 512, 0)

        @pl.when((i >= ST_O) & (i < ST_G))
        def _():
            cols("o", pl.multiple_of((i - ST_O) * 512, 512), 512, 0)

        @pl.when((i >= ST_G) & (i < ST_D))
        def _():
            c0 = pl.multiple_of((i - ST_G) * 256, 256)
            cols("g", c0, 256, 0)
            cols("u", c0, 256, 256)

        j, tile, half, whole, near, far, rest = down_step(i)
        dslot = lax.rem(j + 2 * STEPS, 2)

        def rows_in(src, r0, nr, w0):
            pltpu.make_async_copy(src["d"].at[layer, pl.ds(r0, nr), :], dbuf.at[dslot, pl.ds(w0, nr), :], dsem.at[dslot]).start()

        def chunk_rows(r, tile_no, w0):
            src_core = core if r % 2 == 0 else 1 - core
            rows_in(sources[r], pl.multiple_of(src_core * TAIL + tile_no * 256, 64), 256, w0)

        def rest_rows(r, w0):
            src_core = core if r % 2 == 0 else 1 - core
            rows_in(sources[r], pl.multiple_of((1 - src_core) * 2560, 512), TAIL, pl.multiple_of(w0 + src_core * TAIL, 64))

        @pl.when((whole & (half == 0) & (i != ST_READY + 1)) | (i == ST_READY))
        def _():
            for r in range(3):
                chunk_rows(r, jnp.where(i == ST_READY, N_D - 2, tile), r * 256)

        @pl.when(whole & (half == 0))
        def _():
            chunk_rows(3, tile, 768)

        @pl.when(near & (half == 0))
        def _():
            for r in range(2):
                chunk_rows(r, N_D - 1, r * 256)
                rest_rows(r, 512)

        @pl.when(far & (half == 0) & (layer < LAYERS - 1))
        def _():
            for r in range(2):
                chunk_rows(2 + r, N_D - 1, r * 256)

        @pl.when(far & (half == 0) & (layer == LAYERS - 1))
        def _():
            near_far().start()

        @pl.when(rest & (half == 0))
        def _():
            for r in range(2):
                rest_rows(2 + r, 0)

    def norm(layer, which):
        @pl.loop(0, TOK // NB)
        def _(m):
            rows = pl.ds(pl.multiple_of(m * NB, NB), NB)
            total = jnp.zeros((NB, 1), F32)
            for b in range(4):
                blk = x_ref[rows, pl.ds(b * ROWS, ROWS)]
                total = total + jnp.sum(blk * blk, axis=1, keepdims=True)
            inv = lax.rsqrt(total * (1.0 / D) + EPS)
            for b in range(4):
                blk = x_ref[rows, pl.ds(b * ROWS, ROWS)]
                gain = gain_ref[which * LAYERS + layer, :, pl.ds(b * ROWS, ROWS)]
                c0 = pl.multiple_of(rel(b) * ROWS, ROWS)
                h_ref[rows, pl.ds(c0, ROWS)] = (blk * inv * gain).astype(BF16)

    def rotate(vals, rows):
        vals = vals.astype(BF16).astype(F32)
        turned = pltpu.roll(vals, HEAD // 2, 1)
        return (vals * cos_ref[rows, :] + turned * sin_ref[rows, :]).astype(BF16)

    def tile_product(slot, finish_rows):
        @pl.loop(0, TOK // MB)
        def _(m):
            rows = pl.ds(pl.multiple_of(m * MB, MB), MB)
            finish_rows(rows, jnp.dot(h_ref[rows, :], wbuf[slot], preferred_element_type=F32))

    def kv_step(slot):
        def fin(rows, acc):
            for b in range(2):
                kv_ref[rows, pl.ds(b * HEAD, HEAD)] = rotate(acc[:, b * HEAD:(b + 1) * HEAD], rows)
            kv_ref[rows, pl.ds(256, 256)] = acc[:, 256:].astype(BF16)
        tile_product(slot, fin)

    def q_step(slot, j):
        def fin(rows, acc):
            for b in range(4):
                c0 = pl.multiple_of(j * 512 + b * HEAD, HEAD)
                q_ref[rows, pl.ds(c0, HEAD)] = rotate(acc[:, b * HEAD:(b + 1) * HEAD], rows)
        tile_product(slot, fin)

    def o_step(slot, j):
        def fin(rows, acc):
            c0 = pl.ds(pl.multiple_of(j * 512, 512), 512)
            x_ref[rows, c0] = x_ref[rows, c0] + acc
        tile_product(slot, fin)

    def g_step(slot, j):
        def fin(rows, acc):
            gate = acc[:, :256]
            up = acc[:, 256:]
            c0 = pl.multiple_of(j * 256, 256)
            a_ref[rows, pl.ds(c0, 256)] = (gate * jax.nn.sigmoid(gate) * up).astype(BF16)
        tile_product(slot, fin)

    def attend(head):
        kv = head // 8
        q0 = pl.multiple_of(head * HEAD, HEAD)
        k0 = pl.multiple_of(kv * HEAD, HEAD)
        v0 = pl.multiple_of(256 + kv * HEAD, HEAD)
        o0 = pl.multiple_of(rel(head // 4) * ROWS + lax.rem(head, 4) * HEAD, HEAD)
        scale = HEAD ** -0.5
        for b in range(TOK // QB):
            keys = (b + 1) * QB
            rows = pl.ds(b * QB, QB)
            scores = lax.dot_general(q_ref[rows, pl.ds(q0, HEAD)], kv_ref[pl.ds(0, keys), pl.ds(k0, HEAD)],
                                     (((1,), (1,)), ((), ())), preferred_element_type=F32)
            key_idx = lax.broadcasted_iota(jnp.int32, (QB, keys), 1)
            row_idx = lax.broadcasted_iota(jnp.int32, (QB, keys), 0) + b * QB
            first = jnp.concatenate([first_ref[rows, :]] * (keys // HEAD), axis=1)
            ok = (key_idx >= first) & (key_idx <= row_idx)
            scores = jnp.where(ok, scores, -1e30)
            top = jnp.max(scores, axis=1, keepdims=True)
            probs = jnp.exp((scores - top) * scale)
            inv = 1.0 / jnp.sum(probs, axis=1, keepdims=True)
            probs = (probs * inv).astype(BF16)
            mixed = jnp.dot(probs, kv_ref[pl.ds(0, keys), pl.ds(v0, HEAD)], preferred_element_type=F32)
            h_ref[rows, pl.ds(o0, HEAD)] = mixed.astype(BF16)

    def add_product(dslot, half, cols, tile_ref=None):
        rows = pl.ds(pl.multiple_of(half * MB, MB), MB)
        depth = sum(width for _, width in cols)
        lhs = jnp.concatenate([a_ref[rows, pl.ds(c0, width)] for c0, width in cols], axis=1)
        tile = dbuf[dslot, pl.ds(0, depth), :] if tile_ref is None else tile_ref[...]
        x_ref[rows, :] = x_ref[rows, :] + jnp.dot(lhs, tile, preferred_element_type=F32)

    def wait_d(dslot, half, depth):
        @pl.when(half == 0)
        def _():
            part = dbuf.at[dslot, pl.ds(0, depth), :]
            pltpu.make_async_copy(part, part, dsem.at[dslot]).wait()

    def last_cols(side_no):
        return [(tile_col(side_no, core, N_D - 1), 256), (tile_col(side_no, 1 - core, N_D - 1), 256)]

    def wait_w(slot):
        pltpu.make_async_copy(wbuf.at[slot], wbuf.at[slot], wsem.at[slot]).wait()

    def step(s):
        before = [jnp.where(s == 0, one, two) for one, two in zip(FIRST, targets(s - 1))]
        relays(before, targets(s))

        @pl.when(s + 1 < ALL_STEPS)
        def _():
            load_tile(s + 1)

        with jax.named_scope("comp"):
            compute(s)

    def compute(s):
        layer = s // STEPS
        i = lax.rem(s, STEPS)
        slot = lax.rem(s, 2)

        @pl.when(((i == 0) & (layer > 0)) | (i == ST_G))
        def _():
            norm(layer, jnp.where(i == 0, 0, 1))

        @pl.when((i < ST_A) | ((i >= ST_O) & (i < ST_D)))
        def _():
            wait_w(slot)

        @pl.when(i == 0)
        def _():
            kv_step(slot)

        @pl.when((i >= ST_Q) & (i < ST_A))
        def _():
            q_step(slot, i - ST_Q)

        @pl.when((i >= ST_A) & (i < ST_O))
        def _():
            attend(i - ST_A)

        @pl.when((i >= ST_O) & (i < ST_G))
        def _():
            o_step(slot, i - ST_O)

        @pl.when((i >= ST_G) & (i < ST_D))
        def _():
            g_step(slot, i - ST_G)

        j, tile, half, whole, near, far, rest = down_step(i)
        dslot = lax.rem(j + 2 * STEPS, 2)

        @pl.when(whole)
        def _():
            wait_d(dslot, half, 1024)
            add_product(dslot, half, [(tile_col(lax.rem(side + r // 2, 2), lax.rem(core + r, 2), tile), 256) for r in range(4)])

        @pl.when(near)
        def _():
            wait_d(dslot, half, NEAR_K)
            add_product(dslot, half, last_cols(side) + [(rest_col(side), REST_K)])

        @pl.when(far & (layer < LAYERS - 1))
        def _():
            wait_d(dslot, half, 512)
            add_product(dslot, half, last_cols(1 - side))

        @pl.when(far & (layer == LAYERS - 1))
        def _():
            @pl.when(half == 0)
            def _():
                near_far().wait()
                near_rest().start()
            add_product(dslot, half, last_cols(1 - side), far_ref)

        @pl.when(rest)
        def _():
            wait_d(dslot, half, REST_K)
            add_product(dslot, half, [(rest_col(1 - side), REST_K)])

    @pl.loop(0, AHEAD)
    def _(m):
        for_item(m, start1)

    @pl.loop(0, AHEAD0)
    def _(k):
        for_chunk(k, start0)

    for copy in inputs:
        copy.wait()

    for n, ref in enumerate((ga_ref, gm_ref)):
        for layer in range(LAYERS):
            gain_ref[n * LAYERS + layer] = ref[pl.ds(layer, 1), :].astype(F32)
    ids = seg_ref[...].astype(F32)
    lane = lax.broadcasted_iota(jnp.int32, (128, HEAD), 1)
    for b in range(TOK // 128):
        rows = pl.ds(b * 128, 128)
        mine = jnp.transpose(jnp.broadcast_to(ids[b:b + 1, :], (128, 128)))
        before = jnp.zeros((128, 128), F32)
        for c in range(TOK // 128):
            before = before + jnp.where(ids[c:c + 1, :] < mine, 1.0, 0.0)
        first = jnp.sum(before, axis=1, keepdims=True)
        pos = lax.broadcasted_iota(jnp.int32, (128, 128), 0).astype(F32) + (b * 128.0) - first
        angles = pos * freq_ref[...]
        cos_ref[rows, :] = jnp.cos(angles)
        sin = jnp.sin(angles)
        sin_ref[rows, :] = jnp.where(lane < HEAD // 2, -sin, sin)
        first_ref[rows, :] = jnp.broadcast_to(first, (128, 128)).astype(jnp.int32)

    @pl.loop(0, TOK // NB)
    def _(m):
        rows = pl.ds(pl.multiple_of(m * NB, NB), NB)
        x_ref[rows, :] = q_ref[rows, :].astype(F32)

    relays((0, 0, 0), (2, 0, 0))
    norm(0, 0)

    @pl.loop(0, AHEAD0 - 1)
    def _(k):
        for_chunk(k, wait0)

    relays((2, 0, 0), START)
    relays(START, FIRST)
    load_tile(0)

    @pl.loop(0, ALL_STEPS)
    def _(s):
        with jax.named_scope("step"):
            step(s)

    relays(targets(ALL_STEPS - 1), (ITEMS, PUSHES, CHUNKS))
    near_rest().wait()


def result_kernel(x_ref, a_ref, w_ref, out, y_ref, osem):
    c0 = pl.multiple_of((1 - lax.axis_index("fsdp") // 2) * (2 * FF_ROWS) + 2560, HEAD)

    def store(n, m):
        rows, cols = pl.ds(m * 512, 512), pl.ds(n * 512, 512)
        return pltpu.make_async_copy(y_ref.at[rows, cols], out.at[rows, cols], osem.at[n, m])

    for n in range(4):
        cols = pl.ds(n * 512, 512)
        for m in range(2):
            rows = pl.ds(m * 512, 512)
            y_ref[rows, cols] = x_ref[rows, cols] + jnp.dot(a_ref[rows, pl.ds(c0, REST_K)], w_ref[:, cols], preferred_element_type=F32)
            store(n, m).start()
    for n in range(4):
        for m in range(2):
            store(n, m).wait()


def run_layers(tokens, seg_ids, g_attn, g_mlp, weights):
    shapes = [jax.ShapeDtypeStruct(w.shape, w.dtype) for w in weights]
    half_dim = HEAD // 2
    freq = np.float32(ROPE_BASE) ** (-np.arange(half_dim, dtype=np.float32) / np.float32(half_dim))
    freq = jnp.asarray(np.concatenate([freq, freq]).reshape(1, HEAD))
    sem = pltpu.SemaphoreType.DMA((SLOTS, 2))
    item_sem = pltpu.SemaphoreType.DMA((ITEM_SLOTS,))
    any_spec = pl.BlockSpec(memory_space=pl.ANY)
    vmem_spec = pl.BlockSpec(memory_space=pltpu.VMEM)
    outs = pl.pallas_call(
        layer_kernel,
        out_shape=[pltpu.VMEM((TOK, D), F32), pltpu.VMEM((TOK, FF), BF16), pltpu.VMEM((REST_K, D), BF16)] + shapes * 3,
        in_specs=[any_spec] * 12,
        out_specs=[vmem_spec] * 3 + [any_spec] * 21,
        scratch_shapes=[
            pltpu.VMEM((TOK, D), BF16),
            pltpu.VMEM((TOK, D), BF16),
            pltpu.VMEM((TOK, 512), BF16),
            pltpu.VMEM((2, D, 512), BF16),
            pltpu.VMEM((2, 1024, D), BF16),
            pltpu.VMEM((TOK, HEAD), F32),
            pltpu.VMEM((TOK, HEAD), F32),
            pltpu.VMEM((TOK, HEAD), jnp.int32),
            pltpu.VMEM((2 * LAYERS, 1, D), F32),
            pltpu.VMEM((TOK // 128, 128), jnp.int32),
            pltpu.VMEM((1, HEAD), F32),
            pltpu.VMEM((LAYERS, D), BF16),
            pltpu.VMEM((LAYERS, D), BF16),
            pltpu.VMEM((512, D), BF16),
            pltpu.SemaphoreType.DMA((2,)),
            pltpu.SemaphoreType.DMA((2,)),
            pltpu.SemaphoreType.DMA((5,)),
            pltpu.SemaphoreType.DMA((2,)),
        ] + [sem] * 2 + [item_sem] * 4 + [sem] * 2,
        compiler_params=pltpu.CompilerParams(collective_id=0, has_side_effects=True, vmem_limit_bytes=33 * 1000 * 1000),
        name="two_layers",
    )(tokens, seg_ids.reshape(TOK // 128, 128), freq, g_attn, g_mlp, *weights)
    hidden = pltpu.with_memory_space_constraint(outs[0], pltpu.VMEM)
    act = pltpu.with_memory_space_constraint(outs[1], pltpu.VMEM)
    rest = pltpu.with_memory_space_constraint(outs[2], pltpu.VMEM)
    return pl.pallas_call(
        result_kernel,
        out_shape=jax.ShapeDtypeStruct((TOK, D), F32),
        in_specs=[vmem_spec] * 3,
        out_specs=any_spec,
        scratch_shapes=[
            pltpu.VMEM((TOK, D), F32),
            pltpu.SemaphoreType.DMA((4, 2)),
        ],
        compiler_params=pltpu.CompilerParams(vmem_limit_bytes=24 * 1000 * 1000),
        name="result",
    )(hidden, act, rest)


def solution(mesh):
    tok_spec = P(("rep", "fsdp"), None)
    seg_spec = P(("rep", "fsdp"))
    mat_spec = P(None, "fsdp", None)
    gain_spec = P(None, None)

    def per_device(tokens, seg_ids, w_q, w_k, w_v, w_o, w_gate, w_up, w_down, g_attn, g_mlp):
        return run_layers(tokens, seg_ids, g_attn, g_mlp, (w_q, w_k, w_v, w_o, w_gate, w_up, w_down))

    return jax.shard_map(per_device, mesh=mesh, in_specs=(tok_spec, seg_spec, mat_spec, mat_spec, mat_spec, mat_spec, mat_spec, mat_spec, mat_spec, gain_spec, gain_spec), out_specs=tok_spec, check_vma=False)
```

```python
import functools

import jax
import jax.numpy as jnp
import numpy as np
from jax import lax
from jax.experimental import pallas as pl
from jax.experimental.pallas import tpu as pltpu
from jax.sharding import PartitionSpec as P

D = 2048
FF = 11008
HEADS = 16
HEAD = 128
TOK = 1024
EPS = 1e-5
ROPE_BASE = 10000.0
MESH = pl.DeviceIdType.MESH
F32 = jnp.float32
BF16 = jnp.bfloat16

LAYERS = 2
SLOTS = 8
ITEM_SLOTS = 2 * SLOTS
AHEAD = 8
AHEAD0 = 5
ROWS = D // 4
FF_ROWS = FF // 4
TAIL = 192
NAMES = ("q", "k", "v", "o", "g", "u", "d")

N_Q = 4
N_GU = 21
N_D = 10
CH_Q = 1
CH_O = CH_Q + N_Q
CH_GU = CH_O + N_Q
CH_GL = CH_GU + N_GU
CH_D = CH_GL + 1
CH_DR = CH_D + N_D
PER_LAYER = CH_DR + 1
CHUNKS = LAYERS * PER_LAYER
ITEMS = 2 * CHUNKS
PUSHES = CHUNKS + 1

NEAR_AT = 5

N_GT = FF // 256
ST_Q = 1
ST_A = ST_Q + N_Q
ST_O = ST_A + HEADS
ST_G = ST_O + 4
ST_D = ST_G + N_GT
ST_NEAR = ST_D + 2 * NEAR_AT
ST_READY = ST_D + 2 * (N_D - 1)
ST_IDLE = ST_READY + 3
ST_FAR = ST_IDLE + 1
ST_REST = ST_FAR + 2
STEPS = ST_REST + 2
ALL_STEPS = LAYERS * STEPS - 2
START = (4, 1, 0)
FIRST = (8, 3, 1)
REST_K = 2 * TAIL
WIDE = D // 2
NEAR_K = 512 + REST_K

MB = 512
NB = 128
QB = 256


def layer_kernel(*refs):
    tok, seg, freq, g_attn, g_mlp = refs[:5]
    own = dict(zip(NAMES, refs[5:12]))
    x_ref, a_ref = refs[12:14]
    b1 = dict(zip(NAMES, refs[14:21]))
    b2 = dict(zip(NAMES, refs[21:28]))
    b3 = dict(zip(NAMES, refs[28:35]))
    (h_ref, q_ref, kv_ref, wbuf, dbuf, cos_ref, sin_ref, first_ref, gain_ref,
     seg_ref, freq_ref, ga_ref, gm_ref, far_ref, wsem, dsem, iosem, lsem) = refs[35:53]
    s0s, s0r, s1s, s1r, s2s, s2r, s3s, s3r = refs[53:]
    sources = (own, b1, b2, b3)
    y = lax.axis_index("rep")
    d = lax.axis_index("fsdp")
    side = d // 2
    core = lax.rem(d, 2)
    x_dev = (y, lax.rem(d + 2, 4))
    y_dev = (1 - y, d)
    c_dev = (y, d + 1 - 2 * core)

    def rel(block):
        return 2 * lax.rem(block // 2 + side, 2) + lax.rem(block + core, 2)

    inputs = [pltpu.make_async_copy(src, dst, iosem.at[n]) for n, (src, dst) in enumerate(
        ((tok, q_ref), (seg, seg_ref), (freq, freq_ref), (g_attn, ga_ref), (g_mlp, gm_ref)))]
    for copy in inputs:
        copy.start()

    with jax.named_scope("barrier"):
        barrier = pltpu.get_barrier_semaphore()
        for dev in (x_dev, y_dev, c_dev):
            pl.semaphore_signal(barrier, inc=1, device_id=dev, device_id_type=MESH)
        pl.semaphore_wait(barrier, 3)

    def kinds(k):
        i = lax.rem(k, PER_LAYER)
        jq = pl.multiple_of((i - CH_Q) * 512, 512)
        jo = pl.multiple_of((i - CH_O) * 512, 512)
        jg = pl.multiple_of((i - CH_GU) * 512, 512)
        jd = core * TAIL + (i - CH_D) * 256
        jr = (1 - core) * 2560
        last = N_GU * 512
        kv = [("k", 0, ROWS, 0, 256), ("v", 0, ROWS, 0, 256)]
        gu = [("g", 0, ROWS, jg, 512), ("u", 0, ROWS, jg, 512)]
        gl = [("g", 0, ROWS, last, 256), ("u", 0, ROWS, last, 256)]

        def split_cols(name, c0):
            whole = [(name, 0, ROWS, c0, 512)]
            return [(name, 0, ROWS, c0, 256), (name, 0, ROWS, c0 + 256, 256)], whole, whole

        def split_rows(r0, nr):
            halves = [("d", r0, nr // 2, 0, D), ("d", r0 + nr // 2, nr // 2, 0, D)]
            return halves, [("d", r0, nr, 0, D)], halves

        return [
            (i == 0, kv, kv, kv, 0),
            ((i >= CH_Q) & (i < CH_O), *split_cols("q", jq), 0),
            ((i >= CH_O) & (i < CH_GU), *split_cols("o", jo), 0),
            ((i >= CH_GU) & (i < CH_GL), gu, gu, gu, 0),
            (i == CH_GL, gl, gl, gl, 0),
            ((i >= CH_D) & (i < CH_DR) & (k != CHUNKS - 2), *split_rows(jd, 256), 0),
            (k == CHUNKS - 2, *split_rows(jd, 256), 2),
            ((i == CH_DR) & (k != CHUNKS - 1), *split_rows(jr, TAIL), 0),
            (k == CHUNKS - 1, *split_rows(jr, TAIL)[:2], [("d", jr, TAIL, 0, WIDE), ("d", jr, TAIL, WIDE, WIDE)], 1),
        ]

    def for_chunk(k, fn, form=2, part=None):
        layer = k // PER_LAYER
        slot = lax.rem(k, SLOTS)
        for kind in kinds(k):
            @pl.when((k < CHUNKS) & kind[0])
            def _():
                for n, piece in enumerate(kind[form]):
                    if part is None:
                        fn(kind[4], layer, piece, (slot, n))
                    else:
                        @pl.when(part != 1 - n)
                        def _():
                            fn(kind[4], layer, piece, (slot, n))

    def for_pair(k, fn, part=None):
        layer = k // PER_LAYER
        for cond, pieces, _, _, mark in kinds(k):
            @pl.when((k < CHUNKS) & cond)
            def _():
                for n, piece in enumerate(pieces):
                    args = (mark == 1 and n == 1, layer, piece, (lax.rem(2 * k + n, ITEM_SLOTS),))
                    if part is None:
                        fn(*args)
                    else:
                        @pl.when(part != 1 - n)
                        def _():
                            fn(*args)

    def for_item(m, fn):
        k = m // 2
        n = lax.rem(m, 2)
        layer = k // PER_LAYER
        slot = (lax.rem(m, ITEM_SLOTS),)
        for cond, (one, two), _, _, mark in kinds(k):
            if one[0] == two[0] and mark != 1:
                name, r0, nr, c0, nc = one
                r0, c0 = (r0 + n * nr, c0) if nc == D else (r0, pl.multiple_of(c0 + n * nc, 256))

                @pl.when((m < ITEMS) & cond)
                def _():
                    fn(False, layer, (name, r0, nr, c0, nc), slot)
            else:
                for which, piece in enumerate((one, two)):
                    @pl.when((m < ITEMS) & cond & (n == which))
                    def _():
                        fn(mark == 1 and which == 1, layer, piece, slot)

    def view(bufs, name, layer, r0, nr, c0, nc, half):
        if half:
            nr = nr // 2
            r0 = r0 + y * nr
        r0 = pl.multiple_of(r0, 16)
        return bufs[name].at[layer, pl.ds(r0, nr), pl.ds(c0, nc)]

    def remote(src, dst, ss, rs, dev, half):
        def make(whole, layer, piece, slot):
            part = half and not whole
            return pltpu.make_async_remote_copy(
                src_ref=view(src, piece[0], layer, *piece[1:], part),
                dst_ref=view(dst, piece[0], layer, *piece[1:], part),
                send_sem=ss.at[slot], recv_sem=rs.at[slot], device_id=dev, device_id_type=MESH)
        return make

    copy0 = remote(own, b1, s0s, s0r, c_dev, False)
    copy1 = remote(own, b2, s1s, s1r, x_dev, True)
    copy2 = remote(b2, b2, s2s, s2r, y_dev, True)

    def rest_rows(c0):
        return a_ref.at[pl.ds(pl.multiple_of(c0 // WIDE * REST_K + core * TAIL, 64), TAIL), pl.ds(FF, WIDE)]

    def copy3(mark, layer, piece, slot):
        name, r0, nr, c0, nc = piece
        if mark == 0:
            return remote(b2, b3, s3s, s3r, c_dev, False)(False, layer, piece, slot)
        if mark == 1:
            dst = rest_rows(c0)
        else:
            dst = far_ref.at[pl.ds(pl.multiple_of(r0 - core * TAIL - (N_D - 1) * 256 + 256, 128), nr), :]
        return pltpu.make_async_remote_copy(
            src_ref=view(b2, name, layer, r0, nr, c0, nc, False), dst_ref=dst,
            send_sem=s3s.at[slot], recv_sem=s3r.at[slot], device_id=c_dev, device_id_type=MESH)

    def start0(*a):
        copy0(*a).start()

    def start1(*a):
        copy1(*a).start()

    def wait0(*a):
        copy0(*a).wait_recv()

    def relay2(*a):
        copy1(*a).wait_recv()
        if not a[0]:
            copy2(*a).start()

    def arrived(*a):
        if not a[0]:
            copy2(*a).wait_recv()
        copy1(*a).wait_send()

    def relay3(*a):
        copy3(*a).start()

    def pushed(*a):
        copy0(*a).wait_send()

    def finish(*a):
        copy3(*a).wait_recv()
        copy3(*a).wait_send()

    def sent(*a):
        if not a[0]:
            copy2(*a).wait_send()

    def targets(s):
        i = lax.rem(s, STEPS)
        layer = s // STEPS
        first = layer == 0
        late = 1 - jnp.minimum(layer, 1)
        t2 = jnp.where(i < ST_A, 9 + 2 * i + late,
             jnp.where(i < ST_G + 1, 18 + late + 3 * (i - ST_A) // 5,
             jnp.where(i < ST_D, jnp.maximum(i + 4, 31 + late + (i - ST_G - 1) // 2),
             jnp.where(i < ST_NEAR, jnp.maximum(i, ST_D + 3 + (2 * (i - ST_D) + 1) // 3),
             jnp.where(first, jnp.where(i < ST_NEAR + 2, i, jnp.where(i < ST_READY - 2, 40 + i // 2, jnp.where(i < ST_READY, i - 2, i - 3))),
             jnp.where(i < ST_READY - 2, 38 + (i + 1) // 2, 39 + i // 2))))))
        final = i == STEPS - 1
        t3 = jnp.where(i < ST_D, jnp.where(i < ST_A, 3 + i, (t2 - 3) // 2),
             jnp.where(first, jnp.where(i < ST_IDLE, (t2 - 2) // 2, CH_DR + (i - ST_IDLE + 1) // 2 + jnp.where(final, 1, 0)),
             jnp.where(i < ST_READY - 4, (t2 - 2) // 2, jnp.where(i < ST_READY + 2, 39 + (i - ST_READY + 4) // 3, i - ST_READY + 39 + jnp.where(i == ST_FAR, 1, 0)))))
        end = s >= ALL_STEPS - 2
        t2 = jnp.minimum(t2 + layer * 2 * PER_LAYER, jnp.where(end, ITEMS, ITEMS - 1))
        t3 = jnp.minimum(t3 + layer * PER_LAYER, PUSHES)
        nxt = jnp.minimum(s + 1, ALL_STEPS - 1)
        i = lax.rem(nxt, STEPS)
        base = nxt // STEPS * PER_LAYER
        done = jnp.where(i < ST_A, 1 + i,
               jnp.where(i < ST_O, ST_A,
               jnp.where(i < ST_G, 1 + CH_O + i - ST_O,
               jnp.where(i < ST_D, 1 + CH_GU + (i - ST_G) // 2,
               jnp.where(i < ST_NEAR, 1 + CH_D + (i - ST_D) // 2,
               jnp.where(i < ST_READY, CH_D + (i - ST_D) // 2,
               jnp.where(i < ST_READY + 1, CH_DR - 2,
               jnp.where(i < ST_FAR, CH_DR - 1,
               jnp.where(i < ST_REST, CH_DR, PER_LAYER)))))))))
        tf = jnp.maximum(jnp.minimum(t3 - 2, CHUNKS - 2), done + base)
        pushes = tf + jnp.where(tf == CHUNKS - 1, 1, 0)
        t3 = jnp.maximum(jnp.maximum(t3, pushes), base + jnp.where((i >= ST_READY) & (i < ST_FAR), CH_DR - 1, 0))
        return jnp.maximum(t2, 2 * jnp.minimum(t3, CHUNKS - 2)), t3, tf

    def relays(old, new):
        @pl.loop(old[0], new[0])
        def _(m):
            with jax.named_scope("r2"):
                for_item(m, relay2)
                for_item(m + AHEAD, start1)
                n = lax.rem(m, 2)
                for_chunk(m // 2 + jnp.where(n == 0, AHEAD0, CHUNKS), start0)
                for_chunk(m // 2 + jnp.where(n == 0, CHUNKS, AHEAD0 - 1), wait0)

        @pl.loop(old[1], new[1])
        def _(p):
            with jax.named_scope("r3"):
                extra = jnp.maximum(p - (CHUNKS - 2), 0)
                k = p - jnp.minimum(extra, 1)
                part = jnp.where((p < CHUNKS - 2) | (extra > 1), 2, extra)
                for_pair(k, arrived, part)
                for_chunk(k, relay3, 3, part)
                for_chunk(jnp.where(part == 1, CHUNKS, k), pushed)

        @pl.loop(old[2], new[2])
        def _(k):
            with jax.named_scope("fin"):
                for_chunk(k, finish, 3)
                for_pair(k, sent)

    def down_step(i):
        n = i - ST_D - jnp.where(i > ST_READY, 1, 0) - jnp.where(i > ST_IDLE, 1, 0)
        j = n // 2
        near = (i >= ST_NEAR) & (i < ST_NEAR + 2)
        far = (i >= ST_FAR) & (i < ST_REST)
        rest = i >= ST_REST
        whole = (i >= ST_D) & (i < ST_IDLE) & ~near & (i != ST_READY)
        return j, jnp.where(i > ST_NEAR, j - 1, j), lax.rem(n + 2 * STEPS, 2), whole, near, far, rest

    def rest_col(side_no):
        return pl.multiple_of(side_no * (2 * FF_ROWS) + 2560, HEAD)

    def tile_col(side_no, core_no, tile):
        return pl.multiple_of(side_no * (2 * FF_ROWS) + core_no * (FF_ROWS + TAIL) + tile * 256, HEAD)

    def near_far():
        r0 = pl.multiple_of(core * TAIL + (N_D - 1) * 256, 64)
        return pltpu.make_async_copy(b2["d"].at[LAYERS - 1, pl.ds(r0, 256), :], far_ref.at[pl.ds(0, 256), :], lsem.at[0])

    def near_rest():
        r0 = pl.multiple_of((1 - core) * 2560, 512)
        return [pltpu.make_async_copy(b2["d"].at[LAYERS - 1, pl.ds(r0, TAIL), pl.ds(n * WIDE, WIDE)], rest_rows(n * WIDE), lsem.at[1 + n])
                for n in range(2)]

    def load_tile(s):
        layer = s // STEPS
        i = lax.rem(s, STEPS)
        slot = lax.rem(s, 2)

        def cols(name, c0, nc, w0):
            for r, src in enumerate(sources):
                pltpu.make_async_copy(src[name].at[layer, :, pl.ds(c0, nc)],
                                      wbuf.at[slot, pl.ds(r * ROWS, ROWS), pl.ds(w0, nc)], wsem.at[slot]).start()

        @pl.when(i == 0)
        def _():
            cols("k", 0, 256, 0)
            cols("v", 0, 256, 256)

        @pl.when((i >= ST_Q) & (i < ST_A))
        def _():
            cols("q", pl.multiple_of((i - ST_Q) * 512, 512), 512, 0)

        @pl.when((i >= ST_O) & (i < ST_G))
        def _():
            cols("o", pl.multiple_of((i - ST_O) * 512, 512), 512, 0)

        @pl.when((i >= ST_G) & (i < ST_D))
        def _():
            c0 = pl.multiple_of((i - ST_G) * 256, 256)
            cols("g", c0, 256, 0)
            cols("u", c0, 256, 256)

        j, tile, half, whole, near, far, rest = down_step(i)
        dslot = lax.rem(j + 2 * STEPS, 2)

        def rows_in(src, r0, nr, w0):
            pltpu.make_async_copy(src["d"].at[layer, pl.ds(r0, nr), :], dbuf.at[dslot, pl.ds(w0, nr), :], dsem.at[dslot]).start()

        def chunk_rows(r, tile_no, w0):
            src_core = core if r % 2 == 0 else 1 - core
            rows_in(sources[r], pl.multiple_of(src_core * TAIL + tile_no * 256, 64), 256, w0)

        def rest_rows(r, w0):
            src_core = core if r % 2 == 0 else 1 - core
            rows_in(sources[r], pl.multiple_of((1 - src_core) * 2560, 512), TAIL, pl.multiple_of(w0 + src_core * TAIL, 64))

        @pl.when((whole & (half == 0) & (i != ST_READY + 1)) | (i == ST_READY))
        def _():
            for r in range(3):
                chunk_rows(r, jnp.where(i == ST_READY, N_D - 2, tile), r * 256)

        @pl.when(whole & (half == 0))
        def _():
            chunk_rows(3, tile, 768)

        @pl.when(near & (half == 0))
        def _():
            for r in range(2):
                chunk_rows(r, N_D - 1, r * 256)
                rest_rows(r, 512)

        @pl.when(far & (half == 0) & (layer < LAYERS - 1))
        def _():
            for r in range(2):
                chunk_rows(2 + r, N_D - 1, r * 256)

        @pl.when(far & (half == 0) & (layer == LAYERS - 1))
        def _():
            near_far().start()

        @pl.when(rest & (half == 0))
        def _():
            for r in range(2):
                rest_rows(2 + r, 0)

    def norm(layer, which):
        @pl.loop(0, TOK // NB)
        def _(m):
            rows = pl.ds(pl.multiple_of(m * NB, NB), NB)
            total = jnp.zeros((NB, 1), F32)
            for b in range(4):
                blk = x_ref[rows, pl.ds(b * ROWS, ROWS)]
                total = total + jnp.sum(blk * blk, axis=1, keepdims=True)
            inv = lax.rsqrt(total * (1.0 / D) + EPS)
            for b in range(4):
                blk = x_ref[rows, pl.ds(b * ROWS, ROWS)]
                gain = gain_ref[which * LAYERS + layer, :, pl.ds(b * ROWS, ROWS)]
                c0 = pl.multiple_of(rel(b) * ROWS, ROWS)
                h_ref[rows, pl.ds(c0, ROWS)] = (blk * inv * gain).astype(BF16)

    def rotate(vals, rows):
        vals = vals.astype(BF16).astype(F32)
        turned = pltpu.roll(vals, HEAD // 2, 1)
        return (vals * cos_ref[rows, :] + turned * sin_ref[rows, :]).astype(BF16)

    def tile_product(slot, finish_rows):
        @pl.loop(0, TOK // MB)
        def _(m):
            rows = pl.ds(pl.multiple_of(m * MB, MB), MB)
            finish_rows(rows, jnp.dot(h_ref[rows, :], wbuf[slot], preferred_element_type=F32))

    def kv_step(slot):
        def fin(rows, acc):
            for b in range(2):
                kv_ref[rows, pl.ds(b * HEAD, HEAD)] = rotate(acc[:, b * HEAD:(b + 1) * HEAD], rows)
            kv_ref[rows, pl.ds(256, 256)] = acc[:, 256:].astype(BF16)
        tile_product(slot, fin)

    def q_step(slot, j):
        def fin(rows, acc):
            for b in range(4):
                c0 = pl.multiple_of(j * 512 + b * HEAD, HEAD)
                q_ref[rows, pl.ds(c0, HEAD)] = rotate(acc[:, b * HEAD:(b + 1) * HEAD], rows)
        tile_product(slot, fin)

    def o_step(slot, j):
        def fin(rows, acc):
            c0 = pl.ds(pl.multiple_of(j * 512, 512), 512)
            x_ref[rows, c0] = x_ref[rows, c0] + acc
        tile_product(slot, fin)

    def g_step(slot, j):
        def fin(rows, acc):
            gate = acc[:, :256]
            up = acc[:, 256:]
            c0 = pl.multiple_of(j * 256, 256)
            a_ref[rows, pl.ds(c0, 256)] = (gate * jax.nn.sigmoid(gate) * up).astype(BF16)
        tile_product(slot, fin)

    def attend(head):
        kv = head // 8
        q0 = pl.multiple_of(head * HEAD, HEAD)
        k0 = pl.multiple_of(kv * HEAD, HEAD)
        v0 = pl.multiple_of(256 + kv * HEAD, HEAD)
        o0 = pl.multiple_of(rel(head // 4) * ROWS + lax.rem(head, 4) * HEAD, HEAD)
        scale = HEAD ** -0.5
        for b in range(TOK // QB):
            keys = (b + 1) * QB
            rows = pl.ds(b * QB, QB)
            scores = lax.dot_general(q_ref[rows, pl.ds(q0, HEAD)], kv_ref[pl.ds(0, keys), pl.ds(k0, HEAD)],
                                     (((1,), (1,)), ((), ())), preferred_element_type=F32)
            key_idx = lax.broadcasted_iota(jnp.int32, (QB, keys), 1)
            row_idx = lax.broadcasted_iota(jnp.int32, (QB, keys), 0) + b * QB
            first = jnp.concatenate([first_ref[rows, :]] * (keys // HEAD), axis=1)
            ok = (key_idx >= first) & (key_idx <= row_idx)
            scores = jnp.where(ok, scores, -1e30)
            top = jnp.max(scores, axis=1, keepdims=True)
            probs = jnp.exp((scores - top) * scale)
            inv = 1.0 / jnp.sum(probs, axis=1, keepdims=True)
            probs = (probs * inv).astype(BF16)
            mixed = jnp.dot(probs, kv_ref[pl.ds(0, keys), pl.ds(v0, HEAD)], preferred_element_type=F32)
            h_ref[rows, pl.ds(o0, HEAD)] = mixed.astype(BF16)

    def add_product(dslot, half, cols, tile_ref=None):
        rows = pl.ds(pl.multiple_of(half * MB, MB), MB)
        depth = sum(width for _, width in cols)
        lhs = jnp.concatenate([a_ref[rows, pl.ds(c0, width)] for c0, width in cols], axis=1)
        tile = dbuf[dslot, pl.ds(0, depth), :] if tile_ref is None else tile_ref[...]
        x_ref[rows, :] = x_ref[rows, :] + jnp.dot(lhs, tile, preferred_element_type=F32)

    def wait_d(dslot, half, depth):
        @pl.when(half == 0)
        def _():
            part = dbuf.at[dslot, pl.ds(0, depth), :]
            pltpu.make_async_copy(part, part, dsem.at[dslot]).wait()

    def last_cols(side_no):
        return [(tile_col(side_no, core, N_D - 1), 256), (tile_col(side_no, 1 - core, N_D - 1), 256)]

    def wait_w(slot):
        pltpu.make_async_copy(wbuf.at[slot], wbuf.at[slot], wsem.at[slot]).wait()

    def step(s):
        before = [jnp.where(s == 0, one, two) for one, two in zip(FIRST, targets(s - 1))]
        relays(before, targets(s))

        @pl.when(s + 1 < ALL_STEPS)
        def _():
            load_tile(s + 1)

        with jax.named_scope("comp"):
            compute(s)

    def compute(s):
        layer = s // STEPS
        i = lax.rem(s, STEPS)
        slot = lax.rem(s, 2)

        @pl.when(((i == 0) & (layer > 0)) | (i == ST_G))
        def _():
            norm(layer, jnp.where(i == 0, 0, 1))

        @pl.when((i < ST_A) | ((i >= ST_O) & (i < ST_D)))
        def _():
            wait_w(slot)

        @pl.when(i == 0)
        def _():
            kv_step(slot)

        @pl.when((i >= ST_Q) & (i < ST_A))
        def _():
            q_step(slot, i - ST_Q)

        @pl.when((i >= ST_A) & (i < ST_O))
        def _():
            attend(i - ST_A)

        @pl.when((i >= ST_O) & (i < ST_G))
        def _():
            o_step(slot, i - ST_O)

        @pl.when((i >= ST_G) & (i < ST_D))
        def _():
            g_step(slot, i - ST_G)

        j, tile, half, whole, near, far, rest = down_step(i)
        dslot = lax.rem(j + 2 * STEPS, 2)

        @pl.when(whole)
        def _():
            wait_d(dslot, half, 1024)
            add_product(dslot, half, [(tile_col(lax.rem(side + r // 2, 2), lax.rem(core + r, 2), tile), 256) for r in range(4)])

        @pl.when(near)
        def _():
            wait_d(dslot, half, NEAR_K)
            add_product(dslot, half, last_cols(side) + [(rest_col(side), REST_K)])

        @pl.when(far & (layer < LAYERS - 1))
        def _():
            wait_d(dslot, half, 512)
            add_product(dslot, half, last_cols(1 - side))

        @pl.when(far & (layer == LAYERS - 1))
        def _():
            @pl.when(half == 0)
            def _():
                near_far().wait()
                for copy in near_rest():
                    copy.start()
            add_product(dslot, half, last_cols(1 - side), far_ref)

        @pl.when(rest)
        def _():
            wait_d(dslot, half, REST_K)
            add_product(dslot, half, [(rest_col(1 - side), REST_K)])

    @pl.loop(0, AHEAD)
    def _(m):
        for_item(m, start1)

    @pl.loop(0, AHEAD0)
    def _(k):
        for_chunk(k, start0)

    for copy in inputs:
        copy.wait()

    for n, ref in enumerate((ga_ref, gm_ref)):
        for layer in range(LAYERS):
            gain_ref[n * LAYERS + layer] = ref[pl.ds(layer, 1), :].astype(F32)
    ids = seg_ref[...].astype(F32)
    lane = lax.broadcasted_iota(jnp.int32, (128, HEAD), 1)
    for b in range(TOK // 128):
        rows = pl.ds(b * 128, 128)
        mine = jnp.transpose(jnp.broadcast_to(ids[b:b + 1, :], (128, 128)))
        before = jnp.zeros((128, 128), F32)
        for c in range(TOK // 128):
            before = before + jnp.where(ids[c:c + 1, :] < mine, 1.0, 0.0)
        first = jnp.sum(before, axis=1, keepdims=True)
        pos = lax.broadcasted_iota(jnp.int32, (128, 128), 0).astype(F32) + (b * 128.0) - first
        angles = pos * freq_ref[...]
        cos_ref[rows, :] = jnp.cos(angles)
        sin = jnp.sin(angles)
        sin_ref[rows, :] = jnp.where(lane < HEAD // 2, -sin, sin)
        first_ref[rows, :] = jnp.broadcast_to(first, (128, 128)).astype(jnp.int32)

    @pl.loop(0, TOK // NB)
    def _(m):
        rows = pl.ds(pl.multiple_of(m * NB, NB), NB)
        x_ref[rows, :] = q_ref[rows, :].astype(F32)

    relays((0, 0, 0), (2, 0, 0))
    norm(0, 0)

    @pl.loop(0, AHEAD0 - 1)
    def _(k):
        for_chunk(k, wait0)

    relays((2, 0, 0), START)
    relays(START, FIRST)
    load_tile(0)

    @pl.loop(0, ALL_STEPS)
    def _(s):
        with jax.named_scope("step"):
            step(s)

    relays(targets(ALL_STEPS - 1), (ITEMS, PUSHES, CHUNKS))
    for copy in near_rest():
        copy.wait()


def result_kernel(x_ref, a_ref, out, y_ref, osem):
    c0 = pl.multiple_of((1 - lax.axis_index("fsdp") // 2) * (2 * FF_ROWS) + 2560, HEAD)

    def store(n, m):
        rows, cols = pl.ds(m * 512, 512), pl.ds(n * 512, 512)
        return pltpu.make_async_copy(y_ref.at[rows, cols], out.at[rows, cols], osem.at[n, m])

    for n in range(4):
        cols = pl.ds(n * 512, 512)
        tile = a_ref[pl.ds(n // 2 * REST_K, REST_K), pl.ds(FF + n % 2 * 512, 512)]
        for m in range(2):
            rows = pl.ds(m * 512, 512)
            y_ref[rows, cols] = x_ref[rows, cols] + jnp.dot(a_ref[rows, pl.ds(c0, REST_K)], tile, preferred_element_type=F32)
            store(n, m).start()
    for n in range(4):
        for m in range(2):
            store(n, m).wait()


def run_layers(tokens, seg_ids, g_attn, g_mlp, weights):
    shapes = [jax.ShapeDtypeStruct(w.shape, w.dtype) for w in weights]
    half_dim = HEAD // 2
    freq = np.float32(ROPE_BASE) ** (-np.arange(half_dim, dtype=np.float32) / np.float32(half_dim))
    freq = jnp.asarray(np.concatenate([freq, freq]).reshape(1, HEAD))
    sem = pltpu.SemaphoreType.DMA((SLOTS, 2))
    item_sem = pltpu.SemaphoreType.DMA((ITEM_SLOTS,))
    any_spec = pl.BlockSpec(memory_space=pl.ANY)
    vmem_spec = pl.BlockSpec(memory_space=pltpu.VMEM)
    outs = pl.pallas_call(
        layer_kernel,
        out_shape=[pltpu.VMEM((TOK, D), F32), pltpu.VMEM((TOK, FF + WIDE), BF16)] + shapes * 3,
        in_specs=[any_spec] * 12,
        out_specs=[vmem_spec] * 2 + [any_spec] * 21,
        scratch_shapes=[
            pltpu.VMEM((TOK, D), BF16),
            pltpu.VMEM((TOK, D), BF16),
            pltpu.VMEM((TOK, 512), BF16),
            pltpu.VMEM((2, D, 512), BF16),
            pltpu.VMEM((2, 1024, D), BF16),
            pltpu.VMEM((TOK, HEAD), F32),
            pltpu.VMEM((TOK, HEAD), F32),
            pltpu.VMEM((TOK, HEAD), jnp.int32),
            pltpu.VMEM((2 * LAYERS, 1, D), F32),
            pltpu.VMEM((TOK // 128, 128), jnp.int32),
            pltpu.VMEM((1, HEAD), F32),
            pltpu.VMEM((LAYERS, D), BF16),
            pltpu.VMEM((LAYERS, D), BF16),
            pltpu.VMEM((512, D), BF16),
            pltpu.SemaphoreType.DMA((2,)),
            pltpu.SemaphoreType.DMA((2,)),
            pltpu.SemaphoreType.DMA((5,)),
            pltpu.SemaphoreType.DMA((3,)),
        ] + [sem] * 2 + [item_sem] * 4 + [sem] * 2,
        compiler_params=pltpu.CompilerParams(collective_id=0, has_side_effects=True, vmem_limit_bytes=32 * 1000 * 1000),
        name="two_layers",
    )(tokens, seg_ids.reshape(TOK // 128, 128), freq, g_attn, g_mlp, *weights)
    hidden = pltpu.with_memory_space_constraint(outs[0], pltpu.VMEM)
    act = pltpu.with_memory_space_constraint(outs[1], pltpu.VMEM)
    return pl.pallas_call(
        result_kernel,
        out_shape=jax.ShapeDtypeStruct((TOK, D), F32),
        in_specs=[vmem_spec] * 2,
        out_specs=any_spec,
        scratch_shapes=[
            pltpu.VMEM((TOK, D), F32),
            pltpu.SemaphoreType.DMA((4, 2)),
        ],
        compiler_params=pltpu.CompilerParams(vmem_limit_bytes=24 * 1000 * 1000),
        name="result",
    )(hidden, act)


def solution(mesh):
    tok_spec = P(("rep", "fsdp"), None)
    seg_spec = P(("rep", "fsdp"))
    mat_spec = P(None, "fsdp", None)
    gain_spec = P(None, None)

    def per_device(tokens, seg_ids, w_q, w_k, w_v, w_o, w_gate, w_up, w_down, g_attn, g_mlp):
        return run_layers(tokens, seg_ids, g_attn, g_mlp, (w_q, w_k, w_v, w_o, w_gate, w_up, w_down))

    return jax.shard_map(per_device, mesh=mesh, in_specs=(tok_spec, seg_spec, mat_spec, mat_spec, mat_spec, mat_spec, mat_spec, mat_spec, mat_spec, gain_spec, gain_spec), out_specs=tok_spec, check_vma=False)
```

```python
import functools

import jax
import jax.numpy as jnp
import numpy as np
from jax import lax
from jax.experimental import pallas as pl
from jax.experimental.pallas import tpu as pltpu
from jax.sharding import PartitionSpec as P

D = 2048
FF = 11008
HEADS = 16
HEAD = 128
TOK = 1024
EPS = 1e-5
ROPE_BASE = 10000.0
MESH = pl.DeviceIdType.MESH
F32 = jnp.float32
BF16 = jnp.bfloat16

LAYERS = 2
SLOTS = 8
ITEM_SLOTS = 2 * SLOTS
AHEAD = 8
AHEAD0 = 5
ROWS = D // 4
FF_ROWS = FF // 4
TAIL = 192
NAMES = ("q", "k", "v", "o", "g", "u", "d")

N_Q = 4
N_GU = 21
N_D = 10
CH_Q = 1
CH_O = CH_Q + N_Q
CH_GU = CH_O + N_Q
CH_GL = CH_GU + N_GU
CH_D = CH_GL + 1
CH_DR = CH_D + N_D
PER_LAYER = CH_DR + 1
CHUNKS = LAYERS * PER_LAYER
ITEMS = 2 * CHUNKS
PUSHES = CHUNKS + 1

NEAR_AT = 5

N_GT = FF // 256
ST_Q = 1
ST_A = ST_Q + N_Q
ST_O = ST_A + HEADS
ST_G = ST_O + 4
ST_D = ST_G + N_GT
ST_NEAR = ST_D + 2 * NEAR_AT
ST_READY = ST_D + 2 * (N_D - 1)
ST_IDLE = ST_READY + 3
ST_FAR = ST_IDLE + 1
ST_REST = ST_FAR + 2
STEPS = ST_REST + 2
ALL_STEPS = LAYERS * STEPS - 2
START = (4, 1, 0)
FIRST = (8, 3, 1)
REST_K = 2 * TAIL
WIDE = D // 2
NEAR_K = 512 + REST_K

MB = 512
NB = 128
QB = 256


def layer_kernel(*refs):
    tok, seg, freq, g_attn, g_mlp = refs[:5]
    own = dict(zip(NAMES, refs[5:12]))
    x_ref, a_ref = refs[12:14]
    b1 = dict(zip(NAMES, refs[14:21]))
    b2 = dict(zip(NAMES, refs[21:28]))
    b3 = dict(zip(NAMES, refs[28:35]))
    (h_ref, q_ref, kv_ref, wbuf, dbuf, cos_ref, sin_ref, first_ref, gain_ref,
     seg_ref, freq_ref, ga_ref, gm_ref, far_ref, wsem, dsem, iosem, lsem) = refs[35:53]
    s0s, s0r, s1s, s1r, s2s, s2r, s3s, s3r = refs[53:]
    sources = (own, b1, b2, b3)
    y = lax.axis_index("rep")
    d = lax.axis_index("fsdp")
    side = d // 2
    core = lax.rem(d, 2)
    x_dev = (y, lax.rem(d + 2, 4))
    y_dev = (1 - y, d)
    c_dev = (y, d + 1 - 2 * core)

    def rel(block):
        return 2 * lax.rem(block // 2 + side, 2) + lax.rem(block + core, 2)

    inputs = [pltpu.make_async_copy(src, dst, iosem.at[n]) for n, (src, dst) in enumerate(
        ((tok, q_ref), (seg, seg_ref), (freq, freq_ref), (g_attn, ga_ref), (g_mlp, gm_ref)))]
    for copy in inputs:
        copy.start()

    with jax.named_scope("barrier"):
        barrier = pltpu.get_barrier_semaphore()
        for dev in (x_dev, y_dev, c_dev):
            pl.semaphore_signal(barrier, inc=1, device_id=dev, device_id_type=MESH)
        pl.semaphore_wait(barrier, 3)

    def kinds(k):
        i = lax.rem(k, PER_LAYER)
        jq = pl.multiple_of((i - CH_Q) * 512, 512)
        jo = pl.multiple_of((i - CH_O) * 512, 512)
        jg = pl.multiple_of((i - CH_GU) * 512, 512)
        jd = core * TAIL + (i - CH_D) * 256
        jr = (1 - core) * 2560
        last = N_GU * 512
        kv = [("k", 0, ROWS, 0, 256), ("v", 0, ROWS, 0, 256)]
        gu = [("g", 0, ROWS, jg, 512), ("u", 0, ROWS, jg, 512)]
        gl = [("g", 0, ROWS, last, 256), ("u", 0, ROWS, last, 256)]

        def split_cols(name, c0):
            whole = [(name, 0, ROWS, c0, 512)]
            return [(name, 0, ROWS, c0, 256), (name, 0, ROWS, c0 + 256, 256)], whole, whole

        def split_rows(r0, nr):
            halves = [("d", r0, nr // 2, 0, D), ("d", r0 + nr // 2, nr // 2, 0, D)]
            return halves, [("d", r0, nr, 0, D)], halves

        return [
            (i == 0, kv, kv, kv, 0),
            ((i >= CH_Q) & (i < CH_O), *split_cols("q", jq), 0),
            ((i >= CH_O) & (i < CH_GU), *split_cols("o", jo), 0),
            ((i >= CH_GU) & (i < CH_GL), gu, gu, gu, 0),
            (i == CH_GL, gl, gl, gl, 0),
            ((i >= CH_D) & (i < CH_DR) & (k != CHUNKS - 2), *split_rows(jd, 256), 0),
            (k == CHUNKS - 2, *split_rows(jd, 256), 2),
            ((i == CH_DR) & (k != CHUNKS - 1), *split_rows(jr, TAIL), 0),
            (k == CHUNKS - 1, *split_rows(jr, TAIL)[:2], [("d", jr, TAIL, 0, WIDE), ("d", jr, TAIL, WIDE, WIDE)], 1),
        ]

    def for_chunk(k, fn, form=2, part=None):
        layer = k // PER_LAYER
        slot = lax.rem(k, SLOTS)
        for kind in kinds(k):
            @pl.when((k < CHUNKS) & kind[0])
            def _():
                for n, piece in enumerate(kind[form]):
                    if part is None:
                        fn(kind[4], layer, piece, (slot, n))
                    else:
                        @pl.when(part != 1 - n)
                        def _():
                            fn(kind[4], layer, piece, (slot, n))

    def for_pair(k, fn, part=None):
        layer = k // PER_LAYER
        for cond, pieces, _, _, mark in kinds(k):
            @pl.when((k < CHUNKS) & cond)
            def _():
                for n, piece in enumerate(pieces):
                    args = (mark == 1 and n == 1, layer, piece, (lax.rem(2 * k + n, ITEM_SLOTS),))
                    if part is None:
                        fn(*args)
                    else:
                        @pl.when(part != 1 - n)
                        def _():
                            fn(*args)

    def for_item(m, fn):
        k = m // 2
        n = lax.rem(m, 2)
        layer = k // PER_LAYER
        slot = (lax.rem(m, ITEM_SLOTS),)
        for cond, (one, two), _, _, mark in kinds(k):
            if one[0] == two[0] and mark != 1:
                name, r0, nr, c0, nc = one
                r0, c0 = (r0 + n * nr, c0) if nc == D else (r0, pl.multiple_of(c0 + n * nc, 256))

                @pl.when((m < ITEMS) & cond)
                def _():
                    fn(False, layer, (name, r0, nr, c0, nc), slot)
            else:
                for which, piece in enumerate((one, two)):
                    @pl.when((m < ITEMS) & cond & (n == which))
                    def _():
                        fn(mark == 1 and which == 1, layer, piece, slot)

    def view(bufs, name, layer, r0, nr, c0, nc, half):
        if half:
            nr = nr // 2
            r0 = r0 + y * nr
        r0 = pl.multiple_of(r0, 16)
        return bufs[name].at[layer, pl.ds(r0, nr), pl.ds(c0, nc)]

    def remote(src, dst, ss, rs, dev, half):
        def make(whole, layer, piece, slot):
            part = half and not whole
            return pltpu.make_async_remote_copy(
                src_ref=view(src, piece[0], layer, *piece[1:], part),
                dst_ref=view(dst, piece[0], layer, *piece[1:], part),
                send_sem=ss.at[slot], recv_sem=rs.at[slot], device_id=dev, device_id_type=MESH)
        return make

    copy0 = remote(own, b1, s0s, s0r, c_dev, False)
    copy1 = remote(own, b2, s1s, s1r, x_dev, True)
    copy2 = remote(b2, b2, s2s, s2r, y_dev, True)

    def rest_rows(c0):
        return a_ref.at[pl.ds(pl.multiple_of(c0 // WIDE * REST_K + core * TAIL, 64), TAIL), pl.ds(FF, WIDE)]

    def copy3(mark, layer, piece, slot):
        name, r0, nr, c0, nc = piece
        if mark == 0:
            return remote(b2, b3, s3s, s3r, c_dev, False)(False, layer, piece, slot)
        if mark == 1:
            dst = rest_rows(c0)
        else:
            dst = far_ref.at[pl.ds(pl.multiple_of(r0 - core * TAIL - (N_D - 1) * 256 + 256, 128), nr), :]
        return pltpu.make_async_remote_copy(
            src_ref=view(b2, name, layer, r0, nr, c0, nc, False), dst_ref=dst,
            send_sem=s3s.at[slot], recv_sem=s3r.at[slot], device_id=c_dev, device_id_type=MESH)

    def start0(*a):
        copy0(*a).start()

    def start1(*a):
        copy1(*a).start()

    def wait0(*a):
        copy0(*a).wait_recv()

    def relay2(*a):
        copy1(*a).wait_recv()
        if not a[0]:
            copy2(*a).start()

    def arrived(*a):
        if not a[0]:
            copy2(*a).wait_recv()
        copy1(*a).wait_send()

    def relay3(*a):
        copy3(*a).start()

    def pushed(*a):
        copy0(*a).wait_send()

    def finish(*a):
        copy3(*a).wait_recv()
        copy3(*a).wait_send()

    def sent(*a):
        if not a[0]:
            copy2(*a).wait_send()

    def targets(s):
        i = lax.rem(s, STEPS)
        layer = s // STEPS
        first = layer == 0
        late = 1 - jnp.minimum(layer, 1)
        t2 = jnp.where(i < ST_A, 9 + 2 * i + late,
             jnp.where(i < ST_G + 1, 19 + late + 3 * (i - ST_A) // 5,
             jnp.where(i < ST_D, jnp.maximum(i + 4, 32 + late + (i - ST_G - 1) // 2),
             jnp.where(i < ST_NEAR, jnp.maximum(i, ST_D + 3 + (2 * (i - ST_D) + 1) // 3),
             jnp.where(first, jnp.where(i < ST_NEAR + 2, i, jnp.where(i < ST_READY - 2, 40 + i // 2, jnp.where(i < ST_READY, i - 2, i - 3))),
             jnp.where(i < ST_READY - 4, 38 + (i + 1) // 2, 39 + i // 2))))))
        final = i == STEPS - 1
        t3 = jnp.where(i < ST_D, jnp.where(i < ST_A, 3 + i, (t2 - 3) // 2),
             jnp.where(first, jnp.where(i < ST_IDLE, (t2 - 2) // 2, CH_DR + (i - ST_IDLE + 1) // 2 + jnp.where(final, 1, 0)),
             jnp.where(i < ST_READY - 4, (t2 - 2) // 2, jnp.where(i < ST_READY + 2, 39 + (i - ST_READY + 4) // 3, i - ST_READY + 39 + jnp.where(i == ST_FAR, 1, 0)))))
        end = s >= ALL_STEPS - 2
        t2 = jnp.minimum(t2 + layer * 2 * PER_LAYER, jnp.where(end, ITEMS, ITEMS - 1))
        t3 = jnp.minimum(t3 + layer * PER_LAYER, PUSHES)
        nxt = jnp.minimum(s + 1, ALL_STEPS - 1)
        i = lax.rem(nxt, STEPS)
        base = nxt // STEPS * PER_LAYER
        done = jnp.where(i < ST_A, 1 + i,
               jnp.where(i < ST_O, ST_A,
               jnp.where(i < ST_G, 1 + CH_O + i - ST_O,
               jnp.where(i < ST_D, 1 + CH_GU + (i - ST_G) // 2,
               jnp.where(i < ST_NEAR, 1 + CH_D + (i - ST_D) // 2,
               jnp.where(i < ST_READY, CH_D + (i - ST_D) // 2,
               jnp.where(i < ST_READY + 1, CH_DR - 2,
               jnp.where(i < ST_FAR, CH_DR - 1,
               jnp.where(i < ST_REST, CH_DR, PER_LAYER)))))))))
        tf = jnp.maximum(jnp.minimum(t3 - 2, CHUNKS - 2), done + base)
        pushes = tf + jnp.where(tf == CHUNKS - 1, 1, 0)
        t3 = jnp.maximum(jnp.maximum(t3, pushes), base + jnp.where((i >= ST_READY) & (i < ST_FAR), CH_DR - 1, 0))
        return jnp.maximum(t2, 2 * jnp.minimum(t3, CHUNKS - 2)), t3, tf

    def relays(old, new):
        @pl.loop(old[0], new[0])
        def _(m):
            with jax.named_scope("r2"):
                for_item(m, relay2)
                for_item(m + AHEAD, start1)
                n = lax.rem(m, 2)
                for_chunk(m // 2 + jnp.where(n == 0, AHEAD0, CHUNKS), start0)
                for_chunk(m // 2 + jnp.where(n == 0, CHUNKS, AHEAD0 - 1), wait0)

        @pl.loop(old[1], new[1])
        def _(p):
            with jax.named_scope("r3"):
                extra = jnp.maximum(p - (CHUNKS - 2), 0)
                k = p - jnp.minimum(extra, 1)
                part = jnp.where((p < CHUNKS - 2) | (extra > 1), 2, extra)
                for_pair(k, arrived, part)
                for_chunk(k, relay3, 3, part)
                for_chunk(jnp.where(part == 1, CHUNKS, k), pushed)

        @pl.loop(old[2], new[2])
        def _(k):
            with jax.named_scope("fin"):
                for_chunk(k, finish, 3)
                for_pair(k, sent)

    def down_step(i):
        n = i - ST_D - jnp.where(i > ST_READY, 1, 0) - jnp.where(i > ST_IDLE, 1, 0)
        j = n // 2
        near = (i >= ST_NEAR) & (i < ST_NEAR + 2)
        far = (i >= ST_FAR) & (i < ST_REST)
        rest = i >= ST_REST
        whole = (i >= ST_D) & (i < ST_IDLE) & ~near & (i != ST_READY)
        return j, jnp.where(i > ST_NEAR, j - 1, j), lax.rem(n + 2 * STEPS, 2), whole, near, far, rest

    def rest_col(side_no):
        return pl.multiple_of(side_no * (2 * FF_ROWS) + 2560, HEAD)

    def tile_col(side_no, core_no, tile):
        return pl.multiple_of(side_no * (2 * FF_ROWS) + core_no * (FF_ROWS + TAIL) + tile * 256, HEAD)

    def near_far():
        r0 = pl.multiple_of(core * TAIL + (N_D - 1) * 256, 64)
        return pltpu.make_async_copy(b2["d"].at[LAYERS - 1, pl.ds(r0, 256), :], far_ref.at[pl.ds(0, 256), :], lsem.at[0])

    def near_rest():
        r0 = pl.multiple_of((1 - core) * 2560, 512)
        return [pltpu.make_async_copy(b2["d"].at[LAYERS - 1, pl.ds(r0, TAIL), pl.ds(n * WIDE, WIDE)], rest_rows(n * WIDE), lsem.at[1 + n])
                for n in range(2)]

    def load_tile(s):
        layer = s // STEPS
        i = lax.rem(s, STEPS)
        slot = lax.rem(s, 2)

        def cols(name, c0, nc, w0):
            for r, src in enumerate(sources):
                pltpu.make_async_copy(src[name].at[layer, :, pl.ds(c0, nc)],
                                      wbuf.at[slot, pl.ds(r * ROWS, ROWS), pl.ds(w0, nc)], wsem.at[slot]).start()

        @pl.when(i == 0)
        def _():
            cols("k", 0, 256, 0)
            cols("v", 0, 256, 256)

        @pl.when((i >= ST_Q) & (i < ST_A))
        def _():
            cols("q", pl.multiple_of((i - ST_Q) * 512, 512), 512, 0)

        @pl.when((i >= ST_O) & (i < ST_G))
        def _():
            cols("o", pl.multiple_of((i - ST_O) * 512, 512), 512, 0)

        @pl.when((i >= ST_G) & (i < ST_D))
        def _():
            c0 = pl.multiple_of((i - ST_G) * 256, 256)
            cols("g", c0, 256, 0)
            cols("u", c0, 256, 256)

        j, tile, half, whole, near, far, rest = down_step(i)
        dslot = lax.rem(j + 2 * STEPS, 2)

        def rows_in(src, r0, nr, w0):
            pltpu.make_async_copy(src["d"].at[layer, pl.ds(r0, nr), :], dbuf.at[dslot, pl.ds(w0, nr), :], dsem.at[dslot]).start()

        def chunk_rows(r, tile_no, w0):
            src_core = core if r % 2 == 0 else 1 - core
            rows_in(sources[r], pl.multiple_of(src_core * TAIL + tile_no * 256, 64), 256, w0)

        def rest_rows(r, w0):
            src_core = core if r % 2 == 0 else 1 - core
            rows_in(sources[r], pl.multiple_of((1 - src_core) * 2560, 512), TAIL, pl.multiple_of(w0 + src_core * TAIL, 64))

        @pl.when((whole & (half == 0) & (i != ST_READY + 1)) | (i == ST_READY))
        def _():
            for r in range(3):
                chunk_rows(r, jnp.where(i == ST_READY, N_D - 2, tile), r * 256)

        @pl.when(whole & (half == 0))
        def _():
            chunk_rows(3, tile, 768)

        @pl.when(near & (half == 0))
        def _():
            for r in range(2):
                chunk_rows(r, N_D - 1, r * 256)
                rest_rows(r, 512)

        @pl.when(far & (half == 0) & (layer < LAYERS - 1))
        def _():
            for r in range(2):
                chunk_rows(2 + r, N_D - 1, r * 256)

        @pl.when(far & (half == 0) & (layer == LAYERS - 1))
        def _():
            near_far().start()

        @pl.when(rest & (half == 0))
        def _():
            for r in range(2):
                rest_rows(2 + r, 0)

    def norm(layer, which):
        @pl.loop(0, TOK // NB)
        def _(m):
            rows = pl.ds(pl.multiple_of(m * NB, NB), NB)
            total = jnp.zeros((NB, 1), F32)
            for b in range(4):
                blk = x_ref[rows, pl.ds(b * ROWS, ROWS)]
                total = total + jnp.sum(blk * blk, axis=1, keepdims=True)
            inv = lax.rsqrt(total * (1.0 / D) + EPS)
            for b in range(4):
                blk = x_ref[rows, pl.ds(b * ROWS, ROWS)]
                gain = gain_ref[which * LAYERS + layer, :, pl.ds(b * ROWS, ROWS)]
                c0 = pl.multiple_of(rel(b) * ROWS, ROWS)
                h_ref[rows, pl.ds(c0, ROWS)] = (blk * inv * gain).astype(BF16)

    def rotate(vals, rows):
        vals = vals.astype(BF16).astype(F32)
        turned = pltpu.roll(vals, HEAD // 2, 1)
        return (vals * cos_ref[rows, :] + turned * sin_ref[rows, :]).astype(BF16)

    def tile_product(slot, finish_rows):
        @pl.loop(0, TOK // MB)
        def _(m):
            rows = pl.ds(pl.multiple_of(m * MB, MB), MB)
            finish_rows(rows, jnp.dot(h_ref[rows, :], wbuf[slot], preferred_element_type=F32))

    def kv_step(slot):
        def fin(rows, acc):
            for b in range(2):
                kv_ref[rows, pl.ds(b * HEAD, HEAD)] = rotate(acc[:, b * HEAD:(b + 1) * HEAD], rows)
            kv_ref[rows, pl.ds(256, 256)] = acc[:, 256:].astype(BF16)
        tile_product(slot, fin)

    def q_step(slot, j):
        def fin(rows, acc):
            for b in range(4):
                c0 = pl.multiple_of(j * 512 + b * HEAD, HEAD)
                q_ref[rows, pl.ds(c0, HEAD)] = rotate(acc[:, b * HEAD:(b + 1) * HEAD], rows)
        tile_product(slot, fin)

    def o_step(slot, j):
        def fin(rows, acc):
            c0 = pl.ds(pl.multiple_of(j * 512, 512), 512)
            x_ref[rows, c0] = x_ref[rows, c0] + acc
        tile_product(slot, fin)

    def g_step(slot, j):
        def fin(rows, acc):
            gate = acc[:, :256]
            up = acc[:, 256:]
            c0 = pl.multiple_of(j * 256, 256)
            a_ref[rows, pl.ds(c0, 256)] = (gate * jax.nn.sigmoid(gate) * up).astype(BF16)
        tile_product(slot, fin)

    def attend(head):
        kv = head // 8
        q0 = pl.multiple_of(head * HEAD, HEAD)
        k0 = pl.multiple_of(kv * HEAD, HEAD)
        v0 = pl.multiple_of(256 + kv * HEAD, HEAD)
        o0 = pl.multiple_of(rel(head // 4) * ROWS + lax.rem(head, 4) * HEAD, HEAD)
        scale = HEAD ** -0.5
        for b in range(TOK // QB):
            keys = (b + 1) * QB
            rows = pl.ds(b * QB, QB)
            scores = lax.dot_general(q_ref[rows, pl.ds(q0, HEAD)], kv_ref[pl.ds(0, keys), pl.ds(k0, HEAD)],
                                     (((1,), (1,)), ((), ())), preferred_element_type=F32)
            key_idx = lax.broadcasted_iota(jnp.int32, (QB, keys), 1)
            row_idx = lax.broadcasted_iota(jnp.int32, (QB, keys), 0) + b * QB
            first = jnp.concatenate([first_ref[rows, :]] * (keys // HEAD), axis=1)
            ok = (key_idx >= first) & (key_idx <= row_idx)
            scores = jnp.where(ok, scores, -1e30)
            top = jnp.max(scores, axis=1, keepdims=True)
            probs = jnp.exp((scores - top) * scale)
            inv = 1.0 / jnp.sum(probs, axis=1, keepdims=True)
            probs = (probs * inv).astype(BF16)
            mixed = jnp.dot(probs, kv_ref[pl.ds(0, keys), pl.ds(v0, HEAD)], preferred_element_type=F32)
            h_ref[rows, pl.ds(o0, HEAD)] = mixed.astype(BF16)

    def add_product(dslot, half, cols, tile_ref=None):
        rows = pl.ds(pl.multiple_of(half * MB, MB), MB)
        depth = sum(width for _, width in cols)
        lhs = jnp.concatenate([a_ref[rows, pl.ds(c0, width)] for c0, width in cols], axis=1)
        tile = dbuf[dslot, pl.ds(0, depth), :] if tile_ref is None else tile_ref[...]
        x_ref[rows, :] = x_ref[rows, :] + jnp.dot(lhs, tile, preferred_element_type=F32)

    def wait_d(dslot, half, depth):
        @pl.when(half == 0)
        def _():
            part = dbuf.at[dslot, pl.ds(0, depth), :]
            pltpu.make_async_copy(part, part, dsem.at[dslot]).wait()

    def last_cols(side_no):
        return [(tile_col(side_no, core, N_D - 1), 256), (tile_col(side_no, 1 - core, N_D - 1), 256)]

    def wait_w(slot):
        pltpu.make_async_copy(wbuf.at[slot], wbuf.at[slot], wsem.at[slot]).wait()

    def step(s):
        before = [jnp.where(s == 0, one, two) for one, two in zip(FIRST, targets(s - 1))]
        relays(before, targets(s))

        @pl.when(s + 1 < ALL_STEPS)
        def _():
            load_tile(s + 1)

        with jax.named_scope("comp"):
            compute(s)

    def compute(s):
        layer = s // STEPS
        i = lax.rem(s, STEPS)
        slot = lax.rem(s, 2)

        @pl.when(((i == 0) & (layer > 0)) | (i == ST_G))
        def _():
            norm(layer, jnp.where(i == 0, 0, 1))

        @pl.when((i < ST_A) | ((i >= ST_O) & (i < ST_D)))
        def _():
            wait_w(slot)

        @pl.when(i == 0)
        def _():
            kv_step(slot)

        @pl.when((i >= ST_Q) & (i < ST_A))
        def _():
            q_step(slot, i - ST_Q)

        @pl.when((i >= ST_A) & (i < ST_O))
        def _():
            attend(i - ST_A)

        @pl.when((i >= ST_O) & (i < ST_G))
        def _():
            o_step(slot, i - ST_O)

        @pl.when((i >= ST_G) & (i < ST_D))
        def _():
            g_step(slot, i - ST_G)

        j, tile, half, whole, near, far, rest = down_step(i)
        dslot = lax.rem(j + 2 * STEPS, 2)

        @pl.when(whole)
        def _():
            wait_d(dslot, half, 1024)
            add_product(dslot, half, [(tile_col(lax.rem(side + r // 2, 2), lax.rem(core + r, 2), tile), 256) for r in range(4)])

        @pl.when(near)
        def _():
            wait_d(dslot, half, NEAR_K)
            add_product(dslot, half, last_cols(side) + [(rest_col(side), REST_K)])

        @pl.when(far & (layer < LAYERS - 1))
        def _():
            wait_d(dslot, half, 512)
            add_product(dslot, half, last_cols(1 - side))

        @pl.when(far & (layer == LAYERS - 1))
        def _():
            @pl.when(half == 0)
            def _():
                near_far().wait()
                for copy in near_rest():
                    copy.start()
            add_product(dslot, half, last_cols(1 - side), far_ref)

        @pl.when(rest)
        def _():
            wait_d(dslot, half, REST_K)
            add_product(dslot, half, [(rest_col(1 - side), REST_K)])

    @pl.loop(0, AHEAD)
    def _(m):
        for_item(m, start1)

    @pl.loop(0, AHEAD0)
    def _(k):
        for_chunk(k, start0)

    for copy in inputs:
        copy.wait()

    for n, ref in enumerate((ga_ref, gm_ref)):
        for layer in range(LAYERS):
            gain_ref[n * LAYERS + layer] = ref[pl.ds(layer, 1), :].astype(F32)
    ids = seg_ref[...].astype(F32)
    lane = lax.broadcasted_iota(jnp.int32, (128, HEAD), 1)
    for b in range(TOK // 128):
        rows = pl.ds(b * 128, 128)
        mine = jnp.transpose(jnp.broadcast_to(ids[b:b + 1, :], (128, 128)))
        before = jnp.zeros((128, 128), F32)
        for c in range(TOK // 128):
            before = before + jnp.where(ids[c:c + 1, :] < mine, 1.0, 0.0)
        first = jnp.sum(before, axis=1, keepdims=True)
        pos = lax.broadcasted_iota(jnp.int32, (128, 128), 0).astype(F32) + (b * 128.0) - first
        angles = pos * freq_ref[...]
        cos_ref[rows, :] = jnp.cos(angles)
        sin = jnp.sin(angles)
        sin_ref[rows, :] = jnp.where(lane < HEAD // 2, -sin, sin)
        first_ref[rows, :] = jnp.broadcast_to(first, (128, 128)).astype(jnp.int32)

    @pl.loop(0, TOK // NB)
    def _(m):
        rows = pl.ds(pl.multiple_of(m * NB, NB), NB)
        x_ref[rows, :] = q_ref[rows, :].astype(F32)

    relays((0, 0, 0), (2, 0, 0))
    norm(0, 0)

    @pl.loop(0, AHEAD0 - 1)
    def _(k):
        for_chunk(k, wait0)

    relays((2, 0, 0), START)
    relays(START, FIRST)
    load_tile(0)

    @pl.loop(0, ALL_STEPS)
    def _(s):
        with jax.named_scope("step"):
            step(s)

    relays(targets(ALL_STEPS - 1), (ITEMS, PUSHES, CHUNKS))
    for copy in near_rest():
        copy.wait()


def result_kernel(x_ref, a_ref, out, y_ref, osem):
    c0 = pl.multiple_of((1 - lax.axis_index("fsdp") // 2) * (2 * FF_ROWS) + 2560, HEAD)

    def store(n, m):
        rows, cols = pl.ds(m * 512, 512), pl.ds(n * 512, 512)
        return pltpu.make_async_copy(y_ref.at[rows, cols], out.at[rows, cols], osem.at[n, m])

    for n in range(4):
        cols = pl.ds(n * 512, 512)
        tile = a_ref[pl.ds(n // 2 * REST_K, REST_K), pl.ds(FF + n % 2 * 512, 512)]
        for m in range(2):
            rows = pl.ds(m * 512, 512)
            y_ref[rows, cols] = x_ref[rows, cols] + jnp.dot(a_ref[rows, pl.ds(c0, REST_K)], tile, preferred_element_type=F32)
            store(n, m).start()
    for n in range(4):
        for m in range(2):
            store(n, m).wait()


def run_layers(tokens, seg_ids, g_attn, g_mlp, weights):
    shapes = [jax.ShapeDtypeStruct(w.shape, w.dtype) for w in weights]
    half_dim = HEAD // 2
    freq = np.float32(ROPE_BASE) ** (-np.arange(half_dim, dtype=np.float32) / np.float32(half_dim))
    freq = jnp.asarray(np.concatenate([freq, freq]).reshape(1, HEAD))
    sem = pltpu.SemaphoreType.DMA((SLOTS, 2))
    item_sem = pltpu.SemaphoreType.DMA((ITEM_SLOTS,))
    any_spec = pl.BlockSpec(memory_space=pl.ANY)
    vmem_spec = pl.BlockSpec(memory_space=pltpu.VMEM)
    outs = pl.pallas_call(
        layer_kernel,
        out_shape=[pltpu.VMEM((TOK, D), F32), pltpu.VMEM((TOK, FF + WIDE), BF16)] + shapes * 3,
        in_specs=[any_spec] * 12,
        out_specs=[vmem_spec] * 2 + [any_spec] * 21,
        scratch_shapes=[
            pltpu.VMEM((TOK, D), BF16),
            pltpu.VMEM((TOK, D), BF16),
            pltpu.VMEM((TOK, 512), BF16),
            pltpu.VMEM((2, D, 512), BF16),
            pltpu.VMEM((2, 1024, D), BF16),
            pltpu.VMEM((TOK, HEAD), F32),
            pltpu.VMEM((TOK, HEAD), F32),
            pltpu.VMEM((TOK, HEAD), jnp.int32),
            pltpu.VMEM((2 * LAYERS, 1, D), F32),
            pltpu.VMEM((TOK // 128, 128), jnp.int32),
            pltpu.VMEM((1, HEAD), F32),
            pltpu.VMEM((LAYERS, D), BF16),
            pltpu.VMEM((LAYERS, D), BF16),
            pltpu.VMEM((512, D), BF16),
            pltpu.SemaphoreType.DMA((2,)),
            pltpu.SemaphoreType.DMA((2,)),
            pltpu.SemaphoreType.DMA((5,)),
            pltpu.SemaphoreType.DMA((3,)),
        ] + [sem] * 2 + [item_sem] * 4 + [sem] * 2,
        compiler_params=pltpu.CompilerParams(collective_id=0, has_side_effects=True, vmem_limit_bytes=32 * 1000 * 1000),
        name="two_layers",
    )(tokens, seg_ids.reshape(TOK // 128, 128), freq, g_attn, g_mlp, *weights)
    hidden = pltpu.with_memory_space_constraint(outs[0], pltpu.VMEM)
    act = pltpu.with_memory_space_constraint(outs[1], pltpu.VMEM)
    return pl.pallas_call(
        result_kernel,
        out_shape=jax.ShapeDtypeStruct((TOK, D), F32),
        in_specs=[vmem_spec] * 2,
        out_specs=any_spec,
        scratch_shapes=[
            pltpu.VMEM((TOK, D), F32),
            pltpu.SemaphoreType.DMA((4, 2)),
        ],
        compiler_params=pltpu.CompilerParams(vmem_limit_bytes=24 * 1000 * 1000),
        name="result",
    )(hidden, act)


def solution(mesh):
    tok_spec = P(("rep", "fsdp"), None)
    seg_spec = P(("rep", "fsdp"))
    mat_spec = P(None, "fsdp", None)
    gain_spec = P(None, None)

    def per_device(tokens, seg_ids, w_q, w_k, w_v, w_o, w_gate, w_up, w_down, g_attn, g_mlp):
        return run_layers(tokens, seg_ids, g_attn, g_mlp, (w_q, w_k, w_v, w_o, w_gate, w_up, w_down))

    return jax.shard_map(per_device, mesh=mesh, in_specs=(tok_spec, seg_spec, mat_spec, mat_spec, mat_spec, mat_spec, mat_spec, mat_spec, mat_spec, gain_spec, gain_spec), out_specs=tok_spec, check_vma=False)
```

```python
import jax
import jax.numpy as jnp
import numpy as np
from jax import lax
from jax.experimental import pallas as pl
from jax.experimental.pallas import tpu as pltpu
from jax.sharding import PartitionSpec as P

D = 2048
FF = 11008
HEADS = 16
HEAD = 128
TOK = 1024
EPS = 1e-5
ROPE_BASE = 10000.0
MESH = pl.DeviceIdType.MESH
F32 = jnp.float32
BF16 = jnp.bfloat16

LAYERS = 2
SLOTS = 8
ITEM_SLOTS = 2 * SLOTS
AHEAD = 8
AHEAD0 = 5
ROWS = D // 4
FF_ROWS = FF // 4
TAIL = 192
NAMES = ("q", "k", "v", "o", "g", "u", "d")

N_Q = 4
N_GU = 21
N_D = 10
CH_Q = 1
CH_O = CH_Q + N_Q
CH_GU = CH_O + N_Q
CH_GL = CH_GU + N_GU
CH_D = CH_GL + 1
CH_DR = CH_D + N_D
PER_LAYER = CH_DR + 1
CHUNKS = LAYERS * PER_LAYER
ITEMS = 2 * CHUNKS
PUSHES = CHUNKS + 1

NEAR_AT = 5

N_GT = FF // 256
ST_Q = 1
ST_A = ST_Q + N_Q
ST_O = ST_A + HEADS
ST_G = ST_O + 4
ST_D = ST_G + N_GT
ST_NEAR = ST_D + 2 * NEAR_AT
ST_READY = ST_D + 2 * (N_D - 1)
ST_IDLE = ST_READY + 3
ST_FAR = ST_IDLE + 1
ST_REST = ST_FAR + 2
STEPS = ST_REST + 2
ALL_STEPS = LAYERS * STEPS - 2
START = (4, 1, 0)
FIRST = (8, 3, 1)
REST_K = 2 * TAIL
WIDE = D // 2
NEAR_K = 512 + REST_K

MB = 512
NB = 128
QB = 256


def layer_kernel(*refs):
    tok, seg, freq, g_attn, g_mlp = refs[:5]
    own = dict(zip(NAMES, refs[5:12]))
    x_ref, a_ref = refs[12:14]
    b1 = dict(zip(NAMES, refs[14:21]))
    b2 = dict(zip(NAMES, refs[21:28]))
    b3 = dict(zip(NAMES, refs[28:35]))
    (h_ref, q_ref, kv_ref, wbuf, dbuf, cos_ref, sin_ref, first_ref, gain_ref,
     seg_ref, freq_ref, ga_ref, gm_ref, far_ref, wsem, dsem, iosem, lsem) = refs[35:53]
    s0s, s0r, s1s, s1r, s2s, s2r, s3s, s3r = refs[53:]
    sources = (own, b1, b2, b3)
    y = lax.axis_index("rep")
    d = lax.axis_index("fsdp")
    side = d // 2
    core = lax.rem(d, 2)
    x_dev = (y, lax.rem(d + 2, 4))
    y_dev = (1 - y, d)
    c_dev = (y, d + 1 - 2 * core)

    def rel(block):
        return 2 * lax.rem(block // 2 + side, 2) + lax.rem(block + core, 2)

    inputs = [pltpu.make_async_copy(src, dst, iosem.at[n]) for n, (src, dst) in enumerate(
        ((tok, q_ref), (seg, seg_ref), (freq, freq_ref), (g_attn, ga_ref), (g_mlp, gm_ref)))]
    for copy in inputs:
        copy.start()

    barrier = pltpu.get_barrier_semaphore()
    for dev in (x_dev, y_dev, c_dev):
        pl.semaphore_signal(barrier, inc=1, device_id=dev, device_id_type=MESH)
    pl.semaphore_wait(barrier, 3)

    def kinds(k):
        i = lax.rem(k, PER_LAYER)
        jq = pl.multiple_of((i - CH_Q) * 512, 512)
        jo = pl.multiple_of((i - CH_O) * 512, 512)
        jg = pl.multiple_of((i - CH_GU) * 512, 512)
        jd = core * TAIL + (i - CH_D) * 256
        jr = (1 - core) * 2560
        last = N_GU * 512
        kv = [("k", 0, ROWS, 0, 256), ("v", 0, ROWS, 0, 256)]
        gu = [("g", 0, ROWS, jg, 512), ("u", 0, ROWS, jg, 512)]
        gl = [("g", 0, ROWS, last, 256), ("u", 0, ROWS, last, 256)]

        def split_cols(name, c0):
            whole = [(name, 0, ROWS, c0, 512)]
            return [(name, 0, ROWS, c0, 256), (name, 0, ROWS, c0 + 256, 256)], whole, whole

        def split_rows(r0, nr):
            halves = [("d", r0, nr // 2, 0, D), ("d", r0 + nr // 2, nr // 2, 0, D)]
            return halves, [("d", r0, nr, 0, D)], halves

        return [
            (i == 0, kv, kv, kv, 0),
            ((i >= CH_Q) & (i < CH_O), *split_cols("q", jq), 0),
            ((i >= CH_O) & (i < CH_GU), *split_cols("o", jo), 0),
            ((i >= CH_GU) & (i < CH_GL), gu, gu, gu, 0),
            (i == CH_GL, gl, gl, gl, 0),
            ((i >= CH_D) & (i < CH_DR) & (k != CHUNKS - 2), *split_rows(jd, 256), 0),
            (k == CHUNKS - 2, *split_rows(jd, 256), 2),
            ((i == CH_DR) & (k != CHUNKS - 1), *split_rows(jr, TAIL), 0),
            (k == CHUNKS - 1, *split_rows(jr, TAIL)[:2], [("d", jr, TAIL, 0, WIDE), ("d", jr, TAIL, WIDE, WIDE)], 1),
        ]

    def for_chunk(k, fn, form=2, part=None):
        layer = k // PER_LAYER
        slot = lax.rem(k, SLOTS)
        for kind in kinds(k):
            @pl.when((k < CHUNKS) & kind[0])
            def _():
                for n, piece in enumerate(kind[form]):
                    if part is None:
                        fn(kind[4], layer, piece, (slot, n))
                    else:
                        @pl.when(part != 1 - n)
                        def _():
                            fn(kind[4], layer, piece, (slot, n))

    def for_pair(k, fn, part=None):
        layer = k // PER_LAYER
        for cond, pieces, _, _, mark in kinds(k):
            @pl.when((k < CHUNKS) & cond)
            def _():
                for n, piece in enumerate(pieces):
                    args = (mark == 1 and n == 1, layer, piece, (lax.rem(2 * k + n, ITEM_SLOTS),))
                    if part is None:
                        fn(*args)
                    else:
                        @pl.when(part != 1 - n)
                        def _():
                            fn(*args)

    def for_item(m, fn):
        k = m // 2
        n = lax.rem(m, 2)
        layer = k // PER_LAYER
        slot = (lax.rem(m, ITEM_SLOTS),)
        for cond, (one, two), _, _, mark in kinds(k):
            if one[0] == two[0] and mark != 1:
                name, r0, nr, c0, nc = one
                r0, c0 = (r0 + n * nr, c0) if nc == D else (r0, pl.multiple_of(c0 + n * nc, 256))

                @pl.when((m < ITEMS) & cond)
                def _():
                    fn(False, layer, (name, r0, nr, c0, nc), slot)
            else:
                for which, piece in enumerate((one, two)):
                    @pl.when((m < ITEMS) & cond & (n == which))
                    def _():
                        fn(mark == 1 and which == 1, layer, piece, slot)

    def view(bufs, name, layer, r0, nr, c0, nc, half):
        if half:
            nr = nr // 2
            r0 = r0 + y * nr
        r0 = pl.multiple_of(r0, 16)
        return bufs[name].at[layer, pl.ds(r0, nr), pl.ds(c0, nc)]

    def remote(src, dst, ss, rs, dev, half):
        def make(whole, layer, piece, slot):
            part = half and not whole
            return pltpu.make_async_remote_copy(
                src_ref=view(src, piece[0], layer, *piece[1:], part),
                dst_ref=view(dst, piece[0], layer, *piece[1:], part),
                send_sem=ss.at[slot], recv_sem=rs.at[slot], device_id=dev, device_id_type=MESH)
        return make

    copy0 = remote(own, b1, s0s, s0r, c_dev, False)
    copy1 = remote(own, b2, s1s, s1r, x_dev, True)
    copy2 = remote(b2, b2, s2s, s2r, y_dev, True)

    def rest_rows(c0):
        return a_ref.at[pl.ds(pl.multiple_of(c0 // WIDE * REST_K + core * TAIL, 64), TAIL), pl.ds(FF, WIDE)]

    def copy3(mark, layer, piece, slot):
        name, r0, nr, c0, nc = piece
        if mark == 0:
            return remote(b2, b3, s3s, s3r, c_dev, False)(False, layer, piece, slot)
        if mark == 1:
            dst = rest_rows(c0)
        else:
            dst = far_ref.at[pl.ds(pl.multiple_of(r0 - core * TAIL - (N_D - 1) * 256 + 256, 128), nr), :]
        return pltpu.make_async_remote_copy(
            src_ref=view(b2, name, layer, r0, nr, c0, nc, False), dst_ref=dst,
            send_sem=s3s.at[slot], recv_sem=s3r.at[slot], device_id=c_dev, device_id_type=MESH)

    def start0(*a):
        copy0(*a).start()

    def start1(*a):
        copy1(*a).start()

    def wait0(*a):
        copy0(*a).wait_recv()

    def relay2(*a):
        copy1(*a).wait_recv()
        if not a[0]:
            copy2(*a).start()

    def arrived(*a):
        if not a[0]:
            copy2(*a).wait_recv()
        copy1(*a).wait_send()

    def relay3(*a):
        copy3(*a).start()

    def pushed(*a):
        copy0(*a).wait_send()

    def finish(*a):
        copy3(*a).wait_recv()
        copy3(*a).wait_send()

    def sent(*a):
        if not a[0]:
            copy2(*a).wait_send()

    def targets(s):
        i = lax.rem(s, STEPS)
        layer = s // STEPS
        first = layer == 0
        late = 1 - jnp.minimum(layer, 1)
        t2 = jnp.where(i < ST_A, 9 + 2 * i + late,
             jnp.where(i < ST_G + 1, 19 + late + 3 * (i - ST_A) // 5,
             jnp.where(i < ST_D, jnp.maximum(i + 4, 32 + late + (i - ST_G - 1) // 2),
             jnp.where(i < ST_NEAR, jnp.maximum(i, ST_D + 3 + (2 * (i - ST_D) + 1) // 3),
             jnp.where(first, jnp.where(i < ST_NEAR + 2, i, jnp.where(i < ST_READY - 2, 40 + i // 2, jnp.where(i < ST_READY, i - 2, i - 3))),
             jnp.where(i < ST_READY - 4, 38 + (i + 1) // 2, 39 + i // 2))))))
        final = i == STEPS - 1
        t3 = jnp.where(i < ST_D, jnp.where(i < ST_A, 3 + i, (t2 - 3) // 2),
             jnp.where(first, jnp.where(i < ST_IDLE, (t2 - 2) // 2, CH_DR + (i - ST_IDLE + 1) // 2 + jnp.where(final, 1, 0)),
             jnp.where(i < ST_READY - 4, (t2 - 2) // 2, jnp.where(i < ST_READY + 2, 39 + (i - ST_READY + 4) // 3, i - ST_READY + 39 + jnp.where(i == ST_FAR, 1, 0)))))
        end = s >= ALL_STEPS - 2
        t2 = jnp.minimum(t2 + layer * 2 * PER_LAYER, jnp.where(end, ITEMS, ITEMS - 1))
        t3 = jnp.minimum(t3 + layer * PER_LAYER, PUSHES)
        nxt = jnp.minimum(s + 1, ALL_STEPS - 1)
        i = lax.rem(nxt, STEPS)
        base = nxt // STEPS * PER_LAYER
        done = jnp.where(i < ST_A, 1 + i,
               jnp.where(i < ST_O, ST_A,
               jnp.where(i < ST_G, 1 + CH_O + i - ST_O,
               jnp.where(i < ST_D, 1 + CH_GU + (i - ST_G) // 2,
               jnp.where(i < ST_NEAR, 1 + CH_D + (i - ST_D) // 2,
               jnp.where(i < ST_READY, CH_D + (i - ST_D) // 2,
               jnp.where(i < ST_READY + 1, CH_DR - 2,
               jnp.where(i < ST_FAR, CH_DR - 1,
               jnp.where(i < ST_REST, CH_DR, PER_LAYER)))))))))
        tf = jnp.maximum(jnp.minimum(t3 - 2, CHUNKS - 2), done + base)
        pushes = tf + jnp.where(tf == CHUNKS - 1, 1, 0)
        t3 = jnp.maximum(jnp.maximum(t3, pushes), base + jnp.where((i >= ST_READY) & (i < ST_FAR), CH_DR - 1, 0))
        return jnp.maximum(t2, 2 * jnp.minimum(t3, CHUNKS - 2)), t3, tf

    def relays(old, new):
        @pl.loop(old[0], new[0])
        def _(m):
            for_item(m, relay2)
            for_item(m + AHEAD, start1)
            n = lax.rem(m, 2)
            for_chunk(m // 2 + jnp.where(n == 0, AHEAD0, CHUNKS), start0)
            for_chunk(m // 2 + jnp.where(n == 0, CHUNKS, AHEAD0 - 1), wait0)

        @pl.loop(old[1], new[1])
        def _(p):
            extra = jnp.maximum(p - (CHUNKS - 2), 0)
            k = p - jnp.minimum(extra, 1)
            part = jnp.where((p < CHUNKS - 2) | (extra > 1), 2, extra)
            for_pair(k, arrived, part)
            for_chunk(k, relay3, 3, part)
            for_chunk(jnp.where(part == 1, CHUNKS, k), pushed)

        @pl.loop(old[2], new[2])
        def _(k):
            for_chunk(k, finish, 3)
            for_pair(k, sent)

    def down_step(i):
        n = i - ST_D - jnp.where(i > ST_READY, 1, 0) - jnp.where(i > ST_IDLE, 1, 0)
        j = n // 2
        near = (i >= ST_NEAR) & (i < ST_NEAR + 2)
        far = (i >= ST_FAR) & (i < ST_REST)
        rest = i >= ST_REST
        whole = (i >= ST_D) & (i < ST_IDLE) & ~near & (i != ST_READY)
        return j, jnp.where(i > ST_NEAR, j - 1, j), lax.rem(n + 2 * STEPS, 2), whole, near, far, rest

    def rest_col(side_no):
        return pl.multiple_of(side_no * (2 * FF_ROWS) + 2560, HEAD)

    def tile_col(side_no, core_no, tile):
        return pl.multiple_of(side_no * (2 * FF_ROWS) + core_no * (FF_ROWS + TAIL) + tile * 256, HEAD)

    def near_far():
        r0 = pl.multiple_of(core * TAIL + (N_D - 1) * 256, 64)
        return pltpu.make_async_copy(b2["d"].at[LAYERS - 1, pl.ds(r0, 256), :], far_ref.at[pl.ds(0, 256), :], lsem.at[0])

    def near_rest():
        r0 = pl.multiple_of((1 - core) * 2560, 512)
        return [pltpu.make_async_copy(b2["d"].at[LAYERS - 1, pl.ds(r0, TAIL), pl.ds(n * WIDE, WIDE)], rest_rows(n * WIDE), lsem.at[1 + n])
                for n in range(2)]

    def load_tile(s):
        layer = s // STEPS
        i = lax.rem(s, STEPS)
        slot = lax.rem(s, 2)

        def cols(name, c0, nc, w0):
            for r, src in enumerate(sources):
                pltpu.make_async_copy(src[name].at[layer, :, pl.ds(c0, nc)],
                                      wbuf.at[slot, pl.ds(r * ROWS, ROWS), pl.ds(w0, nc)], wsem.at[slot]).start()

        @pl.when(i == 0)
        def _():
            cols("k", 0, 256, 0)
            cols("v", 0, 256, 256)

        @pl.when((i >= ST_Q) & (i < ST_A))
        def _():
            cols("q", pl.multiple_of((i - ST_Q) * 512, 512), 512, 0)

        @pl.when((i >= ST_O) & (i < ST_G))
        def _():
            cols("o", pl.multiple_of((i - ST_O) * 512, 512), 512, 0)

        @pl.when((i >= ST_G) & (i < ST_D))
        def _():
            c0 = pl.multiple_of((i - ST_G) * 256, 256)
            cols("g", c0, 256, 0)
            cols("u", c0, 256, 256)

        j, tile, half, whole, near, far, rest = down_step(i)
        dslot = lax.rem(j + 2 * STEPS, 2)

        def rows_in(src, r0, nr, w0):
            pltpu.make_async_copy(src["d"].at[layer, pl.ds(r0, nr), :], dbuf.at[dslot, pl.ds(w0, nr), :], dsem.at[dslot]).start()

        def chunk_rows(r, tile_no, w0):
            src_core = core if r % 2 == 0 else 1 - core
            rows_in(sources[r], pl.multiple_of(src_core * TAIL + tile_no * 256, 64), 256, w0)

        def rest_rows(r, w0):
            src_core = core if r % 2 == 0 else 1 - core
            rows_in(sources[r], pl.multiple_of((1 - src_core) * 2560, 512), TAIL, pl.multiple_of(w0 + src_core * TAIL, 64))

        @pl.when((whole & (half == 0) & (i != ST_READY + 1)) | (i == ST_READY))
        def _():
            for r in range(3):
                chunk_rows(r, jnp.where(i == ST_READY, N_D - 2, tile), r * 256)

        @pl.when(whole & (half == 0))
        def _():
            chunk_rows(3, tile, 768)

        @pl.when(near & (half == 0))
        def _():
            for r in range(2):
                chunk_rows(r, N_D - 1, r * 256)
                rest_rows(r, 512)

        @pl.when(far & (half == 0) & (layer < LAYERS - 1))
        def _():
            for r in range(2):
                chunk_rows(2 + r, N_D - 1, r * 256)

        @pl.when(far & (half == 0) & (layer == LAYERS - 1))
        def _():
            near_far().start()

        @pl.when(rest & (half == 0))
        def _():
            for r in range(2):
                rest_rows(2 + r, 0)

    def norm(layer, which):
        @pl.loop(0, TOK // NB)
        def _(m):
            rows = pl.ds(pl.multiple_of(m * NB, NB), NB)
            total = jnp.zeros((NB, 1), F32)
            for b in range(4):
                blk = x_ref[rows, pl.ds(b * ROWS, ROWS)]
                total = total + jnp.sum(blk * blk, axis=1, keepdims=True)
            inv = lax.rsqrt(total * (1.0 / D) + EPS)
            for b in range(4):
                blk = x_ref[rows, pl.ds(b * ROWS, ROWS)]
                gain = gain_ref[which * LAYERS + layer, :, pl.ds(b * ROWS, ROWS)]
                c0 = pl.multiple_of(rel(b) * ROWS, ROWS)
                h_ref[rows, pl.ds(c0, ROWS)] = (blk * inv * gain).astype(BF16)

    def rotate(vals, rows):
        vals = vals.astype(BF16).astype(F32)
        turned = pltpu.roll(vals, HEAD // 2, 1)
        return (vals * cos_ref[rows, :] + turned * sin_ref[rows, :]).astype(BF16)

    def tile_product(slot, finish_rows):
        @pl.loop(0, TOK // MB)
        def _(m):
            rows = pl.ds(pl.multiple_of(m * MB, MB), MB)
            finish_rows(rows, jnp.dot(h_ref[rows, :], wbuf[slot], preferred_element_type=F32))

    def kv_step(slot):
        def fin(rows, acc):
            for b in range(2):
                kv_ref[rows, pl.ds(b * HEAD, HEAD)] = rotate(acc[:, b * HEAD:(b + 1) * HEAD], rows)
            kv_ref[rows, pl.ds(256, 256)] = acc[:, 256:].astype(BF16)
        tile_product(slot, fin)

    def q_step(slot, j):
        def fin(rows, acc):
            for b in range(4):
                c0 = pl.multiple_of(j * 512 + b * HEAD, HEAD)
                q_ref[rows, pl.ds(c0, HEAD)] = rotate(acc[:, b * HEAD:(b + 1) * HEAD], rows)
        tile_product(slot, fin)

    def o_step(slot, j):
        def fin(rows, acc):
            c0 = pl.ds(pl.multiple_of(j * 512, 512), 512)
            x_ref[rows, c0] = x_ref[rows, c0] + acc
        tile_product(slot, fin)

    def g_step(slot, j):
        def fin(rows, acc):
            gate = acc[:, :256]
            up = acc[:, 256:]
            c0 = pl.multiple_of(j * 256, 256)
            a_ref[rows, pl.ds(c0, 256)] = (gate * jax.nn.sigmoid(gate) * up).astype(BF16)
        tile_product(slot, fin)

    def attend(head):
        kv = head // 8
        q0 = pl.multiple_of(head * HEAD, HEAD)
        k0 = pl.multiple_of(kv * HEAD, HEAD)
        v0 = pl.multiple_of(256 + kv * HEAD, HEAD)
        o0 = pl.multiple_of(rel(head // 4) * ROWS + lax.rem(head, 4) * HEAD, HEAD)
        scale = HEAD ** -0.5
        for b in range(TOK // QB):
            keys = (b + 1) * QB
            rows = pl.ds(b * QB, QB)
            scores = lax.dot_general(q_ref[rows, pl.ds(q0, HEAD)], kv_ref[pl.ds(0, keys), pl.ds(k0, HEAD)],
                                     (((1,), (1,)), ((), ())), preferred_element_type=F32)
            key_idx = lax.broadcasted_iota(jnp.int32, (QB, keys), 1)
            row_idx = lax.broadcasted_iota(jnp.int32, (QB, keys), 0) + b * QB
            first = jnp.concatenate([first_ref[rows, :]] * (keys // HEAD), axis=1)
            ok = (key_idx >= first) & (key_idx <= row_idx)
            scores = jnp.where(ok, scores, -1e30)
            top = jnp.max(scores, axis=1, keepdims=True)
            probs = jnp.exp((scores - top) * scale)
            inv = 1.0 / jnp.sum(probs, axis=1, keepdims=True)
            probs = (probs * inv).astype(BF16)
            mixed = jnp.dot(probs, kv_ref[pl.ds(0, keys), pl.ds(v0, HEAD)], preferred_element_type=F32)
            h_ref[rows, pl.ds(o0, HEAD)] = mixed.astype(BF16)

    def add_product(dslot, half, cols, tile_ref=None):
        rows = pl.ds(pl.multiple_of(half * MB, MB), MB)
        depth = sum(width for _, width in cols)
        lhs = jnp.concatenate([a_ref[rows, pl.ds(c0, width)] for c0, width in cols], axis=1)
        tile = dbuf[dslot, pl.ds(0, depth), :] if tile_ref is None else tile_ref[...]
        x_ref[rows, :] = x_ref[rows, :] + jnp.dot(lhs, tile, preferred_element_type=F32)

    def wait_d(dslot, half, depth):
        @pl.when(half == 0)
        def _():
            part = dbuf.at[dslot, pl.ds(0, depth), :]
            pltpu.make_async_copy(part, part, dsem.at[dslot]).wait()

    def last_cols(side_no):
        return [(tile_col(side_no, core, N_D - 1), 256), (tile_col(side_no, 1 - core, N_D - 1), 256)]

    def wait_w(slot):
        pltpu.make_async_copy(wbuf.at[slot], wbuf.at[slot], wsem.at[slot]).wait()

    def step(s):
        before = [jnp.where(s == 0, one, two) for one, two in zip(FIRST, targets(s - 1))]
        relays(before, targets(s))

        @pl.when(s + 1 < ALL_STEPS)
        def _():
            load_tile(s + 1)

        compute(s)

    def compute(s):
        layer = s // STEPS
        i = lax.rem(s, STEPS)
        slot = lax.rem(s, 2)

        @pl.when(((i == 0) & (layer > 0)) | (i == ST_G))
        def _():
            norm(layer, jnp.where(i == 0, 0, 1))

        @pl.when((i < ST_A) | ((i >= ST_O) & (i < ST_D)))
        def _():
            wait_w(slot)

        @pl.when(i == 0)
        def _():
            kv_step(slot)

        @pl.when((i >= ST_Q) & (i < ST_A))
        def _():
            q_step(slot, i - ST_Q)

        @pl.when((i >= ST_A) & (i < ST_O))
        def _():
            attend(i - ST_A)

        @pl.when((i >= ST_O) & (i < ST_G))
        def _():
            o_step(slot, i - ST_O)

        @pl.when((i >= ST_G) & (i < ST_D))
        def _():
            g_step(slot, i - ST_G)

        j, tile, half, whole, near, far, rest = down_step(i)
        dslot = lax.rem(j + 2 * STEPS, 2)

        @pl.when(whole)
        def _():
            wait_d(dslot, half, 1024)
            add_product(dslot, half, [(tile_col(lax.rem(side + r // 2, 2), lax.rem(core + r, 2), tile), 256) for r in range(4)])

        @pl.when(near)
        def _():
            wait_d(dslot, half, NEAR_K)
            add_product(dslot, half, last_cols(side) + [(rest_col(side), REST_K)])

        @pl.when(far & (layer < LAYERS - 1))
        def _():
            wait_d(dslot, half, 512)
            add_product(dslot, half, last_cols(1 - side))

        @pl.when(far & (layer == LAYERS - 1))
        def _():
            @pl.when(half == 0)
            def _():
                near_far().wait()
                for copy in near_rest():
                    copy.start()
            add_product(dslot, half, last_cols(1 - side), far_ref)

        @pl.when(rest)
        def _():
            wait_d(dslot, half, REST_K)
            add_product(dslot, half, [(rest_col(1 - side), REST_K)])

    @pl.loop(0, AHEAD)
    def _(m):
        for_item(m, start1)

    @pl.loop(0, AHEAD0)
    def _(k):
        for_chunk(k, start0)

    for copy in inputs:
        copy.wait()

    for n, ref in enumerate((ga_ref, gm_ref)):
        for layer in range(LAYERS):
            gain_ref[n * LAYERS + layer] = ref[pl.ds(layer, 1), :].astype(F32)
    ids = seg_ref[...].astype(F32)
    lane = lax.broadcasted_iota(jnp.int32, (128, HEAD), 1)
    for b in range(TOK // 128):
        rows = pl.ds(b * 128, 128)
        mine = jnp.transpose(jnp.broadcast_to(ids[b:b + 1, :], (128, 128)))
        before = jnp.zeros((128, 128), F32)
        for c in range(TOK // 128):
            before = before + jnp.where(ids[c:c + 1, :] < mine, 1.0, 0.0)
        first = jnp.sum(before, axis=1, keepdims=True)
        pos = lax.broadcasted_iota(jnp.int32, (128, 128), 0).astype(F32) + (b * 128.0) - first
        angles = pos * freq_ref[...]
        cos_ref[rows, :] = jnp.cos(angles)
        sin = jnp.sin(angles)
        sin_ref[rows, :] = jnp.where(lane < HEAD // 2, -sin, sin)
        first_ref[rows, :] = jnp.broadcast_to(first, (128, 128)).astype(jnp.int32)

    @pl.loop(0, TOK // NB)
    def _(m):
        rows = pl.ds(pl.multiple_of(m * NB, NB), NB)
        x_ref[rows, :] = q_ref[rows, :].astype(F32)

    relays((0, 0, 0), (2, 0, 0))
    norm(0, 0)

    @pl.loop(0, AHEAD0 - 1)
    def _(k):
        for_chunk(k, wait0)

    relays((2, 0, 0), START)
    relays(START, FIRST)
    load_tile(0)

    @pl.loop(0, ALL_STEPS)
    def _(s):
        step(s)

    relays(targets(ALL_STEPS - 1), (ITEMS, PUSHES, CHUNKS))
    for copy in near_rest():
        copy.wait()


def result_kernel(x_ref, a_ref, out, y_ref, osem):
    c0 = pl.multiple_of((1 - lax.axis_index("fsdp") // 2) * (2 * FF_ROWS) + 2560, HEAD)

    def store(n, m):
        rows, cols = pl.ds(m * 512, 512), pl.ds(n * 512, 512)
        return pltpu.make_async_copy(y_ref.at[rows, cols], out.at[rows, cols], osem.at[n, m])

    for n in range(4):
        cols = pl.ds(n * 512, 512)
        tile = a_ref[pl.ds(n // 2 * REST_K, REST_K), pl.ds(FF + n % 2 * 512, 512)]
        for m in range(2):
            rows = pl.ds(m * 512, 512)
            y_ref[rows, cols] = x_ref[rows, cols] + jnp.dot(a_ref[rows, pl.ds(c0, REST_K)], tile, preferred_element_type=F32)
            store(n, m).start()
    for n in range(4):
        for m in range(2):
            store(n, m).wait()


def run_layers(tokens, seg_ids, g_attn, g_mlp, weights):
    shapes = [jax.ShapeDtypeStruct(w.shape, w.dtype) for w in weights]
    half_dim = HEAD // 2
    freq = np.float32(ROPE_BASE) ** (-np.arange(half_dim, dtype=np.float32) / np.float32(half_dim))
    freq = jnp.asarray(np.concatenate([freq, freq]).reshape(1, HEAD))
    sem = pltpu.SemaphoreType.DMA((SLOTS, 2))
    item_sem = pltpu.SemaphoreType.DMA((ITEM_SLOTS,))
    any_spec = pl.BlockSpec(memory_space=pl.ANY)
    vmem_spec = pl.BlockSpec(memory_space=pltpu.VMEM)
    outs = pl.pallas_call(
        layer_kernel,
        out_shape=[pltpu.VMEM((TOK, D), F32), pltpu.VMEM((TOK, FF + WIDE), BF16)] + shapes * 3,
        in_specs=[any_spec] * 12,
        out_specs=[vmem_spec] * 2 + [any_spec] * 21,
        scratch_shapes=[
            pltpu.VMEM((TOK, D), BF16),
            pltpu.VMEM((TOK, D), BF16),
            pltpu.VMEM((TOK, 512), BF16),
            pltpu.VMEM((2, D, 512), BF16),
            pltpu.VMEM((2, 1024, D), BF16),
            pltpu.VMEM((TOK, HEAD), F32),
            pltpu.VMEM((TOK, HEAD), F32),
            pltpu.VMEM((TOK, HEAD), jnp.int32),
            pltpu.VMEM((2 * LAYERS, 1, D), F32),
            pltpu.VMEM((TOK // 128, 128), jnp.int32),
            pltpu.VMEM((1, HEAD), F32),
            pltpu.VMEM((LAYERS, D), BF16),
            pltpu.VMEM((LAYERS, D), BF16),
            pltpu.VMEM((512, D), BF16),
            pltpu.SemaphoreType.DMA((2,)),
            pltpu.SemaphoreType.DMA((2,)),
            pltpu.SemaphoreType.DMA((5,)),
            pltpu.SemaphoreType.DMA((3,)),
        ] + [sem] * 2 + [item_sem] * 4 + [sem] * 2,
        compiler_params=pltpu.CompilerParams(collective_id=0, has_side_effects=True, vmem_limit_bytes=32 * 1000 * 1000),
        name="two_layers",
    )(tokens, seg_ids.reshape(TOK // 128, 128), freq, g_attn, g_mlp, *weights)
    hidden = pltpu.with_memory_space_constraint(outs[0], pltpu.VMEM)
    act = pltpu.with_memory_space_constraint(outs[1], pltpu.VMEM)
    return pl.pallas_call(
        result_kernel,
        out_shape=jax.ShapeDtypeStruct((TOK, D), F32),
        in_specs=[vmem_spec] * 2,
        out_specs=any_spec,
        scratch_shapes=[
            pltpu.VMEM((TOK, D), F32),
            pltpu.SemaphoreType.DMA((4, 2)),
        ],
        compiler_params=pltpu.CompilerParams(vmem_limit_bytes=24 * 1000 * 1000),
        name="result",
    )(hidden, act)


def solution(mesh):
    tok_spec = P(("rep", "fsdp"), None)
    seg_spec = P(("rep", "fsdp"))
    mat_spec = P(None, "fsdp", None)
    gain_spec = P(None, None)

    def per_device(tokens, seg_ids, w_q, w_k, w_v, w_o, w_gate, w_up, w_down, g_attn, g_mlp):
        return run_layers(tokens, seg_ids, g_attn, g_mlp, (w_q, w_k, w_v, w_o, w_gate, w_up, w_down))

    return jax.shard_map(per_device, mesh=mesh, in_specs=(tok_spec, seg_spec, mat_spec, mat_spec, mat_spec, mat_spec, mat_spec, mat_spec, mat_spec, gain_spec, gain_spec), out_specs=tok_spec, check_vma=False)
```

```python
import functools

import jax
import jax.numpy as jnp
import numpy as np
from jax import lax
from jax.experimental import pallas as pl
from jax.experimental.pallas import tpu as pltpu
from jax.sharding import PartitionSpec as P

D = 2048
WIDTH = 512
PART = 256
LANES = 128
FF = 11008
HEADS = 16
HEAD = LANES
TOK = 1024
EPS = 1e-5
ROPE_BASE = 10000.0
MESH = pl.DeviceIdType.MESH
F32 = jnp.float32
BF16 = jnp.bfloat16

LAYERS = 2
SLOTS = 8
ITEM_SLOTS = 2 * SLOTS
AHEAD = 8
AHEAD0 = 5
ROWS = D // 4
FF_ROWS = FF // 4
TAIL = 192
NAMES = ("q", "k", "v", "o", "g", "u", "d")

N_Q = 4
N_GU = 21
N_D = 10
CH_Q = 1
CH_O = CH_Q + N_Q
CH_GU = CH_O + N_Q
CH_GL = CH_GU + N_GU
CH_D = CH_GL + 1
CH_DR = CH_D + N_D
PER_LAYER = CH_DR + 1
CHUNKS = LAYERS * PER_LAYER
ITEMS = 2 * CHUNKS
PUSHES = CHUNKS + 1

NEAR_AT = 5

N_GT = FF // PART
ST_Q = 1
ST_A = ST_Q + N_Q
ST_O = ST_A + HEADS
ST_G = ST_O + 4
ST_D = ST_G + N_GT
ST_NEAR = ST_D + 2 * NEAR_AT
ST_READY = ST_D + 2 * (N_D - 1)
ST_IDLE = ST_READY + 3
ST_FAR = ST_IDLE + 1
ST_REST = ST_FAR + 2
STEPS = ST_REST + 2
ALL_STEPS = LAYERS * STEPS - 2
START = (4, 1, 0)
FIRST = (8, 3, 1)
REST_K = 2 * TAIL
WIDE = D // 2
NEAR_K = WIDTH + REST_K

MB = WIDTH
NB = LANES
QB = PART


def layer_kernel(*refs):
    tok, seg, freq, g_attn, g_mlp = refs[:5]
    own = dict(zip(NAMES, refs[5:12]))
    x_ref, a_ref = refs[12:14]
    b1 = dict(zip(NAMES, refs[14:21]))
    b2 = dict(zip(NAMES, refs[21:28]))
    b3 = dict(zip(NAMES, refs[28:35]))
    (h_ref, q_ref, kv_ref, wbuf, dbuf, cos_ref, sin_ref, first_ref, gain_ref,
     seg_ref, freq_ref, ga_ref, gm_ref, far_ref, wsem, dsem, iosem, lsem) = refs[35:53]
    s0s, s0r, s1s, s1r, s2s, s2r, s3s, s3r = refs[53:]
    sources = (own, b1, b2, b3)
    y = lax.axis_index("rep")
    d = lax.axis_index("fsdp")
    side = d // 2
    core = lax.rem(d, 2)
    x_dev = (y, lax.rem(d + 2, 4))
    y_dev = (1 - y, d)
    c_dev = (y, d + 1 - 2 * core)

    def rel(block):
        return 2 * lax.rem(block // 2 + side, 2) + lax.rem(block + core, 2)

    inputs = [pltpu.make_async_copy(src, dst, iosem.at[n]) for n, (src, dst) in enumerate(
        ((tok, q_ref), (seg, seg_ref), (freq, freq_ref), (g_attn, ga_ref), (g_mlp, gm_ref)))]
    for copy in inputs:
        copy.start()

    with jax.named_scope("barrier"):
        barrier = pltpu.get_barrier_semaphore()
        for dev in (x_dev, y_dev, c_dev):
            pl.semaphore_signal(barrier, inc=1, device_id=dev, device_id_type=MESH)
        pl.semaphore_wait(barrier, 3)

    def kinds(k):
        i = lax.rem(k, PER_LAYER)
        jq = pl.multiple_of((i - CH_Q) * WIDTH, WIDTH)
        jo = pl.multiple_of((i - CH_O) * WIDTH, WIDTH)
        jg = pl.multiple_of((i - CH_GU) * WIDTH, WIDTH)
        jd = core * TAIL + (i - CH_D) * PART
        jr = (1 - core) * 2560
        last = N_GU * WIDTH
        kv = [("k", 0, ROWS, 0, PART), ("v", 0, ROWS, 0, PART)]
        gu = [("g", 0, ROWS, jg, WIDTH), ("u", 0, ROWS, jg, WIDTH)]
        gl = [("g", 0, ROWS, last, PART), ("u", 0, ROWS, last, PART)]

        def split_cols(name, c0):
            whole = [(name, 0, ROWS, c0, WIDTH)]
            return [(name, 0, ROWS, c0, PART), (name, 0, ROWS, c0 + PART, PART)], whole, whole

        def split_rows(r0, nr):
            halves = [("d", r0, nr // 2, 0, D), ("d", r0 + nr // 2, nr // 2, 0, D)]
            return halves, [("d", r0, nr, 0, D)], halves

        return [
            (i == 0, kv, kv, kv, 0),
            ((i >= CH_Q) & (i < CH_O), *split_cols("q", jq), 0),
            ((i >= CH_O) & (i < CH_GU), *split_cols("o", jo), 0),
            ((i >= CH_GU) & (i < CH_GL), gu, gu, gu, 0),
            (i == CH_GL, gl, gl, gl, 0),
            ((i >= CH_D) & (i < CH_DR) & (k != CHUNKS - 2), *split_rows(jd, PART), 0),
            (k == CHUNKS - 2, *split_rows(jd, PART), 2),
            ((i == CH_DR) & (k != CHUNKS - 1), *split_rows(jr, TAIL), 0),
            (k == CHUNKS - 1, *split_rows(jr, TAIL)[:2], [("d", jr, TAIL, 0, WIDE), ("d", jr, TAIL, WIDE, WIDE)], 1),
        ]

    def for_chunk(k, fn, form=2, part=None):
        layer = k // PER_LAYER
        slot = lax.rem(k, SLOTS)
        for kind in kinds(k):
            @pl.when((k < CHUNKS) & kind[0])
            def _():
                for n, piece in enumerate(kind[form]):
                    if part is None:
                        fn(kind[4], layer, piece, (slot, n))
                    else:
                        @pl.when(part != 1 - n)
                        def _():
                            fn(kind[4], layer, piece, (slot, n))

    def for_pair(k, fn, part=None):
        layer = k // PER_LAYER
        for cond, pieces, _, _, mark in kinds(k):
            @pl.when((k < CHUNKS) & cond)
            def _():
                for n, piece in enumerate(pieces):
                    args = (mark == 1 and n == 1, layer, piece, (lax.rem(2 * k + n, ITEM_SLOTS),))
                    if part is None:
                        fn(*args)
                    else:
                        @pl.when(part != 1 - n)
                        def _():
                            fn(*args)

    def for_item(m, fn):
        k = m // 2
        n = lax.rem(m, 2)
        layer = k // PER_LAYER
        slot = (lax.rem(m, ITEM_SLOTS),)
        for cond, (one, two), _, _, mark in kinds(k):
            if one[0] == two[0] and mark != 1:
                name, r0, nr, c0, nc = one
                r0, c0 = (r0 + n * nr, c0) if nc == D else (r0, pl.multiple_of(c0 + n * nc, PART))

                @pl.when((m < ITEMS) & cond)
                def _():
                    fn(False, layer, (name, r0, nr, c0, nc), slot)
            else:
                for which, piece in enumerate((one, two)):
                    @pl.when((m < ITEMS) & cond & (n == which))
                    def _():
                        fn(mark == 1 and which == 1, layer, piece, slot)

    def view(bufs, name, layer, r0, nr, c0, nc, half):
        if half:
            nr = nr // 2
            r0 = r0 + y * nr
        r0 = pl.multiple_of(r0, 16)
        return bufs[name].at[layer, pl.ds(r0, nr), pl.ds(c0, nc)]

    def remote(src, dst, ss, rs, dev, half):
        def make(whole, layer, piece, slot):
            part = half and not whole
            return pltpu.make_async_remote_copy(
                src_ref=view(src, piece[0], layer, *piece[1:], part),
                dst_ref=view(dst, piece[0], layer, *piece[1:], part),
                send_sem=ss.at[slot], recv_sem=rs.at[slot], device_id=dev, device_id_type=MESH)
        return make

    copy0 = remote(own, b1, s0s, s0r, c_dev, False)
    copy1 = remote(own, b2, s1s, s1r, x_dev, True)
    copy2 = remote(b2, b2, s2s, s2r, y_dev, True)

    def rest_rows(c0):
        return a_ref.at[pl.ds(pl.multiple_of(c0 // WIDE * REST_K + core * TAIL, 64), TAIL), pl.ds(FF, WIDE)]

    def copy3(mark, layer, piece, slot):
        name, r0, nr, c0, nc = piece
        if mark == 0:
            return remote(b2, b3, s3s, s3r, c_dev, False)(False, layer, piece, slot)
        if mark == 1:
            dst = rest_rows(c0)
        else:
            dst = far_ref.at[pl.ds(pl.multiple_of(r0 - core * TAIL - (N_D - 1) * PART + PART, LANES), nr), :]
        return pltpu.make_async_remote_copy(
            src_ref=view(b2, name, layer, r0, nr, c0, nc, False), dst_ref=dst,
            send_sem=s3s.at[slot], recv_sem=s3r.at[slot], device_id=c_dev, device_id_type=MESH)

    def start0(*a):
        copy0(*a).start()

    def start1(*a):
        copy1(*a).start()

    def wait0(*a):
        copy0(*a).wait_recv()

    def relay2(*a):
        copy1(*a).wait_recv()
        if not a[0]:
            copy2(*a).start()

    def arrived(*a):
        if not a[0]:
            copy2(*a).wait_recv()
        copy1(*a).wait_send()

    def relay3(*a):
        copy3(*a).start()

    def pushed(*a):
        copy0(*a).wait_send()

    def finish(*a):
        copy3(*a).wait_recv()
        copy3(*a).wait_send()

    def sent(*a):
        if not a[0]:
            copy2(*a).wait_send()

    def targets(s):
        i = lax.rem(s, STEPS)
        layer = s // STEPS
        first = layer == 0
        late = 1 - jnp.minimum(layer, 1)
        t2 = jnp.where(i < ST_A, 9 + 2 * i + late,
             jnp.where(i < ST_G + 1, 18 + late + 3 * (i - ST_A) // 5,
             jnp.where(i < ST_D, jnp.maximum(i + 4, 31 + late + (i - ST_G - 1) // 2),
             jnp.where(i < ST_NEAR, jnp.maximum(i, ST_D + 3 + (2 * (i - ST_D) + 1) // 3),
             jnp.where(first, jnp.where(i < ST_NEAR + 2, i, jnp.where(i < ST_READY - 2, 40 + i // 2, jnp.where(i < ST_READY, i - 2, i - 3))),
             jnp.where(i < ST_READY - 2, 38 + (i + 1) // 2, 39 + i // 2))))))
        final = i == STEPS - 1
        t3 = jnp.where(i < ST_D, jnp.where(i < ST_A, 3 + i, (t2 - 3) // 2),
             jnp.where(first, jnp.where(i < ST_IDLE, (t2 - 2) // 2, CH_DR + (i - ST_IDLE + 1) // 2 + jnp.where(final, 1, 0)),
             jnp.where(i < ST_READY - 4, (t2 - 2) // 2, jnp.where(i < ST_READY + 2, 39 + (i - ST_READY + 4) // 3, i - ST_READY + 39 + jnp.where(i == ST_FAR, 1, 0)))))
        end = s >= ALL_STEPS - 2
        t2 = jnp.minimum(t2 + layer * 2 * PER_LAYER, jnp.where(end, ITEMS, ITEMS - 1))
        t3 = jnp.minimum(t3 + layer * PER_LAYER, PUSHES)
        nxt = jnp.minimum(s + 1, ALL_STEPS - 1)
        i = lax.rem(nxt, STEPS)
        base = nxt // STEPS * PER_LAYER
        done = jnp.where(i < ST_A, 1 + i,
               jnp.where(i < ST_O, ST_A,
               jnp.where(i < ST_G, 1 + CH_O + i - ST_O,
               jnp.where(i < ST_D, 1 + CH_GU + (i - ST_G) // 2,
               jnp.where(i < ST_NEAR, 1 + CH_D + (i - ST_D) // 2,
               jnp.where(i < ST_READY, CH_D + (i - ST_D) // 2,
               jnp.where(i < ST_READY + 1, CH_DR - 2,
               jnp.where(i < ST_FAR, CH_DR - 1,
               jnp.where(i < ST_REST, CH_DR, PER_LAYER)))))))))
        tf = jnp.maximum(jnp.minimum(t3 - 2, CHUNKS - 2), done + base)
        pushes = tf + jnp.where(tf == CHUNKS - 1, 1, 0)
        t3 = jnp.maximum(jnp.maximum(t3, pushes), base + jnp.where((i >= ST_READY) & (i < ST_FAR), CH_DR - 1, 0))
        return jnp.maximum(t2, 2 * jnp.minimum(t3, CHUNKS - 2)), t3, tf

    def relays(old, new):
        @pl.loop(old[0], new[0])
        def _(m):
            with jax.named_scope("r2"):
                for_item(m, relay2)
                for_item(m + AHEAD, start1)
                n = lax.rem(m, 2)
                for_chunk(m // 2 + jnp.where(n == 0, AHEAD0, CHUNKS), start0)
                for_chunk(m // 2 + jnp.where(n == 0, CHUNKS, AHEAD0 - 1), wait0)

        @pl.loop(old[1], new[1])
        def _(p):
            with jax.named_scope("r3"):
                extra = jnp.maximum(p - (CHUNKS - 2), 0)
                k = p - jnp.minimum(extra, 1)
                part = jnp.where((p < CHUNKS - 2) | (extra > 1), 2, extra)
                for_pair(k, arrived, part)
                for_chunk(k, relay3, 3, part)
                for_chunk(jnp.where(part == 1, CHUNKS, k), pushed)

        @pl.loop(old[2], new[2])
        def _(k):
            with jax.named_scope("fin"):
                for_chunk(k, finish, 3)
                for_pair(k, sent)

    def down_step(i):
        n = i - ST_D - jnp.where(i > ST_READY, 1, 0) - jnp.where(i > ST_IDLE, 1, 0)
        j = n // 2
        near = (i >= ST_NEAR) & (i < ST_NEAR + 2)
        far = (i >= ST_FAR) & (i < ST_REST)
        rest = i >= ST_REST
        whole = (i >= ST_D) & (i < ST_IDLE) & ~near & (i != ST_READY)
        return j, jnp.where(i > ST_NEAR, j - 1, j), lax.rem(n + 2 * STEPS, 2), whole, near, far, rest

    def rest_col(side_no):
        return pl.multiple_of(side_no * (2 * FF_ROWS) + 2560, HEAD)

    def tile_col(side_no, core_no, tile):
        return pl.multiple_of(side_no * (2 * FF_ROWS) + core_no * (FF_ROWS + TAIL) + tile * PART, HEAD)

    def near_far():
        r0 = pl.multiple_of(core * TAIL + (N_D - 1) * PART, 64)
        return pltpu.make_async_copy(b2["d"].at[LAYERS - 1, pl.ds(r0, PART), :], far_ref.at[pl.ds(0, PART), :], lsem.at[0])

    def near_rest():
        r0 = pl.multiple_of((1 - core) * 2560, WIDTH)
        return [pltpu.make_async_copy(b2["d"].at[LAYERS - 1, pl.ds(r0, TAIL), pl.ds(n * WIDE, WIDE)], rest_rows(n * WIDE), lsem.at[1 + n])
                for n in range(2)]

    def load_tile(s):
        layer = s // STEPS
        i = lax.rem(s, STEPS)
        slot = lax.rem(s, 2)

        def cols(name, c0, nc, w0):
            for r, src in enumerate(sources):
                pltpu.make_async_copy(src[name].at[layer, :, pl.ds(c0, nc)],
                                      wbuf.at[slot, pl.ds(r * ROWS, ROWS), pl.ds(w0, nc)], wsem.at[slot]).start()

        @pl.when(i == 0)
        def _():
            cols("k", 0, PART, 0)
            cols("v", 0, PART, PART)

        @pl.when((i >= ST_Q) & (i < ST_A))
        def _():
            cols("q", pl.multiple_of((i - ST_Q) * WIDTH, WIDTH), WIDTH, 0)

        @pl.when((i >= ST_O) & (i < ST_G))
        def _():
            cols("o", pl.multiple_of((i - ST_O) * WIDTH, WIDTH), WIDTH, 0)

        @pl.when((i >= ST_G) & (i < ST_D))
        def _():
            c0 = pl.multiple_of((i - ST_G) * PART, PART)
            cols("g", c0, PART, 0)
            cols("u", c0, PART, PART)

        j, tile, half, whole, near, far, rest = down_step(i)
        dslot = lax.rem(j + 2 * STEPS, 2)

        def rows_in(src, r0, nr, w0):
            pltpu.make_async_copy(src["d"].at[layer, pl.ds(r0, nr), :], dbuf.at[dslot, pl.ds(w0, nr), :], dsem.at[dslot]).start()

        def chunk_rows(r, tile_no, w0):
            src_core = core if r % 2 == 0 else 1 - core
            rows_in(sources[r], pl.multiple_of(src_core * TAIL + tile_no * PART, 64), PART, w0)

        def rest_rows(r, w0):
            src_core = core if r % 2 == 0 else 1 - core
            rows_in(sources[r], pl.multiple_of((1 - src_core) * 2560, WIDTH), TAIL, pl.multiple_of(w0 + src_core * TAIL, 64))

        @pl.when((whole & (half == 0) & (i != ST_READY + 1)) | (i == ST_READY))
        def _():
            for r in range(3):
                chunk_rows(r, jnp.where(i == ST_READY, N_D - 2, tile), r * PART)

        @pl.when(whole & (half == 0))
        def _():
            chunk_rows(3, tile, 768)

        @pl.when(near & (half == 0))
        def _():
            for r in range(2):
                chunk_rows(r, N_D - 1, r * PART)
                rest_rows(r, WIDTH)

        @pl.when(far & (half == 0) & (layer < LAYERS - 1))
        def _():
            for r in range(2):
                chunk_rows(2 + r, N_D - 1, r * PART)

        @pl.when(far & (half == 0) & (layer == LAYERS - 1))
        def _():
            near_far().start()

        @pl.when(rest & (half == 0))
        def _():
            for r in range(2):
                rest_rows(2 + r, 0)

    def norm(layer, which):
        @pl.loop(0, TOK // NB)
        def _(m):
            rows = pl.ds(pl.multiple_of(m * NB, NB), NB)
            total = jnp.zeros((NB, 1), F32)
            for b in range(4):
                blk = x_ref[rows, pl.ds(b * ROWS, ROWS)]
                total = total + jnp.sum(blk * blk, axis=1, keepdims=True)
            inv = lax.rsqrt(total * (1.0 / D) + EPS)
            for b in range(4):
                blk = x_ref[rows, pl.ds(b * ROWS, ROWS)]
                gain = gain_ref[which * LAYERS + layer, :, pl.ds(b * ROWS, ROWS)]
                c0 = pl.multiple_of(rel(b) * ROWS, ROWS)
                h_ref[rows, pl.ds(c0, ROWS)] = (blk * inv * gain).astype(BF16)

    def rotate(vals, rows):
        vals = vals.astype(BF16).astype(F32)
        turned = pltpu.roll(vals, HEAD // 2, 1)
        return (vals * cos_ref[rows, :] + turned * sin_ref[rows, :]).astype(BF16)

    def tile_product(slot, finish_rows):
        @pl.loop(0, TOK // MB)
        def _(m):
            rows = pl.ds(pl.multiple_of(m * MB, MB), MB)
            finish_rows(rows, jnp.dot(h_ref[rows, :], wbuf[slot], preferred_element_type=F32))

    def kv_step(slot):
        def fin(rows, acc):
            for b in range(2):
                kv_ref[rows, pl.ds(b * HEAD, HEAD)] = rotate(acc[:, b * HEAD:(b + 1) * HEAD], rows)
            kv_ref[rows, pl.ds(PART, PART)] = acc[:, PART:].astype(BF16)
        tile_product(slot, fin)

    def q_step(slot, j):
        def fin(rows, acc):
            for b in range(4):
                c0 = pl.multiple_of(j * WIDTH + b * HEAD, HEAD)
                q_ref[rows, pl.ds(c0, HEAD)] = rotate(acc[:, b * HEAD:(b + 1) * HEAD], rows)
        tile_product(slot, fin)

    def o_step(slot, j):
        def fin(rows, acc):
            c0 = pl.ds(pl.multiple_of(j * WIDTH, WIDTH), WIDTH)
            x_ref[rows, c0] = x_ref[rows, c0] + acc
        tile_product(slot, fin)

    def g_step(slot, j):
        def fin(rows, acc):
            gate = acc[:, :PART]
            up = acc[:, PART:]
            c0 = pl.multiple_of(j * PART, PART)
            a_ref[rows, pl.ds(c0, PART)] = (gate * jax.nn.sigmoid(gate) * up).astype(BF16)
        tile_product(slot, fin)

    def attend(head):
        kv = head // 8
        q0 = pl.multiple_of(head * HEAD, HEAD)
        k0 = pl.multiple_of(kv * HEAD, HEAD)
        v0 = pl.multiple_of(PART + kv * HEAD, HEAD)
        o0 = pl.multiple_of(rel(head // 4) * ROWS + lax.rem(head, 4) * HEAD, HEAD)
        scale = HEAD ** -0.5
        for b in range(TOK // QB):
            keys = (b + 1) * QB
            rows = pl.ds(b * QB, QB)
            scores = lax.dot_general(q_ref[rows, pl.ds(q0, HEAD)], kv_ref[pl.ds(0, keys), pl.ds(k0, HEAD)],
                                     (((1,), (1,)), ((), ())), preferred_element_type=F32)
            key_idx = lax.broadcasted_iota(jnp.int32, (QB, keys), 1)
            row_idx = lax.broadcasted_iota(jnp.int32, (QB, keys), 0) + b * QB
            first = jnp.concatenate([first_ref[rows, :]] * (keys // HEAD), axis=1)
            ok = (key_idx >= first) & (key_idx <= row_idx)
            scores = jnp.where(ok, scores, -1e30)
            top = jnp.max(scores, axis=1, keepdims=True)
            probs = jnp.exp((scores - top) * scale)
            inv = 1.0 / jnp.sum(probs, axis=1, keepdims=True)
            probs = (probs * inv).astype(BF16)
            mixed = jnp.dot(probs, kv_ref[pl.ds(0, keys), pl.ds(v0, HEAD)], preferred_element_type=F32)
            h_ref[rows, pl.ds(o0, HEAD)] = mixed.astype(BF16)

    def add_product(dslot, half, cols, tile_ref=None):
        rows = pl.ds(pl.multiple_of(half * MB, MB), MB)
        depth = sum(width for _, width in cols)
        lhs = jnp.concatenate([a_ref[rows, pl.ds(c0, width)] for c0, width in cols], axis=1)
        tile = dbuf[dslot, pl.ds(0, depth), :] if tile_ref is None else tile_ref[...]
        x_ref[rows, :] = x_ref[rows, :] + jnp.dot(lhs, tile, preferred_element_type=F32)

    def wait_d(dslot, half, depth):
        @pl.when(half == 0)
        def _():
            part = dbuf.at[dslot, pl.ds(0, depth), :]
            pltpu.make_async_copy(part, part, dsem.at[dslot]).wait()

    def last_cols(side_no):
        return [(tile_col(side_no, core, N_D - 1), PART), (tile_col(side_no, 1 - core, N_D - 1), PART)]

    def wait_w(slot):
        pltpu.make_async_copy(wbuf.at[slot], wbuf.at[slot], wsem.at[slot]).wait()

    def step(s):
        before = [jnp.where(s == 0, one, two) for one, two in zip(FIRST, targets(s - 1))]
        relays(before, targets(s))

        @pl.when(s + 1 < ALL_STEPS)
        def _():
            load_tile(s + 1)

        with jax.named_scope("comp"):
            compute(s)

    def compute(s):
        layer = s // STEPS
        i = lax.rem(s, STEPS)
        slot = lax.rem(s, 2)

        @pl.when(((i == 0) & (layer > 0)) | (i == ST_G))
        def _():
            norm(layer, jnp.where(i == 0, 0, 1))

        @pl.when((i < ST_A) | ((i >= ST_O) & (i < ST_D)))
        def _():
            wait_w(slot)

        @pl.when(i == 0)
        def _():
            kv_step(slot)

        @pl.when((i >= ST_Q) & (i < ST_A))
        def _():
            q_step(slot, i - ST_Q)

        @pl.when((i >= ST_A) & (i < ST_O))
        def _():
            attend(i - ST_A)

        @pl.when((i >= ST_O) & (i < ST_G))
        def _():
            o_step(slot, i - ST_O)

        @pl.when((i >= ST_G) & (i < ST_D))
        def _():
            g_step(slot, i - ST_G)

        j, tile, half, whole, near, far, rest = down_step(i)
        dslot = lax.rem(j + 2 * STEPS, 2)

        @pl.when(whole)
        def _():
            wait_d(dslot, half, 1024)
            add_product(dslot, half, [(tile_col(lax.rem(side + r // 2, 2), lax.rem(core + r, 2), tile), PART) for r in range(4)])

        @pl.when(near)
        def _():
            wait_d(dslot, half, NEAR_K)
            add_product(dslot, half, last_cols(side) + [(rest_col(side), REST_K)])

        @pl.when(far & (layer < LAYERS - 1))
        def _():
            wait_d(dslot, half, WIDTH)
            add_product(dslot, half, last_cols(1 - side))

        @pl.when(far & (layer == LAYERS - 1))
        def _():
            @pl.when(half == 0)
            def _():
                near_far().wait()
                for copy in near_rest():
                    copy.start()
            add_product(dslot, half, last_cols(1 - side), far_ref)

        @pl.when(rest)
        def _():
            wait_d(dslot, half, REST_K)
            add_product(dslot, half, [(rest_col(1 - side), REST_K)])

    @pl.loop(0, AHEAD)
    def _(m):
        for_item(m, start1)

    @pl.loop(0, AHEAD0)
    def _(k):
        for_chunk(k, start0)

    for copy in inputs:
        copy.wait()

    for n, ref in enumerate((ga_ref, gm_ref)):
        for layer in range(LAYERS):
            gain_ref[n * LAYERS + layer] = ref[pl.ds(layer, 1), :].astype(F32)
    ids = seg_ref[...].astype(F32)
    lane = lax.broadcasted_iota(jnp.int32, (LANES, HEAD), 1)
    for b in range(TOK // LANES):
        rows = pl.ds(b * LANES, LANES)
        mine = jnp.transpose(jnp.broadcast_to(ids[b:b + 1, :], (LANES, LANES)))
        before = jnp.zeros((LANES, LANES), F32)
        for c in range(TOK // LANES):
            before = before + jnp.where(ids[c:c + 1, :] < mine, 1.0, 0.0)
        first = jnp.sum(before, axis=1, keepdims=True)
        pos = lax.broadcasted_iota(jnp.int32, (LANES, LANES), 0).astype(F32) + (b * 128.0) - first
        angles = pos * freq_ref[...]
        cos_ref[rows, :] = jnp.cos(angles)
        sin = jnp.sin(angles)
        sin_ref[rows, :] = jnp.where(lane < HEAD // 2, -sin, sin)
        first_ref[rows, :] = jnp.broadcast_to(first, (LANES, LANES)).astype(jnp.int32)

    @pl.loop(0, TOK // NB)
    def _(m):
        rows = pl.ds(pl.multiple_of(m * NB, NB), NB)
        x_ref[rows, :] = q_ref[rows, :].astype(F32)

    relays((0, 0, 0), (2, 0, 0))
    norm(0, 0)

    @pl.loop(0, AHEAD0 - 1)
    def _(k):
        for_chunk(k, wait0)

    relays((2, 0, 0), START)
    relays(START, FIRST)
    load_tile(0)

    @pl.loop(0, ALL_STEPS)
    def _(s):
        with jax.named_scope("step"):
            step(s)

    relays(targets(ALL_STEPS - 1), (ITEMS, PUSHES, CHUNKS))
    for copy in near_rest():
        copy.wait()


def result_kernel(x_ref, a_ref, out, y_ref, osem):
    c0 = pl.multiple_of((1 - lax.axis_index("fsdp") // 2) * (2 * FF_ROWS) + 2560, HEAD)

    def store(n, m):
        rows, cols = pl.ds(m * WIDTH, WIDTH), pl.ds(n * WIDTH, WIDTH)
        return pltpu.make_async_copy(y_ref.at[rows, cols], out.at[rows, cols], osem.at[n, m])

    for n in range(4):
        cols = pl.ds(n * WIDTH, WIDTH)
        tile = a_ref[pl.ds(n // 2 * REST_K, REST_K), pl.ds(FF + n % 2 * WIDTH, WIDTH)]
        for m in range(2):
            rows = pl.ds(m * WIDTH, WIDTH)
            y_ref[rows, cols] = x_ref[rows, cols] + jnp.dot(a_ref[rows, pl.ds(c0, REST_K)], tile, preferred_element_type=F32)
            store(n, m).start()
    for n in range(4):
        for m in range(2):
            store(n, m).wait()


def run_layers(tokens, seg_ids, g_attn, g_mlp, weights):
    shapes = [jax.ShapeDtypeStruct(w.shape, w.dtype) for w in weights]
    half_dim = HEAD // 2
    freq = np.float32(ROPE_BASE) ** (-np.arange(half_dim, dtype=np.float32) / np.float32(half_dim))
    freq = jnp.asarray(np.concatenate([freq, freq]).reshape(1, HEAD))
    sem = pltpu.SemaphoreType.DMA((SLOTS, 2))
    item_sem = pltpu.SemaphoreType.DMA((ITEM_SLOTS,))
    any_spec = pl.BlockSpec(memory_space=pl.ANY)
    vmem_spec = pl.BlockSpec(memory_space=pltpu.VMEM)
    outs = pl.pallas_call(
        layer_kernel,
        out_shape=[pltpu.VMEM((TOK, D), F32), pltpu.VMEM((TOK, FF + WIDE), BF16)] + shapes * 3,
        in_specs=[any_spec] * 12,
        out_specs=[vmem_spec] * 2 + [any_spec] * 21,
        scratch_shapes=[
            pltpu.VMEM((TOK, D), BF16),
            pltpu.VMEM((TOK, D), BF16),
            pltpu.VMEM((TOK, WIDTH), BF16),
            pltpu.VMEM((2, D, WIDTH), BF16),
            pltpu.VMEM((2, 1024, D), BF16),
            pltpu.VMEM((TOK, HEAD), F32),
            pltpu.VMEM((TOK, HEAD), F32),
            pltpu.VMEM((TOK, HEAD), jnp.int32),
            pltpu.VMEM((2 * LAYERS, 1, D), F32),
            pltpu.VMEM((TOK // LANES, LANES), jnp.int32),
            pltpu.VMEM((1, HEAD), F32),
            pltpu.VMEM((LAYERS, D), BF16),
            pltpu.VMEM((LAYERS, D), BF16),
            pltpu.VMEM((WIDTH, D), BF16),
            pltpu.SemaphoreType.DMA((2,)),
            pltpu.SemaphoreType.DMA((2,)),
            pltpu.SemaphoreType.DMA((5,)),
            pltpu.SemaphoreType.DMA((3,)),
        ] + [sem] * 2 + [item_sem] * 4 + [sem] * 2,
        compiler_params=pltpu.CompilerParams(collective_id=0, has_side_effects=True, vmem_limit_bytes=32 * 1000 * 1000),
        name="two_layers",
    )(tokens, seg_ids.reshape(TOK // LANES, LANES), freq, g_attn, g_mlp, *weights)
    hidden = pltpu.with_memory_space_constraint(outs[0], pltpu.VMEM)
    act = pltpu.with_memory_space_constraint(outs[1], pltpu.VMEM)
    return pl.pallas_call(
        result_kernel,
        out_shape=jax.ShapeDtypeStruct((TOK, D), F32),
        in_specs=[vmem_spec] * 2,
        out_specs=any_spec,
        scratch_shapes=[
            pltpu.VMEM((TOK, D), F32),
            pltpu.SemaphoreType.DMA((4, 2)),
        ],
        compiler_params=pltpu.CompilerParams(vmem_limit_bytes=24 * 1000 * 1000),
        name="result",
    )(hidden, act)


def solution(mesh):
    tok_spec = P(("rep", "fsdp"), None)
    seg_spec = P(("rep", "fsdp"))
    mat_spec = P(None, "fsdp", None)
    gain_spec = P(None, None)

    def per_device(tokens, seg_ids, w_q, w_k, w_v, w_o, w_gate, w_up, w_down, g_attn, g_mlp):
        return run_layers(tokens, seg_ids, g_attn, g_mlp, (w_q, w_k, w_v, w_o, w_gate, w_up, w_down))

    return jax.shard_map(per_device, mesh=mesh, in_specs=(tok_spec, seg_spec, mat_spec, mat_spec, mat_spec, mat_spec, mat_spec, mat_spec, mat_spec, gain_spec, gain_spec), out_specs=tok_spec, check_vma=False)
```

```python
import functools

import jax
import jax.numpy as jnp
import numpy as np
from jax import lax
from jax.experimental import pallas as pl
from jax.experimental.pallas import tpu as pltpu
from jax.sharding import PartitionSpec as P

D = 2048
WIDTH = 512
PART = 256
LANES = 128
FF = 11008
HEADS = 16
HEAD = LANES
TOK = 1024
EPS = 1e-5
ROPE_BASE = 10000.0
MESH = pl.DeviceIdType.MESH
F32 = jnp.float32
BF16 = jnp.bfloat16

LAYERS = 2
SLOTS = 8
ITEM_SLOTS = 2 * SLOTS
AHEAD = 8
AHEAD0 = 5
ROWS = D // 4
FF_ROWS = FF // 4
TAIL = 192
NAMES = ("q", "k", "v", "o", "g", "u", "d")

N_Q = 4
N_GU = 21
N_D = 10
CH_Q = 1
CH_O = CH_Q + N_Q
CH_GU = CH_O + N_Q
CH_GL = CH_GU + N_GU
CH_D = CH_GL + 1
CH_DR = CH_D + N_D
PER_LAYER = CH_DR + 1
CHUNKS = LAYERS * PER_LAYER
ITEMS = 2 * CHUNKS
PUSHES = CHUNKS + 1

NEAR_AT = 5

N_GT = FF // PART
ST_Q = 1
ST_A = ST_Q + N_Q
ST_O = ST_A + HEADS
ST_G = ST_O + 4
ST_D = ST_G + N_GT
ST_NEAR = ST_D + 2 * NEAR_AT
ST_READY = ST_D + 2 * (N_D - 1)
ST_IDLE = ST_READY + 3
ST_FAR = ST_IDLE + 1
ST_REST = ST_FAR + 2
STEPS = ST_REST + 2
ALL_STEPS = LAYERS * STEPS - 2
START = (4, 1, 0)
FIRST = (8, 3, 1)
REST_K = 2 * TAIL
WIDE = D // 2
NEAR_K = WIDTH + REST_K

MB = WIDTH
NB = LANES
QB = PART


def layer_kernel(*refs):
    tok, seg, freq, g_attn, g_mlp = refs[:5]
    own = dict(zip(NAMES, refs[5:12]))
    x_ref, a_ref = refs[12:14]
    b1 = dict(zip(NAMES, refs[14:21]))
    b2 = dict(zip(NAMES, refs[21:28]))
    b3 = dict(zip(NAMES, refs[28:35]))
    (h_ref, q_ref, kv_ref, wbuf, dbuf, cos_ref, sin_ref, first_ref, gain_ref,
     seg_ref, freq_ref, ga_ref, gm_ref, far_ref, wsem, dsem, iosem, lsem) = refs[35:53]
    s0s, s0r, s1s, s1r, s2s, s2r, s3s, s3r = refs[53:]
    sources = (own, b1, b2, b3)
    y = lax.axis_index("rep")
    d = lax.axis_index("fsdp")
    side = d // 2
    core = lax.rem(d, 2)
    x_dev = (y, lax.rem(d + 2, 4))
    y_dev = (1 - y, d)
    c_dev = (y, d + 1 - 2 * core)

    def rel(block):
        return 2 * lax.rem(block // 2 + side, 2) + lax.rem(block + core, 2)

    inputs = [pltpu.make_async_copy(src, dst, iosem.at[n]) for n, (src, dst) in enumerate(
        ((tok, q_ref), (seg, seg_ref), (freq, freq_ref), (g_attn, ga_ref), (g_mlp, gm_ref)))]
    for copy in inputs:
        copy.start()

    with jax.named_scope("barrier"):
        barrier = pltpu.get_barrier_semaphore()
        for dev in (x_dev, y_dev, c_dev):
            pl.semaphore_signal(barrier, inc=1, device_id=dev, device_id_type=MESH)
        pl.semaphore_wait(barrier, 3)

    def kinds(k):
        i = lax.rem(k, PER_LAYER)
        jq = pl.multiple_of((i - CH_Q) * WIDTH, WIDTH)
        jo = pl.multiple_of((i - CH_O) * WIDTH, WIDTH)
        jg = pl.multiple_of((i - CH_GU) * WIDTH, WIDTH)
        jd = core * TAIL + (i - CH_D) * PART
        jr = (1 - core) * 2560
        last = N_GU * WIDTH
        kv = [("k", 0, ROWS, 0, PART), ("v", 0, ROWS, 0, PART)]
        gu = [("g", 0, ROWS, jg, WIDTH), ("u", 0, ROWS, jg, WIDTH)]
        gl = [("g", 0, ROWS, last, PART), ("u", 0, ROWS, last, PART)]

        def split_cols(name, c0):
            whole = [(name, 0, ROWS, c0, WIDTH)]
            return [(name, 0, ROWS, c0, PART), (name, 0, ROWS, c0 + PART, PART)], whole, whole

        def split_rows(r0, nr):
            halves = [("d", r0, nr // 2, 0, D), ("d", r0 + nr // 2, nr // 2, 0, D)]
            return halves, [("d", r0, nr, 0, D)], halves

        return [
            (i == 0, kv, kv, kv, 0),
            ((i >= CH_Q) & (i < CH_O), *split_cols("q", jq), 0),
            ((i >= CH_O) & (i < CH_GU), *split_cols("o", jo), 0),
            ((i >= CH_GU) & (i < CH_GL), gu, gu, gu, 0),
            (i == CH_GL, gl, gl, gl, 0),
            ((i >= CH_D) & (i < CH_DR) & (k != CHUNKS - 2), *split_rows(jd, PART), 0),
            (k == CHUNKS - 2, *split_rows(jd, PART), 2),
            ((i == CH_DR) & (k != CHUNKS - 1), *split_rows(jr, TAIL), 0),
            (k == CHUNKS - 1, *split_rows(jr, TAIL)[:2], [("d", jr, TAIL, 0, WIDE), ("d", jr, TAIL, WIDE, WIDE)], 1),
        ]

    def for_chunk(k, fn, form=2, part=None):
        layer = k // PER_LAYER
        slot = lax.rem(k, SLOTS)
        for kind in kinds(k):
            @pl.when((k < CHUNKS) & kind[0])
            def _():
                for n, piece in enumerate(kind[form]):
                    if part is None:
                        fn(kind[4], layer, piece, (slot, n))
                    else:
                        @pl.when(part != 1 - n)
                        def _():
                            fn(kind[4], layer, piece, (slot, n))

    def for_pair(k, fn, part=None):
        layer = k // PER_LAYER
        for cond, pieces, _, _, mark in kinds(k):
            @pl.when((k < CHUNKS) & cond)
            def _():
                for n, piece in enumerate(pieces):
                    args = (mark == 1 and n == 1, layer, piece, (lax.rem(2 * k + n, ITEM_SLOTS),))
                    if part is None:
                        fn(*args)
                    else:
                        @pl.when(part != 1 - n)
                        def _():
                            fn(*args)

    def for_item(m, fn):
        k = m // 2
        n = lax.rem(m, 2)
        layer = k // PER_LAYER
        slot = (lax.rem(m, ITEM_SLOTS),)
        for cond, (one, two), _, _, mark in kinds(k):
            if one[0] == two[0] and mark != 1:
                name, r0, nr, c0, nc = one
                r0, c0 = (r0 + n * nr, c0) if nc == D else (r0, pl.multiple_of(c0 + n * nc, PART))

                @pl.when((m < ITEMS) & cond)
                def _():
                    fn(False, layer, (name, r0, nr, c0, nc), slot)
            else:
                for which, piece in enumerate((one, two)):
                    @pl.when((m < ITEMS) & cond & (n == which))
                    def _():
                        fn(mark == 1 and which == 1, layer, piece, slot)

    def view(bufs, name, layer, r0, nr, c0, nc, half):
        if half:
            nr = nr // 2
            r0 = r0 + y * nr
        r0 = pl.multiple_of(r0, 16)
        return bufs[name].at[layer, pl.ds(r0, nr), pl.ds(c0, nc)]

    def remote(src, dst, ss, rs, dev, half):
        def make(whole, layer, piece, slot):
            part = half and not whole
            return pltpu.make_async_remote_copy(
                src_ref=view(src, piece[0], layer, *piece[1:], part),
                dst_ref=view(dst, piece[0], layer, *piece[1:], part),
                send_sem=ss.at[slot], recv_sem=rs.at[slot], device_id=dev, device_id_type=MESH)
        return make

    copy0 = remote(own, b1, s0s, s0r, c_dev, False)
    copy1 = remote(own, b2, s1s, s1r, x_dev, True)
    copy2 = remote(b2, b2, s2s, s2r, y_dev, True)

    def rest_rows(c0):
        return a_ref.at[pl.ds(pl.multiple_of(c0 // WIDE * REST_K + core * TAIL, 64), TAIL), pl.ds(FF, WIDE)]

    def copy3(mark, layer, piece, slot):
        name, r0, nr, c0, nc = piece
        if mark == 0:
            return remote(b2, b3, s3s, s3r, c_dev, False)(False, layer, piece, slot)
        if mark == 1:
            dst = rest_rows(c0)
        else:
            dst = far_ref.at[pl.ds(pl.multiple_of(r0 - core * TAIL - (N_D - 1) * PART + PART, LANES), nr), :]
        return pltpu.make_async_remote_copy(
            src_ref=view(b2, name, layer, r0, nr, c0, nc, False), dst_ref=dst,
            send_sem=s3s.at[slot], recv_sem=s3r.at[slot], device_id=c_dev, device_id_type=MESH)

    def start0(*a):
        copy0(*a).start()

    def start1(*a):
        copy1(*a).start()

    def wait0(*a):
        copy0(*a).wait_recv()

    def relay2(*a):
        copy1(*a).wait_recv()
        if not a[0]:
            copy2(*a).start()

    def arrived(*a):
        if not a[0]:
            copy2(*a).wait_recv()
        copy1(*a).wait_send()

    def relay3(*a):
        copy3(*a).start()

    def pushed(*a):
        copy0(*a).wait_send()

    def finish(*a):
        copy3(*a).wait_recv()
        copy3(*a).wait_send()

    def sent(*a):
        if not a[0]:
            copy2(*a).wait_send()

    def targets(s):
        i = lax.rem(s, STEPS)
        layer = s // STEPS
        first = layer == 0
        late = 1 - jnp.minimum(layer, 1)
        t2 = jnp.where(i < ST_A, 9 + 2 * i + late,
             jnp.where(i < ST_G + 1, 18 + late + 3 * (i - ST_A) // 5,
             jnp.where(i < ST_D, jnp.maximum(i + 4, 31 + late + (i - ST_G - 1) // 2),
             jnp.where(i < ST_NEAR, jnp.maximum(i, ST_D + 3 + (2 * (i - ST_D) + 1) // 3),
             jnp.where(first, jnp.where(i < ST_NEAR + 2, i, jnp.where(i < ST_READY - 2, 40 + i // 2, jnp.where(i < ST_READY, i - 2, i - 3))),
             jnp.where(i < ST_READY - 2, 38 + (i + 1) // 2, 39 + i // 2))))))
        final = i == STEPS - 1
        t3 = jnp.where(i < ST_D, jnp.where(i < ST_A, 3 + i, (t2 - 3) // 2),
             jnp.where(first, jnp.where(i < ST_IDLE, (t2 - 2) // 2, CH_DR + (i - ST_IDLE + 1) // 2 + jnp.where(final, 1, 0)),
             jnp.where(i < ST_READY - 4, (t2 - 2) // 2, jnp.where(i < ST_READY + 2, 39 + (i - ST_READY + 4) // 3, i - ST_READY + 39))))
        end = s >= ALL_STEPS - 1
        t2 = jnp.minimum(t2 + layer * 2 * PER_LAYER, jnp.where(end, ITEMS, ITEMS - 1))
        t3 = jnp.minimum(t3 + layer * PER_LAYER, jnp.where(end, PUSHES, PUSHES - 1))
        nxt = jnp.minimum(s + 1, ALL_STEPS - 1)
        i = lax.rem(nxt, STEPS)
        base = nxt // STEPS * PER_LAYER
        done = jnp.where(i < ST_A, 1 + i,
               jnp.where(i < ST_O, ST_A,
               jnp.where(i < ST_G, 1 + CH_O + i - ST_O,
               jnp.where(i < ST_D, 1 + CH_GU + (i - ST_G) // 2,
               jnp.where(i < ST_NEAR, 1 + CH_D + (i - ST_D) // 2,
               jnp.where(i < ST_READY, CH_D + (i - ST_D) // 2,
               jnp.where(i < ST_READY + 1, CH_DR - 2,
               jnp.where(i < ST_FAR, CH_DR - 1,
               jnp.where(i < ST_REST, CH_DR, PER_LAYER)))))))))
        tf = jnp.maximum(jnp.minimum(t3 - 2, CHUNKS - 2), done + base)
        pushes = tf + jnp.where(tf == CHUNKS - 1, 1, 0)
        t3 = jnp.maximum(jnp.maximum(t3, pushes), base + jnp.where((i >= ST_READY) & (i < ST_FAR), CH_DR - 1, 0))
        return jnp.maximum(t2, 2 * jnp.minimum(t3, CHUNKS - 2)), t3, tf

    def relays(old, new):
        @pl.loop(old[0], new[0])
        def _(m):
            with jax.named_scope("r2"):
                for_item(m, relay2)
                for_item(m + AHEAD, start1)
                n = lax.rem(m, 2)
                for_chunk(m // 2 + jnp.where(n == 0, AHEAD0, CHUNKS), start0)
                for_chunk(m // 2 + jnp.where(n == 0, CHUNKS, AHEAD0 - 1), wait0)

        @pl.loop(old[1], new[1])
        def _(p):
            with jax.named_scope("r3"):
                extra = jnp.maximum(p - (CHUNKS - 2), 0)
                k = p - jnp.minimum(extra, 1)
                part = jnp.where((p < CHUNKS - 2) | (extra > 1), 2, extra)
                for_pair(k, arrived, part)

                @pl.when(p == CHUNKS - 1)
                def _():
                    near_far().start()

                for_chunk(k, relay3, 3, part)
                for_chunk(jnp.where(part == 1, CHUNKS, k), pushed)

        @pl.loop(old[2], new[2])
        def _(k):
            with jax.named_scope("fin"):
                for_chunk(k, finish, 3)
                for_pair(k, sent)

    def down_step(i):
        n = i - ST_D - jnp.where(i > ST_READY, 1, 0) - jnp.where(i > ST_IDLE, 1, 0)
        j = n // 2
        near = (i >= ST_NEAR) & (i < ST_NEAR + 2)
        far = (i >= ST_FAR) & (i < ST_REST)
        rest = i >= ST_REST
        whole = (i >= ST_D) & (i < ST_IDLE) & ~near & (i != ST_READY)
        return j, jnp.where(i > ST_NEAR, j - 1, j), lax.rem(n + 2 * STEPS, 2), whole, near, far, rest

    def rest_col(side_no):
        return pl.multiple_of(side_no * (2 * FF_ROWS) + 2560, HEAD)

    def tile_col(side_no, core_no, tile):
        return pl.multiple_of(side_no * (2 * FF_ROWS) + core_no * (FF_ROWS + TAIL) + tile * PART, HEAD)

    def near_far():
        r0 = pl.multiple_of(core * TAIL + (N_D - 1) * PART, 64)
        return pltpu.make_async_copy(b2["d"].at[LAYERS - 1, pl.ds(r0, PART), :], far_ref.at[pl.ds(0, PART), :], lsem.at[0])

    def near_rest():
        r0 = pl.multiple_of((1 - core) * 2560, WIDTH)
        return [pltpu.make_async_copy(b2["d"].at[LAYERS - 1, pl.ds(r0, TAIL), pl.ds(n * WIDE, WIDE)], rest_rows(n * WIDE), lsem.at[1 + n])
                for n in range(2)]

    def load_tile(s):
        layer = s // STEPS
        i = lax.rem(s, STEPS)
        slot = lax.rem(s, 2)

        def cols(name, c0, nc, w0):
            for r, src in enumerate(sources):
                pltpu.make_async_copy(src[name].at[layer, :, pl.ds(c0, nc)],
                                      wbuf.at[slot, pl.ds(r * ROWS, ROWS), pl.ds(w0, nc)], wsem.at[slot]).start()

        @pl.when(i == 0)
        def _():
            cols("k", 0, PART, 0)
            cols("v", 0, PART, PART)

        @pl.when((i >= ST_Q) & (i < ST_A))
        def _():
            cols("q", pl.multiple_of((i - ST_Q) * WIDTH, WIDTH), WIDTH, 0)

        @pl.when((i >= ST_O) & (i < ST_G))
        def _():
            cols("o", pl.multiple_of((i - ST_O) * WIDTH, WIDTH), WIDTH, 0)

        @pl.when((i >= ST_G) & (i < ST_D))
        def _():
            c0 = pl.multiple_of((i - ST_G) * PART, PART)
            cols("g", c0, PART, 0)
            cols("u", c0, PART, PART)

        j, tile, half, whole, near, far, rest = down_step(i)
        dslot = lax.rem(j + 2 * STEPS, 2)

        def rows_in(src, r0, nr, w0):
            pltpu.make_async_copy(src["d"].at[layer, pl.ds(r0, nr), :], dbuf.at[dslot, pl.ds(w0, nr), :], dsem.at[dslot]).start()

        def chunk_rows(r, tile_no, w0):
            src_core = core if r % 2 == 0 else 1 - core
            rows_in(sources[r], pl.multiple_of(src_core * TAIL + tile_no * PART, 64), PART, w0)

        def rest_rows(r, w0):
            src_core = core if r % 2 == 0 else 1 - core
            rows_in(sources[r], pl.multiple_of((1 - src_core) * 2560, WIDTH), TAIL, pl.multiple_of(w0 + src_core * TAIL, 64))

        @pl.when((whole & (half == 0) & (i != ST_READY + 1)) | (i == ST_READY))
        def _():
            for r in range(3):
                chunk_rows(r, jnp.where(i == ST_READY, N_D - 2, tile), r * PART)

        @pl.when(whole & (half == 0))
        def _():
            chunk_rows(3, tile, 768)

        @pl.when(near & (half == 0))
        def _():
            for r in range(2):
                chunk_rows(r, N_D - 1, r * PART)
                rest_rows(r, WIDTH)

        @pl.when(far & (half == 0) & (layer < LAYERS - 1))
        def _():
            for r in range(2):
                chunk_rows(2 + r, N_D - 1, r * PART)

        @pl.when(rest & (half == 0))
        def _():
            for r in range(2):
                rest_rows(2 + r, 0)

    def norm(layer, which):
        @pl.loop(0, TOK // NB)
        def _(m):
            rows = pl.ds(pl.multiple_of(m * NB, NB), NB)
            total = jnp.zeros((NB, 1), F32)
            for b in range(4):
                blk = x_ref[rows, pl.ds(b * ROWS, ROWS)]
                total = total + jnp.sum(blk * blk, axis=1, keepdims=True)
            inv = lax.rsqrt(total * (1.0 / D) + EPS)
            for b in range(4):
                blk = x_ref[rows, pl.ds(b * ROWS, ROWS)]
                gain = gain_ref[which * LAYERS + layer, :, pl.ds(b * ROWS, ROWS)]
                c0 = pl.multiple_of(rel(b) * ROWS, ROWS)
                h_ref[rows, pl.ds(c0, ROWS)] = (blk * inv * gain).astype(BF16)

    def rotate(vals, rows):
        vals = vals.astype(BF16).astype(F32)
        turned = pltpu.roll(vals, HEAD // 2, 1)
        return (vals * cos_ref[rows, :] + turned * sin_ref[rows, :]).astype(BF16)

    def tile_product(slot, finish_rows):
        @pl.loop(0, TOK // MB)
        def _(m):
            rows = pl.ds(pl.multiple_of(m * MB, MB), MB)
            finish_rows(rows, jnp.dot(h_ref[rows, :], wbuf[slot], preferred_element_type=F32))

    def kv_step(slot):
        def fin(rows, acc):
            for b in range(2):
                kv_ref[rows, pl.ds(b * HEAD, HEAD)] = rotate(acc[:, b * HEAD:(b + 1) * HEAD], rows)
            kv_ref[rows, pl.ds(PART, PART)] = acc[:, PART:].astype(BF16)
        tile_product(slot, fin)

    def q_step(slot, j):
        def fin(rows, acc):
            for b in range(4):
                c0 = pl.multiple_of(j * WIDTH + b * HEAD, HEAD)
                q_ref[rows, pl.ds(c0, HEAD)] = rotate(acc[:, b * HEAD:(b + 1) * HEAD], rows)
        tile_product(slot, fin)

    def o_step(slot, j):
        def fin(rows, acc):
            c0 = pl.ds(pl.multiple_of(j * WIDTH, WIDTH), WIDTH)
            x_ref[rows, c0] = x_ref[rows, c0] + acc
        tile_product(slot, fin)

    def g_step(slot, j):
        def fin(rows, acc):
            gate = acc[:, :PART]
            up = acc[:, PART:]
            c0 = pl.multiple_of(j * PART, PART)
            a_ref[rows, pl.ds(c0, PART)] = (gate * jax.nn.sigmoid(gate) * up).astype(BF16)
        tile_product(slot, fin)

    def attend(head):
        kv = head // 8
        q0 = pl.multiple_of(head * HEAD, HEAD)
        k0 = pl.multiple_of(kv * HEAD, HEAD)
        v0 = pl.multiple_of(PART + kv * HEAD, HEAD)
        o0 = pl.multiple_of(rel(head // 4) * ROWS + lax.rem(head, 4) * HEAD, HEAD)
        scale = HEAD ** -0.5
        for b in range(TOK // QB):
            keys = (b + 1) * QB
            rows = pl.ds(b * QB, QB)
            scores = lax.dot_general(q_ref[rows, pl.ds(q0, HEAD)], kv_ref[pl.ds(0, keys), pl.ds(k0, HEAD)],
                                     (((1,), (1,)), ((), ())), preferred_element_type=F32)
            key_idx = lax.broadcasted_iota(jnp.int32, (QB, keys), 1)
            row_idx = lax.broadcasted_iota(jnp.int32, (QB, keys), 0) + b * QB
            first = jnp.concatenate([first_ref[rows, :]] * (keys // HEAD), axis=1)
            ok = (key_idx >= first) & (key_idx <= row_idx)
            scores = jnp.where(ok, scores, -1e30)
            top = jnp.max(scores, axis=1, keepdims=True)
            probs = jnp.exp((scores - top) * scale)
            inv = 1.0 / jnp.sum(probs, axis=1, keepdims=True)
            probs = (probs * inv).astype(BF16)
            mixed = jnp.dot(probs, kv_ref[pl.ds(0, keys), pl.ds(v0, HEAD)], preferred_element_type=F32)
            h_ref[rows, pl.ds(o0, HEAD)] = mixed.astype(BF16)

    def add_product(dslot, half, cols, tile_ref=None):
        rows = pl.ds(pl.multiple_of(half * MB, MB), MB)
        depth = sum(width for _, width in cols)
        lhs = jnp.concatenate([a_ref[rows, pl.ds(c0, width)] for c0, width in cols], axis=1)
        tile = dbuf[dslot, pl.ds(0, depth), :] if tile_ref is None else tile_ref[...]
        x_ref[rows, :] = x_ref[rows, :] + jnp.dot(lhs, tile, preferred_element_type=F32)

    def wait_d(dslot, half, depth):
        @pl.when(half == 0)
        def _():
            part = dbuf.at[dslot, pl.ds(0, depth), :]
            pltpu.make_async_copy(part, part, dsem.at[dslot]).wait()

    def last_cols(side_no):
        return [(tile_col(side_no, core, N_D - 1), PART), (tile_col(side_no, 1 - core, N_D - 1), PART)]

    def wait_w(slot):
        pltpu.make_async_copy(wbuf.at[slot], wbuf.at[slot], wsem.at[slot]).wait()

    def step(s):
        before = [jnp.where(s == 0, one, two) for one, two in zip(FIRST, targets(s - 1))]
        relays(before, targets(s))

        @pl.when(s + 1 < ALL_STEPS)
        def _():
            load_tile(s + 1)

        with jax.named_scope("comp"):
            compute(s)

    def compute(s):
        layer = s // STEPS
        i = lax.rem(s, STEPS)
        slot = lax.rem(s, 2)

        @pl.when(((i == 0) & (layer > 0)) | (i == ST_G))
        def _():
            norm(layer, jnp.where(i == 0, 0, 1))

        @pl.when((i < ST_A) | ((i >= ST_O) & (i < ST_D)))
        def _():
            wait_w(slot)

        @pl.when(i == 0)
        def _():
            kv_step(slot)

        @pl.when((i >= ST_Q) & (i < ST_A))
        def _():
            q_step(slot, i - ST_Q)

        @pl.when((i >= ST_A) & (i < ST_O))
        def _():
            attend(i - ST_A)

        @pl.when((i >= ST_O) & (i < ST_G))
        def _():
            o_step(slot, i - ST_O)

        @pl.when((i >= ST_G) & (i < ST_D))
        def _():
            g_step(slot, i - ST_G)

        j, tile, half, whole, near, far, rest = down_step(i)
        dslot = lax.rem(j + 2 * STEPS, 2)

        @pl.when(whole)
        def _():
            wait_d(dslot, half, 1024)
            add_product(dslot, half, [(tile_col(lax.rem(side + r // 2, 2), lax.rem(core + r, 2), tile), PART) for r in range(4)])

        @pl.when(near)
        def _():
            wait_d(dslot, half, NEAR_K)
            add_product(dslot, half, last_cols(side) + [(rest_col(side), REST_K)])

        @pl.when(far & (layer < LAYERS - 1))
        def _():
            wait_d(dslot, half, WIDTH)
            add_product(dslot, half, last_cols(1 - side))

        @pl.when(far & (layer == LAYERS - 1))
        def _():
            @pl.when(half == 0)
            def _():
                near_far().wait()

            @pl.when(half == 1)
            def _():
                for copy in near_rest():
                    copy.start()
            add_product(dslot, half, last_cols(1 - side), far_ref)

        @pl.when(rest)
        def _():
            wait_d(dslot, half, REST_K)
            add_product(dslot, half, [(rest_col(1 - side), REST_K)])

    @pl.loop(0, AHEAD)
    def _(m):
        for_item(m, start1)

    @pl.loop(0, AHEAD0)
    def _(k):
        for_chunk(k, start0)

    for copy in inputs:
        copy.wait()

    for n, ref in enumerate((ga_ref, gm_ref)):
        for layer in range(LAYERS):
            gain_ref[n * LAYERS + layer] = ref[pl.ds(layer, 1), :].astype(F32)
    ids = seg_ref[...].astype(F32)
    lane = lax.broadcasted_iota(jnp.int32, (LANES, HEAD), 1)
    for b in range(TOK // LANES):
        rows = pl.ds(b * LANES, LANES)
        mine = jnp.transpose(jnp.broadcast_to(ids[b:b + 1, :], (LANES, LANES)))
        before = jnp.zeros((LANES, LANES), F32)
        for c in range(TOK // LANES):
            before = before + jnp.where(ids[c:c + 1, :] < mine, 1.0, 0.0)
        first = jnp.sum(before, axis=1, keepdims=True)
        pos = lax.broadcasted_iota(jnp.int32, (LANES, LANES), 0).astype(F32) + (b * 128.0) - first
        angles = pos * freq_ref[...]
        cos_ref[rows, :] = jnp.cos(angles)
        sin = jnp.sin(angles)
        sin_ref[rows, :] = jnp.where(lane < HEAD // 2, -sin, sin)
        first_ref[rows, :] = jnp.broadcast_to(first, (LANES, LANES)).astype(jnp.int32)

    @pl.loop(0, TOK // NB)
    def _(m):
        rows = pl.ds(pl.multiple_of(m * NB, NB), NB)
        x_ref[rows, :] = q_ref[rows, :].astype(F32)

    relays((0, 0, 0), (2, 0, 0))
    norm(0, 0)

    @pl.loop(0, AHEAD0 - 1)
    def _(k):
        for_chunk(k, wait0)

    relays((2, 0, 0), START)
    relays(START, FIRST)
    load_tile(0)

    @pl.loop(0, ALL_STEPS)
    def _(s):
        with jax.named_scope("step"):
            step(s)

    relays(targets(ALL_STEPS - 1), (ITEMS, PUSHES, CHUNKS))
    for copy in near_rest():
        copy.wait()


def result_kernel(x_ref, a_ref, out, y_ref, osem):
    c0 = pl.multiple_of((1 - lax.axis_index("fsdp") // 2) * (2 * FF_ROWS) + 2560, HEAD)

    def store(n, m):
        rows, cols = pl.ds(m * WIDTH, WIDTH), pl.ds(n * WIDTH, WIDTH)
        return pltpu.make_async_copy(y_ref.at[rows, cols], out.at[rows, cols], osem.at[n, m])

    for n in range(4):
        cols = pl.ds(n * WIDTH, WIDTH)
        tile = a_ref[pl.ds(n // 2 * REST_K, REST_K), pl.ds(FF + n % 2 * WIDTH, WIDTH)]
        for m in range(2):
            rows = pl.ds(m * WIDTH, WIDTH)
            y_ref[rows, cols] = x_ref[rows, cols] + jnp.dot(a_ref[rows, pl.ds(c0, REST_K)], tile, preferred_element_type=F32)
            store(n, m).start()
    for n in range(4):
        for m in range(2):
            store(n, m).wait()


def run_layers(tokens, seg_ids, g_attn, g_mlp, weights):
    shapes = [jax.ShapeDtypeStruct(w.shape, w.dtype) for w in weights]
    half_dim = HEAD // 2
    freq = np.float32(ROPE_BASE) ** (-np.arange(half_dim, dtype=np.float32) / np.float32(half_dim))
    freq = jnp.asarray(np.concatenate([freq, freq]).reshape(1, HEAD))
    sem = pltpu.SemaphoreType.DMA((SLOTS, 2))
    item_sem = pltpu.SemaphoreType.DMA((ITEM_SLOTS,))
    any_spec = pl.BlockSpec(memory_space=pl.ANY)
    vmem_spec = pl.BlockSpec(memory_space=pltpu.VMEM)
    outs = pl.pallas_call(
        layer_kernel,
        out_shape=[pltpu.VMEM((TOK, D), F32), pltpu.VMEM((TOK, FF + WIDE), BF16)] + shapes * 3,
        in_specs=[any_spec] * 12,
        out_specs=[vmem_spec] * 2 + [any_spec] * 21,
        scratch_shapes=[
            pltpu.VMEM((TOK, D), BF16),
            pltpu.VMEM((TOK, D), BF16),
            pltpu.VMEM((TOK, WIDTH), BF16),
            pltpu.VMEM((2, D, WIDTH), BF16),
            pltpu.VMEM((2, 1024, D), BF16),
            pltpu.VMEM((TOK, HEAD), F32),
            pltpu.VMEM((TOK, HEAD), F32),
            pltpu.VMEM((TOK, HEAD), jnp.int32),
            pltpu.VMEM((2 * LAYERS, 1, D), F32),
            pltpu.VMEM((TOK // LANES, LANES), jnp.int32),
            pltpu.VMEM((1, HEAD), F32),
            pltpu.VMEM((LAYERS, D), BF16),
            pltpu.VMEM((LAYERS, D), BF16),
            pltpu.VMEM((WIDTH, D), BF16),
            pltpu.SemaphoreType.DMA((2,)),
            pltpu.SemaphoreType.DMA((2,)),
            pltpu.SemaphoreType.DMA((5,)),
            pltpu.SemaphoreType.DMA((3,)),
        ] + [sem] * 2 + [item_sem] * 4 + [sem] * 2,
        compiler_params=pltpu.CompilerParams(collective_id=0, has_side_effects=True, vmem_limit_bytes=32 * 1000 * 1000),
        name="two_layers",
    )(tokens, seg_ids.reshape(TOK // LANES, LANES), freq, g_attn, g_mlp, *weights)
    hidden = pltpu.with_memory_space_constraint(outs[0], pltpu.VMEM)
    act = pltpu.with_memory_space_constraint(outs[1], pltpu.VMEM)
    return pl.pallas_call(
        result_kernel,
        out_shape=jax.ShapeDtypeStruct((TOK, D), F32),
        in_specs=[vmem_spec] * 2,
        out_specs=any_spec,
        scratch_shapes=[
            pltpu.VMEM((TOK, D), F32),
            pltpu.SemaphoreType.DMA((4, 2)),
        ],
        compiler_params=pltpu.CompilerParams(vmem_limit_bytes=24 * 1000 * 1000),
        name="result",
    )(hidden, act)


def solution(mesh):
    tok_spec = P(("rep", "fsdp"), None)
    seg_spec = P(("rep", "fsdp"))
    mat_spec = P(None, "fsdp", None)
    gain_spec = P(None, None)

    def per_device(tokens, seg_ids, w_q, w_k, w_v, w_o, w_gate, w_up, w_down, g_attn, g_mlp):
        return run_layers(tokens, seg_ids, g_attn, g_mlp, (w_q, w_k, w_v, w_o, w_gate, w_up, w_down))

    return jax.shard_map(per_device, mesh=mesh, in_specs=(tok_spec, seg_spec, mat_spec, mat_spec, mat_spec, mat_spec, mat_spec, mat_spec, mat_spec, gain_spec, gain_spec), out_specs=tok_spec, check_vma=False)
```
